128 devices in a mesh: datb: 4 (over z), model: 4 (over y), data: 8 (over x, core).
Axes of the slice: x: 4, y: 4, z: 4, core: 2. Of those that a mesh axis runs over, the one named last changes fastest.
Arguments:
- tokens: bfloat16 [8192, 3584], P(('datb', 'data', 'model'))
- w_gate: bfloat16 [3584, 18944], P(('datb', 'data'), 'model')
- w_up: bfloat16 [3584, 18944], P(('datb', 'data'), 'model')
- w_down: bfloat16 [18944, 3584], P('model', ('datb', 'data'))
- grad_out: bfloat16 [8192, 3584], P(('datb', 'data', 'model'))
Outputs:
- output 1: bfloat16 [8192, 3584], P(('datb', 'data', 'model'))
- output 2: bfloat16 [8192, 3584], P(('datb', 'data', 'model'))
- output 3: float32 [3584, 18944], P(('datb', 'data'), 'model')
- output 4: float32 [3584, 18944], P(('datb', 'data'), 'model')
- output 5: float32 [18944, 3584], P('model', ('datb', 'data'))
All inputs are finite; a program needn't handle non-finite values.
Results may differ from the reference program's by a relative error of at most 0.02.
Values are sent between devices in bfloat16 or wider.
A program may use at most 1 GiB of HBM per device.

```python
import jax
import jax.numpy as jnp
from jax import lax

D_MODEL = 3584
D_FF = 18944
TOKENS = 8192
BLOCK_ROWS = 512


def setup_inputs(seed: int = 0) -> dict:
    key = jax.random.key(seed)
    k_tok, k_gate, k_up, k_down, k_grad = jax.random.split(key, 5)
    tokens = jax.random.normal(k_tok, (TOKENS, D_MODEL), jnp.float32)
    w_gate = jax.random.normal(k_gate, (D_MODEL, D_FF), jnp.float32) * (D_MODEL ** -0.5)
    w_up = jax.random.normal(k_up, (D_MODEL, D_FF), jnp.float32) * (D_MODEL ** -0.5)
    w_down = jax.random.normal(k_down, (D_FF, D_MODEL), jnp.float32) * (1.5 * D_FF ** -0.5)
    grad_out = jax.random.normal(k_grad, (TOKENS, D_MODEL), jnp.float32)
    return {"tokens": tokens.astype(jnp.bfloat16), "w_gate": w_gate.astype(jnp.bfloat16), "w_up": w_up.astype(jnp.bfloat16), "w_down": w_down.astype(jnp.bfloat16), "grad_out": grad_out.astype(jnp.bfloat16)}


def block_pass(tok_rows, grad_rows, w_gate, w_up, w_down):
    gate_pre = jnp.dot(tok_rows, w_gate, preferred_element_type=jnp.float32).astype(jnp.bfloat16).astype(jnp.float32)
    up_pre = jnp.dot(tok_rows, w_up, preferred_element_type=jnp.float32).astype(jnp.bfloat16).astype(jnp.float32)
    gate_sig = jax.nn.sigmoid(gate_pre)
    silu_gate = gate_pre * gate_sig
    hidden = (silu_gate * up_pre).astype(jnp.bfloat16)
    down_out = jnp.dot(hidden, w_down, preferred_element_type=jnp.float32)
    out_rows = (tok_rows.astype(jnp.float32) + down_out).astype(jnp.bfloat16)
    grad_hidden = jnp.dot(grad_rows, w_down.T, preferred_element_type=jnp.float32).astype(jnp.bfloat16).astype(jnp.float32)
    grad_gate_pre = (grad_hidden * up_pre * gate_sig * (1.0 + gate_pre * (1.0 - gate_sig))).astype(jnp.bfloat16)
    grad_up_pre = (grad_hidden * silu_gate).astype(jnp.bfloat16)
    back_sum = jnp.dot(grad_gate_pre, w_gate.T, preferred_element_type=jnp.float32) + jnp.dot(grad_up_pre, w_up.T, preferred_element_type=jnp.float32)
    grad_in = (grad_rows.astype(jnp.float32) + back_sum).astype(jnp.bfloat16)
    part_gate = jnp.dot(tok_rows.T, grad_gate_pre, preferred_element_type=jnp.float32)
    part_up = jnp.dot(tok_rows.T, grad_up_pre, preferred_element_type=jnp.float32)
    part_down = jnp.dot(hidden.T, grad_rows, preferred_element_type=jnp.float32)
    return out_rows, grad_in, part_gate, part_up, part_down


def reference(tokens, w_gate, w_up, w_down, grad_out):
    block_count = TOKENS // BLOCK_ROWS
    tok_blocks = tokens.reshape(block_count, BLOCK_ROWS, D_MODEL)
    grad_blocks = grad_out.reshape(block_count, BLOCK_ROWS, D_MODEL)

    def scan_step(acc_carry, block_pair):
        acc_gate, acc_up, acc_down = acc_carry
        tok_rows, grad_rows = block_pair
        out_rows, grad_in, part_gate, part_up, part_down = block_pass(tok_rows, grad_rows, w_gate, w_up, w_down)
        return (acc_gate + part_gate, acc_up + part_up, acc_down + part_down), (out_rows, grad_in)

    zero_acc = (jnp.zeros((D_MODEL, D_FF), jnp.float32), jnp.zeros((D_MODEL, D_FF), jnp.float32), jnp.zeros((D_FF, D_MODEL), jnp.float32))
    acc_final, row_outs = lax.scan(scan_step, zero_acc, (tok_blocks, grad_blocks))
    grad_gate, grad_up, grad_down = acc_final
    out_blocks, grad_in_blocks = row_outs
    return (out_blocks.reshape(TOKENS, D_MODEL), grad_in_blocks.reshape(TOKENS, D_MODEL), grad_gate, grad_up, grad_down)
```

```python
import jax
import jax.numpy as jnp
from jax import lax
from jax.sharding import PartitionSpec as P

ROW_SPEC = P(("datb", "data", "model"), None)
GATE_SPEC = P(("datb", "data"), "model")
DOWN_SPEC = P("model", ("datb", "data"))


def solution(mesh):
    data_size = mesh.shape["data"]

    def local_step(tok_loc, wg_loc, wu_loc, wd_loc, grad_loc):
        def gate_like(w):
            w = lax.all_to_all(w, "data", 1, 0, tiled=True)
            return lax.all_gather(w, "datb", axis=0, tiled=True)

        wg = gate_like(wg_loc)
        wu = gate_like(wu_loc)
        wd = lax.all_gather(lax.all_to_all(wd_loc, "data", 0, 1, tiled=True), "datb", axis=1, tiled=True)

        tok = lax.all_gather(tok_loc, ("data", "model"), axis=0, tiled=True)
        grad = lax.all_gather(grad_loc, ("data", "model"), axis=0, tiled=True)

        gate_pre = jnp.dot(tok, wg, preferred_element_type=jnp.float32).astype(jnp.bfloat16).astype(jnp.float32)
        up_pre = jnp.dot(tok, wu, preferred_element_type=jnp.float32).astype(jnp.bfloat16).astype(jnp.float32)
        grad_hid = jnp.dot(grad, wd.T, preferred_element_type=jnp.float32).astype(jnp.bfloat16).astype(jnp.float32)
        sig = jax.nn.sigmoid(gate_pre)
        silu = gate_pre * sig
        hidden = (silu * up_pre).astype(jnp.bfloat16)
        dgate = (grad_hid * up_pre * sig * (1.0 + gate_pre * (1.0 - sig))).astype(jnp.bfloat16)
        dup = (grad_hid * silu).astype(jnp.bfloat16)

        g_gate = jnp.dot(tok.T, dgate, preferred_element_type=jnp.float32)
        g_up = jnp.dot(tok.T, dup, preferred_element_type=jnp.float32)
        g_down = jnp.dot(hidden.T, grad, preferred_element_type=jnp.float32)

        down_part = jnp.dot(hidden, wd, preferred_element_type=jnp.float32).astype(jnp.bfloat16)
        back_part = (jnp.dot(dgate, wg.T, preferred_element_type=jnp.float32) + jnp.dot(dup, wu.T, preferred_element_type=jnp.float32)).astype(jnp.bfloat16)

        def to_rows(part):
            return lax.psum_scatter(part, ("data", "model"), scatter_dimension=0, tiled=True)

        out = (tok_loc.astype(jnp.float32) + to_rows(down_part).astype(jnp.float32)).astype(jnp.bfloat16)
        grad_in = (grad_loc.astype(jnp.float32) + to_rows(back_part).astype(jnp.float32)).astype(jnp.bfloat16)

        def grad_gate_like(g):
            g = lax.psum_scatter(g, "datb", scatter_dimension=0, tiled=True)
            return lax.all_to_all(g, "data", 0, 1, tiled=True)

        grad_gate = grad_gate_like(g_gate)
        grad_up = grad_gate_like(g_up)
        grad_down = lax.all_to_all(lax.psum_scatter(g_down, "datb", scatter_dimension=1, tiled=True), "data", 1, 0, tiled=True)
        return out, grad_in, grad_gate, grad_up, grad_down

    return jax.shard_map(local_step, mesh=mesh, in_specs=(ROW_SPEC, GATE_SPEC, GATE_SPEC, DOWN_SPEC, ROW_SPEC), out_specs=(ROW_SPEC, ROW_SPEC, GATE_SPEC, GATE_SPEC, DOWN_SPEC), check_vma=False)
```

```python
import jax
import jax.numpy as jnp
from jax import lax
from jax.sharding import Mesh
from jax.sharding import PartitionSpec as P

ROW_SPEC = P(("datb", "x", "core", "model"), None)
GATE_SPEC = P(("datb", "x", "core"), "model")
DOWN_SPEC = P("model", ("datb", "x", "core"))
BF16 = jnp.bfloat16
F32 = jnp.float32


def dot(a, b, ca, cb):
    return lax.dot_general(a, b, (((ca,), (cb,)), ((), ())), preferred_element_type=F32)


def solution(mesh):
    nz, ny, nd = mesh.shape["datb"], mesh.shape["model"], mesh.shape["data"]
    nx, nc = nd // 2, 2
    fine = Mesh(mesh.devices.reshape(nz, ny, nx, nc), ("datb", "model", "x", "core"))
    up = [(i, (i + 1) % nz) for i in range(nz)]
    down = [(i, (i - 1) % nz) for i in range(nz)]
    swap = [(0, 1), (1, 0)]

    def local_step(tok_loc, wg_loc, wu_loc, wd_loc, grad_loc):
        z = lax.axis_index("datb")
        core = lax.axis_index("core")
        rows, d = tok_loc.shape

        def gate_like(w):
            w = lax.all_to_all(w, ("x", "core"), 1, 0, tiled=True)
            return lax.all_gather(w, "datb", axis=0, tiled=True)

        wg = gate_like(wg_loc)
        wu = gate_like(wu_loc)
        wdt = gate_like(wd_loc.T)

        def gather_rows(loc):
            mine = lax.all_gather(loc, ("x", "model"), axis=0, tiled=True)
            other = lax.ppermute(mine, "core", swap)
            first = jnp.where(core == 0, mine, other)
            second = jnp.where(core == 0, other, mine)
            return jnp.concatenate([first, second], axis=0)

        tok = gather_rows(tok_loc)
        grad = gather_rows(grad_loc)

        gate_t = dot(wg, tok, 0, 1).astype(BF16).astype(F32)
        up_t = dot(wu, tok, 0, 1).astype(BF16).astype(F32)
        gh_t = dot(wdt, grad, 0, 1).astype(BF16).astype(F32)
        sig = jax.nn.sigmoid(gate_t)
        silu = gate_t * sig
        hid_t = (silu * up_t).astype(BF16)
        dgate_t = (gh_t * up_t * sig * (1.0 + gate_t * (1.0 - sig))).astype(BF16)
        dup_t = (gh_t * silu).astype(BF16)

        def ring_reduce(ff_t, rows_full):
            cols = d // nz
            half = ff_t.shape[0] // 2

            def piece(k):
                return dot(ff_t, lax.dynamic_slice_in_dim(rows_full, lax.rem(z + k, nz) * cols, cols, 1), 1, 0)

            far = piece(2)
            far_up = lax.ppermute(far[:half], "datb", up)
            far_dn = lax.ppermute(far[half:], "datb", down)
            nxt, prv = piece(1), piece(3)
            free_up = lax.ppermute(nxt[half:], "datb", up)
            free_dn = lax.ppermute(prv[:half], "datb", down)
            dep_up = lax.ppermute(nxt[:half] + far_up, "datb", up)
            dep_dn = lax.ppermute(prv[half:] + far_dn, "datb", down)
            own = piece(0)
            lo = own[:half] + dep_up + free_dn
            hi = own[half:] + free_up + dep_dn
            return jnp.concatenate([lo, hi], axis=0)

        def to_shard(total_t):
            return lax.all_to_all(total_t.T, ("x", "core"), 0, 1, tiled=True)

        grad_gate = to_shard(ring_reduce(dgate_t, tok))
        grad_up = to_shard(ring_reduce(dup_t, tok))
        grad_down = to_shard(ring_reduce(hid_t, grad)).T

        down_part = dot(hid_t, wdt, 0, 1)
        back_part = dot(dgate_t, wg, 0, 1) + dot(dup_t, wu, 0, 1)

        def to_rows(part):
            half = part.shape[0] // 2
            part = part.astype(BF16)
            give = lax.dynamic_slice_in_dim(part, (1 - core) * half, half, 0)
            keep = lax.dynamic_slice_in_dim(part, core * half, half, 0)
            got = lax.ppermute(give, "core", swap)
            return lax.psum_scatter((keep.astype(F32) + got.astype(F32)).astype(BF16), ("x", "model"), scatter_dimension=0, tiled=True)

        out = (tok_loc.astype(F32) + to_rows(down_part).astype(F32)).astype(BF16)
        grad_in = (grad_loc.astype(F32) + to_rows(back_part).astype(F32)).astype(BF16)
        return out, grad_in, grad_gate, grad_up, grad_down

    return jax.shard_map(local_step, mesh=fine, in_specs=(ROW_SPEC, GATE_SPEC, GATE_SPEC, DOWN_SPEC, ROW_SPEC), out_specs=(ROW_SPEC, ROW_SPEC, GATE_SPEC, GATE_SPEC, DOWN_SPEC), check_vma=False)
```

```python
import functools

import jax
import jax.numpy as jnp
from jax import lax
from jax.experimental import pallas as pl
from jax.experimental.pallas import tpu as pltpu
from jax.sharding import Mesh
from jax.sharding import PartitionSpec as P

ROW_SPEC = P(("datb", "x", "core", "model"), None)
GATE_SPEC = P(("datb", "x", "core"), "model")
DOWN_SPEC = P("model", ("datb", "x", "core"))
BF16 = jnp.bfloat16
F32 = jnp.float32
MESH_ID = pl.DeviceIdType.MESH
RING = 4
NEAR = ((0, 0), (0, 1), (1, 0), (3, 0), (1, 1), (3, 1), (2, 0), (2, 1))
DELTAS = (0, 3, 1, 2)


def dot(a, b, ca, cb):
    return lax.dot_general(a, b, (((ca,), (cb,)), ((), ())), preferred_element_type=F32)


def gather_kernel(pg, pu, pd, tok, grad, wg, wu, wd, tok_all, grad_all,
                  own_sem, ex_s, ex_r, z1_s, z1_r, z2_s, z2_r, p1_s, p1_r, p2_s, p2_r, q1_s, q1_r, q2_s, q2_r, cc_s, cc_r):
    z, y = lax.axis_index("datb"), lax.axis_index("model")
    x, core = lax.axis_index("x"), lax.axis_index("core")
    i8 = 2 * x + core
    n8 = 2 * RING
    rows = tok.shape[0]
    half = rows // 2

    def peer(dx, dc):
        return 2 * lax.rem(x + dx, RING) + lax.rem(core + dc, 2)

    def zdev(k):
        return {"datb": lax.rem(z + k, RING)}

    def near(dx, dc):
        return {"x": lax.rem(x + dx, RING), "core": lax.rem(core + dc, 2)}

    def xdev(k):
        return {"x": lax.rem(x + k, RING)}

    def ydev(k):
        return {"model": lax.rem(y + k, RING)}

    def copy(src, dst, s, r, dev):
        return pltpu.make_async_remote_copy(src_ref=src, dst_ref=dst, send_sem=s, recv_sem=r, device_id=dev, device_id_type=MESH_ID)

    barrier = pltpu.get_barrier_semaphore()
    others = [zdev(1), zdev(3), ydev(1), ydev(3)] + [near(*n) for n in NEAR[1:]]
    for dev in others:
        pl.semaphore_signal(barrier, inc=1, device_id=dev, device_id_type=MESH_ID)
    pl.semaphore_wait(barrier, len(others))

    pieces, fulls = (pg, pu, pd), (wg, wu, wd)
    started = []

    def go(c):
        c.start()
        started.append(c)
        return c

    local = []
    for t in range(3):
        local.append(pltpu.make_async_copy(pieces[t].at[i8], fulls[t].at[z * n8 + i8], own_sem.at[t]))
    rings = ((tok, tok_all), (grad, grad_all))

    def row_block(px, py, lo=0, size=rows):
        start = (lax.rem(px, RING) * 2 + core) * RING + lax.rem(py, RING)
        return pl.ds(pl.multiple_of(start * rows + lo, half), size)

    for t, (own, full) in enumerate(rings):
        local.append(pltpu.make_async_copy(own, full.at[row_block(x, y)], own_sem.at[3 + t]))
    for c in local:
        c.start()

    def exchange(t):
        for k in range(1, n8):
            go(copy(pieces[t].at[peer(*NEAR[k])], fulls[t].at[z * n8 + i8], ex_s.at[t, k], ex_r.at[t, k], near(*NEAR[k])))

    def from_peer(k):
        dx, dc = NEAR[k]
        return peer(RING - dx, dc)

    def wait_exchange(t, k):
        slot = fulls[t].at[z * n8 + from_peer(k)]
        copy(slot, slot, ex_s.at[t, k], ex_r.at[t, k], {"datb": z}).wait_recv()

    def z_first(t, k):
        src = pieces[t].at[i8] if k == 0 else fulls[t].at[z * n8 + from_peer(k)]
        dst = fulls[t].at[z * n8 + from_peer(k)]
        for side, step in enumerate((1, 3)):
            go(copy(src, dst, z1_s.at[t, side, k], z1_r.at[t, side, k], zdev(step)))

    def wait_z_first(t, side, k):
        back = 3 if side == 0 else 1
        slot = fulls[t].at[lax.rem(z + back, RING) * n8 + from_peer(k)]
        copy(slot, slot, z1_s.at[t, side, k], z1_r.at[t, side, k], {"datb": z}).wait_recv()

    def z_second(t):
        for k in range(n8 // 2):
            for side, step in enumerate((1, 3)):
                kk = k + side * (n8 // 2)
                wait_z_first(t, side, kk)
                back = 3 if side == 0 else 1
                slot = fulls[t].at[lax.rem(z + back, RING) * n8 + from_peer(kk)]
                go(copy(slot, slot, z2_s.at[t, side, k], z2_r.at[t, side, k], zdev(step)))

    def axes(r):
        return (ydev, xdev) if r == 0 else (xdev, ydev)

    def block(r, da, db, lo=0, size=rows):
        return row_block(x + db, y + da, lo, size) if r == 0 else row_block(x + da, y + db, lo, size)

    def to_core(r, ia, ib):
        own, full = rings[r]
        rb = block(r, DELTAS[ia], DELTAS[ib])
        src = own if ia == 0 and ib == 0 else full.at[rb]
        go(copy(src, full.at[rb], cc_s.at[r, ia, ib], cc_r.at[r, ia, ib], near(0, 1)))

    def first_own(r):
        own, full = rings[r]
        for side, step in enumerate((1, 3)):
            go(copy(own, full.at[block(r, 0, 0)], p1_s.at[r, side], p1_r.at[r, side], axes(r)[0](step)))

    def first_forward(r):
        own, full = rings[r]
        for side, step in enumerate((1, 3)):
            back = 3 if side == 0 else 1
            rb = full.at[block(r, back, 0)]
            copy(rb, rb, p1_s.at[r, side], p1_r.at[r, side], {"datb": z}).wait_recv()
            hb = full.at[block(r, back, 0, side * half, half)]
            go(copy(hb, hb, p2_s.at[r, side], p2_r.at[r, side], axes(r)[0](step)))

    def first_wait_far(r):
        own, full = rings[r]
        for side in range(2):
            hb = full.at[block(r, 2, 0, side * half, half)]
            copy(hb, hb, p2_s.at[r, side], p2_r.at[r, side], {"datb": z}).wait_recv()

    def second_send(r, ia):
        own, full = rings[r]
        rb = full.at[block(r, DELTAS[ia], 0)]
        src = own if ia == 0 else rb
        for side, step in enumerate((1, 3)):
            go(copy(src, rb, q1_s.at[r, side, ia], q1_r.at[r, side, ia], axes(r)[1](step)))

    def second_forward(r):
        own, full = rings[r]
        for ia in range(RING):
            for side, step in enumerate((1, 3)):
                back = 3 if side == 0 else 1
                rb = full.at[block(r, DELTAS[ia], back)]
                copy(rb, rb, q1_s.at[r, side, ia], q1_r.at[r, side, ia], {"datb": z}).wait_recv()
                if ia // 2 == side:
                    go(copy(rb, rb, q2_s.at[r, ia], q2_r.at[r, ia], axes(r)[1](step)))
                to_core(r, ia, 1 if side == 0 else 2)

    def second_wait_far(r):
        own, full = rings[r]
        for ia in range(RING):
            rb = full.at[block(r, DELTAS[ia], 2)]
            copy(rb, rb, q2_s.at[r, ia], q2_r.at[r, ia], {"datb": z}).wait_recv()
            to_core(r, ia, 3)

    exchange(0)
    z_first(0, 0)
    first_own(0)
    first_own(1)
    second_send(0, 0)
    second_send(1, 0)
    exchange(1)
    z_first(1, 0)
    exchange(2)
    z_first(2, 0)
    to_core(0, 0, 0)
    to_core(1, 0, 0)
    for k in range(1, n8):
        wait_exchange(0, k)
        z_first(0, k)
    for r in range(2):
        first_forward(r)
        for ia in (1, 2):
            second_send(r, ia)
            to_core(r, ia, 0)
    for k in range(1, n8):
        wait_exchange(1, k)
        z_first(1, k)
    for r in range(2):
        first_wait_far(r)
        second_send(r, 3)
        to_core(r, 3, 0)
    z_second(0)
    for k in range(1, n8):
        wait_exchange(2, k)
        z_first(2, k)
    for r in range(2):
        second_forward(r)
    z_second(1)
    for r in range(2):
        second_wait_far(r)
    z_second(2)

    for c in local:
        c.wait()
    for t in range(3):
        for k in range(n8 // 2):
            wait_z_first(t, 0, n8 // 2 + k)
            wait_z_first(t, 1, k)
            for side in range(2):
                slot = fulls[t].at[lax.rem(z + 2, RING) * n8 + from_peer(k + side * (n8 // 2))]
                copy(slot, slot, z2_s.at[t, side, k], z2_r.at[t, side, k], {"datb": z}).wait_recv()
    for r in range(2):
        own, full = rings[r]
        for ia in range(RING):
            for ib in range(RING):
                rb = full.at[other_core_rows(r, x, y, core, DELTAS[ia], DELTAS[ib], rows, half)]
                copy(rb, rb, cc_s.at[r, ia, ib], cc_r.at[r, ia, ib], {"datb": z}).wait_recv()
    for c in started:
        c.wait_send()


def other_core_rows(r, x, y, core, da, db, rows, half):
    px, py = (x + db, y + da) if r == 0 else (x + da, y + db)
    start = (lax.rem(px, RING) * 2 + 1 - core) * RING + lax.rem(py, RING)
    return pl.ds(pl.multiple_of(start * rows, half), rows)


def gather_all(pg, pu, pd, tok, grad):
    n8, dp, f8 = pg.shape
    rows, d = tok.shape
    hbm = pl.BlockSpec(memory_space=pl.ANY)
    dma = pltpu.SemaphoreType.DMA
    return pl.pallas_call(
        gather_kernel,
        out_shape=[jax.ShapeDtypeStruct((RING * n8, dp, f8), BF16)] * 3 + [jax.ShapeDtypeStruct((rows * RING * n8, d), BF16)] * 2,
        in_specs=[hbm] * 5,
        out_specs=[hbm] * 5,
        scratch_shapes=[
            dma((5,)),
            dma((3, n8)), dma((3, n8)),
            dma((3, 2, n8)), dma((3, 2, n8)),
            dma((3, 2, n8 // 2)), dma((3, 2, n8 // 2)),
            dma((2, 2)), dma((2, 2)),
            dma((2, 2)), dma((2, 2)),
            dma((2, 2, RING)), dma((2, 2, RING)),
            dma((2, RING)), dma((2, RING)),
            dma((2, RING, RING)), dma((2, RING, RING)),
        ],
        compiler_params=pltpu.CompilerParams(collective_id=0, has_side_effects=True),
        name="gather_all",
    )(pg, pu, pd, tok, grad)


def solution(mesh):
    nz, ny, nd = mesh.shape["datb"], mesh.shape["model"], mesh.shape["data"]
    nx, nc = nd // 2, 2
    fine = Mesh(mesh.devices.reshape(nz, ny, nx, nc), ("datb", "model", "x", "core"))
    up = [(i, (i + 1) % nz) for i in range(nz)]
    down = [(i, (i - 1) % nz) for i in range(nz)]
    swap = [(0, 1), (1, 0)]

    def local_step(tok_loc, wg_loc, wu_loc, wd_loc, grad_loc):
        z = lax.axis_index("datb")
        core = lax.axis_index("core")
        rows, d = tok_loc.shape

        def by_owner(w):
            return w.reshape(w.shape[0], nd, w.shape[1] // nd).transpose(1, 0, 2)

        full = gather_all(by_owner(wg_loc), by_owner(wu_loc), by_owner(wd_loc.T), tok_loc, grad_loc)
        wg, wu, wdt = (w.reshape(-1, w.shape[2]) for w in full[:3])
        tok, grad = full[3:]

        gate_t = dot(wg, tok, 0, 1).astype(BF16).astype(F32)
        up_t = dot(wu, tok, 0, 1).astype(BF16).astype(F32)
        gh_t = dot(wdt, grad, 0, 1).astype(BF16).astype(F32)
        sig = jax.nn.sigmoid(gate_t)
        silu = gate_t * sig
        hid_t = (silu * up_t).astype(BF16)
        dgate_t = (gh_t * up_t * sig * (1.0 + gate_t * (1.0 - sig))).astype(BF16)
        dup_t = (gh_t * silu).astype(BF16)

        def ring_reduce(ff_t, rows_full):
            cols = d // nz
            half = ff_t.shape[0] // 2

            def piece(k):
                return dot(ff_t, lax.dynamic_slice_in_dim(rows_full, lax.rem(z + k, nz) * cols, cols, 1), 1, 0)

            far = piece(2)
            far_up = lax.ppermute(far[:half], "datb", up)
            far_dn = lax.ppermute(far[half:], "datb", down)
            nxt, prv = piece(1), piece(3)
            free_up = lax.ppermute(nxt[half:], "datb", up)
            free_dn = lax.ppermute(prv[:half], "datb", down)
            dep_up = lax.ppermute(nxt[:half] + far_up, "datb", up)
            dep_dn = lax.ppermute(prv[half:] + far_dn, "datb", down)
            own = piece(0)
            lo = own[:half] + dep_up + free_dn
            hi = own[half:] + free_up + dep_dn
            return jnp.concatenate([lo, hi], axis=0)

        def to_shard(total_t):
            return lax.all_to_all(total_t.T, ("x", "core"), 0, 1, tiled=True)

        grad_gate = to_shard(ring_reduce(dgate_t, tok))
        grad_up = to_shard(ring_reduce(dup_t, tok))
        grad_down = to_shard(ring_reduce(hid_t, grad)).T

        down_part = dot(hid_t, wdt, 0, 1)
        back_part = dot(dgate_t, wg, 0, 1) + dot(dup_t, wu, 0, 1)

        def to_rows(part):
            part = part.astype(BF16).reshape(nx, nc, ny * rows, d)
            give = lax.dynamic_slice_in_dim(part, 1 - core, 1, 1).reshape(-1, d)
            keep = lax.dynamic_slice_in_dim(part, core, 1, 1).reshape(-1, d)
            got = lax.ppermute(give, "core", swap)
            return lax.psum_scatter((keep.astype(F32) + got.astype(F32)).astype(BF16), ("x", "model"), scatter_dimension=0, tiled=True)

        out = (tok_loc.astype(F32) + to_rows(down_part).astype(F32)).astype(BF16)
        grad_in = (grad_loc.astype(F32) + to_rows(back_part).astype(F32)).astype(BF16)
        return out, grad_in, grad_gate, grad_up, grad_down

    return jax.shard_map(local_step, mesh=fine, in_specs=(ROW_SPEC, GATE_SPEC, GATE_SPEC, DOWN_SPEC, ROW_SPEC), out_specs=(ROW_SPEC, ROW_SPEC, GATE_SPEC, GATE_SPEC, DOWN_SPEC), check_vma=False)
```

```python
import functools

import jax
import jax.numpy as jnp
from jax import lax
from jax.experimental import pallas as pl
from jax.experimental.pallas import tpu as pltpu
from jax.sharding import Mesh
from jax.sharding import PartitionSpec as P

ROW_SPEC = P(("datb", "x", "core", "model"), None)
GATE_SPEC = P(("datb", "x", "core"), "model")
DOWN_SPEC = P("model", ("datb", "x", "core"))
BF16 = jnp.bfloat16
F32 = jnp.float32
MESH_ID = pl.DeviceIdType.MESH
RING = 4
NEAR = ((0, 0), (0, 1), (1, 0), (3, 0), (1, 1), (3, 1), (2, 0), (2, 1))
DELTAS = (0, 3, 1, 2)


def dot(a, b, ca, cb):
    return lax.dot_general(a, b, (((ca,), (cb,)), ((), ())), preferred_element_type=F32)


def gather_kernel(pg, pu, pd, tok, grad, wg, wu, wd, tok_all, grad_all,
                  own_sem, ex_s, ex_r, z1_s, z1_r, z2_s, z2_r, p1_s, p1_r, p2_s, p2_r, q1_s, q1_r, q2_s, q2_r, cc_s, cc_r):
    z, y = lax.axis_index("datb"), lax.axis_index("model")
    x, core = lax.axis_index("x"), lax.axis_index("core")
    i8 = 2 * x + core
    n8 = 2 * RING
    rows = tok.shape[0]
    half = rows // 2

    def peer(dx, dc):
        return 2 * lax.rem(x + dx, RING) + lax.rem(core + dc, 2)

    def zdev(k):
        return {"datb": lax.rem(z + k, RING)}

    def near(dx, dc):
        return {"x": lax.rem(x + dx, RING), "core": lax.rem(core + dc, 2)}

    def xdev(k):
        return {"x": lax.rem(x + k, RING)}

    def ydev(k):
        return {"model": lax.rem(y + k, RING)}

    def copy(src, dst, s, r, dev):
        return pltpu.make_async_remote_copy(src_ref=src, dst_ref=dst, send_sem=s, recv_sem=r, device_id=dev, device_id_type=MESH_ID)

    barrier = pltpu.get_barrier_semaphore()
    others = [zdev(1), zdev(3), ydev(1), ydev(3)] + [near(*n) for n in NEAR[1:]]
    for dev in others:
        pl.semaphore_signal(barrier, inc=1, device_id=dev, device_id_type=MESH_ID)
    pl.semaphore_wait(barrier, len(others))

    pieces, fulls = (pg, pu, pd), (wg, wu, wd)
    started = []

    def go(c):
        c.start()
        started.append(c)
        return c

    local = []
    for t in range(3):
        local.append(pltpu.make_async_copy(pieces[t].at[i8], fulls[t].at[z * n8 + i8], own_sem.at[t]))
    rings = ((tok, tok_all), (grad, grad_all))

    def row_block(px, py, lo=0, size=rows):
        start = (lax.rem(px, RING) * 2 + core) * RING + lax.rem(py, RING)
        return pl.ds(pl.multiple_of(start * rows + lo, half), size)

    for t, (own, full) in enumerate(rings):
        local.append(pltpu.make_async_copy(own, full.at[row_block(x, y)], own_sem.at[3 + t]))
    for c in local:
        c.start()

    def exchange(t):
        for k in range(1, n8):
            go(copy(pieces[t].at[peer(*NEAR[k])], fulls[t].at[z * n8 + i8], ex_s.at[t, k], ex_r.at[t, k], near(*NEAR[k])))

    def from_peer(k):
        dx, dc = NEAR[k]
        return peer(RING - dx, dc)

    def wait_exchange(t, k):
        slot = fulls[t].at[z * n8 + from_peer(k)]
        copy(slot, slot, ex_s.at[t, k], ex_r.at[t, k], {"datb": z}).wait_recv()

    def z_first(t, k):
        src = pieces[t].at[i8] if k == 0 else fulls[t].at[z * n8 + from_peer(k)]
        dst = fulls[t].at[z * n8 + from_peer(k)]
        for side, step in enumerate((1, 3)):
            go(copy(src, dst, z1_s.at[t, side, k], z1_r.at[t, side, k], zdev(step)))

    def wait_z_first(t, side, k):
        back = 3 if side == 0 else 1
        slot = fulls[t].at[lax.rem(z + back, RING) * n8 + from_peer(k)]
        copy(slot, slot, z1_s.at[t, side, k], z1_r.at[t, side, k], {"datb": z}).wait_recv()

    def z_second(t):
        for k in range(n8 // 2):
            for side, step in enumerate((1, 3)):
                kk = k + side * (n8 // 2)
                wait_z_first(t, side, kk)
                back = 3 if side == 0 else 1
                slot = fulls[t].at[lax.rem(z + back, RING) * n8 + from_peer(kk)]
                go(copy(slot, slot, z2_s.at[t, side, k], z2_r.at[t, side, k], zdev(step)))

    def axes(r):
        return (ydev, xdev) if r == 0 else (xdev, ydev)

    def block(r, da, db, lo=0, size=rows):
        return row_block(x + db, y + da, lo, size) if r == 0 else row_block(x + da, y + db, lo, size)

    def to_core(r, ia, ib):
        own, full = rings[r]
        rb = block(r, DELTAS[ia], DELTAS[ib])
        src = own if ia == 0 and ib == 0 else full.at[rb]
        go(copy(src, full.at[rb], cc_s.at[r, ia, ib], cc_r.at[r, ia, ib], near(0, 1)))

    def first_own(r):
        own, full = rings[r]
        for side, step in enumerate((1, 3)):
            go(copy(own, full.at[block(r, 0, 0)], p1_s.at[r, side], p1_r.at[r, side], axes(r)[0](step)))

    def first_forward(r):
        own, full = rings[r]
        for side, step in enumerate((1, 3)):
            back = 3 if side == 0 else 1
            rb = full.at[block(r, back, 0)]
            copy(rb, rb, p1_s.at[r, side], p1_r.at[r, side], {"datb": z}).wait_recv()
            hb = full.at[block(r, back, 0, side * half, half)]
            go(copy(hb, hb, p2_s.at[r, side], p2_r.at[r, side], axes(r)[0](step)))

    def first_wait_far(r):
        own, full = rings[r]
        for side in range(2):
            hb = full.at[block(r, 2, 0, side * half, half)]
            copy(hb, hb, p2_s.at[r, side], p2_r.at[r, side], {"datb": z}).wait_recv()

    def second_send(r, ia):
        own, full = rings[r]
        rb = full.at[block(r, DELTAS[ia], 0)]
        src = own if ia == 0 else rb
        for side, step in enumerate((1, 3)):
            go(copy(src, rb, q1_s.at[r, side, ia], q1_r.at[r, side, ia], axes(r)[1](step)))

    def second_forward(r):
        own, full = rings[r]
        for ia in range(RING):
            for side, step in enumerate((1, 3)):
                back = 3 if side == 0 else 1
                rb = full.at[block(r, DELTAS[ia], back)]
                copy(rb, rb, q1_s.at[r, side, ia], q1_r.at[r, side, ia], {"datb": z}).wait_recv()
                if ia // 2 == side:
                    go(copy(rb, rb, q2_s.at[r, ia], q2_r.at[r, ia], axes(r)[1](step)))
                to_core(r, ia, 1 if side == 0 else 2)

    def second_wait_far(r):
        own, full = rings[r]
        for ia in range(RING):
            rb = full.at[block(r, DELTAS[ia], 2)]
            copy(rb, rb, q2_s.at[r, ia], q2_r.at[r, ia], {"datb": z}).wait_recv()
            to_core(r, ia, 3)

    exchange(0)
    z_first(0, 0)
    first_own(0)
    first_own(1)
    second_send(0, 0)
    second_send(1, 0)
    exchange(1)
    z_first(1, 0)
    exchange(2)
    z_first(2, 0)
    to_core(0, 0, 0)
    to_core(1, 0, 0)
    for k in range(1, n8):
        wait_exchange(0, k)
        z_first(0, k)
    for r in range(2):
        first_forward(r)
        for ia in (1, 2):
            second_send(r, ia)
            to_core(r, ia, 0)
    for k in range(1, n8):
        wait_exchange(1, k)
        z_first(1, k)
    for r in range(2):
        first_wait_far(r)
        second_send(r, 3)
        to_core(r, 3, 0)
    z_second(0)
    for k in range(1, n8):
        wait_exchange(2, k)
        z_first(2, k)
    for r in range(2):
        second_forward(r)
    z_second(1)
    for r in range(2):
        second_wait_far(r)
    z_second(2)

    for c in local:
        c.wait()
    for t in range(3):
        for k in range(n8 // 2):
            wait_z_first(t, 0, n8 // 2 + k)
            wait_z_first(t, 1, k)
            for side in range(2):
                slot = fulls[t].at[lax.rem(z + 2, RING) * n8 + from_peer(k + side * (n8 // 2))]
                copy(slot, slot, z2_s.at[t, side, k], z2_r.at[t, side, k], {"datb": z}).wait_recv()
    for r in range(2):
        own, full = rings[r]
        for ia in range(RING):
            for ib in range(RING):
                rb = full.at[other_core_rows(r, x, y, core, DELTAS[ia], DELTAS[ib], rows, half)]
                copy(rb, rb, cc_s.at[r, ia, ib], cc_r.at[r, ia, ib], {"datb": z}).wait_recv()
    for c in started:
        c.wait_send()


def other_core_rows(r, x, y, core, da, db, rows, half):
    px, py = (x + db, y + da) if r == 0 else (x + da, y + db)
    start = (lax.rem(px, RING) * 2 + 1 - core) * RING + lax.rem(py, RING)
    return pl.ds(pl.multiple_of(start * rows, half), rows)


def gather_all(pg, pu, pd, tok, grad):
    n8, dp, f8 = pg.shape
    rows, d = tok.shape
    hbm = pl.BlockSpec(memory_space=pl.ANY)
    dma = pltpu.SemaphoreType.DMA
    return pl.pallas_call(
        gather_kernel,
        out_shape=[jax.ShapeDtypeStruct((RING * n8, dp, f8), BF16)] * 3 + [jax.ShapeDtypeStruct((rows * RING * n8, d), BF16)] * 2,
        in_specs=[hbm] * 5,
        out_specs=[hbm] * 5,
        scratch_shapes=[
            dma((5,)),
            dma((3, n8)), dma((3, n8)),
            dma((3, 2, n8)), dma((3, 2, n8)),
            dma((3, 2, n8 // 2)), dma((3, 2, n8 // 2)),
            dma((2, 2)), dma((2, 2)),
            dma((2, 2)), dma((2, 2)),
            dma((2, 2, RING)), dma((2, 2, RING)),
            dma((2, RING)), dma((2, RING)),
            dma((2, RING, RING)), dma((2, RING, RING)),
        ],
        compiler_params=pltpu.CompilerParams(collective_id=0, has_side_effects=True),
        name="gather_all",
    )(pg, pu, pd, tok, grad)


LANE = 128


def reduce_kernel(f_ref, tok, grad, og, ou, od, ra, rb,
                  ff, blk, far, nxt, tmp, stage,
                  ff_sem, blk_sem, tmp_sem, a_s, a_r, f_s, f_r, d_s, d_r, e_s, e_r, own_sem):
    z, y = lax.axis_index("datb"), lax.axis_index("model")
    x, core = lax.axis_index("x"), lax.axis_index("core")
    i8 = 2 * x + core
    n8 = 2 * RING
    nf = ff.shape[1]
    half = nf // 2
    cols = blk.shape[2]
    dp = cols // n8
    outs = (og, ou, od)

    def zdev(k):
        return {"datb": lax.rem(z + k, RING)}

    def near(dx, dc):
        return {"x": lax.rem(x + dx, RING), "core": lax.rem(core + dc, 2)}

    def peer(dx, dc):
        return 2 * lax.rem(x + dx, RING) + lax.rem(core + dc, 2)

    def rcopy(src, dst, s, r, dev):
        return pltpu.make_async_remote_copy(src_ref=src, dst_ref=dst, send_sem=s, recv_sem=r, device_id=dev, device_id_type=MESH_ID)

    barrier = pltpu.get_barrier_semaphore()
    others = [zdev(1), zdev(3)] + [near(*n) for n in NEAR[1:]]
    for dev in others:
        pl.semaphore_signal(barrier, inc=1, device_id=dev, device_id_type=MESH_ID)

    def ff_load(t):
        return pltpu.make_async_copy(f_ref.at[t], ff.at[t], ff_sem.at[t])

    def blk_copy(src, slot, k):
        lanes = pl.ds(pl.multiple_of(lax.rem(z + k, RING) * cols, LANE), cols)
        return pltpu.make_async_copy(src.at[:, lanes], blk.at[slot], blk_sem.at[slot])

    def blk_load(t, slot, k):
        @pl.when(t < 2)
        def _():
            blk_copy(tok, slot, k).start()

        @pl.when(t == 2)
        def _():
            blk_copy(grad, slot, k).start()

    def blk_wait(slot):
        blk_copy(tok, slot, 0).wait()

    def product(t, slot, dst):
        step = 2 * LANE

        def one(n, carry):
            lanes = pl.ds(pl.multiple_of(jnp.minimum(n * step, cols - step), LANE), step)
            dst[:nf, lanes] = jnp.dot(ff[t], blk[slot, :, lanes], preferred_element_type=F32)
            return carry

        lax.fori_loop(0, -(-cols // step), one, 0)

    lo, hi = pl.ds(0, half), pl.ds(half, half)

    def a_copies(t):
        return [rcopy(far.at[t, rows], ra.at[t, rows], a_s.at[t, s], a_r.at[t, s], zdev(k)) for s, rows, k in ((0, lo, 1), (1, hi, 3))]

    def f_copies(t):
        return [rcopy(nxt.at[t, s, rows], rb.at[t, s, rows], f_s.at[t, s], f_r.at[t, s], zdev(k)) for s, rows, k in ((0, hi, 1), (1, lo, 3))]

    def d_rows(t):
        if t < 2:
            return [(0, 0, 0, half), (1, 0, half, half)]
        out = []
        for p, (u, v) in enumerate(TAIL):
            out += [(0, p, u[0], u[1] - u[0]), (1, p, v[0], v[1] - v[0])]
        return out

    def d_copies(t):
        out = []
        for s, p, start, size in d_rows(t):
            rows = pl.ds(start, size)
            out.append(rcopy(nxt.at[t, s, rows], rb.at[t, s, rows], d_s.at[t, s, p], d_r.at[t, s, p], zdev(1 if s == 0 else 3)))
        return out

    for t in range(3):
        ff_load(t).start()
    blk_load(0, 0, 2)
    blk_load(2, 1, 2)
    pl.semaphore_wait(barrier, len(others))

    for t in range(3):
        ff_load(t).wait()
        if t != 1:
            blk_wait(t // 2)
        product(t, t // 2, far.at[t])
        for c in a_copies(t):
            c.start()
    for t in range(3):
        if t != 1:
            blk_load(t, 0, 1)
            blk_load(t, 1, 3)
        for s in range(2):
            if t != 1:
                blk_wait(s)
            product(t, s, nxt.at[t, s])
        for c in f_copies(t):
            c.start()
        for c in a_copies(t):
            c.wait_recv()
        for s, rows in ((0, lo), (1, hi)):
            pltpu.make_async_copy(ra.at[t, rows], tmp.at[s, rows], tmp_sem.at[s]).start()
        for s, rows in ((0, lo), (1, hi)):
            pltpu.make_async_copy(ra.at[t, rows], tmp.at[s, rows], tmp_sem.at[s]).wait()
            nxt[t, s, rows] += tmp[s, rows]
        for c in d_copies(t):
            c.start()
    for t in range(3):
        for c in a_copies(t):
            c.wait_send()
    blk_load(0, 0, 0)
    blk_load(2, 1, 0)
    for t in range(3):
        if t != 1:
            blk_wait(t // 2)
        product(t, t // 2, far.at[t])

    def load_sums(t, start, size):
        cs = [pltpu.make_async_copy(rb.at[t, s, pl.ds(start, size)], tmp.at[s, pl.ds(start, size)], tmp_sem.at[s]) for s in range(2)]
        for c in cs:
            c.start()
        for c in cs:
            c.wait()

    def turn(t, tile, slot):
        rows = pl.ds(pl.multiple_of(tile * LANE, LANE), LANE)
        total = far[t, rows] + tmp[0, rows] + tmp[1, rows]
        stage[slot, :, rows] = total.T

    def hand_out(t, slot, p, lanes):
        cs = []
        for k in range(1, n8):
            rows = pl.ds(pl.multiple_of(peer(*NEAR[k]) * dp, 8), dp)
            cs.append(rcopy(stage.at[slot, rows, lanes], outs[t].at[i8, :, lanes], e_s.at[t, p, k], e_r.at[t, p, k], near(*NEAR[k])))
        rows = pl.ds(pl.multiple_of(i8 * dp, 8), dp)
        mine = pltpu.make_async_copy(stage.at[slot, rows, lanes], outs[t].at[i8, :, lanes], own_sem.at[t, p])
        return cs, mine

    def start_all(pair):
        for c in pair[0]:
            c.start()
        pair[1].start()

    tiles = stage.shape[2] // LANE
    for t in range(2):
        for c in f_copies(t) + d_copies(t):
            c.wait_recv()
        load_sums(t, 0, nf)
        lax.fori_loop(0, tiles, lambda i, c: (turn(t, i, t), c)[1], 0)
        start_all(hand_out(t, t, 0, pl.ds(0, tiles * LANE)))
    pair = hand_out(0, 0, 0, pl.ds(0, tiles * LANE))
    for c in pair[0]:
        c.wait_send()
    pair[1].wait()
    for c in f_copies(2):
        c.wait_recv()
    dcs = d_copies(2)
    for p, group in enumerate(TAIL_TILES):
        for c in dcs[2 * p:2 * p + 2]:
            c.wait_recv()
        for tile in group:
            load_sums(2, tile * LANE, min(LANE, nf - tile * LANE))
            turn(2, tile, 0)
            start_all(hand_out(2, 0, tile, pl.ds(tile * LANE, LANE)))

    last = [hand_out(1, 1, 0, pl.ds(0, tiles * LANE))] + [hand_out(2, 0, tile, pl.ds(tile * LANE, LANE)) for tile in range(tiles)]
    for pair in last:
        for c in pair[0]:
            c.wait_send()
        pair[1].wait()
    for pair in [hand_out(0, 0, 0, pl.ds(0, tiles * LANE))] + last:
        for c in pair[0]:
            c.wait_recv()
    for t in range(3):
        for c in f_copies(t) + d_copies(t):
            c.wait_send()


TAIL = (((0, 128), (384, 512)), ((128, 256), (512, 592)), ((256, 296), (296, 384)))
TAIL_TILES = ((0, 3), (1, 4), (2,))


def reduce_weights(f_all, tok, grad):
    _, nf, rows = f_all.shape
    d = tok.shape[1]
    cols = d // RING
    n8 = 2 * RING
    padded = -(-nf // LANE) * LANE
    hbm = pl.BlockSpec(memory_space=pl.ANY)
    dma = pltpu.SemaphoreType.DMA
    out = jax.ShapeDtypeStruct((n8, cols // n8, padded), F32)
    res = pl.pallas_call(
        reduce_kernel,
        out_shape=[out] * 3 + [jax.ShapeDtypeStruct((3, nf, cols), F32), jax.ShapeDtypeStruct((3, 2, nf, cols), F32)],
        in_specs=[hbm] * 3,
        out_specs=[hbm] * 5,
        scratch_shapes=[
            pltpu.VMEM((3, nf, rows), BF16),
            pltpu.VMEM((2, rows, cols), BF16),
            pltpu.VMEM((3, padded, cols), F32),
            pltpu.VMEM((3, 2, nf, cols), F32),
            pltpu.VMEM((2, padded, cols), F32),
            pltpu.VMEM((2, cols, padded), F32),
            dma((3,)), dma((2,)), dma((2,)),
            dma((3, 2)), dma((3, 2)),
            dma((3, 2)), dma((3, 2)),
            dma((3, 2, 3)), dma((3, 2, 3)),
            dma((3, 5, n8)), dma((3, 5, n8)),
            dma((3, 5)),
        ],
        compiler_params=pltpu.CompilerParams(collective_id=1, has_side_effects=True, vmem_limit_bytes=60 * 1024 * 1024),
        cost_estimate=pl.CostEstimate(flops=6 * nf * rows * d, bytes_accessed=100_000_000, transcendentals=0),
        name="reduce_weights",
    )(f_all, tok, grad)
    return res[:3]


def solution(mesh):
    nz, ny, nd = mesh.shape["datb"], mesh.shape["model"], mesh.shape["data"]
    nx, nc = nd // 2, 2
    fine = Mesh(mesh.devices.reshape(nz, ny, nx, nc), ("datb", "model", "x", "core"))
    swap = [(0, 1), (1, 0)]

    def local_step(tok_loc, wg_loc, wu_loc, wd_loc, grad_loc):
        core = lax.axis_index("core")
        rows, d = tok_loc.shape

        def by_owner(w):
            return w.reshape(w.shape[0], nd, w.shape[1] // nd).transpose(1, 0, 2)

        full = gather_all(by_owner(wg_loc), by_owner(wu_loc), by_owner(wd_loc.T), tok_loc, grad_loc)
        wg, wu, wdt = (w.reshape(-1, w.shape[2]) for w in full[:3])
        tok, grad = full[3:]

        gate_t = dot(wg, tok, 0, 1).astype(BF16).astype(F32)
        up_t = dot(wu, tok, 0, 1).astype(BF16).astype(F32)
        gh_t = dot(wdt, grad, 0, 1).astype(BF16).astype(F32)
        sig = jax.nn.sigmoid(gate_t)
        silu = gate_t * sig
        hid_t = (silu * up_t).astype(BF16)
        dgate_t = (gh_t * up_t * sig * (1.0 + gate_t * (1.0 - sig))).astype(BF16)
        dup_t = (gh_t * silu).astype(BF16)

        down_part = dot(hid_t, wdt, 0, 1)
        back_part = dot(dgate_t, wg, 0, 1) + dot(dup_t, wu, 0, 1)

        def to_rows(part):
            part = part.astype(BF16).reshape(nx, nc, ny * rows, d)
            give = lax.dynamic_slice_in_dim(part, 1 - core, 1, 1).reshape(-1, d)
            keep = lax.dynamic_slice_in_dim(part, core, 1, 1).reshape(-1, d)
            got = lax.ppermute(give, "core", swap)
            return lax.psum_scatter((keep.astype(F32) + got.astype(F32)).astype(BF16), ("x", "model"), scatter_dimension=0, tiled=True)

        out_rows, back_rows = to_rows(down_part), to_rows(back_part)
        f_all, _ = lax.optimization_barrier((jnp.stack([dgate_t, dup_t, hid_t]), back_part))
        sums = reduce_weights(f_all, tok, grad)
        grad_gate, grad_up, grad_down_t = (s[:, :, :wg.shape[1]].transpose(1, 0, 2).reshape(s.shape[1], -1) for s in sums)
        grad_down = grad_down_t.T

        out = (tok_loc.astype(F32) + out_rows.astype(F32)).astype(BF16)
        grad_in = (grad_loc.astype(F32) + back_rows.astype(F32)).astype(BF16)
        return out, grad_in, grad_gate, grad_up, grad_down

    return jax.shard_map(local_step, mesh=fine, in_specs=(ROW_SPEC, GATE_SPEC, GATE_SPEC, DOWN_SPEC, ROW_SPEC), out_specs=(ROW_SPEC, ROW_SPEC, GATE_SPEC, GATE_SPEC, DOWN_SPEC), check_vma=False)
```

```python
import functools

import jax
import jax.numpy as jnp
from jax import lax
from jax.experimental import pallas as pl
from jax.experimental.pallas import tpu as pltpu
from jax.sharding import Mesh
from jax.sharding import PartitionSpec as P

ROW_SPEC = P(("datb", "x", "core", "model"), None)
GATE_SPEC = P(("datb", "x", "core"), "model")
DOWN_SPEC = P("model", ("datb", "x", "core"))
BF16 = jnp.bfloat16
F32 = jnp.float32
MESH_ID = pl.DeviceIdType.MESH
RING = 4
NEAR = ((0, 0), (0, 1), (1, 0), (3, 0), (1, 1), (3, 1), (2, 0), (2, 1))
DELTAS = (0, 3, 1, 2)


def dot(a, b, ca, cb):
    return lax.dot_general(a, b, (((ca,), (cb,)), ((), ())), preferred_element_type=F32)


def gather_kernel(pg, pu, pd, tok, grad, wg, wu, wd, tok_all, grad_all,
                  own_sem, ex_s, ex_r, z1_s, z1_r, z2_s, z2_r, p1_s, p1_r, p2_s, p2_r, q1_s, q1_r, q2_s, q2_r, cc_s, cc_r):
    z, y = lax.axis_index("datb"), lax.axis_index("model")
    x, core = lax.axis_index("x"), lax.axis_index("core")
    i8 = 2 * x + core
    n8 = 2 * RING
    rows = tok.shape[0]
    half = rows // 2

    def peer(dx, dc):
        return 2 * lax.rem(x + dx, RING) + lax.rem(core + dc, 2)

    def zdev(k):
        return {"datb": lax.rem(z + k, RING)}

    def near(dx, dc):
        return {"x": lax.rem(x + dx, RING), "core": lax.rem(core + dc, 2)}

    def xdev(k):
        return {"x": lax.rem(x + k, RING)}

    def ydev(k):
        return {"model": lax.rem(y + k, RING)}

    def copy(src, dst, s, r, dev):
        return pltpu.make_async_remote_copy(src_ref=src, dst_ref=dst, send_sem=s, recv_sem=r, device_id=dev, device_id_type=MESH_ID)

    barrier = pltpu.get_barrier_semaphore()
    others = [zdev(1), zdev(3), ydev(1), ydev(3)] + [near(*n) for n in NEAR[1:]]
    for dev in others:
        pl.semaphore_signal(barrier, inc=1, device_id=dev, device_id_type=MESH_ID)
    pl.semaphore_wait(barrier, len(others))

    pieces, fulls = (pg, pu, pd), (wg, wu, wd)
    started = []

    def go(c):
        c.start()
        started.append(c)
        return c

    local = []
    for t in range(3):
        local.append(pltpu.make_async_copy(pieces[t].at[i8], fulls[t].at[z * n8 + i8], own_sem.at[t]))
    rings = ((tok, tok_all), (grad, grad_all))

    def row_block(px, py, lo=0, size=rows):
        start = (lax.rem(px, RING) * 2 + core) * RING + lax.rem(py, RING)
        return pl.ds(pl.multiple_of(start * rows + lo, half), size)

    for t, (own, full) in enumerate(rings):
        local.append(pltpu.make_async_copy(own, full.at[row_block(x, y)], own_sem.at[3 + t]))
    for c in local:
        c.start()

    def exchange(t):
        for k in range(1, n8):
            go(copy(pieces[t].at[peer(*NEAR[k])], fulls[t].at[z * n8 + i8], ex_s.at[t, k], ex_r.at[t, k], near(*NEAR[k])))

    def from_peer(k):
        dx, dc = NEAR[k]
        return peer(RING - dx, dc)

    def wait_exchange(t, k):
        slot = fulls[t].at[z * n8 + from_peer(k)]
        copy(slot, slot, ex_s.at[t, k], ex_r.at[t, k], {"datb": z}).wait_recv()

    def z_first(t, k):
        src = pieces[t].at[i8] if k == 0 else fulls[t].at[z * n8 + from_peer(k)]
        dst = fulls[t].at[z * n8 + from_peer(k)]
        for side, step in enumerate((1, 3)):
            go(copy(src, dst, z1_s.at[t, side, k], z1_r.at[t, side, k], zdev(step)))

    def wait_z_first(t, side, k):
        back = 3 if side == 0 else 1
        slot = fulls[t].at[lax.rem(z + back, RING) * n8 + from_peer(k)]
        copy(slot, slot, z1_s.at[t, side, k], z1_r.at[t, side, k], {"datb": z}).wait_recv()

    def z_second(t):
        for k in range(n8 // 2):
            for side, step in enumerate((1, 3)):
                kk = k + side * (n8 // 2)
                wait_z_first(t, side, kk)
                back = 3 if side == 0 else 1
                slot = fulls[t].at[lax.rem(z + back, RING) * n8 + from_peer(kk)]
                go(copy(slot, slot, z2_s.at[t, side, k], z2_r.at[t, side, k], zdev(step)))

    def axes(r):
        return (ydev, xdev) if r == 0 else (xdev, ydev)

    def block(r, da, db, lo=0, size=rows):
        return row_block(x + db, y + da, lo, size) if r == 0 else row_block(x + da, y + db, lo, size)

    def to_core(r, ia, ib):
        own, full = rings[r]
        rb = block(r, DELTAS[ia], DELTAS[ib])
        src = own if ia == 0 and ib == 0 else full.at[rb]
        go(copy(src, full.at[rb], cc_s.at[r, ia, ib], cc_r.at[r, ia, ib], near(0, 1)))

    def first_own(r):
        own, full = rings[r]
        for side, step in enumerate((1, 3)):
            go(copy(own, full.at[block(r, 0, 0)], p1_s.at[r, side], p1_r.at[r, side], axes(r)[0](step)))

    def first_forward(r):
        own, full = rings[r]
        for side, step in enumerate((1, 3)):
            back = 3 if side == 0 else 1
            rb = full.at[block(r, back, 0)]
            copy(rb, rb, p1_s.at[r, side], p1_r.at[r, side], {"datb": z}).wait_recv()
            hb = full.at[block(r, back, 0, side * half, half)]
            go(copy(hb, hb, p2_s.at[r, side], p2_r.at[r, side], axes(r)[0](step)))

    def first_wait_far(r):
        own, full = rings[r]
        for side in range(2):
            hb = full.at[block(r, 2, 0, side * half, half)]
            copy(hb, hb, p2_s.at[r, side], p2_r.at[r, side], {"datb": z}).wait_recv()

    def second_send(r, ia):
        own, full = rings[r]
        rb = full.at[block(r, DELTAS[ia], 0)]
        src = own if ia == 0 else rb
        for side, step in enumerate((1, 3)):
            go(copy(src, rb, q1_s.at[r, side, ia], q1_r.at[r, side, ia], axes(r)[1](step)))

    def second_forward(r):
        own, full = rings[r]
        for ia in range(RING):
            for side, step in enumerate((1, 3)):
                back = 3 if side == 0 else 1
                rb = full.at[block(r, DELTAS[ia], back)]
                copy(rb, rb, q1_s.at[r, side, ia], q1_r.at[r, side, ia], {"datb": z}).wait_recv()
                if ia // 2 == side:
                    go(copy(rb, rb, q2_s.at[r, ia], q2_r.at[r, ia], axes(r)[1](step)))
                to_core(r, ia, 1 if side == 0 else 2)

    def second_wait_far(r):
        own, full = rings[r]
        for ia in range(RING):
            rb = full.at[block(r, DELTAS[ia], 2)]
            copy(rb, rb, q2_s.at[r, ia], q2_r.at[r, ia], {"datb": z}).wait_recv()
            to_core(r, ia, 3)

    exchange(0)
    z_first(0, 0)
    first_own(0)
    first_own(1)
    second_send(0, 0)
    second_send(1, 0)
    exchange(1)
    z_first(1, 0)
    exchange(2)
    z_first(2, 0)
    to_core(0, 0, 0)
    to_core(1, 0, 0)
    for k in range(1, n8):
        wait_exchange(0, k)
        z_first(0, k)
    for r in range(2):
        first_forward(r)
        for ia in (1, 2):
            second_send(r, ia)
            to_core(r, ia, 0)
    for k in range(1, n8):
        wait_exchange(1, k)
        z_first(1, k)
    for r in range(2):
        first_wait_far(r)
        second_send(r, 3)
        to_core(r, 3, 0)
    z_second(0)
    for k in range(1, n8):
        wait_exchange(2, k)
        z_first(2, k)
    for r in range(2):
        second_forward(r)
    z_second(1)
    for r in range(2):
        second_wait_far(r)
    z_second(2)

    for c in local:
        c.wait()
    for t in range(3):
        for k in range(n8 // 2):
            wait_z_first(t, 0, n8 // 2 + k)
            wait_z_first(t, 1, k)
            for side in range(2):
                slot = fulls[t].at[lax.rem(z + 2, RING) * n8 + from_peer(k + side * (n8 // 2))]
                copy(slot, slot, z2_s.at[t, side, k], z2_r.at[t, side, k], {"datb": z}).wait_recv()
    for r in range(2):
        own, full = rings[r]
        for ia in range(RING):
            for ib in range(RING):
                rb = full.at[other_core_rows(r, x, y, core, DELTAS[ia], DELTAS[ib], rows, half)]
                copy(rb, rb, cc_s.at[r, ia, ib], cc_r.at[r, ia, ib], {"datb": z}).wait_recv()
    for c in started:
        c.wait_send()


def other_core_rows(r, x, y, core, da, db, rows, half):
    px, py = (x + db, y + da) if r == 0 else (x + da, y + db)
    start = (lax.rem(px, RING) * 2 + 1 - core) * RING + lax.rem(py, RING)
    return pl.ds(pl.multiple_of(start * rows, half), rows)


def gather_all(pg, pu, pd, tok, grad):
    n8, dp, f8 = pg.shape
    rows, d = tok.shape
    hbm = pl.BlockSpec(memory_space=pl.ANY)
    dma = pltpu.SemaphoreType.DMA
    return pl.pallas_call(
        gather_kernel,
        out_shape=[jax.ShapeDtypeStruct((RING * n8, dp, f8), BF16)] * 3 + [jax.ShapeDtypeStruct((rows * RING * n8, d), BF16)] * 2,
        in_specs=[hbm] * 5,
        out_specs=[hbm] * 5,
        scratch_shapes=[
            dma((5,)),
            dma((3, n8)), dma((3, n8)),
            dma((3, 2, n8)), dma((3, 2, n8)),
            dma((3, 2, n8 // 2)), dma((3, 2, n8 // 2)),
            dma((2, 2)), dma((2, 2)),
            dma((2, 2)), dma((2, 2)),
            dma((2, 2, RING)), dma((2, 2, RING)),
            dma((2, RING)), dma((2, RING)),
            dma((2, RING, RING)), dma((2, RING, RING)),
        ],
        compiler_params=pltpu.CompilerParams(collective_id=0, has_side_effects=True),
        name="gather_all",
    )(pg, pu, pd, tok, grad)


LANE = 128
TAIL = (((0, 128), (384, 512)), ((128, 256), (512, 592)), ((256, 296), (296, 384)))
TAIL_TILES = ((0, 3), (1, 4), (2,))
OUT_COLS = 512


def reduce_kernel(f_ref, h_ref, wg, wu, wd, tok, grad, tok_own, grad_own,
                  og, ou, od, out, gin, ra, rb, give, rc, part, ra1, rb1, sd1, mid, ra2, rb2, sd2,
                  ff, blk, far, nxt, tmp, stage,
                  ff_sem, blk_sem, tmp_sem, a_s, a_r, f_s, f_r, d_s, d_r, e_s, e_r, own_sem,
                  c_s, c_r, a1_s, a1_r, f1_s, f1_r, d1_s, d1_r, a2_s, a2_r, f2_s, f2_r, d2_s, d2_r):
    z, y = lax.axis_index("datb"), lax.axis_index("model")
    x, core = lax.axis_index("x"), lax.axis_index("core")
    i8 = 2 * x + core
    n8 = 2 * RING
    nf = ff.shape[1]
    half = nf // 2
    cols = blk.shape[2]
    dp = cols // n8
    outs = (og, ou, od)

    def zdev(k):
        return {"datb": lax.rem(z + k, RING)}

    def xdev(k):
        return {"x": lax.rem(x + k, RING)}

    def ydev(k):
        return {"model": lax.rem(y + k, RING)}

    def near(dx, dc):
        return {"x": lax.rem(x + dx, RING), "core": lax.rem(core + dc, 2)}

    def peer(dx, dc):
        return 2 * lax.rem(x + dx, RING) + lax.rem(core + dc, 2)

    def rcopy(src, dst, s, r, dev):
        return pltpu.make_async_remote_copy(src_ref=src, dst_ref=dst, send_sem=s, recv_sem=r, device_id=dev, device_id_type=MESH_ID)

    def start(copies):
        for c in copies:
            c.start()

    def received(copies):
        for c in copies:
            c.wait_recv()

    def sent(copies):
        for c in copies:
            c.wait_send()

    barrier = pltpu.get_barrier_semaphore()
    others = [zdev(1), zdev(3), ydev(1), ydev(3)] + [near(*n) for n in NEAR[1:]]
    for dev in others:
        pl.semaphore_signal(barrier, inc=1, device_id=dev, device_id_type=MESH_ID)

    def ff_load(t):
        return pltpu.make_async_copy(f_ref.at[t], ff.at[t], ff_sem.at[t])

    def blk_load(t, slot, k):
        src = tok if t < 2 else grad
        lanes = pl.ds(pl.multiple_of(lax.rem(z + k, RING) * cols, LANE), cols)
        return pltpu.make_async_copy(src.at[:, lanes], blk.at[slot], blk_sem.at[slot])

    def product(t, slot, dst):
        step = 2 * LANE

        def one(n, carry):
            lanes = pl.ds(pl.multiple_of(jnp.minimum(n * step, cols - step), LANE), step)
            dst[:nf, lanes] = jnp.dot(ff[t], blk[slot, :, lanes], preferred_element_type=F32)
            return carry

        lax.fori_loop(0, -(-cols // step), one, 0)

    lo, hi = pl.ds(0, half), pl.ds(half, half)

    def a_copies(t):
        return [rcopy(far.at[t, rows], ra.at[t, rows], a_s.at[t, s], a_r.at[t, s], zdev(k)) for s, rows, k in ((0, lo, 1), (1, hi, 3))]

    def f_copies(t):
        return [rcopy(nxt.at[t, s, rows], rb.at[t, s, rows], f_s.at[t, s], f_r.at[t, s], zdev(k)) for s, rows, k in ((0, hi, 1), (1, lo, 3))]

    def d_rows(t):
        if t < 2:
            return [(0, 0, 0, half), (1, 0, half, half)]
        rows = []
        for p, (u, v) in enumerate(TAIL):
            rows += [(0, p, u[0], u[1] - u[0]), (1, p, v[0], v[1] - v[0])]
        return rows

    def d_copies(t):
        cs = []
        for s, p, first, size in d_rows(t):
            rows = pl.ds(first, size)
            cs.append(rcopy(nxt.at[t, s, rows], rb.at[t, s, rows], d_s.at[t, s, p], d_r.at[t, s, p], zdev(1 if s == 0 else 3)))
        return cs

    def far_blocks():
        for t in range(3):
            ff_load(t).wait()
            if t != 1:
                blk_load(t, t // 2, 2).wait()
            product(t, t // 2, far.at[t])
            start(a_copies(t))

    def next_blocks(t):
        if t != 1:
            blk_load(t, 0, 1).start()
            blk_load(t, 1, 3).start()
        for s in range(2):
            if t != 1:
                blk_load(t, s, 1 + 2 * s).wait()
            product(t, s, nxt.at[t, s])
        start(f_copies(t))
        received(a_copies(t))
        cs = [pltpu.make_async_copy(ra.at[t, rows], tmp.at[s, rows], tmp_sem.at[s]) for s, rows in ((0, lo), (1, hi))]
        start(cs)
        for c, (s, rows) in zip(cs, ((0, lo), (1, hi))):
            c.wait()
            nxt[t, s, rows] += tmp[s, rows]
        start(d_copies(t))

    def own_blocks():
        blk_load(0, 0, 0).start()
        blk_load(2, 1, 0).start()
        for t in range(3):
            sent(a_copies(t))
            if t != 1:
                blk_load(t, t // 2, 0).wait()
            product(t, t // 2, far.at[t])

    def load_sums(t, first, size):
        cs = [pltpu.make_async_copy(rb.at[t, s, pl.ds(first, size)], tmp.at[s, pl.ds(first, size)], tmp_sem.at[s]) for s in range(2)]
        start(cs)
        for c in cs:
            c.wait()

    def turn(t, tile, slot):
        rows = pl.ds(pl.multiple_of(tile * LANE, LANE), LANE)
        total = far[t, rows] + tmp[0, rows] + tmp[1, rows]
        stage[slot, :, rows] = total.T

    def hand_out(t, slot, p, lanes):
        cs = []
        for k in range(1, n8):
            rows = pl.ds(pl.multiple_of(peer(*NEAR[k]) * dp, 8), dp)
            cs.append(rcopy(stage.at[slot, rows, lanes], outs[t].at[i8, :, lanes], e_s.at[t, p, k], e_r.at[t, p, k], near(*NEAR[k])))
        rows = pl.ds(pl.multiple_of(i8 * dp, 8), dp)
        return cs, pltpu.make_async_copy(stage.at[slot, rows, lanes], outs[t].at[i8, :, lanes], own_sem.at[t, p])

    def handed(pair):
        sent(pair[0])
        pair[1].wait()

    tiles = stage.shape[2] // LANE
    every = pl.ds(0, tiles * LANE)

    def finish(t):
        received(f_copies(t) + d_copies(t))
        load_sums(t, 0, nf)

        def one(i, carry):
            turn(t, i, t)
            return carry

        lax.fori_loop(0, tiles, one, 0)
        cs, mine = hand_out(t, t, 0, every)
        start(cs + [mine])

    def finish_last():
        handed(hand_out(0, 0, 0, every))
        received(f_copies(2))
        dcs = d_copies(2)
        for p, group in enumerate(TAIL_TILES):
            received(dcs[2 * p:2 * p + 2])
            for tile in group:
                load_sums(2, tile * LANE, min(LANE, nf - tile * LANE))
                turn(2, tile, 0)
                cs, mine = hand_out(2, 0, tile, pl.ds(tile * LANE, LANE))
                start(cs + [mine])

    d = tok.shape[1]
    half_rows = tok_own.shape[1]
    rows = 2 * half_rows
    blocks = d // min(OUT_COLS, d)
    width = d // blocks

    def row_products(r, keep):
        side = core if keep else 1 - core
        terms = ((2, wd),) if r == 0 else ((0, wg), (1, wu))
        specs, args = [], []
        for t, w in terms:
            specs += [pl.BlockSpec((1, RING, 1, RING * rows, nf), lambda j, t=t: (t, 0, side, 0, 0)), pl.BlockSpec((width, nf), lambda j: (j, 0))]
            args += [h_ref, w]
        wide = pl.BlockSpec((RING, RING, rows, width), lambda j: (0, 0, 0, j))
        if keep:
            specs.append(wide)
            args.append(rc.at[r])

        def body(*refs):
            total = None
            for i in range(len(terms)):
                h = refs[2 * i][...].reshape(RING * RING * rows, nf)
                prod = dot(h, refs[2 * i + 1][...], 1, 1)
                total = prod if total is None else total + prod
            if keep:
                total = total + refs[-2][...].astype(F32).reshape(total.shape)
            refs[-1][...] = total.astype(BF16).reshape(RING, RING, rows, width)

        pltpu.emit_pipeline(body, grid=(blocks,), in_specs=specs, out_specs=[wide])(*args, (part if keep else give).at[r])

    def core_copy(r):
        return rcopy(give.at[r], rc.at[r], c_s.at[r], c_r.at[r], near(0, 1))

    def level(r, n):
        first = r == 0 if n == 1 else r == 1
        dev = ydev if first else xdev
        here = y if first else x
        if n == 1:
            def piece(k, h):
                at = lax.rem(here + k, RING)
                return part.at[r, pl.ds(2 * h, 2), at] if r == 0 else part.at[r, at, pl.ds(2 * h, 2)]
            return dev, piece, ra1, rb1, sd1, (a1_s, a1_r, f1_s, f1_r, d1_s, d1_r), (1, rows)

        def piece(k, h):
            return mid.at[r, lax.rem(here + k, RING), pl.ds(h, 1)]
        return dev, piece, ra2, rb2, sd2, (a2_s, a2_r, f2_s, f2_r, d2_s, d2_r), (1, half_rows)

    def ring_a(r, n):
        dev, piece, rfar, _, _, sems, _ = level(r, n)
        return [rcopy(piece(2, s), rfar.at[r, s], sems[0].at[r, s], sems[1].at[r, s], dev(1 + 2 * s)) for s in range(2)]

    def ring_f(r, n):
        dev, piece, _, rnear, _, sems, _ = level(r, n)
        return [rcopy(piece(1 + 2 * s, 1 - s), rnear.at[r, s, 1 - s], sems[2].at[r, s], sems[3].at[r, s], dev(1 + 2 * s)) for s in range(2)]

    def ring_d(r, n):
        dev, _, _, rnear, dep, sems, _ = level(r, n)
        return [rcopy(dep.at[r, s], rnear.at[r, s, s], sems[4].at[r, s], sems[5].at[r, s], dev(1 + 2 * s)) for s in range(2)]

    def add(srcs, dst):
        n = dst.shape[0]
        specs = [pl.BlockSpec((1,) + tuple(ref.shape[1:]), lambda i, rank=len(ref.shape): (i,) + (0,) * (rank - 1)) for ref in [*srcs, dst]]

        def body(*refs):
            total = refs[0][...].astype(F32)
            for ref in refs[1:-1]:
                total = total + ref[...].astype(F32)
            refs[-1][...] = total.astype(BF16).reshape(refs[-1].shape)

        pltpu.emit_pipeline(body, grid=(n,), in_specs=specs[:-1], out_specs=specs[-1:])(*srcs, dst)

    def ring_first(r, n):
        start(ring_a(r, n) + ring_f(r, n))

    def ring_dependent(r, n):
        _, piece, rfar, _, dep, _, _ = level(r, n)
        received(ring_a(r, n))
        for s in range(2):
            add([piece(1 + 2 * s, s), rfar.at[r, s]], dep.at[r, s])
            ring_d(r, n)[s].start()

    def ring_last(r, n):
        _, piece, _, rnear, _, _, _ = level(r, n)
        received(ring_f(r, n) + ring_d(r, n))
        for h in range(2):
            if n == 1:
                add([piece(0, h), rnear.at[r, 0, h], rnear.at[r, 1, h]], mid.at[r, pl.ds(2 * h, 2)])
            else:
                own, res = ((tok_own, out), (grad_own, gin))[r]
                hs = pl.ds(h, 1)
                add([own.at[hs], piece(0, h), rnear.at[r, 0, h], rnear.at[r, 1, h]], res.at[hs])

    for t in range(3):
        ff_load(t).start()
    blk_load(0, 0, 2).start()
    blk_load(2, 1, 2).start()
    pl.semaphore_wait(barrier, len(others))

    far_blocks()
    for r in range(2):
        row_products(r, False)
        core_copy(r).start()
    next_blocks(0)
    core_copy(0).wait_recv()
    row_products(0, True)
    ring_first(0, 1)
    next_blocks(1)
    core_copy(1).wait_recv()
    row_products(1, True)
    ring_first(1, 1)
    next_blocks(2)
    own_blocks()
    ring_dependent(0, 1)
    ring_dependent(1, 1)
    ring_last(0, 1)
    ring_first(0, 2)
    finish(0)
    ring_last(1, 1)
    ring_first(1, 2)
    ring_dependent(0, 2)
    ring_dependent(1, 2)
    ring_last(0, 2)
    ring_last(1, 2)
    finish(1)
    finish_last()

    last = [hand_out(1, 1, 0, every)] + [hand_out(2, 0, tile, pl.ds(tile * LANE, LANE)) for tile in range(tiles)]
    for pair in last:
        handed(pair)
    for pair in [hand_out(0, 0, 0, every)] + last:
        received(pair[0])
    for t in range(3):
        sent(f_copies(t) + d_copies(t))
    for r in range(2):
        core_copy(r).wait_send()
        for n in (1, 2):
            sent(ring_a(r, n) + ring_f(r, n) + ring_d(r, n))


def backward_reduce(f_all, h_all, wg, wu, wd, tok, grad, tok_own, grad_own):
    _, nf, tokens = f_all.shape
    rows, d = tok_own.shape
    cols = d // RING
    n8 = 2 * RING
    padded = -(-nf // LANE) * LANE
    hbm = pl.BlockSpec(memory_space=pl.ANY)
    dma = pltpu.SemaphoreType.DMA
    sds = jax.ShapeDtypeStruct
    halves = (2, rows // 2, d)
    res = pl.pallas_call(
        reduce_kernel,
        out_shape=[sds((n8, cols // n8, padded), F32)] * 3 + [sds(halves, BF16)] * 2 + [
            sds((3, nf, cols), F32), sds((3, 2, nf, cols), F32),
            sds((2, RING, RING, rows, d), BF16), sds((2, RING, RING, rows, d), BF16), sds((2, RING, RING, rows, d), BF16),
            sds((2, 2, 2, rows, d), BF16), sds((2, 2, 2, 2, rows, d), BF16), sds((2, 2, 2, rows, d), BF16),
            sds((2, RING, 2, rows // 2, d), BF16),
            sds((2, 2, 1, rows // 2, d), BF16), sds((2, 2, 2, 1, rows // 2, d), BF16), sds((2, 2, 1, rows // 2, d), BF16),
        ],
        in_specs=[hbm] * 9,
        out_specs=[hbm] * 17,
        scratch_shapes=[
            pltpu.VMEM((3, nf, tokens), BF16),
            pltpu.VMEM((2, tokens, cols), BF16),
            pltpu.VMEM((3, padded, cols), F32),
            pltpu.VMEM((3, 2, nf, cols), F32),
            pltpu.VMEM((2, padded, cols), F32),
            pltpu.VMEM((2, cols, padded), F32),
            dma((3,)), dma((2,)), dma((2,)),
            dma((3, 2)), dma((3, 2)),
            dma((3, 2)), dma((3, 2)),
            dma((3, 2, 3)), dma((3, 2, 3)),
            dma((3, 5, n8)), dma((3, 5, n8)),
            dma((3, 5)),
            dma((2,)), dma((2,)),
        ] + [dma((2, 2))] * 12,
        compiler_params=pltpu.CompilerParams(collective_id=1, has_side_effects=True, vmem_limit_bytes=63 * 1024 * 1024),
        cost_estimate=pl.CostEstimate(flops=12 * nf * tokens * d, bytes_accessed=200_000_000, transcendentals=0),
        name="backward_reduce",
    )(f_all, h_all.reshape(3, RING, 2, RING * rows, nf), wg, wu, wd, tok, grad, tok_own.reshape(halves), grad_own.reshape(halves))
    return res[:3], res[3].reshape(rows, d), res[4].reshape(rows, d)


def solution(mesh):
    nz, ny, nd = mesh.shape["datb"], mesh.shape["model"], mesh.shape["data"]
    nx, nc = nd // 2, 2
    fine = Mesh(mesh.devices.reshape(nz, ny, nx, nc), ("datb", "model", "x", "core"))

    def local_step(tok_loc, wg_loc, wu_loc, wd_loc, grad_loc):
        def by_owner(w):
            return w.reshape(w.shape[0], nd, w.shape[1] // nd).transpose(1, 0, 2)

        full = gather_all(by_owner(wg_loc), by_owner(wu_loc), by_owner(wd_loc.T), tok_loc, grad_loc)
        wg, wu, wdt = (w.reshape(-1, w.shape[2]) for w in full[:3])
        tok, grad = full[3:]

        gate_t = dot(wg, tok, 0, 1).astype(BF16).astype(F32)
        up_t = dot(wu, tok, 0, 1).astype(BF16).astype(F32)
        gh_t = dot(wdt, grad, 0, 1).astype(BF16).astype(F32)
        sig = jax.nn.sigmoid(gate_t)
        silu = gate_t * sig
        hid_t = (silu * up_t).astype(BF16)
        dgate_t = (gh_t * up_t * sig * (1.0 + gate_t * (1.0 - sig))).astype(BF16)
        dup_t = (gh_t * silu).astype(BF16)

        f_all = jnp.stack([dgate_t, dup_t, hid_t])
        h_all = jnp.stack([dgate_t.T, dup_t.T, hid_t.T])
        sums, out, grad_in = backward_reduce(f_all, h_all, wg, wu, wdt, tok, grad, tok_loc, grad_loc)
        grad_gate, grad_up, grad_down_t = (s[:, :, :wg.shape[1]].transpose(1, 0, 2).reshape(s.shape[1], -1) for s in sums)
        grad_down = grad_down_t.T
        return out, grad_in, grad_gate, grad_up, grad_down

    return jax.shard_map(local_step, mesh=fine, in_specs=(ROW_SPEC, GATE_SPEC, GATE_SPEC, DOWN_SPEC, ROW_SPEC), out_specs=(ROW_SPEC, ROW_SPEC, GATE_SPEC, GATE_SPEC, DOWN_SPEC), check_vma=False)
```

```python
import functools

import jax
import jax.numpy as jnp
from jax import lax
from jax.experimental import pallas as pl
from jax.experimental.pallas import tpu as pltpu
from jax.sharding import Mesh
from jax.sharding import PartitionSpec as P

ROW_SPEC = P(("datb", "x", "core", "model"), None)
GATE_SPEC = P(("datb", "x", "core"), "model")
DOWN_SPEC = P("model", ("datb", "x", "core"))
BF16 = jnp.bfloat16
F32 = jnp.float32
MESH_ID = pl.DeviceIdType.MESH
RING = 4
NEAR = ((0, 0), (0, 1), (1, 0), (3, 0), (1, 1), (3, 1), (2, 0), (2, 1))
DELTAS = (0, 3, 1, 2)
CHUNK = 256


def dot(a, b, ca, cb):
    return lax.dot_general(a, b, (((ca,), (cb,)), ((), ())), preferred_element_type=F32)


def forward_kernel(pg, pu, pd, tok, grad, wg, wu, wd, tok_all, grad_all, f_all, h_all,
                   wv, rowbuf, av, bv, hst, fst,
                   own_sem, ex_s, ex_r, z1_s, z1_r, z2_s, z2_r, p1_s, p1_r, p2_s, p2_r, q1_s, q1_r, q2_s, q2_r, cc_s, cc_r,
                   wv_sem, row_sem, hst_sem, fst_sem):
    z, y = lax.axis_index("datb"), lax.axis_index("model")
    x, core = lax.axis_index("x"), lax.axis_index("core")
    i8 = 2 * x + core
    n8 = 2 * RING
    rows, d = tok.shape
    half = rows // 2
    dp, nf = pg.shape[1:]
    tokens = tok_all.shape[0]

    def peer(dx, dc):
        return 2 * lax.rem(x + dx, RING) + lax.rem(core + dc, 2)

    def zdev(k):
        return {"datb": lax.rem(z + k, RING)}

    def near(dx, dc):
        return {"x": lax.rem(x + dx, RING), "core": lax.rem(core + dc, 2)}

    def xdev(k):
        return {"x": lax.rem(x + k, RING)}

    def ydev(k):
        return {"model": lax.rem(y + k, RING)}

    def copy(src, dst, s, r, dev):
        return pltpu.make_async_remote_copy(src_ref=src, dst_ref=dst, send_sem=s, recv_sem=r, device_id=dev, device_id_type=MESH_ID)

    barrier = pltpu.get_barrier_semaphore()
    others = [zdev(1), zdev(3), ydev(1), ydev(3)] + [near(*n) for n in NEAR[1:]]
    for dev in others:
        pl.semaphore_signal(barrier, inc=1, device_id=dev, device_id_type=MESH_ID)

    pieces, fulls = (pg, pu, pd), (wg, wu, wd)
    started = []

    def go(make, *args):
        make(*args).start()
        started.append((make, args))

    def slot(t, zz, j):
        return fulls[t].at[pl.ds(pl.multiple_of((zz * n8 + j) * dp, 16), dp)]

    def from_peer(k):
        dx, dc = NEAR[k]
        return peer(RING - dx, dc)

    def back(side):
        return 3 if side == 0 else 1

    def ahead(side):
        return 1 if side == 0 else 3

    def exchange_copy(t, k):
        return copy(pieces[t].at[peer(*NEAR[k])], slot(t, z, i8), ex_s.at[t, k], ex_r.at[t, k], near(*NEAR[k]))

    def exchange(t):
        for k in range(1, n8):
            go(exchange_copy, t, k)

    def z_first_copy(t, side, k):
        here = slot(t, z, from_peer(k))
        return copy(here if k else pieces[t].at[i8], here, z1_s.at[t, side, k], z1_r.at[t, side, k], zdev(ahead(side)))

    def z_first(t, k):
        if k:
            here = slot(t, z, from_peer(k))
            copy(here, here, ex_s.at[t, k], ex_r.at[t, k], {"datb": z}).wait_recv()
        for side in range(2):
            go(z_first_copy, t, side, k)

    def wait_z_first(t, side, k):
        there = slot(t, lax.rem(z + back(side), RING), from_peer(k))
        copy(there, there, z1_s.at[t, side, k], z1_r.at[t, side, k], {"datb": z}).wait_recv()

    def z_second_copy(t, side, k):
        there = slot(t, lax.rem(z + back(side), RING), from_peer(k + side * (n8 // 2)))
        return copy(there, there, z2_s.at[t, side, k], z2_r.at[t, side, k], zdev(ahead(side)))

    def z_second(t):
        for k in range(n8 // 2):
            for side in range(2):
                wait_z_first(t, side, k + side * (n8 // 2))
                go(z_second_copy, t, side, k)

    def weights_in(t):
        for k in range(n8 // 2):
            wait_z_first(t, 0, n8 // 2 + k)
            wait_z_first(t, 1, k)
            for side in range(2):
                there = slot(t, lax.rem(z + 2, RING), from_peer(k + side * (n8 // 2)))
                copy(there, there, z2_s.at[t, side, k], z2_r.at[t, side, k], {"datb": z}).wait_recv()

    cut = d // 2
    rings = ((tok, tok_all, pl.ds(0, d), True), (grad, grad_all, pl.ds(0, cut), True), (grad, grad_all, pl.ds(cut, d - cut), False))

    def axis(r, n):
        return xdev if rings[r][3] == (n == 1) else ydev

    def block(r, da, db, flip=0, lo=0, size=rows):
        px, py = (x + da, y + db) if rings[r][3] else (x + db, y + da)
        c = 1 - core if flip else core
        first = (lax.rem(px, RING) * 2 + c) * RING + lax.rem(py, RING)
        return rings[r][1].at[pl.ds(pl.multiple_of(first * rows + lo, half), size), rings[r][2]]

    def own_block(r):
        return rings[r][0].at[:, rings[r][2]]

    def to_core_copy(r, ia, ib):
        there = block(r, DELTAS[ia], DELTAS[ib])
        return copy(own_block(r) if ia == 0 and ib == 0 else there, there, cc_s.at[r, ia, ib], cc_r.at[r, ia, ib], near(0, 1))

    def to_core(r, ia, ib):
        go(to_core_copy, r, ia, ib)

    def first_copy(r, side):
        return copy(own_block(r), block(r, 0, 0), p1_s.at[r, side], p1_r.at[r, side], axis(r, 1)(ahead(side)))

    def first_own(r):
        for side in range(2):
            go(first_copy, r, side)

    def first_far_copy(r, side):
        part = block(r, back(side), 0, 0, side * half, half)
        return copy(part, part, p2_s.at[r, side], p2_r.at[r, side], axis(r, 1)(ahead(side)))

    def first_forward(r):
        for side in range(2):
            there = block(r, back(side), 0)
            copy(there, there, p1_s.at[r, side], p1_r.at[r, side], {"datb": z}).wait_recv()
            go(first_far_copy, r, side)
        for ia in (1, 2):
            second_send(r, ia)
            to_core(r, ia, 0)

    def first_far(r):
        for side in range(2):
            part = block(r, 2, 0, 0, side * half, half)
            copy(part, part, p2_s.at[r, side], p2_r.at[r, side], {"datb": z}).wait_recv()
        second_send(r, 3)
        to_core(r, 3, 0)

    def second_copy(r, side, ia):
        there = block(r, DELTAS[ia], 0)
        return copy(there if ia else own_block(r), there, q1_s.at[r, side, ia], q1_r.at[r, side, ia], axis(r, 2)(ahead(side)))

    def second_send(r, ia):
        for side in range(2):
            go(second_copy, r, side, ia)

    def second_far_copy(r, ia):
        side = ia // 2
        there = block(r, DELTAS[ia], back(side))
        return copy(there, there, q2_s.at[r, ia], q2_r.at[r, ia], axis(r, 2)(ahead(side)))

    def second_forward(r, ia):
        for side in range(2):
            there = block(r, DELTAS[ia], back(side))
            copy(there, there, q1_s.at[r, side, ia], q1_r.at[r, side, ia], {"datb": z}).wait_recv()
            if ia // 2 == side:
                go(second_far_copy, r, ia)
            to_core(r, ia, 1 if side == 0 else 2)

    def second_far(r, ia):
        there = block(r, DELTAS[ia], 2)
        copy(there, there, q2_s.at[r, ia], q2_r.at[r, ia], {"datb": z}).wait_recv()
        to_core(r, ia, 3)

    def rows_in(r):
        for ia in range(RING):
            for ib in range(RING):
                there = block(r, DELTAS[ia], DELTAS[ib], 1)
                copy(there, there, cc_s.at[r, ia, ib], cc_r.at[r, ia, ib], {"datb": z}).wait_recv()

    local = [pltpu.make_async_copy(pieces[t].at[i8], slot(t, z, i8), own_sem.at[t]) for t in range(3)]
    local += [pltpu.make_async_copy(own_block(r), block(r, 0, 0), own_sem.at[3 + r]) for r in range(3)]

    n_chunk = tokens // CHUNK

    def w_load(t):
        return pltpu.make_async_copy(fulls[t], wv.at[t], wv_sem.at[t])

    def row_load(src, i, buf):
        first = pl.ds(pl.multiple_of(i * CHUNK, CHUNK), CHUNK)
        return pltpu.make_async_copy(src.at[first], rowbuf.at[buf], row_sem.at[buf])

    def chunk_loop(src, work, between):
        row_load(src, 0, 0).start()

        def body(i, carry):
            buf = lax.rem(i, 2)

            @pl.when(i + 1 < n_chunk)
            def _():
                row_load(src, i + 1, 1 - buf).start()

            for k, step in enumerate(between):
                pl.when(i == k)(step)
            row_load(src, i, buf).wait()
            work(i, buf)
            return carry

        lax.fori_loop(0, n_chunk, body, 0)

    def chunk_rows(i):
        return pl.ds(pl.multiple_of(i * CHUNK, CHUNK), CHUNK)

    def pre_work(i, buf):
        rb = rowbuf[buf]
        av[chunk_rows(i)] = jnp.dot(rb, wv[0], preferred_element_type=F32).astype(BF16)
        bv[chunk_rows(i)] = jnp.dot(rb, wv[1], preferred_element_type=F32).astype(BF16)

    def out_copies(i, buf):
        cs = [pltpu.make_async_copy(hst.at[buf, j], h_all.at[j, chunk_rows(i)], hst_sem.at[buf, j]) for j in range(3)]
        return cs + [pltpu.make_async_copy(fst.at[buf, j], f_all.at[j, :, chunk_rows(i)], fst_sem.at[buf, j]) for j in range(3)]

    def post_work(i, buf):
        g = jnp.dot(rowbuf[buf], wv[2], preferred_element_type=F32).astype(BF16).astype(F32)

        @pl.when(i >= 2)
        def _():
            for c in out_copies(i - 2, buf):
                c.wait()

        a, b = av[chunk_rows(i)].astype(F32), bv[chunk_rows(i)].astype(F32)
        sig = jax.nn.sigmoid(a)
        silu = a * sig
        da = g * b * sig * (1.0 + a * (1.0 - sig))
        for j, v in enumerate((da, g * silu, silu * b)):
            hst[buf, j] = v.astype(BF16)
            fst[buf, j] = v.T.astype(BF16)
        for c in out_copies(i, buf):
            c.start()

    pl.semaphore_wait(barrier, len(others))
    exchange(0)
    z_first(0, 0)
    first_own(0)
    second_send(0, 0)
    first_own(2)
    for c in local:
        c.start()
    exchange(1)
    first_own(1)
    exchange(2)
    second_send(1, 0)
    second_send(2, 0)
    for r in range(3):
        to_core(r, 0, 0)
    for k in range(1, n8):
        z_first(0, k)
    second_forward(0, 0)
    first_forward(0)
    z_first(1, 0)
    z_first(1, 1)
    z_second(0)
    first_far(0)
    first_forward(2)
    for k in range(2, n8):
        z_first(1, k)
    second_forward(0, 1)
    second_forward(0, 2)
    first_forward(1)
    first_far(2)
    second_forward(0, 3)
    first_far(1)
    z_first(2, 0)
    z_first(2, 1)
    z_second(1)
    for k in range(2, n8):
        z_first(2, k)
    weights_in(0)
    for c in local:
        c.wait()
    w_load(0).start()
    for ia in range(RING):
        second_far(0, ia)
    weights_in(1)
    w_load(1).start()
    rows_in(0)
    w_load(0).wait()
    w_load(1).wait()

    def forward_grad(ia):
        second_forward(2, ia)
        second_forward(1, ia)

    chunk_loop(tok_all, pre_work, [functools.partial(forward_grad, ia) for ia in range(RING)] + [functools.partial(z_second, 2)])
    for ia in range(RING):
        second_far(2, ia)
        second_far(1, ia)
    weights_in(2)
    w_load(2).start()
    rows_in(1)
    rows_in(2)
    w_load(2).wait()
    chunk_loop(grad_all, post_work, ())
    for i in (n_chunk - 2, n_chunk - 1):
        for c in out_copies(i, i % 2):
            c.wait()
    for make, args in started:
        make(*args).wait_send()


def forward_gather(pg, pu, pd, tok, grad):
    n8, dp, nf = pg.shape
    rows, d = tok.shape
    tokens = rows * RING * n8
    hbm = pl.BlockSpec(memory_space=pl.ANY)
    dma = pltpu.SemaphoreType.DMA
    sds = jax.ShapeDtypeStruct
    return pl.pallas_call(
        forward_kernel,
        out_shape=[sds((d, nf), BF16)] * 3 + [sds((tokens, d), BF16)] * 2 + [sds((3, nf, tokens), BF16), sds((3, tokens, nf), BF16)],
        in_specs=[hbm] * 5,
        out_specs=[hbm] * 7,
        scratch_shapes=[
            pltpu.VMEM((3, d, nf), BF16),
            pltpu.VMEM((2, CHUNK, d), BF16),
            pltpu.VMEM((tokens, nf), BF16),
            pltpu.VMEM((tokens, nf), BF16),
            pltpu.VMEM((2, 3, CHUNK, nf), BF16),
            pltpu.VMEM((2, 3, nf, CHUNK), BF16),
            dma((6,)),
            dma((3, n8)), dma((3, n8)),
            dma((3, 2, n8)), dma((3, 2, n8)),
            dma((3, 2, n8 // 2)), dma((3, 2, n8 // 2)),
            dma((3, 2)), dma((3, 2)),
            dma((3, 2)), dma((3, 2)),
            dma((3, 2, RING)), dma((3, 2, RING)),
            dma((3, RING)), dma((3, RING)),
            dma((3, RING, RING)), dma((3, RING, RING)),
            dma((3,)), dma((2,)), dma((2, 3)), dma((2, 3)),
        ],
        compiler_params=pltpu.CompilerParams(collective_id=0, has_side_effects=True, vmem_limit_bytes=60 * 1024 * 1024),
        cost_estimate=pl.CostEstimate(flops=6 * nf * tokens * d, bytes_accessed=100_000_000, transcendentals=0),
        name="forward_gather",
    )(pg, pu, pd, tok, grad)


LANE = 128
TAIL = (((0, 128), (384, 512)), ((128, 256), (512, 592)), ((256, 296), (296, 384)))
TAIL_TILES = ((0, 3), (1, 4), (2,))
OUT_COLS = 512


def reduce_kernel(f_ref, h_ref, wg, wu, wd, tok, grad, tok_own, grad_own,
                  og, ou, od, out, gin, ra, rb, give, rc, part, ra1, rb1, sd1, mid, ra2, rb2, sd2,
                  ff, blk, far, nxt, tmp, stage,
                  ff_sem, blk_sem, tmp_sem, a_s, a_r, f_s, f_r, d_s, d_r, e_s, e_r, own_sem,
                  c_s, c_r, a1_s, a1_r, f1_s, f1_r, d1_s, d1_r, a2_s, a2_r, f2_s, f2_r, d2_s, d2_r):
    z, y = lax.axis_index("datb"), lax.axis_index("model")
    x, core = lax.axis_index("x"), lax.axis_index("core")
    i8 = 2 * x + core
    n8 = 2 * RING
    nf = ff.shape[1]
    half = nf // 2
    cols = blk.shape[2]
    dp = cols // n8
    outs = (og, ou, od)

    def zdev(k):
        return {"datb": lax.rem(z + k, RING)}

    def xdev(k):
        return {"x": lax.rem(x + k, RING)}

    def ydev(k):
        return {"model": lax.rem(y + k, RING)}

    def near(dx, dc):
        return {"x": lax.rem(x + dx, RING), "core": lax.rem(core + dc, 2)}

    def peer(dx, dc):
        return 2 * lax.rem(x + dx, RING) + lax.rem(core + dc, 2)

    def rcopy(src, dst, s, r, dev):
        return pltpu.make_async_remote_copy(src_ref=src, dst_ref=dst, send_sem=s, recv_sem=r, device_id=dev, device_id_type=MESH_ID)

    def start(copies):
        for c in copies:
            c.start()

    def received(copies):
        for c in copies:
            c.wait_recv()

    def sent(copies):
        for c in copies:
            c.wait_send()

    barrier = pltpu.get_barrier_semaphore()
    others = [zdev(1), zdev(3), ydev(1), ydev(3)] + [near(*n) for n in NEAR[1:]]
    for dev in others:
        pl.semaphore_signal(barrier, inc=1, device_id=dev, device_id_type=MESH_ID)

    def ff_load(t):
        return pltpu.make_async_copy(f_ref.at[t], ff.at[t], ff_sem.at[t])

    def blk_load(t, slot, k):
        src = tok if t < 2 else grad
        lanes = pl.ds(pl.multiple_of(lax.rem(z + k, RING) * cols, LANE), cols)
        return pltpu.make_async_copy(src.at[:, lanes], blk.at[slot], blk_sem.at[slot])

    def product(t, slot, dst):
        step = 2 * LANE

        def one(n, carry):
            lanes = pl.ds(pl.multiple_of(jnp.minimum(n * step, cols - step), LANE), step)
            dst[:nf, lanes] = jnp.dot(ff[t], blk[slot, :, lanes], preferred_element_type=F32)
            return carry

        lax.fori_loop(0, -(-cols // step), one, 0)

    lo, hi = pl.ds(0, half), pl.ds(half, half)

    def a_copies(t):
        return [rcopy(far.at[t, rows], ra.at[t, rows], a_s.at[t, s], a_r.at[t, s], zdev(k)) for s, rows, k in ((0, lo, 1), (1, hi, 3))]

    def f_copies(t):
        return [rcopy(nxt.at[t, s, rows], rb.at[t, s, rows], f_s.at[t, s], f_r.at[t, s], zdev(k)) for s, rows, k in ((0, hi, 1), (1, lo, 3))]

    def d_rows(t):
        if t < 2:
            return [(0, 0, 0, half), (1, 0, half, half)]
        rows = []
        for p, (u, v) in enumerate(TAIL):
            rows += [(0, p, u[0], u[1] - u[0]), (1, p, v[0], v[1] - v[0])]
        return rows

    def d_copies(t):
        cs = []
        for s, p, first, size in d_rows(t):
            rows = pl.ds(first, size)
            cs.append(rcopy(nxt.at[t, s, rows], rb.at[t, s, rows], d_s.at[t, s, p], d_r.at[t, s, p], zdev(1 if s == 0 else 3)))
        return cs

    def far_blocks():
        for t in range(3):
            ff_load(t).wait()
            if t != 1:
                blk_load(t, t // 2, 2).wait()
            product(t, t // 2, far.at[t])
            start(a_copies(t))

    def next_blocks(t):
        if t != 1:
            blk_load(t, 0, 1).start()
            blk_load(t, 1, 3).start()
        for s in range(2):
            if t != 1:
                blk_load(t, s, 1 + 2 * s).wait()
            product(t, s, nxt.at[t, s])
        start(f_copies(t))
        received(a_copies(t))
        cs = [pltpu.make_async_copy(ra.at[t, rows], tmp.at[s, rows], tmp_sem.at[s]) for s, rows in ((0, lo), (1, hi))]
        start(cs)
        for c, (s, rows) in zip(cs, ((0, lo), (1, hi))):
            c.wait()
            nxt[t, s, rows] += tmp[s, rows]
        start(d_copies(t))

    def own_blocks():
        blk_load(0, 0, 0).start()
        blk_load(2, 1, 0).start()
        for t in range(3):
            sent(a_copies(t))
            if t != 1:
                blk_load(t, t // 2, 0).wait()
            product(t, t // 2, far.at[t])

    def load_sums(t, first, size):
        cs = [pltpu.make_async_copy(rb.at[t, s, pl.ds(first, size)], tmp.at[s, pl.ds(first, size)], tmp_sem.at[s]) for s in range(2)]
        start(cs)
        for c in cs:
            c.wait()

    def turn(t, tile, slot):
        rows = pl.ds(pl.multiple_of(tile * LANE, LANE), LANE)
        total = far[t, rows] + tmp[0, rows] + tmp[1, rows]
        stage[slot, :, rows] = total.T

    def hand_out(t, slot, p, lanes):
        cs = []
        for k in range(1, n8):
            rows = pl.ds(pl.multiple_of(peer(*NEAR[k]) * dp, 8), dp)
            cs.append(rcopy(stage.at[slot, rows, lanes], outs[t].at[i8, :, lanes], e_s.at[t, p, k], e_r.at[t, p, k], near(*NEAR[k])))
        rows = pl.ds(pl.multiple_of(i8 * dp, 8), dp)
        return cs, pltpu.make_async_copy(stage.at[slot, rows, lanes], outs[t].at[i8, :, lanes], own_sem.at[t, p])

    def handed(pair):
        sent(pair[0])
        pair[1].wait()

    tiles = stage.shape[2] // LANE
    every = pl.ds(0, tiles * LANE)

    def finish(t):
        received(f_copies(t) + d_copies(t))
        load_sums(t, 0, nf)

        def one(i, carry):
            turn(t, i, t)
            return carry

        lax.fori_loop(0, tiles, one, 0)
        cs, mine = hand_out(t, t, 0, every)
        start(cs + [mine])

    def finish_last():
        handed(hand_out(0, 0, 0, every))
        received(f_copies(2))
        dcs = d_copies(2)
        for p, group in enumerate(TAIL_TILES):
            received(dcs[2 * p:2 * p + 2])
            for tile in group:
                load_sums(2, tile * LANE, min(LANE, nf - tile * LANE))
                turn(2, tile, 0)
                cs, mine = hand_out(2, 0, tile, pl.ds(tile * LANE, LANE))
                start(cs + [mine])

    d = tok.shape[1]
    half_rows = tok_own.shape[1]
    rows = 2 * half_rows
    blocks = d // min(OUT_COLS, d)
    width = d // blocks

    def row_products(r, keep):
        side = core if keep else 1 - core
        terms = ((2, wd),) if r == 0 else ((0, wg), (1, wu))
        specs, args = [], []
        for t, w in terms:
            specs += [pl.BlockSpec((1, RING, 1, RING * rows, nf), lambda j, t=t: (t, 0, side, 0, 0)), pl.BlockSpec((width, nf), lambda j: (j, 0))]
            args += [h_ref, w]
        wide = pl.BlockSpec((RING, RING, rows, width), lambda j: (0, 0, 0, j))
        if keep:
            specs.append(wide)
            args.append(rc.at[r])

        def body(*refs):
            total = None
            for i in range(len(terms)):
                h = refs[2 * i][...].reshape(RING * RING * rows, nf)
                prod = dot(h, refs[2 * i + 1][...], 1, 1)
                total = prod if total is None else total + prod
            if keep:
                total = total + refs[-2][...].astype(F32).reshape(total.shape)
            refs[-1][...] = total.astype(BF16).reshape(RING, RING, rows, width)

        pltpu.emit_pipeline(body, grid=(blocks,), in_specs=specs, out_specs=[wide])(*args, (part if keep else give).at[r])

    def core_copy(r):
        return rcopy(give.at[r], rc.at[r], c_s.at[r], c_r.at[r], near(0, 1))

    def level(r, n):
        first = r == 0 if n == 1 else r == 1
        dev = ydev if first else xdev
        here = y if first else x
        if n == 1:
            def piece(k, h):
                at = lax.rem(here + k, RING)
                return part.at[r, pl.ds(2 * h, 2), at] if r == 0 else part.at[r, at, pl.ds(2 * h, 2)]
            return dev, piece, ra1, rb1, sd1, (a1_s, a1_r, f1_s, f1_r, d1_s, d1_r), (1, rows)

        def piece(k, h):
            return mid.at[r, lax.rem(here + k, RING), pl.ds(h, 1)]
        return dev, piece, ra2, rb2, sd2, (a2_s, a2_r, f2_s, f2_r, d2_s, d2_r), (1, half_rows)

    def ring_a(r, n):
        dev, piece, rfar, _, _, sems, _ = level(r, n)
        return [rcopy(piece(2, s), rfar.at[r, s], sems[0].at[r, s], sems[1].at[r, s], dev(1 + 2 * s)) for s in range(2)]

    def ring_f(r, n):
        dev, piece, _, rnear, _, sems, _ = level(r, n)
        return [rcopy(piece(1 + 2 * s, 1 - s), rnear.at[r, s, 1 - s], sems[2].at[r, s], sems[3].at[r, s], dev(1 + 2 * s)) for s in range(2)]

    def ring_d(r, n):
        dev, _, _, rnear, dep, sems, _ = level(r, n)
        return [rcopy(dep.at[r, s], rnear.at[r, s, s], sems[4].at[r, s], sems[5].at[r, s], dev(1 + 2 * s)) for s in range(2)]

    def add(srcs, dst):
        n = dst.shape[0]
        specs = [pl.BlockSpec((1,) + tuple(ref.shape[1:]), lambda i, rank=len(ref.shape): (i,) + (0,) * (rank - 1)) for ref in [*srcs, dst]]

        def body(*refs):
            total = refs[0][...].astype(F32)
            for ref in refs[1:-1]:
                total = total + ref[...].astype(F32)
            refs[-1][...] = total.astype(BF16).reshape(refs[-1].shape)

        pltpu.emit_pipeline(body, grid=(n,), in_specs=specs[:-1], out_specs=specs[-1:])(*srcs, dst)

    def ring_first(r, n):
        start(ring_a(r, n) + ring_f(r, n))

    def ring_dependent(r, n):
        _, piece, rfar, _, dep, _, _ = level(r, n)
        received(ring_a(r, n))
        for s in range(2):
            add([piece(1 + 2 * s, s), rfar.at[r, s]], dep.at[r, s])
            ring_d(r, n)[s].start()

    def ring_last(r, n):
        _, piece, _, rnear, _, _, _ = level(r, n)
        received(ring_f(r, n) + ring_d(r, n))
        for h in range(2):
            if n == 1:
                add([piece(0, h), rnear.at[r, 0, h], rnear.at[r, 1, h]], mid.at[r, pl.ds(2 * h, 2)])
            else:
                own, res = ((tok_own, out), (grad_own, gin))[r]
                hs = pl.ds(h, 1)
                add([own.at[hs], piece(0, h), rnear.at[r, 0, h], rnear.at[r, 1, h]], res.at[hs])

    for t in range(3):
        ff_load(t).start()
    blk_load(0, 0, 2).start()
    blk_load(2, 1, 2).start()
    pl.semaphore_wait(barrier, len(others))

    far_blocks()
    for r in range(2):
        row_products(r, False)
        core_copy(r).start()
    next_blocks(0)
    core_copy(0).wait_recv()
    row_products(0, True)
    ring_first(0, 1)
    next_blocks(1)
    core_copy(1).wait_recv()
    row_products(1, True)
    ring_first(1, 1)
    next_blocks(2)
    own_blocks()
    ring_dependent(0, 1)
    ring_dependent(1, 1)
    ring_last(0, 1)
    ring_first(0, 2)
    finish(0)
    ring_last(1, 1)
    ring_first(1, 2)
    ring_dependent(0, 2)
    ring_dependent(1, 2)
    ring_last(0, 2)
    ring_last(1, 2)
    finish(1)
    finish_last()

    last = [hand_out(1, 1, 0, every)] + [hand_out(2, 0, tile, pl.ds(tile * LANE, LANE)) for tile in range(tiles)]
    for pair in last:
        handed(pair)
    for pair in [hand_out(0, 0, 0, every)] + last:
        received(pair[0])
    for t in range(3):
        sent(f_copies(t) + d_copies(t))
    for r in range(2):
        core_copy(r).wait_send()
        for n in (1, 2):
            sent(ring_a(r, n) + ring_f(r, n) + ring_d(r, n))


def backward_reduce(f_all, h_all, wg, wu, wd, tok, grad, tok_own, grad_own):
    _, nf, tokens = f_all.shape
    rows, d = tok_own.shape
    cols = d // RING
    n8 = 2 * RING
    padded = -(-nf // LANE) * LANE
    hbm = pl.BlockSpec(memory_space=pl.ANY)
    dma = pltpu.SemaphoreType.DMA
    sds = jax.ShapeDtypeStruct
    halves = (2, rows // 2, d)
    res = pl.pallas_call(
        reduce_kernel,
        out_shape=[sds((n8, cols // n8, padded), F32)] * 3 + [sds(halves, BF16)] * 2 + [
            sds((3, nf, cols), F32), sds((3, 2, nf, cols), F32),
            sds((2, RING, RING, rows, d), BF16), sds((2, RING, RING, rows, d), BF16), sds((2, RING, RING, rows, d), BF16),
            sds((2, 2, 2, rows, d), BF16), sds((2, 2, 2, 2, rows, d), BF16), sds((2, 2, 2, rows, d), BF16),
            sds((2, RING, 2, rows // 2, d), BF16),
            sds((2, 2, 1, rows // 2, d), BF16), sds((2, 2, 2, 1, rows // 2, d), BF16), sds((2, 2, 1, rows // 2, d), BF16),
        ],
        in_specs=[hbm] * 9,
        out_specs=[hbm] * 17,
        scratch_shapes=[
            pltpu.VMEM((3, nf, tokens), BF16),
            pltpu.VMEM((2, tokens, cols), BF16),
            pltpu.VMEM((3, padded, cols), F32),
            pltpu.VMEM((3, 2, nf, cols), F32),
            pltpu.VMEM((2, padded, cols), F32),
            pltpu.VMEM((2, cols, padded), F32),
            dma((3,)), dma((2,)), dma((2,)),
            dma((3, 2)), dma((3, 2)),
            dma((3, 2)), dma((3, 2)),
            dma((3, 2, 3)), dma((3, 2, 3)),
            dma((3, 5, n8)), dma((3, 5, n8)),
            dma((3, 5)),
            dma((2,)), dma((2,)),
        ] + [dma((2, 2))] * 12,
        compiler_params=pltpu.CompilerParams(collective_id=1, has_side_effects=True, vmem_limit_bytes=63 * 1024 * 1024),
        cost_estimate=pl.CostEstimate(flops=12 * nf * tokens * d, bytes_accessed=200_000_000, transcendentals=0),
        name="backward_reduce",
    )(f_all, h_all.reshape(3, RING, 2, RING * rows, nf), wg, wu, wd, tok, grad, tok_own.reshape(halves), grad_own.reshape(halves))
    return res[:3], res[3].reshape(rows, d), res[4].reshape(rows, d)


def solution(mesh):
    nz, ny, nd = mesh.shape["datb"], mesh.shape["model"], mesh.shape["data"]
    fine = Mesh(mesh.devices.reshape(nz, ny, nd // 2, 2), ("datb", "model", "x", "core"))

    def local_step(tok_loc, wg_loc, wu_loc, wd_loc, grad_loc):
        def by_owner(w):
            return w.reshape(w.shape[0], nd, w.shape[1] // nd).transpose(1, 0, 2)

        wg, wu, wdt, tok, grad, f_all, h_all = forward_gather(by_owner(wg_loc), by_owner(wu_loc), by_owner(wd_loc.T), tok_loc, grad_loc)
        sums, out, grad_in = backward_reduce(f_all, h_all, wg, wu, wdt, tok, grad, tok_loc, grad_loc)
        grad_gate, grad_up, grad_down_t = (s[:, :, :wg.shape[1]].transpose(1, 0, 2).reshape(s.shape[1], -1) for s in sums)
        return out, grad_in, grad_gate, grad_up, grad_down_t.T

    return jax.shard_map(local_step, mesh=fine, in_specs=(ROW_SPEC, GATE_SPEC, GATE_SPEC, DOWN_SPEC, ROW_SPEC), out_specs=(ROW_SPEC, ROW_SPEC, GATE_SPEC, GATE_SPEC, DOWN_SPEC), check_vma=False)
```

```python
import functools

import jax
import jax.numpy as jnp
from jax import lax
from jax.experimental import pallas as pl
from jax.experimental.pallas import tpu as pltpu
from jax.sharding import Mesh
from jax.sharding import PartitionSpec as P

ROW_SPEC = P(("datb", "x", "core", "model"), None)
GATE_SPEC = P(("datb", "x", "core"), "model")
DOWN_SPEC = P("model", ("datb", "x", "core"))
BF16 = jnp.bfloat16
F32 = jnp.float32
MESH_ID = pl.DeviceIdType.MESH
RING = 4
NEAR = ((0, 0), (0, 1), (1, 0), (3, 0), (1, 1), (3, 1), (2, 0), (2, 1))
DELTAS = (0, 3, 1, 2)
CHUNK = 256
EX, Z1, Z2, P1, P2, BL, Q1, Q2, WD = range(9)
GATHER_STEPS = (
    (Z1, 0, 0), (EX, 0, 1), (EX, 0, 2), (EX, 0, 3), (EX, 0, 4), (EX, 0, 5), (EX, 0, 6), (EX, 0, 7), (Z1, 1, 0), (BL, 0, 0), (Z1, 2, 0),
    (EX, 1, 1), (EX, 2, 1), (P1, 2, 0), (P1, 2, 1), (P1, 0, 0), (P1, 0, 1), (Z1, 0, 1), (Z1, 1, 1), (BL, 1, 0), (Z1, 2, 1), (Z2, 0, 0, 0),
    (Z1, 0, 2), (EX, 1, 2), (EX, 1, 3), (Q1, 0, 0, 0), (Q1, 0, 0, 1), (Z1, 0, 3), (EX, 1, 4), (EX, 1, 5), (Z2, 0, 0, 1), (P2, 2, 1),
    (EX, 1, 6), (EX, 1, 7), (P2, 2, 0), (Z1, 0, 4), (Q1, 1, 0, 0), (Q1, 1, 0, 1), (Z1, 0, 5), (EX, 2, 2), (EX, 2, 3), (Z1, 0, 6), (P2, 0, 0),
    (P2, 0, 1), (BL, 0, 1), (Z2, 0, 0, 2), (Z2, 0, 1, 0), (Q2, 0, 0), (EX, 2, 4), (EX, 2, 5), (Z2, 0, 0, 3), (Z2, 0, 1, 1), (EX, 2, 6),
    (EX, 2, 7), (Z1, 0, 7), (Z2, 0, 1, 2), (BL, 0, 2), (Z2, 1, 0, 0), (Q2, 1, 0), (Q1, 0, 1, 1), (P1, 1, 0), (P1, 1, 1), (Z2, 1, 0, 1),
    (Z1, 1, 2), (Z2, 0, 1, 3), (BL, 2, 1), (BL, 0, 3), (Z1, 1, 3), (Q1, 0, 2, 1), (Z1, 1, 4), (BL, 2, 2), (Z1, 1, 5), (WD, 0), (BL, 2, 0),
    (Q1, 0, 1, 0), (Z1, 1, 6), (Q1, 0, 2, 0), (Q1, 0, 3, 1), (Z1, 1, 7), (Z2, 1, 1, 0), (P2, 1, 0), (P2, 1, 1), (Z2, 1, 0, 2), (BL, 2, 3),
    (Z2, 1, 1, 1), (Q1, 2, 1, 1), (Z2, 1, 0, 3), (BL, 1, 1), (Z2, 1, 1, 2), (Q1, 2, 1, 0), (Q1, 2, 2, 0), (Q1, 2, 2, 1), (Q1, 0, 3, 0),
    (Q2, 0, 2), (Z2, 2, 0, 0), (Z2, 1, 1, 3), (BL, 1, 2), (Z2, 2, 0, 1), (Q1, 2, 0, 0), (Q1, 2, 0, 1), (Z1, 2, 2), (BL, 1, 3), (Z1, 2, 3),
    (Q2, 0, 1), (Q2, 0, 3), (Q1, 2, 3, 0), (Q1, 2, 3, 1), (Z1, 2, 4), (WD, 1),
)
CHUNK_STEPS = (
    (
        (Q2, 2, 1), (Q2, 2, 2), (Z1, 2, 5), (Q1, 1, 1, 0), (Q1, 1, 1, 1),
    ),
    (
        (Z1, 2, 6), (Q1, 1, 2, 0), (Q1, 1, 2, 1),
    ),
    (
        (Q2, 2, 0), (Q2, 2, 3), (Z2, 2, 1, 0), (Z2, 2, 0, 2), (Q1, 1, 3, 0), (Q1, 1, 3, 1), (Z1, 2, 7),
    ),
    (
        (Z2, 2, 1, 1), (Z2, 2, 1, 2), (Z2, 2, 0, 3),
    ),
    (
        (Q2, 1, 1), (Q2, 1, 2),
    ),
    (
        (Q2, 1, 3), (Z2, 2, 1, 3),
    ),
    (),
)
LATE_STEPS = (
    (WD, 2),
)


def dot(a, b, ca, cb):
    return lax.dot_general(a, b, (((ca,), (cb,)), ((), ())), preferred_element_type=F32)


def forward_kernel(sg, su, sd, tok, grad, wg, wu, wd, tok_all, grad_all, f_all, h_all,
                   shard, pieces, wv, rowbuf, av, bv, hst, fst,
                   own_sem, ex_s, ex_r, z1_s, z1_r, z2_s, z2_r, p1_s, p1_r, p2_s, p2_r, q1_s, q1_r, q2_s, q2_r, cc_s, cc_r,
                   sh_sem, wv_sem, row_sem, hst_sem, fst_sem):
    z, y = lax.axis_index("datb"), lax.axis_index("model")
    x, core = lax.axis_index("x"), lax.axis_index("core")
    i8 = 2 * x + core
    n8 = 2 * RING
    rows, d = tok.shape
    half = rows // 2
    dp, nf = pieces.shape[2:]
    tokens = tok_all.shape[0]

    def peer(dx, dc):
        return 2 * lax.rem(x + dx, RING) + lax.rem(core + dc, 2)

    def zdev(k):
        return {"datb": lax.rem(z + k, RING)}

    def near(dx, dc):
        return {"x": lax.rem(x + dx, RING), "core": lax.rem(core + dc, 2)}

    def xdev(k):
        return {"x": lax.rem(x + k, RING)}

    def ydev(k):
        return {"model": lax.rem(y + k, RING)}

    def copy(src, dst, s, r, dev):
        return pltpu.make_async_remote_copy(src_ref=src, dst_ref=dst, send_sem=s, recv_sem=r, device_id=dev, device_id_type=MESH_ID)

    barrier = pltpu.get_barrier_semaphore()
    others = [zdev(1), zdev(3), ydev(1), ydev(3)] + [near(*n) for n in NEAR[1:]]
    for dev in others:
        pl.semaphore_signal(barrier, inc=1, device_id=dev, device_id_type=MESH_ID)

    fulls = (wg, wu, wd)
    loads = [pltpu.make_async_copy(src, shard.at[t], sh_sem.at[t]) for t, src in enumerate((sg, su, sd))]
    for c in loads:
        c.start()

    def cut_pieces(t):
        loads[t].wait()
        for j in range(n8):
            pieces[t, j] = shard[t, :, j * nf:(j + 1) * nf]

    started = []

    def go(make, *args):
        make(*args).start()
        started.append((make, args))

    def slot(t, zz, j):
        return fulls[t].at[pl.ds(pl.multiple_of((zz * n8 + j) * dp, 16), dp)]

    def from_peer(k):
        dx, dc = NEAR[k]
        return peer(RING - dx, dc)

    def back(side):
        return 3 if side == 0 else 1

    def ahead(side):
        return 1 if side == 0 else 3

    def exchange_copy(t, k):
        return copy(pieces.at[t, peer(*NEAR[k])], slot(t, z, i8), ex_s.at[t, k], ex_r.at[t, k], near(*NEAR[k]))

    def exchange(t, k):
        go(exchange_copy, t, k)

    def z_first_copy(t, side, k):
        here = slot(t, z, from_peer(k))
        return copy(here if k else pieces.at[t, i8], here, z1_s.at[t, side, k], z1_r.at[t, side, k], zdev(ahead(side)))

    def z_first(t, k):
        if k:
            here = slot(t, z, from_peer(k))
            copy(here, here, ex_s.at[t, k], ex_r.at[t, k], {"datb": z}).wait_recv()
        for side in range(2):
            go(z_first_copy, t, side, k)

    def wait_z_first(t, side, k):
        there = slot(t, lax.rem(z + back(side), RING), from_peer(k))
        copy(there, there, z1_s.at[t, side, k], z1_r.at[t, side, k], {"datb": z}).wait_recv()

    def z_second_copy(t, side, k):
        there = slot(t, lax.rem(z + back(side), RING), from_peer(k + side * (n8 // 2)))
        return copy(there, there, z2_s.at[t, side, k], z2_r.at[t, side, k], zdev(ahead(side)))

    def z_second(t, side, k):
        wait_z_first(t, side, k + side * (n8 // 2))
        go(z_second_copy, t, side, k)

    def weights_done(t):
        local[t].wait()
        for k in range(n8 // 2):
            wait_z_first(t, 0, n8 // 2 + k)
            wait_z_first(t, 1, k)
            for side in range(2):
                there = slot(t, lax.rem(z + 2, RING), from_peer(k + side * (n8 // 2)))
                copy(there, there, z2_s.at[t, side, k], z2_r.at[t, side, k], {"datb": z}).wait_recv()
        w_load(t).start()

    cut = d // 2
    rings = ((tok, tok_all, pl.ds(0, d), True), (grad, grad_all, pl.ds(0, cut), True), (grad, grad_all, pl.ds(cut, d - cut), False))

    def axis(r, n):
        return xdev if rings[r][3] == (n == 1) else ydev

    def block(r, da, db, flip=0, lo=0, size=rows):
        px, py = (x + da, y + db) if rings[r][3] else (x + db, y + da)
        c = 1 - core if flip else core
        first = (lax.rem(px, RING) * 2 + c) * RING + lax.rem(py, RING)
        return rings[r][1].at[pl.ds(pl.multiple_of(first * rows + lo, half), size), rings[r][2]]

    def own_block(r):
        return rings[r][0].at[:, rings[r][2]]

    def to_core_copy(r, ia, ib):
        there = block(r, DELTAS[ia], DELTAS[ib])
        return copy(own_block(r) if ia == 0 and ib == 0 else there, there, cc_s.at[r, ia, ib], cc_r.at[r, ia, ib], near(0, 1))

    def to_core(r, ia, ib):
        go(to_core_copy, r, ia, ib)

    def first_copy(r, side):
        return copy(own_block(r), block(r, 0, 0), p1_s.at[r, side], p1_r.at[r, side], axis(r, 1)(ahead(side)))

    def first_own(r, side):
        go(first_copy, r, side)

    def first_far_copy(r, side):
        part = block(r, back(side), 0, 0, side * half, half)
        return copy(part, part, p2_s.at[r, side], p2_r.at[r, side], axis(r, 1)(ahead(side)))

    def first_forward(r, side):
        there = block(r, back(side), 0)
        copy(there, there, p1_s.at[r, side], p1_r.at[r, side], {"datb": z}).wait_recv()
        go(first_far_copy, r, side)

    def block_on(r, ia):
        for side in range(2 if ia == 3 else 0):
            part = block(r, 2, 0, 0, side * half, half)
            copy(part, part, p2_s.at[r, side], p2_r.at[r, side], {"datb": z}).wait_recv()
        for side in range(2):
            go(second_copy, r, side, ia)
        to_core(r, ia, 0)

    def second_copy(r, side, ia):
        there = block(r, DELTAS[ia], 0)
        return copy(there if ia else own_block(r), there, q1_s.at[r, side, ia], q1_r.at[r, side, ia], axis(r, 2)(ahead(side)))

    def second_far_copy(r, ia):
        side = ia // 2
        there = block(r, DELTAS[ia], back(side))
        return copy(there, there, q2_s.at[r, ia], q2_r.at[r, ia], axis(r, 2)(ahead(side)))

    def second_forward(r, ia, side):
        there = block(r, DELTAS[ia], back(side))
        copy(there, there, q1_s.at[r, side, ia], q1_r.at[r, side, ia], {"datb": z}).wait_recv()
        if ia // 2 == side:
            go(second_far_copy, r, ia)
        to_core(r, ia, 1 if side == 0 else 2)

    def second_far(r, ia):
        there = block(r, DELTAS[ia], 2)
        copy(there, there, q2_s.at[r, ia], q2_r.at[r, ia], {"datb": z}).wait_recv()
        to_core(r, ia, 3)

    def rows_in(r):
        for ia in range(RING):
            for ib in range(RING):
                there = block(r, DELTAS[ia], DELTAS[ib], 1)
                copy(there, there, cc_s.at[r, ia, ib], cc_r.at[r, ia, ib], {"datb": z}).wait_recv()

    local = [pltpu.make_async_copy(pieces.at[t, i8], slot(t, z, i8), own_sem.at[t]) for t in range(3)]
    local += [pltpu.make_async_copy(own_block(r), block(r, 0, 0), own_sem.at[3 + r]) for r in range(3)]

    n_chunk = tokens // CHUNK

    def w_load(t):
        return pltpu.make_async_copy(fulls[t], wv.at[t], wv_sem.at[t])

    def row_load(src, i, buf):
        first = pl.ds(pl.multiple_of(i * CHUNK, CHUNK), CHUNK)
        return pltpu.make_async_copy(src.at[first], rowbuf.at[buf], row_sem.at[buf])

    def chunk_loop(src, work, between):
        row_load(src, 0, 0).start()

        def body(i, carry):
            buf = lax.rem(i, 2)

            @pl.when(i + 1 < n_chunk)
            def _():
                row_load(src, i + 1, 1 - buf).start()

            for k, step in enumerate(between):
                pl.when(i == k)(step)
            row_load(src, i, buf).wait()
            work(i, buf)
            return carry

        lax.fori_loop(0, n_chunk, body, 0)

    def chunk_rows(i):
        return pl.ds(pl.multiple_of(i * CHUNK, CHUNK), CHUNK)

    def pre_work(i, buf):
        rb = rowbuf[buf]
        av[chunk_rows(i)] = jnp.dot(rb, wv[0], preferred_element_type=F32).astype(BF16)
        bv[chunk_rows(i)] = jnp.dot(rb, wv[1], preferred_element_type=F32).astype(BF16)

    def out_copies(i, buf):
        cs = [pltpu.make_async_copy(hst.at[buf, j], h_all.at[j, chunk_rows(i)], hst_sem.at[buf, j]) for j in range(3)]
        return cs + [pltpu.make_async_copy(fst.at[buf, j], f_all.at[j, :, chunk_rows(i)], fst_sem.at[buf, j]) for j in range(3)]

    def post_work(i, buf):
        g = jnp.dot(rowbuf[buf], wv[2], preferred_element_type=F32).astype(BF16).astype(F32)

        @pl.when(i >= 2)
        def _():
            for c in out_copies(i - 2, buf):
                c.wait()

        a, b = av[chunk_rows(i)].astype(F32), bv[chunk_rows(i)].astype(F32)
        sig = jax.nn.sigmoid(a)
        silu = a * sig
        da = g * b * sig * (1.0 + a * (1.0 - sig))
        for j, v in enumerate((da, g * silu, silu * b)):
            hst[buf, j] = v.astype(BF16)
            fst[buf, j] = v.T.astype(BF16)
        for c in out_copies(i, buf):
            c.start()

    steps = (exchange, z_first, z_second, first_own, first_forward, block_on, second_forward, second_far, weights_done)

    def run(group):
        for which, *args in group:
            steps[which](*args)

    with jax.named_scope("begin"):
        for t in range(3):
            cut_pieces(t)
        pl.semaphore_wait(barrier, len(others))
        for c in local:
            c.start()
    with jax.named_scope("gather"):
        run(GATHER_STEPS)
        local[3].wait()
        rows_in(0)
        w_load(0).wait()
        w_load(1).wait()
    with jax.named_scope("gate_up"):
        chunk_loop(tok_all, pre_work, [functools.partial(run, group) for group in CHUNK_STEPS])
    with jax.named_scope("late"):
        run(LATE_STEPS)
        for r in (1, 2):
            local[3 + r].wait()
            rows_in(r)
        w_load(2).wait()
    with jax.named_scope("down"):
        chunk_loop(grad_all, post_work, ())
        for i in (n_chunk - 2, n_chunk - 1):
            for c in out_copies(i, i % 2):
                c.wait()
    for make, args in started:
        make(*args).wait_send()


def forward_gather(sg, su, sd, tok, grad):
    n8 = 2 * RING
    dp, nf = sg.shape[0], sg.shape[1] // n8
    rows, d = tok.shape
    tokens = rows * RING * n8
    hbm = pl.BlockSpec(memory_space=pl.ANY)
    dma = pltpu.SemaphoreType.DMA
    sds = jax.ShapeDtypeStruct
    return pl.pallas_call(
        forward_kernel,
        out_shape=[sds((d, nf), BF16)] * 3 + [sds((tokens, d), BF16)] * 2 + [sds((3, nf, tokens), BF16), sds((3, tokens, nf), BF16)],
        in_specs=[hbm] * 5,
        out_specs=[hbm] * 7,
        scratch_shapes=[
            pltpu.VMEM((3,) + sg.shape, BF16),
            pltpu.VMEM((3, n8, dp, nf), BF16),
            pltpu.VMEM((3, d, nf), BF16),
            pltpu.VMEM((2, CHUNK, d), BF16),
            pltpu.VMEM((tokens, nf), BF16),
            pltpu.VMEM((tokens, nf), BF16),
            pltpu.VMEM((2, 3, CHUNK, nf), BF16),
            pltpu.VMEM((2, 3, nf, CHUNK), BF16),
            dma((6,)),
            dma((3, n8)), dma((3, n8)),
            dma((3, 2, n8)), dma((3, 2, n8)),
            dma((3, 2, n8 // 2)), dma((3, 2, n8 // 2)),
            dma((3, 2)), dma((3, 2)),
            dma((3, 2)), dma((3, 2)),
            dma((3, 2, RING)), dma((3, 2, RING)),
            dma((3, RING)), dma((3, RING)),
            dma((3, RING, RING)), dma((3, RING, RING)),
            dma((3,)), dma((3,)), dma((2,)), dma((2, 3)), dma((2, 3)),
        ],
        compiler_params=pltpu.CompilerParams(collective_id=0, has_side_effects=True, vmem_limit_bytes=60 * 1024 * 1024),
        cost_estimate=pl.CostEstimate(flops=6 * nf * tokens * d, bytes_accessed=100_000_000, transcendentals=0),
        name="forward_gather",
    )(sg, su, sd, tok, grad)


LANE = 128
OUT_COLS = 512


def reduce_kernel(f_ref, h_ref, wg, wu, wd, tok, grad, tok_own, grad_own,
                  og, ou, od, out, gin, ra, rb, give, rc, part, ra1, rb1, sd1, mid, ra2, rb2, sd2,
                  ff, blk, far, nxt, tmp, stage,
                  ff_sem, blk_sem, tmp_sem, a_s, a_r, u_s, u_r, e_s, e_r, own_sem,
                  c_s, c_r, a1_s, a1_r, f1_s, f1_r, d1_s, d1_r, a2_s, a2_r, f2_s, f2_r, d2_s, d2_r):
    z, y = lax.axis_index("datb"), lax.axis_index("model")
    x, core = lax.axis_index("x"), lax.axis_index("core")
    i8 = 2 * x + core
    n8 = 2 * RING
    nf = ff.shape[1]
    half = nf // 2
    cols = blk.shape[2]
    dp = cols // n8
    outs = (og, ou, od)

    def zdev(k):
        return {"datb": lax.rem(z + k, RING)}

    def xdev(k):
        return {"x": lax.rem(x + k, RING)}

    def ydev(k):
        return {"model": lax.rem(y + k, RING)}

    def near(dx, dc):
        return {"x": lax.rem(x + dx, RING), "core": lax.rem(core + dc, 2)}

    def peer(dx, dc):
        return 2 * lax.rem(x + dx, RING) + lax.rem(core + dc, 2)

    def rcopy(src, dst, s, r, dev):
        return pltpu.make_async_remote_copy(src_ref=src, dst_ref=dst, send_sem=s, recv_sem=r, device_id=dev, device_id_type=MESH_ID)

    def start(copies):
        for c in copies:
            c.start()

    def received(copies):
        for c in copies:
            c.wait_recv()

    def sent(copies):
        for c in copies:
            c.wait_send()

    barrier = pltpu.get_barrier_semaphore()
    others = [zdev(1), zdev(3), ydev(1), ydev(3)] + [near(*n) for n in NEAR[1:]]
    for dev in others:
        pl.semaphore_signal(barrier, inc=1, device_id=dev, device_id_type=MESH_ID)

    def ff_load(t):
        return pltpu.make_async_copy(f_ref.at[t], ff.at[t], ff_sem.at[t])

    def blk_load(t, slot, k):
        src = tok if t < 2 else grad
        lanes = pl.ds(pl.multiple_of(lax.rem(z + k, RING) * cols, LANE), cols)
        return pltpu.make_async_copy(src.at[:, lanes], blk.at[slot], blk_sem.at[slot])

    def product(t, slot, dst):
        step = 2 * LANE

        def one(n, carry):
            lanes = pl.ds(pl.multiple_of(jnp.minimum(n * step, cols - step), LANE), step)
            dst[:nf, lanes] = jnp.dot(ff[t], blk[slot, :, lanes], preferred_element_type=F32)
            return carry

        lax.fori_loop(0, -(-cols // step), one, 0)

    lo, hi = pl.ds(0, half), pl.ds(half, half)

    def a_copies(t):
        return [rcopy(far.at[t, rows], ra.at[t, rows], a_s.at[t, s], a_r.at[t, s], zdev(k)) for s, rows, k in ((0, lo, 1), (1, hi, 3))]

    tiles = stage.shape[2] // LANE

    def tile_rows(tile):
        return pl.ds(tile * LANE, min(LANE, nf - tile * LANE))

    def unit_copies(t, tile):
        at = tile_rows(tile)
        return [rcopy(nxt.at[t, s, at], rb.at[t, s, at], u_s.at[t, s, tile], u_r.at[t, s, tile], zdev(1 + 2 * s)) for s in range(2)]

    def far_block(t):
        ff_load(t).wait()
        if t != 1:
            blk_load(t, t // 2, 2).wait()
        product(t, t // 2, far.at[t])
        start(a_copies(t))

    def next_blocks(t):
        for s in range(2):
            blk_load(t, s, 1 + 2 * s).start()
        for s in range(2):
            blk_load(t, s, 1 + 2 * s).wait()
            product(t, s, nxt.at[t, s])
        received(a_copies(t))
        cs = [pltpu.make_async_copy(ra.at[t, rows], tmp.at[s, rows], tmp_sem.at[s]) for s, rows in ((0, lo), (1, hi))]
        start(cs)
        for c, (s, rows) in zip(cs, ((0, lo), (1, hi))):
            c.wait()
            nxt[t, s, rows] += tmp[s, rows]
        for tile in range(tiles):
            start(unit_copies(t, tile))

    def own_block(t):
        blk_load(t, 0, 0).start()
        sent(a_copies(t))
        blk_load(t, 0, 0).wait()
        product(t, 0, far.at[t])

    def hand_out(t, tile):
        lanes = pl.ds(tile * LANE, LANE)
        cs = []
        for k in range(1, n8):
            at = pl.ds(pl.multiple_of(peer(*NEAR[k]) * dp, 8), dp)
            cs.append(rcopy(stage.at[t % 2, at, lanes], outs[t].at[i8, :, lanes], e_s.at[t, tile, k], e_r.at[t, tile, k], near(*NEAR[k])))
        at = pl.ds(pl.multiple_of(i8 * dp, 8), dp)
        return cs, pltpu.make_async_copy(stage.at[t % 2, at, lanes], outs[t].at[i8, :, lanes], own_sem.at[t, tile])

    def handed(t, tile):
        cs, mine = hand_out(t, tile)
        sent(cs)
        mine.wait()

    def finish(t, tile):
        received(unit_copies(t, tile))
        at = tile_rows(tile)
        cs = [pltpu.make_async_copy(rb.at[t, s, at], tmp.at[s, at], tmp_sem.at[s]) for s in range(2)]
        start(cs)
        if t == 2:
            handed(0, tile)
        for c in cs:
            c.wait()
        wide = pl.ds(tile * LANE, LANE)
        stage[t % 2, :, wide] = (far[t, wide] + tmp[0, wide] + tmp[1, wide]).T
        cs, mine = hand_out(t, tile)
        start(cs + [mine])

    d = tok.shape[1]
    half_rows = tok_own.shape[1]
    rows = 2 * half_rows
    blocks = d // min(OUT_COLS, d)
    width = d // blocks

    def row_products(r, keep):
        side = core if keep else 1 - core
        terms = ((2, wd),) if r == 0 else ((0, wg), (1, wu))
        specs, args = [], []
        for t, w in terms:
            specs += [pl.BlockSpec((1, RING, 1, RING * rows, nf), lambda j, t=t: (t, 0, side, 0, 0)), pl.BlockSpec((width, nf), lambda j: (j, 0))]
            args += [h_ref, w]
        wide = pl.BlockSpec((RING, RING, rows, width), lambda j: (0, 0, 0, j))
        if keep:
            specs.append(wide)
            args.append(rc.at[r])

        def body(*refs):
            total = None
            for i in range(len(terms)):
                h = refs[2 * i][...].reshape(RING * RING * rows, nf)
                prod = dot(h, refs[2 * i + 1][...], 1, 1)
                total = prod if total is None else total + prod
            if keep:
                total = total + refs[-2][...].astype(F32).reshape(total.shape)
            refs[-1][...] = total.astype(BF16).reshape(RING, RING, rows, width)

        pltpu.emit_pipeline(body, grid=(blocks,), in_specs=specs, out_specs=[wide])(*args, (part if keep else give).at[r])

    def core_copy(r):
        return rcopy(give.at[r], rc.at[r], c_s.at[r], c_r.at[r], near(0, 1))

    def level(n):
        if n == 1:
            def piece(r, k, h):
                return part.at[r, pl.ds(2 * h, 2), lax.rem(y + k, RING)]
            return ydev, piece, ra1, rb1, sd1, (a1_s, a1_r, f1_s, f1_r, d1_s, d1_r)

        def piece(r, k, h):
            return mid.at[r, lax.rem(x + k, RING), pl.ds(h, 1)]
        return xdev, piece, ra2, rb2, sd2, (a2_s, a2_r, f2_s, f2_r, d2_s, d2_r)

    def ring_a(r, n):
        dev, piece, rfar, _, _, sems = level(n)
        return [rcopy(piece(r, 2, s), rfar.at[r, s], sems[0].at[r, s], sems[1].at[r, s], dev(1 + 2 * s)) for s in range(2)]

    def ring_f(r, n):
        dev, piece, _, rnear, _, sems = level(n)
        return [rcopy(piece(r, 1 + 2 * s, 1 - s), rnear.at[r, s, 1 - s], sems[2].at[r, s], sems[3].at[r, s], dev(1 + 2 * s)) for s in range(2)]

    def ring_d(r, n):
        dev, _, _, rnear, dep, sems = level(n)
        return [rcopy(dep.at[r, s], rnear.at[r, s, s], sems[4].at[r, s], sems[5].at[r, s], dev(1 + 2 * s)) for s in range(2)]

    def add(srcs, dst):
        n = dst.shape[0]
        specs = [pl.BlockSpec((1,) + tuple(ref.shape[1:]), lambda i, rank=len(ref.shape): (i,) + (0,) * (rank - 1)) for ref in [*srcs, dst]]

        def body(*refs):
            total = refs[0][...].astype(F32)
            for ref in refs[1:-1]:
                total = total + ref[...].astype(F32)
            refs[-1][...] = total.astype(BF16).reshape(refs[-1].shape)

        pltpu.emit_pipeline(body, grid=(n,), in_specs=specs[:-1], out_specs=specs[-1:])(*srcs, dst)

    def ring_first(r, n):
        start(ring_a(r, n) + ring_f(r, n))

    def ring_dependent(r, n):
        _, piece, rfar, _, dep, _ = level(n)
        received(ring_a(r, n))
        for s in range(2):
            add([piece(r, 1 + 2 * s, s), rfar.at[r, s]], dep.at[r, s])
            ring_d(r, n)[s].start()

    def ring_last(r, n):
        _, piece, _, rnear, _, _ = level(n)
        received(ring_f(r, n) + ring_d(r, n))
        for h in range(2):
            if n == 1:
                add([piece(r, 0, h), rnear.at[r, 0, h], rnear.at[r, 1, h]], mid.at[r, pl.ds(2 * h, 2)])
            else:
                own, res = ((tok_own, out), (grad_own, gin))[r]
                hs = pl.ds(h, 1)
                add([own.at[hs], piece(r, 0, h), rnear.at[r, 0, h], rnear.at[r, 1, h]], res.at[hs])

    for t in range(3):
        ff_load(t).start()
    blk_load(0, 0, 2).start()
    blk_load(2, 1, 2).start()
    pl.semaphore_wait(barrier, len(others))

    def give_rows(r):
        row_products(r, False)
        core_copy(r).start()

    def keep_rows(r):
        core_copy(r).wait_recv()
        row_products(r, True)

    order = [
        (far_block, 0), (far_block, 1), (far_block, 2), (give_rows, 0), (give_rows, 1), (keep_rows, 0), (ring_first, 0, 1),
        (next_blocks, 0), (own_block, 0), (next_blocks, 1), (own_block, 1), (ring_dependent, 0, 1), (keep_rows, 1), (ring_first, 1, 1),
        (finish, 0, 0), (finish, 0, 1), (next_blocks, 2), (finish, 0, 2), (own_block, 2), (finish, 0, 3), (ring_last, 0, 1),
        (ring_first, 0, 2), (finish, 0, 4), (ring_dependent, 0, 2), (finish, 1, 0), (ring_dependent, 1, 1), (finish, 1, 1),
        (ring_last, 0, 2), (finish, 1, 2), (finish, 1, 3), (finish, 1, 4), (ring_last, 1, 1), (ring_first, 1, 2), (finish, 2, 0),
        (ring_dependent, 1, 2), (finish, 2, 1), (finish, 2, 2), (ring_last, 1, 2), (finish, 2, 3), (finish, 2, 4),
    ]
    for fn, *args in order:
        with jax.named_scope("_".join(str(v) for v in [fn.__name__, *args])):
            fn(*args)

    for t in range(3):
        for tile in range(tiles):
            sent(unit_copies(t, tile))
            received(hand_out(t, tile)[0])
            if t:
                handed(t, tile)
    for r in range(2):
        core_copy(r).wait_send()
        for n in (1, 2):
            sent(ring_a(r, n) + ring_f(r, n) + ring_d(r, n))


def backward_reduce(f_all, h_all, wg, wu, wd, tok, grad, tok_own, grad_own):
    _, nf, tokens = f_all.shape
    rows, d = tok_own.shape
    cols = d // RING
    n8 = 2 * RING
    tiles = -(-nf // LANE)
    padded = tiles * LANE
    hbm = pl.BlockSpec(memory_space=pl.ANY)
    dma = pltpu.SemaphoreType.DMA
    sds = jax.ShapeDtypeStruct
    halves = (2, rows // 2, d)
    res = pl.pallas_call(
        reduce_kernel,
        out_shape=[sds((n8, cols // n8, padded), F32)] * 3 + [sds(halves, BF16)] * 2 + [
            sds((3, nf, cols), F32), sds((3, 2, nf, cols), F32),
            sds((2, RING, RING, rows, d), BF16), sds((2, RING, RING, rows, d), BF16), sds((2, RING, RING, rows, d), BF16),
            sds((2, 2, 2, rows, d), BF16), sds((2, 2, 2, 2, rows, d), BF16), sds((2, 2, 2, rows, d), BF16),
            sds((2, RING, 2, rows // 2, d), BF16),
            sds((2, 2, 1, rows // 2, d), BF16), sds((2, 2, 2, 1, rows // 2, d), BF16), sds((2, 2, 1, rows // 2, d), BF16),
        ],
        in_specs=[hbm] * 9,
        out_specs=[hbm] * 17,
        scratch_shapes=[
            pltpu.VMEM((3, nf, tokens), BF16),
            pltpu.VMEM((2, tokens, cols), BF16),
            pltpu.VMEM((3, padded, cols), F32),
            pltpu.VMEM((3, 2, nf, cols), F32),
            pltpu.VMEM((2, padded, cols), F32),
            pltpu.VMEM((2, cols, padded), F32),
            dma((3,)), dma((2,)), dma((2,)),
            dma((3, 2)), dma((3, 2)),
            dma((3, 2, tiles)), dma((3, 2, tiles)),
            dma((3, tiles, n8)), dma((3, tiles, n8)),
            dma((3, tiles)),
            dma((2,)), dma((2,)),
        ] + [dma((2, 2))] * 12,
        compiler_params=pltpu.CompilerParams(collective_id=1, has_side_effects=True, vmem_limit_bytes=63 * 1024 * 1024),
        cost_estimate=pl.CostEstimate(flops=12 * nf * tokens * d, bytes_accessed=200_000_000, transcendentals=0),
        name="backward_reduce",
    )(f_all, h_all.reshape(3, RING, 2, RING * rows, nf), wg, wu, wd, tok, grad, tok_own.reshape(halves), grad_own.reshape(halves))
    return res[:3], res[3].reshape(rows, d), res[4].reshape(rows, d)


def assemble_kernel(og, ou, od, out, gin, g, u, w, res, gres, buf, flat, in_sem, out_sem, row_buf, row_sem):
    n8, nf = og.shape[0], g.shape[1] // og.shape[0]
    srcs, dsts = (og, ou, od), (g, u, w)
    rows_in = [pltpu.make_async_copy(src, row_buf.at[r], row_sem.at[r]) for r, src in enumerate((out, gin))]
    loads = [pltpu.make_async_copy(src, buf.at[t], in_sem.at[t]) for t, src in enumerate(srcs)]
    stores = [pltpu.make_async_copy(flat.at[t], dst, out_sem.at[t]) for t, dst in enumerate(dsts)]
    for c in loads + rows_in:
        c.start()
    for t in range(3):
        loads[t].wait()
        for j in range(n8):
            flat[t, :, j * nf:(j + 1) * nf] = buf[t, j, :, :nf]
        stores[t].start()
    rows_out = [pltpu.make_async_copy(row_buf.at[r], dst, row_sem.at[r]) for r, dst in enumerate((res, gres))]
    for c in rows_in:
        c.wait()
    for c in rows_out:
        c.start()
    for c in stores + rows_out:
        c.wait()


def assemble(sums, out, gin, ff):
    n8, dp, padded = sums[0].shape
    hbm = pl.BlockSpec(memory_space=pl.ANY)
    dma = pltpu.SemaphoreType.DMA
    sds = jax.ShapeDtypeStruct
    return pl.pallas_call(
        assemble_kernel,
        out_shape=[sds((dp, ff), F32)] * 3 + [sds(out.shape, BF16)] * 2,
        in_specs=[hbm] * 5,
        out_specs=[hbm] * 5,
        scratch_shapes=[
            pltpu.VMEM((3, n8, dp, padded), F32), pltpu.VMEM((3, dp, ff), F32), dma((3,)), dma((3,)),
            pltpu.VMEM((2,) + out.shape, BF16), dma((2,)),
        ],
        compiler_params=pltpu.CompilerParams(vmem_limit_bytes=63 * 1024 * 1024),
        name="assemble",
    )(*sums, out, gin)


def solution(mesh):
    nz, ny, nd = mesh.shape["datb"], mesh.shape["model"], mesh.shape["data"]
    fine = Mesh(mesh.devices.reshape(nz, ny, nd // 2, 2), ("datb", "model", "x", "core"))

    def local_step(tok_loc, wg_loc, wu_loc, wd_loc, grad_loc):
        wg, wu, wdt, tok, grad, f_all, h_all = forward_gather(wg_loc, wu_loc, wd_loc.T, tok_loc, grad_loc)
        sums, out, grad_in = backward_reduce(f_all, h_all, wg, wu, wdt, tok, grad, tok_loc, grad_loc)
        grad_gate, grad_up, grad_down_t, out, grad_in = assemble(sums, out, grad_in, wg_loc.shape[1])
        return out, grad_in, grad_gate, grad_up, grad_down_t.T

    return jax.shard_map(local_step, mesh=fine, in_specs=(ROW_SPEC, GATE_SPEC, GATE_SPEC, DOWN_SPEC, ROW_SPEC), out_specs=(ROW_SPEC, ROW_SPEC, GATE_SPEC, GATE_SPEC, DOWN_SPEC), check_vma=False)
```

```python
import functools

import jax
import jax.numpy as jnp
from jax import lax
from jax.experimental import pallas as pl
from jax.experimental.pallas import tpu as pltpu
from jax.sharding import Mesh
from jax.sharding import PartitionSpec as P

ROW_SPEC = P(("datb", "x", "core", "model"), None)
GATE_SPEC = P(("datb", "x", "core"), "model")
DOWN_SPEC = P("model", ("datb", "x", "core"))
BF16 = jnp.bfloat16
F32 = jnp.float32
MESH_ID = pl.DeviceIdType.MESH
RING = 4
NEAR = ((0, 0), (0, 1), (1, 0), (3, 0), (1, 1), (3, 1), (2, 0), (2, 1))
DELTAS = (0, 3, 1, 2)
LANE = 128
OUT_COLS = 512
EX, Z1, Z2, P1, P2, BL, Q1, Q2, WD = range(9)
GATHER_STEPS = (
    (Z1, 0, 0), (EX, 0, 1), (EX, 0, 2), (EX, 0, 3), (EX, 0, 4), (EX, 0, 5), (EX, 0, 6), (EX, 0, 7), (Z1, 1, 0), (BL, 0, 0), (Z1, 2, 0),
    (EX, 1, 1), (EX, 2, 1), (P1, 2, 0), (P1, 2, 1), (P1, 0, 0), (P1, 0, 1), (Z1, 0, 1), (Z1, 1, 1), (BL, 1, 0), (Z1, 2, 1), (Z2, 0, 0, 0),
    (Z1, 0, 2), (EX, 1, 2), (EX, 1, 3), (Q1, 0, 0, 0), (Q1, 0, 0, 1), (Z1, 0, 3), (EX, 1, 4), (EX, 1, 5), (Z2, 0, 0, 1), (P2, 2, 1),
    (EX, 1, 6), (EX, 1, 7), (P2, 2, 0), (Z1, 0, 4), (Q1, 1, 0, 0), (Q1, 1, 0, 1), (Z1, 0, 5), (EX, 2, 2), (EX, 2, 3), (Z1, 0, 6), (P2, 0, 0),
    (P2, 0, 1), (BL, 0, 1), (Z2, 0, 0, 2), (Z2, 0, 1, 0), (Q2, 0, 0), (EX, 2, 4), (EX, 2, 5), (Z2, 0, 0, 3), (Z2, 0, 1, 1), (EX, 2, 6),
    (EX, 2, 7), (Z1, 0, 7), (Z2, 0, 1, 2), (BL, 0, 2), (Z2, 1, 0, 0), (Q2, 1, 0), (Q1, 0, 1, 1), (P1, 1, 0), (P1, 1, 1), (Z2, 1, 0, 1),
    (Z1, 1, 2), (Z2, 0, 1, 3), (BL, 2, 1), (BL, 0, 3), (Z1, 1, 3), (Q1, 0, 2, 1), (Z1, 1, 4), (BL, 2, 2), (Z1, 1, 5), (WD, 0), (BL, 2, 0),
    (Q1, 0, 1, 0), (Z1, 1, 6), (Q1, 0, 2, 0), (Q1, 0, 3, 1), (Z1, 1, 7), (Z2, 1, 1, 0), (P2, 1, 0), (P2, 1, 1), (Z2, 1, 0, 2), (BL, 2, 3),
    (Z2, 1, 1, 1), (Q1, 2, 1, 1), (Z2, 1, 0, 3), (BL, 1, 1), (Z2, 1, 1, 2), (Q1, 2, 1, 0), (Q1, 2, 2, 0), (Q1, 2, 2, 1), (Q1, 0, 3, 0),
    (Q2, 0, 2), (Z2, 2, 0, 0), (Z2, 1, 1, 3), (BL, 1, 2), (Z2, 2, 0, 1), (Q1, 2, 0, 0), (Q1, 2, 0, 1), (Z1, 2, 2), (BL, 1, 3), (Z1, 2, 3),
    (Q2, 0, 1), (Q2, 0, 3), (Q1, 2, 3, 0), (Q1, 2, 3, 1), (Z1, 2, 4), (WD, 1),
)
CHUNK_STEPS = (
    (
        (Q2, 2, 1), (Q2, 2, 2), (Z1, 2, 5), (Q1, 1, 1, 0), (Q1, 1, 1, 1),
    ),
    (
        (Z1, 2, 6), (Q1, 1, 2, 0), (Q1, 1, 2, 1),
    ),
    (
        (Q2, 2, 0), (Q2, 2, 3), (Z2, 2, 1, 0), (Z2, 2, 0, 2), (Q1, 1, 3, 0), (Q1, 1, 3, 1), (Z1, 2, 7),
    ),
    (
        (Z2, 2, 1, 1), (Z2, 2, 1, 2), (Z2, 2, 0, 3),
    ),
    (
        (Q2, 1, 1), (Q2, 1, 2),
    ),
    (
        (Q2, 1, 3), (Z2, 2, 1, 3),
    ),
    (),
)
LATE_STEPS = (
    (WD, 2),
)
Z_ORDER = (2, 0, 1)


def dot(a, b, ca, cb):
    return lax.dot_general(a, b, (((ca,), (cb,)), ((), ())), preferred_element_type=F32)


def layer_kernel(sg, su, sd, tok, grad, tok_own, grad_own,
                 og, ou, od, out, gin, wg, wu, wd, tok_all, grad_all, h_all, ra, rb, give, rc, part, ra1, rb1, sd1, mid, ra2, rb2, sd2,
                 ff, blk, far, nxt,
                 own_sem, ex_s, ex_r, z1_s, z1_r, z2_s, z2_r, p1_s, p1_r, p2_s, p2_r, q1_s, q1_r, q2_s, q2_r, cc_s, cc_r,
                 sh_sem, wv_sem, row_sem, hst_sem, blk_sem, tmp_sem, a_s, a_r, u_s, u_r, e_s, e_r, out_sem,
                 c_s, c_r, a1_s, a1_r, f1_s, f1_r, d1_s, d1_r, a2_s, a2_r, f2_s, f2_r, d2_s, d2_r):
    z, y = lax.axis_index("datb"), lax.axis_index("model")
    x, core = lax.axis_index("x"), lax.axis_index("core")
    i8 = 2 * x + core
    n8 = 2 * RING
    rows, d = tok.shape
    half_rows = rows // 2
    chunk = RING * rows
    n_chunk = n8
    nf, tokens = ff.shape[1:]
    dp = sg.shape[0]
    half = nf // 2
    cols = blk.shape[2]
    tiles = far.shape[1] // LANE
    outs = (og, ou, od)

    zs, ys, xs = ([v] + [lax.rem(v + k, RING) for k in range(1, RING)] for v in (z, y, x))
    cores = (core, 1 - core)
    peers = [[2 * v + c for c in cores] for v in xs]
    slot_at = [[[pl.multiple_of((zz * n8 + peers[dx][dc]) * dp, 16) for dc in range(2)] for dx in range(RING)] for zz in zs]
    hand_at = [[pl.multiple_of(p * dp, 8) for p in row] for row in peers]
    rows_at = [[[pl.multiple_of((peers[dx][dc] * RING + yy) * rows, half_rows) for dc in range(2)] for yy in ys] for dx in range(RING)]
    lanes_at = [pl.multiple_of(zz * cols, LANE) for zz in zs]

    def peer(dx, dc):
        return peers[dx][dc]

    def zdev(k):
        return {"datb": zs[k]}

    def xdev(k):
        return {"x": xs[k]}

    def ydev(k):
        return {"model": ys[k]}

    def near(dx, dc):
        return {"x": xs[dx], "core": cores[dc]}

    def copy(src, dst, s, r, dev):
        return pltpu.make_async_remote_copy(src_ref=src, dst_ref=dst, send_sem=s, recv_sem=r, device_id=dev, device_id_type=MESH_ID)

    rcopy = copy

    def start(copies):
        for c in copies:
            c.start()

    def received(copies):
        for c in copies:
            c.wait_recv()

    def sent(copies):
        for c in copies:
            c.wait_send()

    barrier = pltpu.get_barrier_semaphore()
    others = [zdev(1), zdev(3), ydev(1), ydev(3)] + [near(*n) for n in NEAR[1:]]
    for dev in others:
        pl.semaphore_signal(barrier, inc=1, device_id=dev, device_id_type=MESH_ID)

    def blk_load(t, slot, k):
        src = tok_all if t < 2 else grad_all
        return pltpu.make_async_copy(src.at[:, pl.ds(lanes_at[k], cols)], blk.at[slot], blk_sem.at[slot])

    def product(t, slot, dst):
        step = 2 * LANE

        def one(n, carry):
            lanes = pl.ds(pl.multiple_of(jnp.minimum(n * step, cols - step), LANE), step)
            dst[:nf, lanes] = jnp.dot(ff[t], blk[slot, :, lanes], preferred_element_type=F32)
            return carry

        lax.fori_loop(0, -(-cols // step), one, 0)

    lo, hi = pl.ds(0, half), pl.ds(half, half)

    def a_copies(t):
        return [rcopy(far.at[t, rows], ra.at[t, rows], a_s.at[t, s], a_r.at[t, s], zdev(k)) for s, rows, k in ((0, lo, 1), (1, hi, 3))]

    def tile_rows(tile):
        return pl.ds(tile * LANE, min(LANE, nf - tile * LANE))

    def unit_copies(t, tile):
        at = tile_rows(tile)
        return [rcopy(nxt.at[t, s, at], rb.at[t, s, at], u_s.at[t, s, tile], u_r.at[t, s, tile], zdev(1 + 2 * s)) for s in range(2)]

    def far_block(t):
        blk_load(t, 0, 2).start()
        blk_load(t, 0, 2).wait()
        product(t, 0, far.at[t])
        start(a_copies(t))

    def forward_phase(shard, pieces, wv, rowbuf, av, bv, hst):
        fulls = (wg, wu, wd)
        loads = [pltpu.make_async_copy(src, shard.at[t], sh_sem.at[t]) for t, src in enumerate((sg, su, sd))]
        for c in loads:
            c.start()

        def cut_pieces(t):
            loads[t].wait()
            for j in range(n8):
                pieces[t, j] = shard[t, :, j * nf:(j + 1) * nf]

        started = []

        def go(make, *args):
            make(*args).start()
            started.append((make, args))

        def slot(t, k, source):
            dx, dc = source
            return fulls[t].at[pl.ds(slot_at[k][dx][dc], dp)]

        def source(k):
            dx, dc = NEAR[k]
            return (RING - dx) % RING, dc

        def back(side):
            return 3 if side == 0 else 1

        def ahead(side):
            return 1 if side == 0 else 3

        def exchange_copy(t, k):
            return copy(pieces.at[t, peer(*NEAR[k])], slot(t, 0, NEAR[0]), ex_s.at[t, k], ex_r.at[t, k], near(*NEAR[k]))

        def exchange(t, k):
            go(exchange_copy, t, k)

        def z_first_copy(t, side, k):
            here = slot(t, 0, source(k))
            return copy(here if k else pieces.at[t, i8], here, z1_s.at[t, side, k], z1_r.at[t, side, k], zdev(ahead(side)))

        def z_first(t, k):
            if k:
                here = slot(t, 0, source(k))
                copy(here, here, ex_s.at[t, k], ex_r.at[t, k], {"datb": z}).wait_recv()
            for side in range(2):
                go(z_first_copy, t, side, k)

        def wait_z_first(t, side, k):
            there = slot(t, back(side), source(k))
            copy(there, there, z1_s.at[t, side, k], z1_r.at[t, side, k], {"datb": z}).wait_recv()

        def z_second_copy(t, side, k):
            there = slot(t, back(side), source(k + side * (n8 // 2)))
            return copy(there, there, z2_s.at[t, side, k], z2_r.at[t, side, k], zdev(ahead(side)))

        def z_second(t, side, k):
            wait_z_first(t, side, k + side * (n8 // 2))
            go(z_second_copy, t, side, k)

        def weights_done(t):
            local[t].wait()
            for k in range(n8 // 2):
                wait_z_first(t, 0, n8 // 2 + k)
                wait_z_first(t, 1, k)
                for side in range(2):
                    there = slot(t, 2, source(k + side * (n8 // 2)))
                    copy(there, there, z2_s.at[t, side, k], z2_r.at[t, side, k], {"datb": z}).wait_recv()
            w_load(t).start()

        cut = d // 2
        rings = ((tok, tok_all, pl.ds(0, d), True), (grad, grad_all, pl.ds(0, cut), True), (grad, grad_all, pl.ds(cut, d - cut), False))

        def axis(r, n):
            return xdev if rings[r][3] == (n == 1) else ydev

        def block(r, da, db, flip=0, lo=0, size=rows):
            dx, dy = (da, db) if rings[r][3] else (db, da)
            first = rows_at[dx][dy][flip]
            return rings[r][1].at[pl.ds(pl.multiple_of(first + lo, half_rows) if lo else first, size), rings[r][2]]

        def own_block(r):
            return rings[r][0].at[:, rings[r][2]]

        def to_core_copy(r, ia, ib):
            there = block(r, DELTAS[ia], DELTAS[ib])
            return copy(own_block(r) if ia == 0 and ib == 0 else there, there, cc_s.at[r, ia, ib], cc_r.at[r, ia, ib], near(0, 1))

        def to_core(r, ia, ib):
            go(to_core_copy, r, ia, ib)

        def first_copy(r, side):
            return copy(own_block(r), block(r, 0, 0), p1_s.at[r, side], p1_r.at[r, side], axis(r, 1)(ahead(side)))

        def first_own(r, side):
            go(first_copy, r, side)

        def first_far_copy(r, side):
            part = block(r, back(side), 0, 0, side * half_rows, half_rows)
            return copy(part, part, p2_s.at[r, side], p2_r.at[r, side], axis(r, 1)(ahead(side)))

        def first_forward(r, side):
            there = block(r, back(side), 0)
            copy(there, there, p1_s.at[r, side], p1_r.at[r, side], {"datb": z}).wait_recv()
            go(first_far_copy, r, side)

        def block_on(r, ia):
            for side in range(2 if ia == 3 else 0):
                part = block(r, 2, 0, 0, side * half_rows, half_rows)
                copy(part, part, p2_s.at[r, side], p2_r.at[r, side], {"datb": z}).wait_recv()
            for side in range(2):
                go(second_copy, r, side, ia)
            to_core(r, ia, 0)

        def second_copy(r, side, ia):
            there = block(r, DELTAS[ia], 0)
            return copy(there if ia else own_block(r), there, q1_s.at[r, side, ia], q1_r.at[r, side, ia], axis(r, 2)(ahead(side)))

        def second_far_copy(r, ia):
            side = ia // 2
            there = block(r, DELTAS[ia], back(side))
            return copy(there, there, q2_s.at[r, ia], q2_r.at[r, ia], axis(r, 2)(ahead(side)))

        def second_forward(r, ia, side):
            there = block(r, DELTAS[ia], back(side))
            copy(there, there, q1_s.at[r, side, ia], q1_r.at[r, side, ia], {"datb": z}).wait_recv()
            if ia // 2 == side:
                go(second_far_copy, r, ia)
            to_core(r, ia, 1 if side == 0 else 2)

        def second_far(r, ia):
            there = block(r, DELTAS[ia], 2)
            copy(there, there, q2_s.at[r, ia], q2_r.at[r, ia], {"datb": z}).wait_recv()
            to_core(r, ia, 3)

        def rows_in(r):
            for ia in range(RING):
                for ib in range(RING):
                    there = block(r, DELTAS[ia], DELTAS[ib], 1)
                    copy(there, there, cc_s.at[r, ia, ib], cc_r.at[r, ia, ib], {"datb": z}).wait_recv()

        local = [pltpu.make_async_copy(pieces.at[t, i8], slot(t, 0, NEAR[0]), own_sem.at[t]) for t in range(3)]
        local += [pltpu.make_async_copy(own_block(r), block(r, 0, 0), own_sem.at[3 + r]) for r in range(3)]

        def w_load(t):
            return pltpu.make_async_copy(fulls[t], wv.at[t % 2], wv_sem.at[t])

        def row_load(src, i, buf):
            return pltpu.make_async_copy(src.at[chunk_rows(i)], rowbuf.at[buf], row_sem.at[buf])

        def chunk_loop(src, work, between):
            row_load(src, 0, 0).start()

            def outer(xx, carry):
                def inner(c, carry):
                    i = 2 * xx + c

                    @pl.when(i + 1 < n_chunk)
                    def _():
                        row_load(src, i + 1, 1 - c).start()

                    for k, step in enumerate(between):
                        pl.when(i == k)(step)
                    row_load(src, i, c).wait()
                    work(i, xx, c)
                    return carry

                return lax.fori_loop(0, 2, inner, carry)

            lax.fori_loop(0, RING, outer, 0)

        def chunk_rows(i):
            return pl.ds(pl.multiple_of(i * chunk, chunk), chunk)

        def h_copy(xx, c, slot, j):
            return pltpu.make_async_copy(hst.at[c, slot], h_all.at[j, xx, c], hst_sem.at[c, slot])

        def keep(i, xx, c, slot, j, value):
            @pl.when(xx >= 1)
            def _():
                h_copy(xx - 1, c, slot, j).wait()

            hst[c, slot] = value.astype(BF16)
            h_copy(xx, c, slot, j).start()
            ff[j, :, chunk_rows(i)] = value.T.astype(BF16)

        def kept(slot, j):
            for c in range(2):
                h_copy(RING - 1, c, slot, j).wait()

        def pre_work(i, xx, c):
            rb_ = rowbuf[c]
            a = jnp.dot(rb_, wv[0], preferred_element_type=F32).astype(BF16)
            b = jnp.dot(rb_, wv[1], preferred_element_type=F32).astype(BF16)
            av[chunk_rows(i)] = a
            bv[chunk_rows(i)] = b
            a, b = a.astype(F32), b.astype(F32)
            keep(i, xx, c, 0, 2, a * jax.nn.sigmoid(a) * b)

        def post_work(i, xx, c):
            g = jnp.dot(rowbuf[c], wv[0], preferred_element_type=F32).astype(BF16).astype(F32)
            a, b = av[chunk_rows(i)].astype(F32), bv[chunk_rows(i)].astype(F32)
            sig = jax.nn.sigmoid(a)
            keep(i, xx, c, 0, 0, g * b * sig * (1.0 + a * (1.0 - sig)))
            keep(i, xx, c, 1, 1, g * (a * sig))

        steps = (exchange, z_first, z_second, first_own, first_forward, block_on, second_forward, second_far, weights_done)

        def run(group):
            for which, *args in group:
                steps[which](*args)

        with jax.named_scope("begin"):
            for t in range(3):
                cut_pieces(t)
            pl.semaphore_wait(barrier, len(others))
            for c in local:
                c.start()
        with jax.named_scope("gather"):
            run(GATHER_STEPS)
            local[3].wait()
            rows_in(0)
            w_load(0).wait()
            w_load(1).wait()
        with jax.named_scope("gate_up"):
            chunk_loop(tok_all, pre_work, [functools.partial(run, group) for group in CHUNK_STEPS])
            kept(0, 2)
        with jax.named_scope("rows"):
            for r in (1, 2):
                local[3 + r].wait()
                rows_in(r)
        far_block(2)
        with jax.named_scope("late"):
            run(LATE_STEPS)
            w_load(2).wait()
        with jax.named_scope("down"):
            chunk_loop(grad_all, post_work, ())
            kept(0, 0)
            kept(1, 1)
        for make, args in started:
            make(*args).wait_send()

    def backward_phase(tmp, stage):
        def next_blocks(t):
            for s in range(2):
                blk_load(t, s, 1 + 2 * s).start()
            for s in range(2):
                blk_load(t, s, 1 + 2 * s).wait()
                product(t, s, nxt.at[t, s])
            received(a_copies(t))
            cs = [pltpu.make_async_copy(ra.at[t, rows], tmp.at[s, rows], tmp_sem.at[s]) for s, rows in ((0, lo), (1, hi))]
            start(cs)
            for c, (s, rows) in zip(cs, ((0, lo), (1, hi))):
                c.wait()
                nxt[t, s, rows] += tmp[s, rows]
            for tile in range(tiles):
                start(unit_copies(t, tile))

        def own_block(t):
            blk_load(t, 0, 0).start()
            sent(a_copies(t))
            blk_load(t, 0, 0).wait()
            product(t, 0, far.at[t])

        def slot(t):
            return Z_ORDER.index(t) % 2

        def hand_out(t, tile):
            lanes = pl.ds(tile * LANE, LANE)
            cs = []
            for k in range(1, n8):
                at = pl.ds(hand_at[NEAR[k][0]][NEAR[k][1]], dp)
                cs.append(rcopy(stage.at[slot(t), at, lanes], outs[t].at[i8, :, lanes], e_s.at[t, tile, k], e_r.at[t, tile, k], near(*NEAR[k])))
            at = pl.ds(hand_at[0][0], dp)
            return cs, pltpu.make_async_copy(stage.at[slot(t), at, lanes], outs[t].at[i8, :, lanes], out_sem.at[t, tile])

        def handed(t, tile):
            cs, mine = hand_out(t, tile)
            sent(cs)
            mine.wait()

        def finish(t, tile):
            received(unit_copies(t, tile))
            at = tile_rows(tile)
            cs = [pltpu.make_async_copy(rb.at[t, s, at], tmp.at[s, at], tmp_sem.at[s]) for s in range(2)]
            start(cs)
            if t == Z_ORDER[2]:
                handed(Z_ORDER[0], tile)
            for c in cs:
                c.wait()
            wide = pl.ds(tile * LANE, LANE)
            stage[slot(t), :, wide] = (far[t, wide] + tmp[0, wide] + tmp[1, wide]).T
            cs, mine = hand_out(t, tile)
            start(cs + [mine])

        blocks = d // min(OUT_COLS, d)
        width = d // blocks

        def row_products(r, keep):
            side = core if keep else 1 - core
            terms = ((2, wd),) if r == 0 else ((0, wg), (1, wu))
            specs, args = [], []
            for t, w in terms:
                specs += [pl.BlockSpec((1, RING, 1, RING * rows, nf), lambda j, t=t: (t, 0, side, 0, 0)), pl.BlockSpec((width, nf), lambda j: (j, 0))]
                args += [h_all, w]
            wide = pl.BlockSpec((RING, RING, rows, width), lambda j: (0, 0, 0, j))
            if keep:
                specs.append(wide)
                args.append(rc.at[r])

            def body(*refs):
                total = None
                for i in range(len(terms)):
                    h = refs[2 * i][...].reshape(RING * RING * rows, nf)
                    prod = dot(h, refs[2 * i + 1][...], 1, 1)
                    total = prod if total is None else total + prod
                if keep:
                    total = total + refs[-2][...].astype(F32).reshape(total.shape)
                refs[-1][...] = total.astype(BF16).reshape(RING, RING, rows, width)

            pltpu.emit_pipeline(body, grid=(blocks,), in_specs=specs, out_specs=[wide])(*args, (part if keep else give).at[r])

        def core_copy(r):
            return rcopy(give.at[r], rc.at[r], c_s.at[r], c_r.at[r], near(0, 1))

        def level(n):
            if n == 1:
                def piece(r, k, h):
                    return part.at[r, pl.ds(2 * h, 2), ys[k]]
                return ydev, piece, ra1, rb1, sd1, (a1_s, a1_r, f1_s, f1_r, d1_s, d1_r)

            def piece(r, k, h):
                return mid.at[r, xs[k], pl.ds(h, 1)]
            return xdev, piece, ra2, rb2, sd2, (a2_s, a2_r, f2_s, f2_r, d2_s, d2_r)

        def ring_a(r, n):
            dev, piece, rfar, _, _, sems = level(n)
            return [rcopy(piece(r, 2, s), rfar.at[r, s], sems[0].at[r, s], sems[1].at[r, s], dev(1 + 2 * s)) for s in range(2)]

        def ring_f(r, n):
            dev, piece, _, rnear, _, sems = level(n)
            return [rcopy(piece(r, 1 + 2 * s, 1 - s), rnear.at[r, s, 1 - s], sems[2].at[r, s], sems[3].at[r, s], dev(1 + 2 * s)) for s in range(2)]

        def ring_d(r, n):
            dev, _, _, rnear, dep, sems = level(n)
            return [rcopy(dep.at[r, s], rnear.at[r, s, s], sems[4].at[r, s], sems[5].at[r, s], dev(1 + 2 * s)) for s in range(2)]

        def add(grid, *terms):
            specs = []
            for ref, at, lead in terms:
                tail = ref.shape[lead:]
                specs.append(pl.BlockSpec((1,) * lead + tuple(tail), lambda *i, at=at, rank=len(tail): tuple(at(*i)) + (0,) * rank))

            def body(*refs):
                total = refs[0][...].astype(F32).reshape(refs[0].shape[-2:])
                for ref in refs[1:-1]:
                    total = total + ref[...].astype(F32).reshape(total.shape)
                refs[-1][...] = total.astype(BF16).reshape(refs[-1].shape)

            pltpu.emit_pipeline(body, grid=grid, in_specs=specs[:-1], out_specs=specs[-1:])(*[ref for ref, _, _ in terms])

        def ring_first(r, n):
            start(ring_a(r, n) + ring_f(r, n))

        def ring_dependent(r, n):
            received(ring_a(r, n))
            if n == 1:
                add((2, 2), (part.at[r], lambda s, i: (2 * s + i, lax.rem(y + 1 + 2 * s, RING)), 2), (ra1.at[r], lambda s, i: (s, i), 2),
                    (sd1.at[r], lambda s, i: (s, i), 2))
            else:
                add((2,), (mid.at[r], lambda s: (lax.rem(x + 1 + 2 * s, RING), s), 2), (ra2.at[r], lambda s: (s, 0), 2),
                    (sd2.at[r], lambda s: (s, 0), 2))
            start(ring_d(r, n))

        def ring_last(r, n):
            received(ring_f(r, n) + ring_d(r, n))
            if n == 1:
                add((2, 2), (part.at[r], lambda h, i: (2 * h + i, y), 2), (rb1.at[r, 0], lambda h, i: (h, i), 2),
                    (rb1.at[r, 1], lambda h, i: (h, i), 2), (mid.at[r], lambda h, i: (2 * h + i,), 1))
            else:
                own, res = ((tok_own, out), (grad_own, gin))[r]
                add((2,), (own, lambda h: (h,), 1), (mid.at[r], lambda h: (x, h), 2), (rb2.at[r, 0], lambda h: (h, 0), 2),
                    (rb2.at[r, 1], lambda h: (h, 0), 2), (res, lambda h: (h,), 1))

        def give_rows(r):
            row_products(r, False)
            core_copy(r).start()

        def keep_rows(r):
            core_copy(r).wait_recv()
            row_products(r, True)

        order = [
            (far_block, 0), (give_rows, 0), (next_blocks, 2), (far_block, 1), (own_block, 2), (keep_rows, 0), (ring_first, 0, 1),
            (finish, 2, 0), (give_rows, 1), (finish, 2, 1), (finish, 2, 2), (next_blocks, 0), (finish, 2, 3), (ring_dependent, 0, 1),
            (finish, 2, 4), (own_block, 0), (keep_rows, 1), (ring_first, 1, 1), (next_blocks, 1), (ring_last, 0, 1), (ring_first, 0, 2),
            (finish, 0, 0), (own_block, 1), (finish, 0, 1), (ring_dependent, 0, 2), (ring_dependent, 1, 1), (finish, 0, 2), (finish, 0, 3),
            (ring_last, 0, 2), (finish, 0, 4), (finish, 1, 0), (finish, 1, 1), (ring_last, 1, 1), (ring_first, 1, 2), (finish, 1, 2),
            (ring_dependent, 1, 2), (finish, 1, 3), (finish, 1, 4), (ring_last, 1, 2),
        ]
        for fn, *args in order:
            with jax.named_scope("_".join(str(v) for v in [fn.__name__, *args])):
                fn(*args)

        for t in range(3):
            for tile in range(tiles):
                sent(unit_copies(t, tile))
                received(hand_out(t, tile)[0])
                if t != Z_ORDER[0]:
                    handed(t, tile)
        for r in range(2):
            core_copy(r).wait_send()
            for n in (1, 2):
                sent(ring_a(r, n) + ring_f(r, n) + ring_d(r, n))

    pl.run_scoped(
        forward_phase,
        pltpu.VMEM((3,) + sg.shape, BF16),
        pltpu.VMEM((3, n8, dp, nf), BF16),
        pltpu.VMEM((2, d, nf), BF16),
        pltpu.VMEM((2, chunk, d), BF16),
        pltpu.VMEM((tokens, nf), BF16),
        pltpu.VMEM((tokens, nf), BF16),
        pltpu.VMEM((2, 2, chunk, nf), BF16),
    )
    pl.run_scoped(backward_phase, pltpu.VMEM((2, tiles * LANE, cols), F32), pltpu.VMEM((2, cols, tiles * LANE), F32))


def layer(sg, su, sd, tok, grad):
    n8 = 2 * RING
    dp, nf = sg.shape[0], sg.shape[1] // n8
    rows, d = tok.shape
    tokens = rows * RING * n8
    cols = d // RING
    tiles = -(-nf // LANE)
    padded = tiles * LANE
    hbm = pl.BlockSpec(memory_space=pl.ANY)
    dma = pltpu.SemaphoreType.DMA
    sds = jax.ShapeDtypeStruct
    halves = (2, rows // 2, d)
    res = pl.pallas_call(
        layer_kernel,
        out_shape=[sds((n8, dp, padded), F32)] * 3 + [sds(halves, BF16)] * 2 + [
            sds((d, nf), BF16), sds((d, nf), BF16), sds((d, nf), BF16), sds((tokens, d), BF16), sds((tokens, d), BF16),
            sds((3, RING, 2, RING * rows, nf), BF16),
            sds((3, nf, cols), F32), sds((3, 2, nf, cols), F32),
            sds((2, RING, RING, rows, d), BF16), sds((2, RING, RING, rows, d), BF16), sds((2, RING, RING, rows, d), BF16),
            sds((2, 2, 2, rows, d), BF16), sds((2, 2, 2, 2, rows, d), BF16), sds((2, 2, 2, rows, d), BF16),
            sds((2, RING, 2, rows // 2, d), BF16),
            sds((2, 2, 1, rows // 2, d), BF16), sds((2, 2, 2, 1, rows // 2, d), BF16), sds((2, 2, 1, rows // 2, d), BF16),
        ],
        in_specs=[hbm] * 7,
        out_specs=[hbm] * 23,
        scratch_shapes=[
            pltpu.VMEM((3, nf, tokens), BF16),
            pltpu.VMEM((2, tokens, cols), BF16),
            pltpu.VMEM((3, padded, cols), F32),
            pltpu.VMEM((3, 2, nf, cols), F32),
            dma((6,)),
            dma((3, n8)), dma((3, n8)),
            dma((3, 2, n8)), dma((3, 2, n8)),
            dma((3, 2, n8 // 2)), dma((3, 2, n8 // 2)),
            dma((3, 2)), dma((3, 2)),
            dma((3, 2)), dma((3, 2)),
            dma((3, 2, RING)), dma((3, 2, RING)),
            dma((3, RING)), dma((3, RING)),
            dma((3, RING, RING)), dma((3, RING, RING)),
            dma((3,)), dma((3,)), dma((2,)), dma((2, 2)), dma((2,)), dma((2,)),
            dma((3, 2)), dma((3, 2)),
            dma((3, 2, tiles)), dma((3, 2, tiles)),
            dma((3, tiles, n8)), dma((3, tiles, n8)),
            dma((3, tiles)),
            dma((2,)), dma((2,)),
        ] + [dma((2, 2))] * 12,
        compiler_params=pltpu.CompilerParams(collective_id=0, has_side_effects=True, vmem_limit_bytes=67043328),
        cost_estimate=pl.CostEstimate(flops=18 * nf * tokens * d, bytes_accessed=300_000_000, transcendentals=0),
        name="layer",
    )(sg, su, sd, tok, grad, tok.reshape(halves), grad.reshape(halves))
    return res[:3], res[3].reshape(rows, d), res[4].reshape(rows, d)


def assemble_kernel(og, ou, od, out, gin, g, u, w, res, gres, buf, flat, in_sem, out_sem, row_buf, row_sem):
    n8, nf = og.shape[0], g.shape[1] // og.shape[0]
    srcs, dsts = (og, ou, od), (g, u, w)
    rows_in = [pltpu.make_async_copy(src, row_buf.at[r], row_sem.at[r]) for r, src in enumerate((out, gin))]
    loads = [pltpu.make_async_copy(src, buf.at[t], in_sem.at[t]) for t, src in enumerate(srcs)]
    stores = [pltpu.make_async_copy(flat.at[t], dst, out_sem.at[t]) for t, dst in enumerate(dsts)]
    for c in loads + rows_in:
        c.start()
    for t in range(3):
        loads[t].wait()
        for j in range(n8):
            flat[t, :, j * nf:(j + 1) * nf] = buf[t, j, :, :nf]
        stores[t].start()
    rows_out = [pltpu.make_async_copy(row_buf.at[r], dst, row_sem.at[r]) for r, dst in enumerate((res, gres))]
    for c in rows_in:
        c.wait()
    for c in rows_out:
        c.start()
    for c in stores + rows_out:
        c.wait()


def assemble(sums, out, gin, ff):
    n8, dp, padded = sums[0].shape
    hbm = pl.BlockSpec(memory_space=pl.ANY)
    dma = pltpu.SemaphoreType.DMA
    sds = jax.ShapeDtypeStruct
    return pl.pallas_call(
        assemble_kernel,
        out_shape=[sds((dp, ff), F32)] * 3 + [sds(out.shape, BF16)] * 2,
        in_specs=[hbm] * 5,
        out_specs=[hbm] * 5,
        scratch_shapes=[
            pltpu.VMEM((3, n8, dp, padded), F32), pltpu.VMEM((3, dp, ff), F32), dma((3,)), dma((3,)),
            pltpu.VMEM((2,) + out.shape, BF16), dma((2,)),
        ],
        compiler_params=pltpu.CompilerParams(vmem_limit_bytes=63 * 1024 * 1024),
        name="assemble",
    )(*sums, out, gin)


def solution(mesh):
    nz, ny, nd = mesh.shape["datb"], mesh.shape["model"], mesh.shape["data"]
    fine = Mesh(mesh.devices.reshape(nz, ny, nd // 2, 2), ("datb", "model", "x", "core"))

    def local_step(tok_loc, wg_loc, wu_loc, wd_loc, grad_loc):
        sums, out, grad_in = layer(wg_loc, wu_loc, wd_loc.T, tok_loc, grad_loc)
        grad_gate, grad_up, grad_down_t, out, grad_in = assemble(sums, out, grad_in, wg_loc.shape[1])
        return out, grad_in, grad_gate, grad_up, grad_down_t.T

    return jax.shard_map(local_step, mesh=fine, in_specs=(ROW_SPEC, GATE_SPEC, GATE_SPEC, DOWN_SPEC, ROW_SPEC), out_specs=(ROW_SPEC, ROW_SPEC, GATE_SPEC, GATE_SPEC, DOWN_SPEC), check_vma=False)
```

```python
import functools

import jax
import jax.numpy as jnp
from jax import lax
from jax.experimental import pallas as pl
from jax.experimental.pallas import tpu as pltpu
from jax.sharding import Mesh
from jax.sharding import PartitionSpec as P

ROW_SPEC = P(("datb", "x", "core", "model"), None)
GATE_SPEC = P(("datb", "x", "core"), "model")
DOWN_SPEC = P("model", ("datb", "x", "core"))
BF16 = jnp.bfloat16
F32 = jnp.float32
MESH_ID = pl.DeviceIdType.MESH
RING = 4
NEAR = ((0, 0), (0, 1), (1, 0), (3, 0), (1, 1), (3, 1), (2, 0), (2, 1))
DELTAS = (0, 3, 1, 2)
LANE = 128
OUT_COLS = 512
EX, Z1, Z2, P1, P2, BL, Q1, Q2, WD, CI = range(10)
GATHER_STEPS = (
    (Z1, 0, 0), (Z1, 1, 0), (P1, 0, 0), (P1, 0, 1), (EX, 0, 1), (EX, 0, 2), (EX, 0, 3), (Z1, 2, 0), (EX, 1, 1), (BL, 0, 0), (EX, 2, 1),
    (P1, 2, 0), (P1, 2, 1), (EX, 0, 4), (EX, 0, 5), (Z1, 0, 1), (Z1, 1, 1), (BL, 1, 0), (Z1, 2, 1), (EX, 0, 6), (EX, 0, 7), (Z2, 0, 0, 0),
    (Z2, 1, 0, 0), (EX, 1, 2), (EX, 1, 3), (Z2, 2, 0, 0), (Q1, 0, 0, 0), (Q1, 0, 0, 1), (EX, 1, 4), (EX, 1, 5), (Z1, 0, 2), (EX, 1, 6),
    (EX, 1, 7), (P2, 2, 1), (P2, 2, 0), (Z1, 0, 3), (Z1, 0, 4), (P2, 0, 0), (P2, 0, 1), (BL, 0, 1), (Q1, 1, 0, 1), (Z1, 0, 5), (EX, 2, 2),
    (EX, 2, 3), (Z1, 0, 6), (Z2, 0, 1, 0), (BL, 0, 2), (EX, 2, 4), (EX, 2, 5), (Z1, 0, 7), (Q2, 0, 0), (Z2, 0, 1, 1), (EX, 2, 6),
    (EX, 2, 7), (Z2, 0, 0, 1), (Q1, 0, 1, 1), (Z2, 0, 1, 2), (Z2, 0, 0, 2), (P1, 1, 0), (P1, 1, 1), (Q1, 1, 0, 0), (Z2, 0, 0, 3),
    (Z2, 0, 1, 3), (Z1, 1, 2), (BL, 2, 1), (Q1, 0, 2, 1), (Q1, 0, 1, 0), (Z1, 1, 3), (Z1, 1, 4), (BL, 2, 2), (Z1, 1, 5), (BL, 2, 0),
    (Q1, 0, 2, 0), (BL, 0, 3), (Z1, 1, 6), (Q2, 0, 2), (WD, 0),
)
GATE_STEPS = (
    (),
    (
        (Q2, 1, 0), (Z1, 1, 7), (Z2, 1, 1, 0), (P2, 1, 0), (P2, 1, 1), (CI, 0),
    ),
    (
        (Z2, 1, 0, 1), (Z2, 1, 1, 1), (Z2, 1, 0, 2), (BL, 1, 1), (BL, 2, 3), (Q1, 2, 1, 1), (Q1, 2, 1, 0), (Z2, 1, 1, 2), (Q1, 0, 3, 1),
        (Z2, 1, 0, 3), (Q1, 2, 2, 0), (Q1, 2, 2, 1), (Q2, 0, 1),
    ),
    (
        (Z2, 1, 1, 3), (Z2, 2, 0, 1), (BL, 1, 2), (Q1, 1, 1, 1), (CI, 1),
    ),
    (
        (Z1, 2, 2), (BL, 1, 3), (Q1, 2, 0, 0), (Q1, 2, 0, 1),
    ),
    (
        (Q1, 0, 3, 0), (Z1, 2, 3), (CI, 2),
    ),
    (
        (Q2, 0, 3), (Z1, 2, 4), (Z1, 2, 5), (Q1, 2, 3, 0), (Q1, 2, 3, 1),
    ),
    (
        (WD, 1), (Q2, 2, 1), (Q2, 2, 2), (Z1, 2, 6), (Q1, 1, 1, 0), (Q1, 1, 2, 1), (CI, 3),
    ),
)
UP_STEPS = (
    (
        (Z1, 2, 7), (Q1, 1, 2, 0),
    ),
    (
        (Q2, 2, 0), (Q2, 2, 3), (Z2, 2, 1, 0), (Z2, 2, 0, 2), (Q1, 1, 3, 1),
    ),
    (
        (Z2, 2, 1, 1), (Q1, 1, 3, 0),
    ),
    (
        (Z2, 2, 0, 3), (Q2, 1, 2),
    ),
    (
        (Q2, 1, 1), (Z2, 2, 1, 2),
    ),
    (
        (Z2, 2, 1, 3),
    ),
    (
        (Q2, 1, 3),
    ),
    (),
)
LATE_STEPS = (
    (WD, 2),
)
Z_ORDER = (2, 0, 1)
EARLY_ORDER = (
    ('far_block', 2), ('next_products', 2),
)
LATE_ORDER = (
    ('next_adds', 2), ('give_rows', 0), ('far_block', 0), ('far_block', 1), ('next_products', 0), ('keep_rows', 0), ('ring_first', 0, 1),
    ('own_block', 2), ('finish', 2, 1), ('finish', 2, 0), ('finish', 2, 3), ('finish', 2, 4), ('give_rows', 1), ('finish', 2, 2),
    ('next_adds', 0), ('own_block', 0), ('ring_dependent', 0, 1), ('keep_rows', 1), ('ring_first', 1, 1), ('next_blocks', 1),
    ('ring_last', 0, 1), ('ring_first', 0, 2), ('own_block', 1), ('finish', 0, 0), ('ring_dependent', 0, 2), ('ring_dependent', 1, 1),
    ('finish', 0, 1), ('finish', 0, 3), ('ring_last', 0, 2), ('finish', 0, 4), ('finish', 0, 2), ('finish', 1, 0), ('finish', 1, 1),
    ('ring_last', 1, 1), ('ring_first', 1, 2), ('finish', 1, 2), ('ring_dependent', 1, 2), ('finish', 1, 3), ('finish', 1, 4),
    ('ring_last', 1, 2),
)


def dot(a, b, ca, cb):
    return lax.dot_general(a, b, (((ca,), (cb,)), ((), ())), preferred_element_type=F32)


def layer_kernel(sg, su, sd, tok, grad, tok_own, grad_own,
                 og, ou, od, out, gin, wg, wu, wd, tok_all, grad_all, h_all, ra, rb, give, rc, part, ra1, rb1, sd1, mid, ra2, rb2, sd2,
                 ff, blk, far, nxt,
                 own_sem, ex_s, ex_r, z1_s, z1_r, z2_s, z2_r, p1_s, p1_r, p2_s, p2_r, q1_s, q1_r, q2_s, q2_r, cc_s, cc_r,
                 sh_sem, wv_sem, row_sem, hst_sem, blk_sem, tmp_sem, a_s, a_r, u_s, u_r, e_s, e_r, out_sem,
                 c_s, c_r, a1_s, a1_r, f1_s, f1_r, d1_s, d1_r, a2_s, a2_r, f2_s, f2_r, d2_s, d2_r):
    z, y = lax.axis_index("datb"), lax.axis_index("model")
    x, core = lax.axis_index("x"), lax.axis_index("core")
    i8 = 2 * x + core
    n8 = 2 * RING
    rows, d = tok.shape
    half_rows = rows // 2
    chunk = RING * rows
    n_chunk = n8
    nf, tokens = ff.shape[1:]
    dp = sg.shape[0]
    half = nf // 2
    cols = blk.shape[2]
    tiles = far.shape[1] // LANE
    outs = (og, ou, od)

    zs, ys, xs = ([v] + [lax.rem(v + k, RING) for k in range(1, RING)] for v in (z, y, x))
    cores = (core, 1 - core)
    peers = [[2 * v + c for c in cores] for v in xs]
    slot_at = [[[pl.multiple_of((zz * n8 + peers[dx][dc]) * dp, 16) for dc in range(2)] for dx in range(RING)] for zz in zs]
    hand_at = [[pl.multiple_of(p * dp, 8) for p in row] for row in peers]
    rows_at = [[[pl.multiple_of((peers[dx][dc] * RING + yy) * rows, half_rows) for dc in range(2)] for yy in ys] for dx in range(RING)]
    lanes_at = [pl.multiple_of(zz * cols, LANE) for zz in zs]

    def peer(dx, dc):
        return peers[dx][dc]

    def zdev(k):
        return {"datb": zs[k]}

    def xdev(k):
        return {"x": xs[k]}

    def ydev(k):
        return {"model": ys[k]}

    def near(dx, dc):
        return {"x": xs[dx], "core": cores[dc]}

    def copy(src, dst, s, r, dev):
        return pltpu.make_async_remote_copy(src_ref=src, dst_ref=dst, send_sem=s, recv_sem=r, device_id=dev, device_id_type=MESH_ID)

    rcopy = copy

    def start(copies):
        for c in copies:
            c.start()

    def received(copies):
        for c in copies:
            c.wait_recv()

    def sent(copies):
        for c in copies:
            c.wait_send()

    def run_order(fns, order):
        for fn, *args in order:
            with jax.named_scope("_".join(str(v) for v in [fn, *args])):
                fns[fn](*args)

    barrier = pltpu.get_barrier_semaphore()
    others = [zdev(1), zdev(3), ydev(1), ydev(3)] + [near(*n) for n in NEAR[1:]]
    for dev in others:
        pl.semaphore_signal(barrier, inc=1, device_id=dev, device_id_type=MESH_ID)

    def blk_load(t, slot, k):
        src = tok_all if t < 2 else grad_all
        return pltpu.make_async_copy(src.at[:, pl.ds(lanes_at[k], cols)], blk.at[slot], blk_sem.at[slot])

    plan = []
    for fn, *args in EARLY_ORDER + LATE_ORDER:
        plan += [(args[0], k) for k in {"far_block": (2,), "next_blocks": (1, 3), "next_products": (1, 3), "own_block": (0,)}.get(fn, ())]
    taken = []

    def next_block():
        n = len(taken)
        taken.append(n)
        if n == 0:
            blk_load(plan[0][0], 0, plan[0][1]).start()
        blk_load(plan[n][0], n % 2, plan[n][1]).wait()
        if n + 1 < len(plan):
            blk_load(plan[n + 1][0], (n + 1) % 2, plan[n + 1][1]).start()
        return n % 2

    def product(t, dst):
        slot = next_block()
        step = 2 * LANE

        def one(n, carry):
            lanes = pl.ds(pl.multiple_of(jnp.minimum(n * step, cols - step), LANE), step)
            dst[:nf, lanes] = jnp.dot(ff[t], blk[slot, :, lanes], preferred_element_type=F32)
            return carry

        lax.fori_loop(0, -(-cols // step), one, 0)

    lo, hi = pl.ds(0, half), pl.ds(half, half)

    def a_copies(t):
        return [rcopy(far.at[t, rows], ra.at[t, rows], a_s.at[t, s], a_r.at[t, s], zdev(k)) for s, rows, k in ((0, lo, 1), (1, hi, 3))]

    def tile_rows(tile):
        return pl.ds(tile * LANE, min(LANE, nf - tile * LANE))

    def unit_copies(t, tile):
        at = tile_rows(tile)
        return [rcopy(nxt.at[t, s, at], rb.at[t, s, at], u_s.at[t, s, tile], u_r.at[t, s, tile], zdev(1 + 2 * s)) for s in range(2)]

    def far_block(t):
        product(t, far.at[t])
        start(a_copies(t))

    def early_units(t):
        if ("next_products", t) not in EARLY_ORDER + LATE_ORDER:
            return ()
        free = [(0, tile) for tile in range(tiles) if tile * LANE >= half]
        return free + [(1, tile) for tile in range(tiles) if (tile + 1) * LANE <= half]

    def next_products(t):
        for s in range(2):
            product(t, nxt.at[t, s])
        for s, tile in early_units(t):
            unit_copies(t, tile)[s].start()

    def forward_phase(shard, pieces, wv, rowbuf, av, bv, hst):
        fulls = (wg, wu, wd)
        loads = [pltpu.make_async_copy(src, shard.at[t], sh_sem.at[t]) for t, src in enumerate((sg, su, sd))]
        for c in loads:
            c.start()

        def cut_pieces(t):
            loads[t].wait()
            for j in range(n8):
                pieces[t, j] = shard[t, :, j * nf:(j + 1) * nf]

        started = []

        def go(make, *args):
            make(*args).start()
            started.append((make, args))

        def slot(t, k, source):
            dx, dc = source
            return fulls[t].at[pl.ds(slot_at[k][dx][dc], dp)]

        def source(k):
            dx, dc = NEAR[k]
            return (RING - dx) % RING, dc

        def back(side):
            return 3 if side == 0 else 1

        def ahead(side):
            return 1 if side == 0 else 3

        def exchange_copy(t, k):
            return copy(pieces.at[t, peer(*NEAR[k])], slot(t, 0, NEAR[0]), ex_s.at[t, k], ex_r.at[t, k], near(*NEAR[k]))

        def exchange(t, k):
            go(exchange_copy, t, k)

        def z_first_copy(t, side, k):
            here = slot(t, 0, source(k))
            return copy(here if k else pieces.at[t, i8], here, z1_s.at[t, side, k], z1_r.at[t, side, k], zdev(ahead(side)))

        def z_first(t, k):
            if k:
                here = slot(t, 0, source(k))
                copy(here, here, ex_s.at[t, k], ex_r.at[t, k], {"datb": z}).wait_recv()
            for side in range(2):
                go(z_first_copy, t, side, k)

        def wait_z_first(t, side, k):
            there = slot(t, back(side), source(k))
            copy(there, there, z1_s.at[t, side, k], z1_r.at[t, side, k], {"datb": z}).wait_recv()

        def z_second_copy(t, side, k):
            there = slot(t, back(side), source(k + side * (n8 // 2)))
            return copy(there, there, z2_s.at[t, side, k], z2_r.at[t, side, k], zdev(ahead(side)))

        def z_second(t, side, k):
            wait_z_first(t, side, k + side * (n8 // 2))
            go(z_second_copy, t, side, k)

        def weights_done(t):
            local[t].wait()
            for k in range(n8 // 2):
                wait_z_first(t, 0, n8 // 2 + k)
                wait_z_first(t, 1, k)
                for side in range(2):
                    there = slot(t, 2, source(k + side * (n8 // 2)))
                    copy(there, there, z2_s.at[t, side, k], z2_r.at[t, side, k], {"datb": z}).wait_recv()
            w_load(t).start()

        cut = d // 2
        rings = ((tok, tok_all, pl.ds(0, d), True), (grad, grad_all, pl.ds(0, cut), True), (grad, grad_all, pl.ds(cut, d - cut), False))

        def axis(r, n):
            return xdev if rings[r][3] == (n == 1) else ydev

        def block(r, da, db, flip=0, lo=0, size=rows):
            dx, dy = (da, db) if rings[r][3] else (db, da)
            first = rows_at[dx][dy][flip]
            return rings[r][1].at[pl.ds(pl.multiple_of(first + lo, half_rows) if lo else first, size), rings[r][2]]

        def own_block(r):
            return rings[r][0].at[:, rings[r][2]]

        def to_core_copy(r, ia, ib):
            there = block(r, DELTAS[ia], DELTAS[ib])
            return copy(own_block(r) if ia == 0 and ib == 0 else there, there, cc_s.at[r, ia, ib], cc_r.at[r, ia, ib], near(0, 1))

        def to_core(r, ia, ib):
            go(to_core_copy, r, ia, ib)

        def first_copy(r, side):
            return copy(own_block(r), block(r, 0, 0), p1_s.at[r, side], p1_r.at[r, side], axis(r, 1)(ahead(side)))

        def first_own(r, side):
            go(first_copy, r, side)

        def first_far_copy(r, side):
            part = block(r, back(side), 0, 0, side * half_rows, half_rows)
            return copy(part, part, p2_s.at[r, side], p2_r.at[r, side], axis(r, 1)(ahead(side)))

        def first_forward(r, side):
            there = block(r, back(side), 0)
            copy(there, there, p1_s.at[r, side], p1_r.at[r, side], {"datb": z}).wait_recv()
            go(first_far_copy, r, side)

        def block_on(r, ia):
            for side in range(2 if ia == 3 else 0):
                part = block(r, 2, 0, 0, side * half_rows, half_rows)
                copy(part, part, p2_s.at[r, side], p2_r.at[r, side], {"datb": z}).wait_recv()
            for side in range(2):
                go(second_copy, r, side, ia)
            to_core(r, ia, 0)

        def second_copy(r, side, ia):
            there = block(r, DELTAS[ia], 0)
            return copy(there if ia else own_block(r), there, q1_s.at[r, side, ia], q1_r.at[r, side, ia], axis(r, 2)(ahead(side)))

        def second_far_copy(r, ia):
            side = ia // 2
            there = block(r, DELTAS[ia], back(side))
            return copy(there, there, q2_s.at[r, ia], q2_r.at[r, ia], axis(r, 2)(ahead(side)))

        def second_forward(r, ia, side):
            there = block(r, DELTAS[ia], back(side))
            copy(there, there, q1_s.at[r, side, ia], q1_r.at[r, side, ia], {"datb": z}).wait_recv()
            if ia // 2 == side:
                go(second_far_copy, r, ia)
            to_core(r, ia, 1 if side == 0 else 2)

        def second_far(r, ia):
            there = block(r, DELTAS[ia], 2)
            copy(there, there, q2_s.at[r, ia], q2_r.at[r, ia], {"datb": z}).wait_recv()
            to_core(r, ia, 3)

        def chunk_in(ia):
            rows_in(0, (ia,))

        def rows_in(r, blocks=range(RING)):
            for ia in blocks:
                for ib in range(RING):
                    there = block(r, DELTAS[ia], DELTAS[ib], 1)
                    copy(there, there, cc_s.at[r, ia, ib], cc_r.at[r, ia, ib], {"datb": z}).wait_recv()

        local = [pltpu.make_async_copy(pieces.at[t, i8], slot(t, 0, NEAR[0]), own_sem.at[t]) for t in range(3)]
        local += [pltpu.make_async_copy(own_block(r), block(r, 0, 0), own_sem.at[3 + r]) for r in range(3)]

        def w_load(t):
            return pltpu.make_async_copy(fulls[t], wv.at[t % 2], wv_sem.at[t])

        def row_load(src, i, buf):
            return pltpu.make_async_copy(src.at[chunk_rows(i)], rowbuf.at[buf], row_sem.at[buf])

        def chunk_loop(src, work, between):
            row_load(src, 0, 0).start()

            def outer(xx, carry):
                def inner(c, carry):
                    i = 2 * xx + c

                    @pl.when(i + 1 < n_chunk)
                    def _():
                        row_load(src, i + 1, 1 - c).start()

                    for k, step in enumerate(between):
                        pl.when(i == k)(step)
                    row_load(src, i, c).wait()
                    work(i, xx, c)
                    return carry

                return lax.fori_loop(0, 2, inner, carry)

            lax.fori_loop(0, RING, outer, 0)

        def chunk_rows(i):
            return pl.ds(pl.multiple_of(i * chunk, chunk), chunk)

        def h_copy(xx, c, slot, j):
            return pltpu.make_async_copy(hst.at[c, slot], h_all.at[j, xx, c], hst_sem.at[c, slot])

        def keep(i, xx, c, slot, j, value):
            @pl.when(xx >= 1)
            def _():
                h_copy(xx - 1, c, slot, j).wait()

            hst[c, slot] = value.astype(BF16)
            h_copy(xx, c, slot, j).start()
            ff[j, :, chunk_rows(i)] = value.T.astype(BF16)

        def kept(slot, j):
            for c in range(2):
                h_copy(RING - 1, c, slot, j).wait()

        def gate_work():
            def outer(ia, carry):
                delta = lax.rem(3 * ia + 3 * lax.div(ia, 2) + 2 * lax.div(ia, 3), RING)

                def inner(flip, carry):
                    for k, group in enumerate(GATE_STEPS):
                        if group:
                            pl.when(2 * ia + flip == k)(functools.partial(run, group))
                    i = 2 * lax.rem(x + delta, RING) + lax.rem(core + flip, 2)
                    row_load(tok_all, i, 0).start()
                    row_load(tok_all, i, 0).wait()
                    av[chunk_rows(i)] = jnp.dot(rowbuf[0], wv[0], preferred_element_type=F32).astype(BF16)
                    return carry

                return lax.fori_loop(0, 2, inner, carry)

            lax.fori_loop(0, RING, outer, 0)

        def up_work(i, xx, c):
            b = jnp.dot(rowbuf[c], wv[1], preferred_element_type=F32).astype(BF16)
            bv[chunk_rows(i)] = b
            a, b = av[chunk_rows(i)].astype(F32), b.astype(F32)
            keep(i, xx, c, 0, 2, a * jax.nn.sigmoid(a) * b)

        def post_work(i, xx, c):
            g = jnp.dot(rowbuf[c], wv[0], preferred_element_type=F32).astype(BF16).astype(F32)
            a, b = av[chunk_rows(i)].astype(F32), bv[chunk_rows(i)].astype(F32)
            sig = jax.nn.sigmoid(a)
            keep(i, xx, c, 0, 0, g * b * sig * (1.0 + a * (1.0 - sig)))
            keep(i, xx, c, 1, 1, g * (a * sig))

        steps = (exchange, z_first, z_second, first_own, first_forward, block_on, second_forward, second_far, weights_done, chunk_in)

        def run(group):
            for which, *args in group:
                steps[which](*args)

        with jax.named_scope("begin"):
            for t in range(3):
                cut_pieces(t)
            pl.semaphore_wait(barrier, len(others))
            for c in local:
                c.start()
        with jax.named_scope("gather"):
            run(GATHER_STEPS)
            local[3].wait()
            w_load(0).wait()
        with jax.named_scope("gate"):
            gate_work()
        with jax.named_scope("up"):
            run(UP_STEPS[0])
            w_load(1).wait()
            chunk_loop(tok_all, up_work, [functools.partial(run, group) for group in ((),) + UP_STEPS[1:]])
            kept(0, 2)
        with jax.named_scope("rows"):
            for r in (1, 2):
                local[3 + r].wait()
                rows_in(r)
        run_order({"far_block": far_block, "next_products": next_products}, EARLY_ORDER)
        with jax.named_scope("late"):
            run(LATE_STEPS)
            w_load(2).wait()
        with jax.named_scope("down"):
            chunk_loop(grad_all, post_work, ())
            kept(0, 0)
            kept(1, 1)
        for make, args in started:
            make(*args).wait_send()

    def backward_phase(tmp, stage):
        def next_adds(t):
            received(a_copies(t))
            cs = [pltpu.make_async_copy(ra.at[t, at], tmp.at[s, at], tmp_sem.at[s]) for s, at in ((0, lo), (1, hi))]
            start(cs)
            for c, (s, at) in zip(cs, ((0, lo), (1, hi))):
                c.wait()
                nxt[t, s, at] += tmp[s, at]
            for tile in range(tiles):
                start(c for s, c in enumerate(unit_copies(t, tile)) if (s, tile) not in early_units(t))

        def next_blocks(t):
            next_products(t)
            next_adds(t)

        def own_block(t):
            sent(a_copies(t))
            product(t, far.at[t])

        def slot(t):
            return Z_ORDER.index(t) % 2

        def hand_out(t, tile):
            cs = []
            for k in range(1, n8):
                at = pl.ds(hand_at[NEAR[k][0]][NEAR[k][1]], dp)
                cs.append(rcopy(stage.at[slot(t), tile, at], outs[t].at[i8, tile], e_s.at[t, tile, k], e_r.at[t, tile, k], near(*NEAR[k])))
            at = pl.ds(hand_at[0][0], dp)
            return cs, pltpu.make_async_copy(stage.at[slot(t), tile, at], outs[t].at[i8, tile], out_sem.at[t, tile])

        def handed(t, tile):
            cs, mine = hand_out(t, tile)
            sent(cs)
            mine.wait()

        def finish(t, tile):
            received(unit_copies(t, tile))
            at = tile_rows(tile)
            cs = [pltpu.make_async_copy(rb.at[t, s, at], tmp.at[s, at], tmp_sem.at[s]) for s in range(2)]
            start(cs)
            if t == Z_ORDER[2]:
                handed(Z_ORDER[0], tile)
            for c in cs:
                c.wait()
            wide = pl.ds(tile * LANE, LANE)
            stage[slot(t), tile] = (far[t, wide] + tmp[0, wide] + tmp[1, wide]).T
            cs, mine = hand_out(t, tile)
            start(cs + [mine])

        blocks = d // min(OUT_COLS, d)
        width = d // blocks

        def row_products(r, keep):
            side = core if keep else 1 - core
            terms = ((2, wd),) if r == 0 else ((0, wg), (1, wu))
            specs, args = [], []
            for t, w in terms:
                specs += [pl.BlockSpec((1, RING, 1, RING * rows, nf), lambda j, t=t: (t, 0, side, 0, 0)), pl.BlockSpec((width, nf), lambda j: (j, 0))]
                args += [h_all, w]
            wide = pl.BlockSpec((RING, RING, rows, width), lambda j: (0, 0, 0, j))
            if keep:
                specs.append(wide)
                args.append(rc.at[r])

            def body(*refs):
                total = None
                for i in range(len(terms)):
                    h = refs[2 * i][...].reshape(RING * RING * rows, nf)
                    prod = dot(h, refs[2 * i + 1][...], 1, 1)
                    total = prod if total is None else total + prod
                if keep:
                    total = total + refs[-2][...].astype(F32).reshape(total.shape)
                refs[-1][...] = total.astype(BF16).reshape(RING, RING, rows, width)

            pltpu.emit_pipeline(body, grid=(blocks,), in_specs=specs, out_specs=[wide])(*args, (part if keep else give).at[r])

        def core_copy(r):
            return rcopy(give.at[r], rc.at[r], c_s.at[r], c_r.at[r], near(0, 1))

        def level(n):
            if n == 1:
                def piece(r, k, h):
                    return part.at[r, pl.ds(2 * h, 2), ys[k]]
                return ydev, piece, ra1, rb1, sd1, (a1_s, a1_r, f1_s, f1_r, d1_s, d1_r)

            def piece(r, k, h):
                return mid.at[r, xs[k], pl.ds(h, 1)]
            return xdev, piece, ra2, rb2, sd2, (a2_s, a2_r, f2_s, f2_r, d2_s, d2_r)

        def ring_a(r, n):
            dev, piece, rfar, _, _, sems = level(n)
            return [rcopy(piece(r, 2, s), rfar.at[r, s], sems[0].at[r, s], sems[1].at[r, s], dev(1 + 2 * s)) for s in range(2)]

        def ring_f(r, n):
            dev, piece, _, rnear, _, sems = level(n)
            return [rcopy(piece(r, 1 + 2 * s, 1 - s), rnear.at[r, s, 1 - s], sems[2].at[r, s], sems[3].at[r, s], dev(1 + 2 * s)) for s in range(2)]

        def ring_d(r, n):
            dev, _, _, rnear, dep, sems = level(n)
            return [rcopy(dep.at[r, s], rnear.at[r, s, s], sems[4].at[r, s], sems[5].at[r, s], dev(1 + 2 * s)) for s in range(2)]

        def add(grid, *terms):
            specs = []
            for ref, at, lead in terms:
                tail = ref.shape[lead:]
                specs.append(pl.BlockSpec((1,) * lead + tuple(tail), lambda *i, at=at, rank=len(tail): tuple(at(*i)) + (0,) * rank))

            def body(*refs):
                total = refs[0][...].astype(F32).reshape(refs[0].shape[-2:])
                for ref in refs[1:-1]:
                    total = total + ref[...].astype(F32).reshape(total.shape)
                refs[-1][...] = total.astype(BF16).reshape(refs[-1].shape)

            pltpu.emit_pipeline(body, grid=grid, in_specs=specs[:-1], out_specs=specs[-1:])(*[ref for ref, _, _ in terms])

        def ring_first(r, n):
            start(ring_a(r, n) + ring_f(r, n))

        def ring_dependent(r, n):
            received(ring_a(r, n))
            if n == 1:
                add((2, 2), (part.at[r], lambda s, i: (2 * s + i, lax.rem(y + 1 + 2 * s, RING)), 2), (ra1.at[r], lambda s, i: (s, i), 2),
                    (sd1.at[r], lambda s, i: (s, i), 2))
            else:
                add((2,), (mid.at[r], lambda s: (lax.rem(x + 1 + 2 * s, RING), s), 2), (ra2.at[r], lambda s: (s, 0), 2),
                    (sd2.at[r], lambda s: (s, 0), 2))
            start(ring_d(r, n))

        def ring_last(r, n):
            received(ring_f(r, n) + ring_d(r, n))
            if n == 1:
                add((2, 2), (part.at[r], lambda h, i: (2 * h + i, y), 2), (rb1.at[r, 0], lambda h, i: (h, i), 2),
                    (rb1.at[r, 1], lambda h, i: (h, i), 2), (mid.at[r], lambda h, i: (2 * h + i,), 1))
            else:
                own, res = ((tok_own, out), (grad_own, gin))[r]
                add((2,), (own, lambda h: (h,), 1), (mid.at[r], lambda h: (x, h), 2), (rb2.at[r, 0], lambda h: (h, 0), 2),
                    (rb2.at[r, 1], lambda h: (h, 0), 2), (res, lambda h: (h,), 1))

        def give_rows(r):
            row_products(r, False)
            core_copy(r).start()

        def keep_rows(r):
            core_copy(r).wait_recv()
            row_products(r, True)

        run_order({
            "far_block": far_block, "next_products": next_products, "next_adds": next_adds, "next_blocks": next_blocks,
            "own_block": own_block, "finish": finish, "give_rows": give_rows, "keep_rows": keep_rows, "ring_first": ring_first,
            "ring_dependent": ring_dependent, "ring_last": ring_last,
        }, LATE_ORDER)

        for t in range(3):
            for tile in range(tiles):
                sent(unit_copies(t, tile))
                received(hand_out(t, tile)[0])
                if t != Z_ORDER[0]:
                    handed(t, tile)
        for r in range(2):
            core_copy(r).wait_send()
            for n in (1, 2):
                sent(ring_a(r, n) + ring_f(r, n) + ring_d(r, n))

    pl.run_scoped(
        forward_phase,
        pltpu.VMEM((3,) + sg.shape, BF16),
        pltpu.VMEM((3, n8, dp, nf), BF16),
        pltpu.VMEM((2, d, nf), BF16),
        pltpu.VMEM((2, chunk, d), BF16),
        pltpu.VMEM((tokens, nf), BF16),
        pltpu.VMEM((tokens, nf), BF16),
        pltpu.VMEM((2, 2, chunk, nf), BF16),
    )
    pl.run_scoped(backward_phase, pltpu.VMEM((2, tiles * LANE, cols), F32), pltpu.VMEM((2, tiles, cols, LANE), F32))


def layer(sg, su, sd, tok, grad):
    n8 = 2 * RING
    dp, nf = sg.shape[0], sg.shape[1] // n8
    rows, d = tok.shape
    tokens = rows * RING * n8
    cols = d // RING
    tiles = -(-nf // LANE)
    padded = tiles * LANE
    hbm = pl.BlockSpec(memory_space=pl.ANY)
    dma = pltpu.SemaphoreType.DMA
    sds = jax.ShapeDtypeStruct
    halves = (2, rows // 2, d)
    res = pl.pallas_call(
        layer_kernel,
        out_shape=[sds((n8, tiles, dp, LANE), F32)] * 3 + [sds(halves, BF16)] * 2 + [
            sds((d, nf), BF16), sds((d, nf), BF16), sds((d, nf), BF16), sds((tokens, d), BF16), sds((tokens, d), BF16),
            sds((3, RING, 2, RING * rows, nf), BF16),
            sds((3, nf, cols), F32), sds((3, 2, nf, cols), F32),
            sds((2, RING, RING, rows, d), BF16), sds((2, RING, RING, rows, d), BF16), sds((2, RING, RING, rows, d), BF16),
            sds((2, 2, 2, rows, d), BF16), sds((2, 2, 2, 2, rows, d), BF16), sds((2, 2, 2, rows, d), BF16),
            sds((2, RING, 2, rows // 2, d), BF16),
            sds((2, 2, 1, rows // 2, d), BF16), sds((2, 2, 2, 1, rows // 2, d), BF16), sds((2, 2, 1, rows // 2, d), BF16),
        ],
        in_specs=[hbm] * 7,
        out_specs=[hbm] * 23,
        scratch_shapes=[
            pltpu.VMEM((3, nf, tokens), BF16),
            pltpu.VMEM((2, tokens, cols), BF16),
            pltpu.VMEM((3, padded, cols), F32),
            pltpu.VMEM((3, 2, nf, cols), F32),
            dma((6,)),
            dma((3, n8)), dma((3, n8)),
            dma((3, 2, n8)), dma((3, 2, n8)),
            dma((3, 2, n8 // 2)), dma((3, 2, n8 // 2)),
            dma((3, 2)), dma((3, 2)),
            dma((3, 2)), dma((3, 2)),
            dma((3, 2, RING)), dma((3, 2, RING)),
            dma((3, RING)), dma((3, RING)),
            dma((3, RING, RING)), dma((3, RING, RING)),
            dma((3,)), dma((3,)), dma((2,)), dma((2, 2)), dma((2,)), dma((2,)),
            dma((3, 2)), dma((3, 2)),
            dma((3, 2, tiles)), dma((3, 2, tiles)),
            dma((3, tiles, n8)), dma((3, tiles, n8)),
            dma((3, tiles)),
            dma((2,)), dma((2,)),
        ] + [dma((2, 2))] * 12,
        compiler_params=pltpu.CompilerParams(collective_id=0, has_side_effects=True, vmem_limit_bytes=67043328),
        cost_estimate=pl.CostEstimate(flops=18 * nf * tokens * d, bytes_accessed=300_000_000, transcendentals=0),
        name="layer",
    )(sg, su, sd, tok, grad, tok.reshape(halves), grad.reshape(halves))
    return res[:3], res[3].reshape(rows, d), res[4].reshape(rows, d)


def assemble_kernel(og, ou, od, out, gin, g, u, w, res, gres, buf, flat, in_sem, out_sem, row_buf, row_sem):
    n8, nf = og.shape[0], g.shape[1] // og.shape[0]
    srcs, dsts = (og, ou, od), (g, u, w)
    rows_in = [pltpu.make_async_copy(src, row_buf.at[r], row_sem.at[r]) for r, src in enumerate((out, gin))]
    loads = [pltpu.make_async_copy(src, buf.at[t], in_sem.at[t]) for t, src in enumerate(srcs)]
    stores = [pltpu.make_async_copy(flat.at[t], dst, out_sem.at[t]) for t, dst in enumerate(dsts)]
    for c in loads + rows_in:
        c.start()
    for t in range(3):
        loads[t].wait()
        for j in range(n8):
            flat[t, :, j * nf:(j + 1) * nf] = jnp.concatenate([buf[t, j, tile] for tile in range(buf.shape[2])], axis=1)[:, :nf]
        stores[t].start()
    rows_out = [pltpu.make_async_copy(row_buf.at[r], dst, row_sem.at[r]) for r, dst in enumerate((res, gres))]
    for c in rows_in:
        c.wait()
    for c in rows_out:
        c.start()
    for c in stores + rows_out:
        c.wait()


def assemble(sums, out, gin, ff):
    dp = sums[0].shape[2]
    hbm = pl.BlockSpec(memory_space=pl.ANY)
    dma = pltpu.SemaphoreType.DMA
    sds = jax.ShapeDtypeStruct
    return pl.pallas_call(
        assemble_kernel,
        out_shape=[sds((dp, ff), F32)] * 3 + [sds(out.shape, BF16)] * 2,
        in_specs=[hbm] * 5,
        out_specs=[hbm] * 5,
        scratch_shapes=[
            pltpu.VMEM((3,) + sums[0].shape, F32), pltpu.VMEM((3, dp, ff), F32), dma((3,)), dma((3,)),
            pltpu.VMEM((2,) + out.shape, BF16), dma((2,)),
        ],
        compiler_params=pltpu.CompilerParams(vmem_limit_bytes=63 * 1024 * 1024),
        name="assemble",
    )(*sums, out, gin)


def solution(mesh):
    nz, ny, nd = mesh.shape["datb"], mesh.shape["model"], mesh.shape["data"]
    fine = Mesh(mesh.devices.reshape(nz, ny, nd // 2, 2), ("datb", "model", "x", "core"))

    def local_step(tok_loc, wg_loc, wu_loc, wd_loc, grad_loc):
        sums, out, grad_in = layer(wg_loc, wu_loc, wd_loc.T, tok_loc, grad_loc)
        grad_gate, grad_up, grad_down_t, out, grad_in = assemble(sums, out, grad_in, wg_loc.shape[1])
        return out, grad_in, grad_gate, grad_up, grad_down_t.T

    return jax.shard_map(local_step, mesh=fine, in_specs=(ROW_SPEC, GATE_SPEC, GATE_SPEC, DOWN_SPEC, ROW_SPEC), out_specs=(ROW_SPEC, ROW_SPEC, GATE_SPEC, GATE_SPEC, DOWN_SPEC), check_vma=False)
```

```python
import functools

import jax
import jax.numpy as jnp
from jax import lax
from jax.experimental import pallas as pl
from jax.experimental.pallas import tpu as pltpu
from jax.sharding import Mesh
from jax.sharding import PartitionSpec as P

ROW_SPEC = P(("datb", "x", "core", "model"), None)
GATE_SPEC = P(("datb", "x", "core"), "model")
DOWN_SPEC = P("model", ("datb", "x", "core"))
BF16 = jnp.bfloat16
F32 = jnp.float32
MESH_ID = pl.DeviceIdType.MESH
RING = 4
NEAR = ((0, 0), (0, 1), (1, 0), (3, 0), (1, 1), (3, 1), (2, 0), (2, 1))
DELTAS = (0, 3, 1, 2)
LANE = 128
OUT_COLS = 512
EX, Z1, Z2, P1, P2, BL, Q1, Q2, WD, CI = range(10)
GATHER_STEPS = (
    (Z1, 0, 0), (Z1, 1, 0), (P1, 0, 0), (P1, 0, 1), (EX, 0, 1), (EX, 0, 2), (EX, 0, 3), (Z1, 2, 0), (EX, 1, 1), (BL, 0, 0), (EX, 2, 1),
    (P1, 2, 0), (P1, 2, 1), (EX, 0, 4), (EX, 0, 5), (Z1, 0, 1), (Z1, 1, 1), (BL, 1, 0), (Z1, 2, 1), (EX, 0, 6), (EX, 0, 7), (Z2, 0, 0, 0),
    (Z2, 1, 0, 0), (EX, 1, 2), (EX, 1, 3), (Z2, 2, 0, 0), (Q1, 0, 0, 0), (Q1, 0, 0, 1), (EX, 1, 4), (EX, 1, 5), (Z1, 0, 2), (EX, 1, 6),
    (EX, 1, 7), (P2, 2, 1), (P2, 2, 0), (Z1, 0, 3), (Z1, 0, 4), (P2, 0, 0), (P2, 0, 1), (BL, 0, 1), (Q1, 1, 0, 1), (Z1, 0, 5), (EX, 2, 2),
    (EX, 2, 3), (Z1, 0, 6), (Z2, 0, 1, 0), (BL, 0, 2), (EX, 2, 4), (EX, 2, 5), (Z1, 0, 7), (Q2, 0, 0), (Z2, 0, 1, 1), (EX, 2, 6),
    (EX, 2, 7), (Z2, 0, 0, 1), (Q1, 0, 1, 1), (Z2, 0, 1, 2), (Z2, 0, 0, 2), (P1, 1, 0), (P1, 1, 1), (Q1, 1, 0, 0), (Z2, 0, 0, 3),
    (Z2, 0, 1, 3), (Z1, 1, 2), (BL, 2, 1), (Q1, 0, 2, 1), (Q1, 0, 1, 0), (Z1, 1, 3), (Z1, 1, 4), (BL, 2, 2), (Z1, 1, 5), (BL, 2, 0),
    (Q1, 0, 2, 0), (BL, 0, 3), (Z1, 1, 6), (Q2, 0, 2), (WD, 0),
)
GATE_STEPS = (
    (),
    (
        (Q2, 1, 0), (Z1, 1, 7), (Z2, 1, 1, 0), (P2, 1, 0), (P2, 1, 1), (CI, 0),
    ),
    (
        (Z2, 1, 0, 1), (Z2, 1, 1, 1), (Z2, 1, 0, 2), (BL, 1, 1), (BL, 2, 3), (Q1, 2, 1, 1), (Q1, 2, 1, 0), (Z2, 1, 1, 2), (Q1, 0, 3, 1),
        (Z2, 1, 0, 3), (Q1, 2, 2, 0), (Q1, 2, 2, 1), (Q2, 0, 1),
    ),
    (
        (Z2, 1, 1, 3), (Z2, 2, 0, 1), (BL, 1, 2), (Q1, 1, 1, 1), (CI, 1),
    ),
    (
        (Z1, 2, 2), (BL, 1, 3), (Q1, 2, 0, 0), (Q1, 2, 0, 1),
    ),
    (
        (Q1, 0, 3, 0), (Z1, 2, 3), (CI, 2),
    ),
    (
        (Q2, 0, 3), (Z1, 2, 4), (Z1, 2, 5), (Q1, 2, 3, 0), (Q1, 2, 3, 1),
    ),
    (
        (WD, 1), (Q2, 2, 1), (Q2, 2, 2), (Z1, 2, 6), (Q1, 1, 1, 0), (Q1, 1, 2, 1), (CI, 3),
    ),
)
UP_STEPS = (
    (
        (Z1, 2, 7), (Q1, 1, 2, 0),
    ),
    (
        (Q2, 2, 0), (Q2, 2, 3), (Z2, 2, 1, 0), (Z2, 2, 0, 2), (Q1, 1, 3, 1),
    ),
    (
        (Z2, 2, 1, 1), (Q1, 1, 3, 0),
    ),
    (
        (Z2, 2, 0, 3), (Q2, 1, 2),
    ),
    (
        (Q2, 1, 1), (Z2, 2, 1, 2),
    ),
    (
        (Z2, 2, 1, 3),
    ),
    (
        (Q2, 1, 3),
    ),
    (),
)
LATE_STEPS = (
    (WD, 2),
)
Z_ORDER = (2, 0, 1)
EARLY_ORDER = (
    ('far_block', 2), ('next_products', 2),
)
LATE_ORDER = (
    ('next_adds', 2), ('far_block', 0), ('far_block', 1), ('own_block', 2), ('give_rows', 1), ('finish', 2, 0), ('give_rows', 0),
    ('finish', 2, 3), ('finish', 2, 1), ('finish', 2, 4), ('finish', 2, 2), ('keep_rows', 1), ('ring_first', 1, 1), ('keep_rows', 0),
    ('ring_first', 0, 1), ('next_blocks', 0), ('own_block', 0), ('ring_dependent', 1, 1), ('next_blocks', 1), ('finish', 0, 0),
    ('own_block', 1), ('finish', 0, 1), ('ring_dependent', 0, 1), ('finish', 0, 2), ('ring_last', 1, 1), ('ring_first', 1, 2),
    ('finish', 0, 3), ('finish', 0, 4), ('ring_last', 0, 1), ('ring_first', 0, 2), ('ring_dependent', 1, 2), ('finish', 1, 0),
    ('ring_last', 1, 2), ('ring_dependent', 0, 2), ('finish', 1, 1), ('finish', 1, 2), ('ring_last', 0, 2), ('finish', 1, 3),
    ('finish', 1, 4),
)


def dot(a, b, ca, cb):
    return lax.dot_general(a, b, (((ca,), (cb,)), ((), ())), preferred_element_type=F32)


def layer_kernel(sg, su, sd, tok, grad, tok_own, grad_own,
                 og, ou, od, out, gin, wg, wu, wd, tok_all, grad_all, h_all, ra, rb, give, rc, part, ra1, rb1, sd1, mid, ra2, rb2, sd2,
                 ff, blk, far, nxt,
                 own_sem, ex_s, ex_r, z1_s, z1_r, z2_s, z2_r, p1_s, p1_r, p2_s, p2_r, q1_s, q1_r, q2_s, q2_r, cc_s, cc_r,
                 sh_sem, wv_sem, row_sem, hst_sem, blk_sem, tmp_sem, a_s, a_r, u_s, u_r, e_s, e_r, out_sem,
                 c_s, c_r, a1_s, a1_r, f1_s, f1_r, d1_s, d1_r, a2_s, a2_r, f2_s, f2_r, d2_s, d2_r):
    z, y = lax.axis_index("datb"), lax.axis_index("model")
    x, core = lax.axis_index("x"), lax.axis_index("core")
    i8 = 2 * x + core
    n8 = 2 * RING
    rows, d = tok.shape
    half_rows = rows // 2
    chunk = RING * rows
    n_chunk = n8
    nf, tokens = ff.shape[1:]
    dp = sg.shape[0]
    half = nf // 2
    cols = blk.shape[2]
    tiles = far.shape[1] // LANE
    outs = (og, ou, od)

    zs, ys, xs = ([v] + [lax.rem(v + k, RING) for k in range(1, RING)] for v in (z, y, x))
    cores = (core, 1 - core)
    peers = [[2 * v + c for c in cores] for v in xs]
    slot_at = [[[pl.multiple_of((zz * n8 + peers[dx][dc]) * dp, 16) for dc in range(2)] for dx in range(RING)] for zz in zs]
    hand_at = [[pl.multiple_of(p * dp, 8) for p in row] for row in peers]
    rows_at = [[[pl.multiple_of((peers[dx][dc] * RING + yy) * rows, half_rows) for dc in range(2)] for yy in ys] for dx in range(RING)]
    lanes_at = [pl.multiple_of(zz * cols, LANE) for zz in zs]

    def peer(dx, dc):
        return peers[dx][dc]

    def zdev(k):
        return {"datb": zs[k]}

    def xdev(k):
        return {"x": xs[k]}

    def ydev(k):
        return {"model": ys[k]}

    def near(dx, dc):
        return {"x": xs[dx], "core": cores[dc]}

    def copy(src, dst, s, r, dev):
        return pltpu.make_async_remote_copy(src_ref=src, dst_ref=dst, send_sem=s, recv_sem=r, device_id=dev, device_id_type=MESH_ID)

    rcopy = copy

    def start(copies):
        for c in copies:
            c.start()

    def received(copies):
        for c in copies:
            c.wait_recv()

    def sent(copies):
        for c in copies:
            c.wait_send()

    def run_order(fns, order):
        for fn, *args in order:
            with jax.named_scope("_".join(str(v) for v in [fn, *args])):
                fns[fn](*args)

    barrier = pltpu.get_barrier_semaphore()
    others = [zdev(1), zdev(3), ydev(1), ydev(3)] + [near(*n) for n in NEAR[1:]]
    for dev in others:
        pl.semaphore_signal(barrier, inc=1, device_id=dev, device_id_type=MESH_ID)

    def blk_load(t, slot, k):
        src = tok_all if t < 2 else grad_all
        return pltpu.make_async_copy(src.at[:, pl.ds(lanes_at[k], cols)], blk.at[slot], blk_sem.at[slot])

    plan = []
    for fn, *args in EARLY_ORDER + LATE_ORDER:
        plan += [(args[0], k) for k in {"far_block": (2,), "next_blocks": (1, 3), "next_products": (1, 3), "own_block": (0,)}.get(fn, ())]
    taken = []

    def next_block():
        n = len(taken)
        taken.append(n)
        if n == 0:
            blk_load(plan[0][0], 0, plan[0][1]).start()
        blk_load(plan[n][0], n % 2, plan[n][1]).wait()
        if n + 1 < len(plan):
            blk_load(plan[n + 1][0], (n + 1) % 2, plan[n + 1][1]).start()
        return n % 2

    def product(t, dst):
        slot = next_block()
        step = 2 * LANE

        def one(n, carry):
            lanes = pl.ds(pl.multiple_of(jnp.minimum(n * step, cols - step), LANE), step)
            dst[:nf, lanes] = jnp.dot(ff[t], blk[slot, :, lanes], preferred_element_type=F32)
            return carry

        lax.fori_loop(0, -(-cols // step), one, 0)

    lo, hi = pl.ds(0, half), pl.ds(half, half)

    def a_copies(t):
        return [rcopy(far.at[t, rows], ra.at[t, rows], a_s.at[t, s], a_r.at[t, s], zdev(k)) for s, rows, k in ((0, lo, 1), (1, hi, 3))]

    def tile_rows(tile):
        return pl.ds(tile * LANE, min(LANE, nf - tile * LANE))

    def unit_copies(t, tile):
        at = tile_rows(tile)
        return [rcopy(nxt.at[t, s, at], rb.at[t, s, at], u_s.at[t, s, tile], u_r.at[t, s, tile], zdev(1 + 2 * s)) for s in range(2)]

    def far_block(t):
        product(t, far.at[t])
        start(a_copies(t))

    def early_units(t):
        if ("next_products", t) not in EARLY_ORDER + LATE_ORDER:
            return ()
        free = [(0, tile) for tile in range(tiles) if tile * LANE >= half]
        return free + [(1, tile) for tile in range(tiles) if (tile + 1) * LANE <= half]

    def next_products(t):
        for s in range(2):
            product(t, nxt.at[t, s])
        for s, tile in early_units(t):
            unit_copies(t, tile)[s].start()

    def forward_phase(shard, pieces, wv, rowbuf, av, bv, hst):
        fulls = (wg, wu, wd)
        loads = [pltpu.make_async_copy(src, shard.at[t], sh_sem.at[t]) for t, src in enumerate((sg, su, sd))]
        for c in loads:
            c.start()

        def cut_pieces(t):
            loads[t].wait()
            for j in range(n8):
                pieces[t, j] = shard[t, :, j * nf:(j + 1) * nf]

        started = []

        def go(make, *args):
            make(*args).start()
            started.append((make, args))

        def slot(t, k, source):
            dx, dc = source
            return fulls[t].at[pl.ds(slot_at[k][dx][dc], dp)]

        def source(k):
            dx, dc = NEAR[k]
            return (RING - dx) % RING, dc

        def back(side):
            return 3 if side == 0 else 1

        def ahead(side):
            return 1 if side == 0 else 3

        def exchange_copy(t, k):
            return copy(pieces.at[t, peer(*NEAR[k])], slot(t, 0, NEAR[0]), ex_s.at[t, k], ex_r.at[t, k], near(*NEAR[k]))

        def exchange(t, k):
            go(exchange_copy, t, k)

        def z_first_copy(t, side, k):
            here = slot(t, 0, source(k))
            return copy(here if k else pieces.at[t, i8], here, z1_s.at[t, side, k], z1_r.at[t, side, k], zdev(ahead(side)))

        def z_first(t, k):
            if k:
                here = slot(t, 0, source(k))
                copy(here, here, ex_s.at[t, k], ex_r.at[t, k], {"datb": z}).wait_recv()
            for side in range(2):
                go(z_first_copy, t, side, k)

        def wait_z_first(t, side, k):
            there = slot(t, back(side), source(k))
            copy(there, there, z1_s.at[t, side, k], z1_r.at[t, side, k], {"datb": z}).wait_recv()

        def z_second_copy(t, side, k):
            there = slot(t, back(side), source(k + side * (n8 // 2)))
            return copy(there, there, z2_s.at[t, side, k], z2_r.at[t, side, k], zdev(ahead(side)))

        def z_second(t, side, k):
            wait_z_first(t, side, k + side * (n8 // 2))
            go(z_second_copy, t, side, k)

        def weights_done(t):
            local[t].wait()
            for k in range(n8 // 2):
                wait_z_first(t, 0, n8 // 2 + k)
                wait_z_first(t, 1, k)
                for side in range(2):
                    there = slot(t, 2, source(k + side * (n8 // 2)))
                    copy(there, there, z2_s.at[t, side, k], z2_r.at[t, side, k], {"datb": z}).wait_recv()
            w_load(t).start()

        cut = d // 2
        rings = ((tok, tok_all, pl.ds(0, d), True), (grad, grad_all, pl.ds(0, cut), True), (grad, grad_all, pl.ds(cut, d - cut), False))

        def axis(r, n):
            return xdev if rings[r][3] == (n == 1) else ydev

        def block(r, da, db, flip=0, lo=0, size=rows):
            dx, dy = (da, db) if rings[r][3] else (db, da)
            first = rows_at[dx][dy][flip]
            return rings[r][1].at[pl.ds(pl.multiple_of(first + lo, half_rows) if lo else first, size), rings[r][2]]

        def own_block(r):
            return rings[r][0].at[:, rings[r][2]]

        def to_core_copy(r, ia, ib):
            there = block(r, DELTAS[ia], DELTAS[ib])
            return copy(own_block(r) if ia == 0 and ib == 0 else there, there, cc_s.at[r, ia, ib], cc_r.at[r, ia, ib], near(0, 1))

        def to_core(r, ia, ib):
            go(to_core_copy, r, ia, ib)

        def first_copy(r, side):
            return copy(own_block(r), block(r, 0, 0), p1_s.at[r, side], p1_r.at[r, side], axis(r, 1)(ahead(side)))

        def first_own(r, side):
            go(first_copy, r, side)

        def first_far_copy(r, side):
            part = block(r, back(side), 0, 0, side * half_rows, half_rows)
            return copy(part, part, p2_s.at[r, side], p2_r.at[r, side], axis(r, 1)(ahead(side)))

        def first_forward(r, side):
            there = block(r, back(side), 0)
            copy(there, there, p1_s.at[r, side], p1_r.at[r, side], {"datb": z}).wait_recv()
            go(first_far_copy, r, side)

        def block_on(r, ia):
            for side in range(2 if ia == 3 else 0):
                part = block(r, 2, 0, 0, side * half_rows, half_rows)
                copy(part, part, p2_s.at[r, side], p2_r.at[r, side], {"datb": z}).wait_recv()
            for side in range(2):
                go(second_copy, r, side, ia)
            to_core(r, ia, 0)

        def second_copy(r, side, ia):
            there = block(r, DELTAS[ia], 0)
            return copy(there if ia else own_block(r), there, q1_s.at[r, side, ia], q1_r.at[r, side, ia], axis(r, 2)(ahead(side)))

        def second_far_copy(r, ia):
            side = ia // 2
            there = block(r, DELTAS[ia], back(side))
            return copy(there, there, q2_s.at[r, ia], q2_r.at[r, ia], axis(r, 2)(ahead(side)))

        def second_forward(r, ia, side):
            there = block(r, DELTAS[ia], back(side))
            copy(there, there, q1_s.at[r, side, ia], q1_r.at[r, side, ia], {"datb": z}).wait_recv()
            if ia // 2 == side:
                go(second_far_copy, r, ia)
            to_core(r, ia, 1 if side == 0 else 2)

        def second_far(r, ia):
            there = block(r, DELTAS[ia], 2)
            copy(there, there, q2_s.at[r, ia], q2_r.at[r, ia], {"datb": z}).wait_recv()
            to_core(r, ia, 3)

        def chunk_in(ia):
            rows_in(0, (ia,))

        def rows_in(r, blocks=range(RING)):
            for ia in blocks:
                for ib in range(RING):
                    there = block(r, DELTAS[ia], DELTAS[ib], 1)
                    copy(there, there, cc_s.at[r, ia, ib], cc_r.at[r, ia, ib], {"datb": z}).wait_recv()

        local = [pltpu.make_async_copy(pieces.at[t, i8], slot(t, 0, NEAR[0]), own_sem.at[t]) for t in range(3)]
        local += [pltpu.make_async_copy(own_block(r), block(r, 0, 0), own_sem.at[3 + r]) for r in range(3)]

        def w_load(t):
            return pltpu.make_async_copy(fulls[t], wv.at[t % 2], wv_sem.at[t])

        def row_load(src, i, buf):
            return pltpu.make_async_copy(src.at[chunk_rows(i)], rowbuf.at[buf], row_sem.at[buf])

        def chunk_loop(src, work, between):
            row_load(src, 0, 0).start()

            def outer(xx, carry):
                def inner(c, carry):
                    i = 2 * xx + c

                    @pl.when(i + 1 < n_chunk)
                    def _():
                        row_load(src, i + 1, 1 - c).start()

                    for k, step in enumerate(between):
                        pl.when(i == k)(step)
                    row_load(src, i, c).wait()
                    work(i, xx, c)
                    return carry

                return lax.fori_loop(0, 2, inner, carry)

            lax.fori_loop(0, RING, outer, 0)

        def chunk_rows(i):
            return pl.ds(pl.multiple_of(i * chunk, chunk), chunk)

        def h_copy(xx, c, slot, j):
            return pltpu.make_async_copy(hst.at[c, slot], h_all.at[j, xx, c], hst_sem.at[c, slot])

        def keep(i, xx, c, slot, j, value):
            @pl.when(xx >= 1)
            def _():
                h_copy(xx - 1, c, slot, j).wait()

            hst[c, slot] = value.astype(BF16)
            h_copy(xx, c, slot, j).start()
            ff[j, :, chunk_rows(i)] = value.T.astype(BF16)

        def kept(slot, j):
            for c in range(2):
                h_copy(RING - 1, c, slot, j).wait()

        def gate_work():
            def outer(ia, carry):
                delta = lax.rem(3 * ia + 3 * lax.div(ia, 2) + 2 * lax.div(ia, 3), RING)

                def inner(flip, carry):
                    for k, group in enumerate(GATE_STEPS):
                        if group:
                            pl.when(2 * ia + flip == k)(functools.partial(run, group))
                    i = 2 * lax.rem(x + delta, RING) + lax.rem(core + flip, 2)
                    row_load(tok_all, i, 0).start()
                    row_load(tok_all, i, 0).wait()
                    av[chunk_rows(i)] = jnp.dot(rowbuf[0], wv[0], preferred_element_type=F32).astype(BF16)
                    return carry

                return lax.fori_loop(0, 2, inner, carry)

            lax.fori_loop(0, RING, outer, 0)

        def up_work(i, xx, c):
            b = jnp.dot(rowbuf[c], wv[1], preferred_element_type=F32).astype(BF16)
            bv[chunk_rows(i)] = b
            a, b = av[chunk_rows(i)].astype(F32), b.astype(F32)
            keep(i, xx, c, 0, 2, a * jax.nn.sigmoid(a) * b)

        def post_work(i, xx, c):
            g = jnp.dot(rowbuf[c], wv[0], preferred_element_type=F32).astype(BF16).astype(F32)
            a, b = av[chunk_rows(i)].astype(F32), bv[chunk_rows(i)].astype(F32)
            sig = jax.nn.sigmoid(a)
            keep(i, xx, c, 0, 0, g * b * sig * (1.0 + a * (1.0 - sig)))
            keep(i, xx, c, 1, 1, g * (a * sig))

        steps = (exchange, z_first, z_second, first_own, first_forward, block_on, second_forward, second_far, weights_done, chunk_in)

        def run(group):
            for which, *args in group:
                steps[which](*args)

        with jax.named_scope("begin"):
            for t in range(3):
                cut_pieces(t)
            pl.semaphore_wait(barrier, len(others))
            for c in local:
                c.start()
        with jax.named_scope("gather"):
            run(GATHER_STEPS)
            local[3].wait()
            w_load(0).wait()
        with jax.named_scope("gate"):
            gate_work()
        with jax.named_scope("up"):
            run(UP_STEPS[0])
            w_load(1).wait()
            chunk_loop(tok_all, up_work, [functools.partial(run, group) for group in ((),) + UP_STEPS[1:]])
            kept(0, 2)
        with jax.named_scope("rows"):
            for r in (1, 2):
                local[3 + r].wait()
                rows_in(r)
        run_order({"far_block": far_block, "next_products": next_products}, EARLY_ORDER)
        with jax.named_scope("late"):
            run(LATE_STEPS)
            w_load(2).wait()
        with jax.named_scope("down"):
            chunk_loop(grad_all, post_work, ())
            kept(0, 0)
            kept(1, 1)
        for make, args in started:
            make(*args).wait_send()

    def backward_phase(tmp, stage):
        def next_adds(t):
            received(a_copies(t))
            cs = [pltpu.make_async_copy(ra.at[t, at], tmp.at[s, at], tmp_sem.at[s]) for s, at in ((0, lo), (1, hi))]
            start(cs)
            for c, (s, at) in zip(cs, ((0, lo), (1, hi))):
                c.wait()
                nxt[t, s, at] += tmp[s, at]
            for tile in range(tiles):
                start(c for s, c in enumerate(unit_copies(t, tile)) if (s, tile) not in early_units(t))

        def next_blocks(t):
            next_products(t)
            next_adds(t)

        def own_block(t):
            sent(a_copies(t))
            product(t, far.at[t])

        def slot(t):
            return Z_ORDER.index(t) % 2

        def hand_out(t, tile):
            cs = []
            for k in range(1, n8):
                at = pl.ds(hand_at[NEAR[k][0]][NEAR[k][1]], dp)
                cs.append(rcopy(stage.at[slot(t), tile, at], outs[t].at[i8, tile], e_s.at[t, tile, k], e_r.at[t, tile, k], near(*NEAR[k])))
            at = pl.ds(hand_at[0][0], dp)
            return cs, pltpu.make_async_copy(stage.at[slot(t), tile, at], outs[t].at[i8, tile], out_sem.at[t, tile])

        def handed(t, tile):
            cs, mine = hand_out(t, tile)
            sent(cs)
            mine.wait()

        def finish(t, tile):
            received(unit_copies(t, tile))
            at = tile_rows(tile)
            cs = [pltpu.make_async_copy(rb.at[t, s, at], tmp.at[s, at], tmp_sem.at[s]) for s in range(2)]
            start(cs)
            if t == Z_ORDER[2]:
                handed(Z_ORDER[0], tile)
            for c in cs:
                c.wait()
            wide = pl.ds(tile * LANE, LANE)
            stage[slot(t), tile] = (far[t, wide] + tmp[0, wide] + tmp[1, wide]).T
            cs, mine = hand_out(t, tile)
            start(cs + [mine])

        blocks = d // min(OUT_COLS, d)
        width = d // blocks

        def row_products(r, keep):
            side = core if keep else 1 - core
            terms = ((2, wd),) if r == 0 else ((0, wg), (1, wu))
            specs, args = [], []
            for t, w in terms:
                specs += [pl.BlockSpec((1, RING, 1, RING * rows, nf), lambda j, t=t: (t, 0, side, 0, 0)), pl.BlockSpec((width, nf), lambda j: (j, 0))]
                args += [h_all, w]
            wide = pl.BlockSpec((RING, RING, rows, width), lambda j: (0, 0, 0, j))
            if keep:
                specs.append(wide)
                args.append(rc.at[r])

            def body(*refs):
                total = None
                for i in range(len(terms)):
                    h = refs[2 * i][...].reshape(RING * RING * rows, nf)
                    prod = dot(h, refs[2 * i + 1][...], 1, 1)
                    total = prod if total is None else total + prod
                if keep:
                    total = total + refs[-2][...].astype(F32).reshape(total.shape)
                refs[-1][...] = total.astype(BF16).reshape(RING, RING, rows, width)

            pltpu.emit_pipeline(body, grid=(blocks,), in_specs=specs, out_specs=[wide])(*args, (part if keep else give).at[r])

        def core_copy(r):
            return rcopy(give.at[r], rc.at[r], c_s.at[r], c_r.at[r], near(0, 1))

        def on_y(r, n):
            return (r == 0) == (n == 1)

        def level(r, n):
            at = ys if on_y(r, n) else xs
            dev = ydev if on_y(r, n) else xdev
            if n == 1:
                def piece(k, h):
                    return part.at[r, pl.ds(2 * h, 2), at[k]] if on_y(r, n) else part.at[r, at[k], pl.ds(2 * h, 2)]
                return dev, piece, ra1, rb1, sd1, (a1_s, a1_r, f1_s, f1_r, d1_s, d1_r)

            def piece(k, h):
                return mid.at[r, at[k], pl.ds(h, 1)]
            return dev, piece, ra2, rb2, sd2, (a2_s, a2_r, f2_s, f2_r, d2_s, d2_r)

        def ring_a(r, n):
            dev, piece, rfar, _, _, sems = level(r, n)
            return [rcopy(piece(2, s), rfar.at[r, s], sems[0].at[r, s], sems[1].at[r, s], dev(1 + 2 * s)) for s in range(2)]

        def ring_f(r, n):
            dev, piece, _, rnear, _, sems = level(r, n)
            return [rcopy(piece(1 + 2 * s, 1 - s), rnear.at[r, s, 1 - s], sems[2].at[r, s], sems[3].at[r, s], dev(1 + 2 * s)) for s in range(2)]

        def ring_d(r, n):
            dev, _, _, rnear, dep, sems = level(r, n)
            return [rcopy(dep.at[r, s], rnear.at[r, s, s], sems[4].at[r, s], sems[5].at[r, s], dev(1 + 2 * s)) for s in range(2)]

        def add(grid, *terms):
            specs = []
            for ref, at, lead in terms:
                tail = ref.shape[lead:]
                specs.append(pl.BlockSpec((1,) * lead + tuple(tail), lambda *i, at=at, rank=len(tail): tuple(at(*i)) + (0,) * rank))

            def body(*refs):
                total = refs[0][...].astype(F32).reshape(refs[0].shape[-2:])
                for ref in refs[1:-1]:
                    total = total + ref[...].astype(F32).reshape(total.shape)
                refs[-1][...] = total.astype(BF16).reshape(refs[-1].shape)

            pltpu.emit_pipeline(body, grid=grid, in_specs=specs[:-1], out_specs=specs[-1:])(*[ref for ref, _, _ in terms])

        def ring_first(r, n):
            start(ring_a(r, n) + ring_f(r, n))

        def ring_dependent(r, n):
            received(ring_a(r, n))
            here = y if on_y(r, n) else x
            if n == 1:
                def near_block(s, i):
                    at = lax.rem(here + 1 + 2 * s, RING)
                    return (2 * s + i, at) if on_y(r, n) else (at, 2 * s + i)

                add((2, 2), (part.at[r], near_block, 2), (ra1.at[r], lambda s, i: (s, i), 2), (sd1.at[r], lambda s, i: (s, i), 2))
            else:
                add((2,), (mid.at[r], lambda s: (lax.rem(here + 1 + 2 * s, RING), s), 2), (ra2.at[r], lambda s: (s, 0), 2),
                    (sd2.at[r], lambda s: (s, 0), 2))
            start(ring_d(r, n))

        def ring_last(r, n):
            received(ring_f(r, n) + ring_d(r, n))
            here = y if on_y(r, n) else x
            if n == 1:
                def own_at(h, i):
                    return (2 * h + i, here) if on_y(r, n) else (here, 2 * h + i)

                add((2, 2), (part.at[r], own_at, 2), (rb1.at[r, 0], lambda h, i: (h, i), 2),
                    (rb1.at[r, 1], lambda h, i: (h, i), 2), (mid.at[r], lambda h, i: (2 * h + i,), 1))
            else:
                own, res = ((tok_own, out), (grad_own, gin))[r]
                add((2,), (own, lambda h: (h,), 1), (mid.at[r], lambda h: (here, h), 2), (rb2.at[r, 0], lambda h: (h, 0), 2),
                    (rb2.at[r, 1], lambda h: (h, 0), 2), (res, lambda h: (h,), 1))

        def give_rows(r):
            row_products(r, False)
            core_copy(r).start()

        def keep_rows(r):
            core_copy(r).wait_recv()
            row_products(r, True)

        run_order({
            "far_block": far_block, "next_products": next_products, "next_adds": next_adds, "next_blocks": next_blocks,
            "own_block": own_block, "finish": finish, "give_rows": give_rows, "keep_rows": keep_rows, "ring_first": ring_first,
            "ring_dependent": ring_dependent, "ring_last": ring_last,
        }, LATE_ORDER)

        for t in range(3):
            for tile in range(tiles):
                sent(unit_copies(t, tile))
                received(hand_out(t, tile)[0])
                if t != Z_ORDER[0]:
                    handed(t, tile)
        for r in range(2):
            core_copy(r).wait_send()
            for n in (1, 2):
                sent(ring_a(r, n) + ring_f(r, n) + ring_d(r, n))

    pl.run_scoped(
        forward_phase,
        pltpu.VMEM((3,) + sg.shape, BF16),
        pltpu.VMEM((3, n8, dp, nf), BF16),
        pltpu.VMEM((2, d, nf), BF16),
        pltpu.VMEM((2, chunk, d), BF16),
        pltpu.VMEM((tokens, nf), BF16),
        pltpu.VMEM((tokens, nf), BF16),
        pltpu.VMEM((2, 2, chunk, nf), BF16),
    )
    pl.run_scoped(backward_phase, pltpu.VMEM((2, tiles * LANE, cols), F32), pltpu.VMEM((2, tiles, cols, LANE), F32))


def layer(sg, su, sd, tok, grad):
    n8 = 2 * RING
    dp, nf = sg.shape[0], sg.shape[1] // n8
    rows, d = tok.shape
    tokens = rows * RING * n8
    cols = d // RING
    tiles = -(-nf // LANE)
    padded = tiles * LANE
    hbm = pl.BlockSpec(memory_space=pl.ANY)
    dma = pltpu.SemaphoreType.DMA
    sds = jax.ShapeDtypeStruct
    halves = (2, rows // 2, d)
    res = pl.pallas_call(
        layer_kernel,
        out_shape=[sds((n8, tiles, dp, LANE), F32)] * 3 + [sds(halves, BF16)] * 2 + [
            sds((d, nf), BF16), sds((d, nf), BF16), sds((d, nf), BF16), sds((tokens, d), BF16), sds((tokens, d), BF16),
            sds((3, RING, 2, RING * rows, nf), BF16),
            sds((3, nf, cols), F32), sds((3, 2, nf, cols), F32),
            sds((2, RING, RING, rows, d), BF16), sds((2, RING, RING, rows, d), BF16), sds((2, RING, RING, rows, d), BF16),
            sds((2, 2, 2, rows, d), BF16), sds((2, 2, 2, 2, rows, d), BF16), sds((2, 2, 2, rows, d), BF16),
            sds((2, RING, 2, rows // 2, d), BF16),
            sds((2, 2, 1, rows // 2, d), BF16), sds((2, 2, 2, 1, rows // 2, d), BF16), sds((2, 2, 1, rows // 2, d), BF16),
        ],
        in_specs=[hbm] * 7,
        out_specs=[hbm] * 23,
        scratch_shapes=[
            pltpu.VMEM((3, nf, tokens), BF16),
            pltpu.VMEM((2, tokens, cols), BF16),
            pltpu.VMEM((3, padded, cols), F32),
            pltpu.VMEM((3, 2, nf, cols), F32),
            dma((6,)),
            dma((3, n8)), dma((3, n8)),
            dma((3, 2, n8)), dma((3, 2, n8)),
            dma((3, 2, n8 // 2)), dma((3, 2, n8 // 2)),
            dma((3, 2)), dma((3, 2)),
            dma((3, 2)), dma((3, 2)),
            dma((3, 2, RING)), dma((3, 2, RING)),
            dma((3, RING)), dma((3, RING)),
            dma((3, RING, RING)), dma((3, RING, RING)),
            dma((3,)), dma((3,)), dma((2,)), dma((2, 2)), dma((2,)), dma((2,)),
            dma((3, 2)), dma((3, 2)),
            dma((3, 2, tiles)), dma((3, 2, tiles)),
            dma((3, tiles, n8)), dma((3, tiles, n8)),
            dma((3, tiles)),
            dma((2,)), dma((2,)),
        ] + [dma((2, 2))] * 12,
        compiler_params=pltpu.CompilerParams(collective_id=0, has_side_effects=True, vmem_limit_bytes=67043328),
        cost_estimate=pl.CostEstimate(flops=18 * nf * tokens * d, bytes_accessed=300_000_000, transcendentals=0),
        name="layer",
    )(sg, su, sd, tok, grad, tok.reshape(halves), grad.reshape(halves))
    return res[:3], res[3].reshape(rows, d), res[4].reshape(rows, d)


def assemble_kernel(og, ou, od, out, gin, g, u, w, res, gres, buf, flat, in_sem, out_sem, row_buf, row_sem):
    n8, nf = og.shape[0], g.shape[1] // og.shape[0]
    srcs, dsts = (og, ou, od), (g, u, w)
    rows_in = [pltpu.make_async_copy(src, row_buf.at[r], row_sem.at[r]) for r, src in enumerate((out, gin))]
    loads = [pltpu.make_async_copy(src, buf.at[t], in_sem.at[t]) for t, src in enumerate(srcs)]
    stores = [pltpu.make_async_copy(flat.at[t], dst, out_sem.at[t]) for t, dst in enumerate(dsts)]
    for c in loads + rows_in:
        c.start()
    for t in range(3):
        loads[t].wait()
        for j in range(n8):
            flat[t, :, j * nf:(j + 1) * nf] = jnp.concatenate([buf[t, j, tile] for tile in range(buf.shape[2])], axis=1)[:, :nf]
        stores[t].start()
    rows_out = [pltpu.make_async_copy(row_buf.at[r], dst, row_sem.at[r]) for r, dst in enumerate((res, gres))]
    for c in rows_in:
        c.wait()
    for c in rows_out:
        c.start()
    for c in stores + rows_out:
        c.wait()


def assemble(sums, out, gin, ff):
    dp = sums[0].shape[2]
    hbm = pl.BlockSpec(memory_space=pl.ANY)
    dma = pltpu.SemaphoreType.DMA
    sds = jax.ShapeDtypeStruct
    return pl.pallas_call(
        assemble_kernel,
        out_shape=[sds((dp, ff), F32)] * 3 + [sds(out.shape, BF16)] * 2,
        in_specs=[hbm] * 5,
        out_specs=[hbm] * 5,
        scratch_shapes=[
            pltpu.VMEM((3,) + sums[0].shape, F32), pltpu.VMEM((3, dp, ff), F32), dma((3,)), dma((3,)),
            pltpu.VMEM((2,) + out.shape, BF16), dma((2,)),
        ],
        compiler_params=pltpu.CompilerParams(vmem_limit_bytes=63 * 1024 * 1024),
        name="assemble",
    )(*sums, out, gin)


def solution(mesh):
    nz, ny, nd = mesh.shape["datb"], mesh.shape["model"], mesh.shape["data"]
    fine = Mesh(mesh.devices.reshape(nz, ny, nd // 2, 2), ("datb", "model", "x", "core"))

    def local_step(tok_loc, wg_loc, wu_loc, wd_loc, grad_loc):
        sums, out, grad_in = layer(wg_loc, wu_loc, wd_loc.T, tok_loc, grad_loc)
        grad_gate, grad_up, grad_down_t, out, grad_in = assemble(sums, out, grad_in, wg_loc.shape[1])
        return out, grad_in, grad_gate, grad_up, grad_down_t.T

    return jax.shard_map(local_step, mesh=fine, in_specs=(ROW_SPEC, GATE_SPEC, GATE_SPEC, DOWN_SPEC, ROW_SPEC), out_specs=(ROW_SPEC, ROW_SPEC, GATE_SPEC, GATE_SPEC, DOWN_SPEC), check_vma=False)
```

```python
import functools

import jax
import jax.numpy as jnp
from jax import lax
from jax.experimental import pallas as pl
from jax.experimental.pallas import tpu as pltpu
from jax.sharding import Mesh
from jax.sharding import PartitionSpec as P

ROW_SPEC = P(("datb", "x", "core", "model"), None)
GATE_SPEC = P(("datb", "x", "core"), "model")
DOWN_SPEC = P("model", ("datb", "x", "core"))
BF16 = jnp.bfloat16
F32 = jnp.float32
MESH_ID = pl.DeviceIdType.MESH
RING = 4
NEAR = ((0, 0), (0, 1), (1, 0), (3, 0), (1, 1), (3, 1), (2, 0), (2, 1))
DELTAS = (0, 3, 1, 2)
LANE = 128
OUT_COLS = 512
EX, Z1, Z2, P1, P2, BL, Q1, Q2, WD, CI = range(10)
GATHER_STEPS = (
    (Z1, 0, 0), (Z1, 1, 0), (P1, 0, 0), (P1, 0, 1), (EX, 0, 1), (EX, 0, 2), (EX, 0, 3), (Z1, 2, 0), (EX, 1, 1), (BL, 0, 0), (EX, 2, 1),
    (P1, 2, 0), (P1, 2, 1), (EX, 0, 4), (EX, 0, 5), (Z1, 0, 1), (Z1, 1, 1), (BL, 1, 0), (Z1, 2, 1), (EX, 0, 6), (EX, 0, 7), (Z2, 0, 0, 0),
    (Z2, 1, 0, 0), (EX, 1, 2), (EX, 1, 3), (Z2, 2, 0, 0), (Q1, 0, 0, 0), (Q1, 0, 0, 1), (EX, 1, 4), (EX, 1, 5), (Z1, 0, 2), (EX, 1, 6),
    (EX, 1, 7), (P2, 2, 1), (P2, 2, 0), (Z1, 0, 3), (Z1, 0, 4), (P2, 0, 0), (P2, 0, 1), (BL, 0, 1), (Q1, 1, 0, 1), (Z1, 0, 5), (EX, 2, 2),
    (EX, 2, 3), (Z1, 0, 6), (Z2, 0, 1, 0), (BL, 0, 2), (EX, 2, 4), (EX, 2, 5), (Z1, 0, 7), (Q2, 0, 0), (Z2, 0, 1, 1), (EX, 2, 6),
    (EX, 2, 7), (Z2, 0, 0, 1), (Q1, 0, 1, 1), (Z2, 0, 1, 2), (Z2, 0, 0, 2), (P1, 1, 0), (P1, 1, 1), (Q1, 1, 0, 0), (Z2, 0, 0, 3),
    (Z2, 0, 1, 3), (Z1, 1, 2), (BL, 2, 1), (Q1, 0, 2, 1), (Q1, 0, 1, 0), (Z1, 1, 3), (Z1, 1, 4), (BL, 2, 2), (Z1, 1, 5), (BL, 2, 0),
    (Q1, 0, 2, 0), (BL, 0, 3), (Z1, 1, 6), (Q2, 0, 2), (WD, 0),
)
GATE_STEPS = (
    (),
    (
        (Q2, 1, 0), (Z1, 1, 7), (Z2, 1, 1, 0), (P2, 1, 0), (P2, 1, 1), (CI, 0),
    ),
    (
        (Z2, 1, 0, 1), (Z2, 1, 1, 1), (Z2, 1, 0, 2), (BL, 1, 1), (BL, 2, 3), (Q1, 2, 1, 1), (Q1, 2, 1, 0), (Z2, 1, 1, 2), (Q1, 0, 3, 1),
        (Z2, 1, 0, 3), (Q1, 2, 2, 0), (Q1, 2, 2, 1), (Q2, 0, 1),
    ),
    (
        (Z2, 1, 1, 3), (Z2, 2, 0, 1), (BL, 1, 2), (Q1, 1, 1, 1), (CI, 1),
    ),
    (
        (Z1, 2, 2), (BL, 1, 3), (Q1, 2, 0, 0), (Q1, 2, 0, 1),
    ),
    (
        (Q1, 0, 3, 0), (Z1, 2, 3), (CI, 2),
    ),
    (
        (Q2, 0, 3), (Z1, 2, 4), (Z1, 2, 5), (Q1, 2, 3, 0), (Q1, 2, 3, 1),
    ),
    (
        (WD, 1), (Q2, 2, 1), (Q2, 2, 2), (Z1, 2, 6), (Q1, 1, 1, 0), (Q1, 1, 2, 1), (CI, 3),
    ),
)
UP_STEPS = (
    (
        (Z1, 2, 7), (Q1, 1, 2, 0),
    ),
    (
        (Q2, 2, 0), (Q2, 2, 3), (Z2, 2, 1, 0), (Z2, 2, 0, 2), (Q1, 1, 3, 1),
    ),
    (
        (Z2, 2, 1, 1), (Q1, 1, 3, 0),
    ),
    (
        (Z2, 2, 0, 3), (Q2, 1, 2),
    ),
    (
        (Q2, 1, 1), (Z2, 2, 1, 2),
    ),
    (
        (Z2, 2, 1, 3),
    ),
    (
        (Q2, 1, 3),
    ),
    (),
)
LATE_STEPS = (
    (WD, 2),
)
Z_ORDER = (2, 1, 0)
EARLY_ORDER = (
    ("far_block", 2), ("next_products", 2), ("late",), ("give_rows", 0),
)
LATE_ORDER = (
    ("next_adds", 2), ("keep_rows", 0), ("ring_first", 0, 1), ("own_block", 2), ("far_block", 1), ("give_rows", 1), ("finish", 2, 3),
    ("finish", 2, 1), ("finish", 2, 4), ("finish", 2, 2), ("finish", 2, 0), ("far_block", 0), ("ring_dependent", 0, 1), ("keep_rows", 1),
    ("ring_first", 1, 1), ("next_blocks", 1), ("own_block", 1), ("next_blocks", 0), ("own_block", 0), ("finish", 1, 0),
    ("ring_dependent", 1, 1), ("finish", 1, 1), ("ring_last", 0, 1), ("ring_first", 0, 2), ("finish", 1, 2), ("finish", 1, 3),
    ("finish", 1, 4), ("ring_last", 1, 1), ("ring_first", 1, 2), ("finish", 0, 0), ("ring_dependent", 0, 2), ("ring_dependent", 1, 2),
    ("finish", 0, 1), ("ring_last", 0, 2), ("finish", 0, 2), ("ring_last", 1, 2), ("finish", 0, 3), ("finish", 0, 4),
)


def dot(a, b, ca, cb):
    return lax.dot_general(a, b, (((ca,), (cb,)), ((), ())), preferred_element_type=F32)


def layer_kernel(sg, su, sd, tok, grad, tok_own, grad_own,
                 og, ou, od, out, gin, wg, wu, wd, tok_all, grad_all, h_all, ra, rb, give, rc, part, ra1, rb1, sd1, mid, ra2, rb2, sd2,
                 ff, blk, far, nxt,
                 own_sem, ex_s, ex_r, z1_s, z1_r, z2_s, z2_r, p1_s, p1_r, p2_s, p2_r, q1_s, q1_r, q2_s, q2_r, cc_s, cc_r,
                 sh_sem, wv_sem, row_sem, hst_sem, blk_sem, tmp_sem, a_s, a_r, u_s, u_r, e_s, e_r, out_sem,
                 c_s, c_r, a1_s, a1_r, f1_s, f1_r, d1_s, d1_r, a2_s, a2_r, f2_s, f2_r, d2_s, d2_r):
    z, y = lax.axis_index("datb"), lax.axis_index("model")
    x, core = lax.axis_index("x"), lax.axis_index("core")
    i8 = 2 * x + core
    n8 = 2 * RING
    rows, d = tok.shape
    half_rows = rows // 2
    chunk = RING * rows
    n_chunk = n8
    nf, tokens = ff.shape[1:]
    dp = sg.shape[0]
    half = nf // 2
    cols = blk.shape[2]
    tiles = far.shape[1] // LANE
    outs = (og, ou, od)

    zs, ys, xs = ([v] + [lax.rem(v + k, RING) for k in range(1, RING)] for v in (z, y, x))
    cores = (core, 1 - core)
    peers = [[2 * v + c for c in cores] for v in xs]
    slot_at = [[[pl.multiple_of((zz * n8 + peers[dx][dc]) * dp, 16) for dc in range(2)] for dx in range(RING)] for zz in zs]
    hand_at = [[pl.multiple_of(p * dp, 8) for p in row] for row in peers]
    rows_at = [[[pl.multiple_of((peers[dx][dc] * RING + yy) * rows, half_rows) for dc in range(2)] for yy in ys] for dx in range(RING)]
    lanes_at = [pl.multiple_of(zz * cols, LANE) for zz in zs]

    def peer(dx, dc):
        return peers[dx][dc]

    def zdev(k):
        return {"datb": zs[k]}

    def xdev(k):
        return {"x": xs[k]}

    def ydev(k):
        return {"model": ys[k]}

    def near(dx, dc):
        return {"x": xs[dx], "core": cores[dc]}

    def copy(src, dst, s, r, dev):
        return pltpu.make_async_remote_copy(src_ref=src, dst_ref=dst, send_sem=s, recv_sem=r, device_id=dev, device_id_type=MESH_ID)

    rcopy = copy

    def start(copies):
        for c in copies:
            c.start()

    def received(copies):
        for c in copies:
            c.wait_recv()

    def sent(copies):
        for c in copies:
            c.wait_send()

    def run_order(fns, order):
        for fn, *args in order:
            with jax.named_scope("_".join(str(v) for v in [fn, *args])):
                fns[fn](*args)

    barrier = pltpu.get_barrier_semaphore()
    others = [zdev(1), zdev(3), ydev(1), ydev(3)] + [near(*n) for n in NEAR[1:]]
    for dev in others:
        pl.semaphore_signal(barrier, inc=1, device_id=dev, device_id_type=MESH_ID)

    def blk_load(t, slot, k):
        src = tok_all if t < 2 else grad_all
        return pltpu.make_async_copy(src.at[:, pl.ds(lanes_at[k], cols)], blk.at[slot], blk_sem.at[slot])

    plan = []
    for fn, *args in EARLY_ORDER + LATE_ORDER:
        plan += [(args[0], k) for k in {"far_block": (2,), "next_blocks": (1, 3), "next_products": (1, 3), "own_block": (0,)}.get(fn, ())]
    taken = []

    def next_block():
        n = len(taken)
        taken.append(n)
        blk_load(plan[n][0], n % 2, plan[n][1]).wait()
        if n + 1 < len(plan):
            blk_load(plan[n + 1][0], (n + 1) % 2, plan[n + 1][1]).start()
        return n % 2

    def product(t, dst):
        slot = next_block()
        step = 2 * LANE

        def one(n, carry):
            lanes = pl.ds(pl.multiple_of(jnp.minimum(n * step, cols - step), LANE), step)
            dst[:nf, lanes] = jnp.dot(ff[t], blk[slot, :, lanes], preferred_element_type=F32)
            return carry

        lax.fori_loop(0, -(-cols // step), one, 0)

    lo, hi = pl.ds(0, half), pl.ds(half, half)

    def a_copies(t):
        return [rcopy(far.at[t, rows], ra.at[t, rows], a_s.at[t, s], a_r.at[t, s], zdev(k)) for s, rows, k in ((0, lo, 1), (1, hi, 3))]

    def tile_rows(tile):
        return pl.ds(tile * LANE, min(LANE, nf - tile * LANE))

    def unit_copies(t, tile):
        at = tile_rows(tile)
        return [rcopy(nxt.at[t, s, at], rb.at[t, s, at], u_s.at[t, s, tile], u_r.at[t, s, tile], zdev(1 + 2 * s)) for s in range(2)]

    def far_block(t):
        product(t, far.at[t])
        start(a_copies(t))

    def early_units(t):
        if ("next_products", t) not in EARLY_ORDER + LATE_ORDER:
            return ()
        free = [(0, tile) for tile in range(tiles) if tile * LANE >= half]
        return free + [(1, tile) for tile in range(tiles) if (tile + 1) * LANE <= half]

    def next_products(t):
        for s in range(2):
            product(t, nxt.at[t, s])
        for s, tile in early_units(t):
            unit_copies(t, tile)[s].start()

    blocks = d // min(OUT_COLS, d)
    width = d // blocks

    def row_products(r, keep):
        side = core if keep else 1 - core
        terms = ((2, wd),) if r == 0 else ((0, wg), (1, wu))
        specs, args = [], []
        for t, w in terms:
            specs += [pl.BlockSpec((1, RING, 1, RING * rows, nf), lambda j, t=t: (t, 0, side, 0, 0)), pl.BlockSpec((width, nf), lambda j: (j, 0))]
            args += [h_all, w]
        wide = pl.BlockSpec((RING, RING, rows, width), lambda j: (0, 0, 0, j))
        if keep:
            specs.append(wide)
            args.append(rc.at[r])

        def body(*refs):
            total = None
            for i in range(len(terms)):
                h = refs[2 * i][...].reshape(RING * RING * rows, nf)
                prod = dot(h, refs[2 * i + 1][...], 1, 1)
                total = prod if total is None else total + prod
            if keep:
                total = total + refs[-2][...].astype(F32).reshape(total.shape)
            refs[-1][...] = total.astype(BF16).reshape(RING, RING, rows, width)

        pltpu.emit_pipeline(body, grid=(blocks,), in_specs=specs, out_specs=[wide])(*args, (part if keep else give).at[r])

    def core_copy(r):
        return rcopy(give.at[r], rc.at[r], c_s.at[r], c_r.at[r], near(0, 1))

    def give_rows(r):
        row_products(r, False)
        core_copy(r).start()

    def forward_phase(rowbuf, av, bv, hst, wv_a):
        held = {}

        fulls = (wg, wu, wd)
        def shard_load(t):
            return pltpu.make_async_copy((sg, su, sd)[t], held["shard"].at[t], sh_sem.at[t])

        def cut_pieces(t):
            shard_load(t).wait()
            for j in range(n8):
                held["pieces"][t, j] = held["shard"][t, :, j * nf:(j + 1) * nf]
            own_piece(t).start()

        def own_piece(t):
            return pltpu.make_async_copy(held["pieces"].at[t, i8], slot(t, 0, NEAR[0]), own_sem.at[t])

        started = []

        def go(make, *args):
            make(*args).start()
            started.append((make, args))

        def slot(t, k, source):
            dx, dc = source
            return fulls[t].at[pl.ds(slot_at[k][dx][dc], dp)]

        def source(k):
            dx, dc = NEAR[k]
            return (RING - dx) % RING, dc

        def back(side):
            return 3 if side == 0 else 1

        def ahead(side):
            return 1 if side == 0 else 3

        def exchange_copy(t, k):
            return copy(held["pieces"].at[t, peer(*NEAR[k])], slot(t, 0, NEAR[0]), ex_s.at[t, k], ex_r.at[t, k], near(*NEAR[k]))

        def exchange(t, k):
            go(exchange_copy, t, k)

        def z_first_copy(t, side, k):
            here = slot(t, 0, source(k))
            return copy(here if k else held["pieces"].at[t, i8], here, z1_s.at[t, side, k], z1_r.at[t, side, k], zdev(ahead(side)))

        def z_first(t, k):
            if k:
                here = slot(t, 0, source(k))
                copy(here, here, ex_s.at[t, k], ex_r.at[t, k], {"datb": z}).wait_recv()
            for side in range(2):
                go(z_first_copy, t, side, k)

        def wait_z_first(t, side, k):
            there = slot(t, back(side), source(k))
            copy(there, there, z1_s.at[t, side, k], z1_r.at[t, side, k], {"datb": z}).wait_recv()

        def z_second_copy(t, side, k):
            there = slot(t, back(side), source(k + side * (n8 // 2)))
            return copy(there, there, z2_s.at[t, side, k], z2_r.at[t, side, k], zdev(ahead(side)))

        def z_second(t, side, k):
            wait_z_first(t, side, k + side * (n8 // 2))
            go(z_second_copy, t, side, k)

        def weights_done(t):
            if (WD, t) not in LATE_STEPS:
                own_wait(t)
            for k in range(n8 // 2):
                wait_z_first(t, 0, n8 // 2 + k)
                wait_z_first(t, 1, k)
                for side in range(2):
                    there = slot(t, 2, source(k + side * (n8 // 2)))
                    copy(there, there, z2_s.at[t, side, k], z2_r.at[t, side, k], {"datb": z}).wait_recv()
            w_load(t).start()

        cut = d // 2
        rings = ((tok, tok_all, pl.ds(0, d), True), (grad, grad_all, pl.ds(0, cut), True), (grad, grad_all, pl.ds(cut, d - cut), False))

        def axis(r, n):
            return xdev if rings[r][3] == (n == 1) else ydev

        def block(r, da, db, flip=0, lo=0, size=rows):
            dx, dy = (da, db) if rings[r][3] else (db, da)
            first = rows_at[dx][dy][flip]
            return rings[r][1].at[pl.ds(pl.multiple_of(first + lo, half_rows) if lo else first, size), rings[r][2]]

        def own_block(r):
            return rings[r][0].at[:, rings[r][2]]

        def to_core_copy(r, ia, ib):
            there = block(r, DELTAS[ia], DELTAS[ib])
            return copy(own_block(r) if ia == 0 and ib == 0 else there, there, cc_s.at[r, ia, ib], cc_r.at[r, ia, ib], near(0, 1))

        def to_core(r, ia, ib):
            go(to_core_copy, r, ia, ib)

        def first_copy(r, side):
            return copy(own_block(r), block(r, 0, 0), p1_s.at[r, side], p1_r.at[r, side], axis(r, 1)(ahead(side)))

        def first_own(r, side):
            go(first_copy, r, side)

        def first_far_copy(r, side):
            part = block(r, back(side), 0, 0, side * half_rows, half_rows)
            return copy(part, part, p2_s.at[r, side], p2_r.at[r, side], axis(r, 1)(ahead(side)))

        def first_forward(r, side):
            there = block(r, back(side), 0)
            copy(there, there, p1_s.at[r, side], p1_r.at[r, side], {"datb": z}).wait_recv()
            go(first_far_copy, r, side)

        def block_on(r, ia):
            for side in range(2 if ia == 3 else 0):
                part = block(r, 2, 0, 0, side * half_rows, half_rows)
                copy(part, part, p2_s.at[r, side], p2_r.at[r, side], {"datb": z}).wait_recv()
            for side in range(2):
                go(second_copy, r, side, ia)
            to_core(r, ia, 0)

        def second_copy(r, side, ia):
            there = block(r, DELTAS[ia], 0)
            return copy(there if ia else own_block(r), there, q1_s.at[r, side, ia], q1_r.at[r, side, ia], axis(r, 2)(ahead(side)))

        def second_far_copy(r, ia):
            side = ia // 2
            there = block(r, DELTAS[ia], back(side))
            return copy(there, there, q2_s.at[r, ia], q2_r.at[r, ia], axis(r, 2)(ahead(side)))

        def second_forward(r, ia, side):
            there = block(r, DELTAS[ia], back(side))
            copy(there, there, q1_s.at[r, side, ia], q1_r.at[r, side, ia], {"datb": z}).wait_recv()
            if ia // 2 == side:
                go(second_far_copy, r, ia)
            to_core(r, ia, 1 if side == 0 else 2)

        def second_far(r, ia):
            there = block(r, DELTAS[ia], 2)
            copy(there, there, q2_s.at[r, ia], q2_r.at[r, ia], {"datb": z}).wait_recv()
            to_core(r, ia, 3)

        def chunk_in(ia):
            rows_in(0, (ia,))

        def rows_in(r, blocks=range(RING)):
            for ia in blocks:
                for ib in range(RING):
                    there = block(r, DELTAS[ia], DELTAS[ib], 1)
                    copy(there, there, cc_s.at[r, ia, ib], cc_r.at[r, ia, ib], {"datb": z}).wait_recv()

        def own_wait(t):
            there = slot(t, 0, NEAR[0])
            pltpu.make_async_copy(there, there, own_sem.at[t]).wait()

        def own_rows(r):
            return pltpu.make_async_copy(own_block(r), block(r, 0, 0), own_sem.at[3 + r])

        def w_load(t):
            return pltpu.make_async_copy(fulls[t], held["wv_b"] if t == 1 else wv_a, wv_sem.at[t])

        def row_load(src, i, buf):
            return pltpu.make_async_copy(src.at[chunk_rows(i)], rowbuf.at[buf], row_sem.at[buf])

        def chunk_loop(src, work, between):
            row_load(src, 0, 0).start()

            def outer(xx, carry):
                def inner(c, carry):
                    i = 2 * xx + c

                    @pl.when(i + 1 < n_chunk)
                    def _():
                        row_load(src, i + 1, 1 - c).start()

                    for k, step in enumerate(between):
                        pl.when(i == k)(step)
                    row_load(src, i, c).wait()
                    work(i, xx, c)
                    return carry

                return lax.fori_loop(0, 2, inner, carry)

            lax.fori_loop(0, RING, outer, 0)

        def chunk_rows(i):
            return pl.ds(pl.multiple_of(i * chunk, chunk), chunk)

        def h_copy(xx, c, slot, j):
            return pltpu.make_async_copy(hst.at[c, slot], h_all.at[j, xx, c], hst_sem.at[c, slot])

        def keep(i, xx, c, slot, j, value):
            @pl.when(xx >= 1)
            def _():
                h_copy(xx - 1, c, slot, j).wait()

            hst[c, slot] = value.astype(BF16)
            h_copy(xx, c, slot, j).start()
            ff[j, :, chunk_rows(i)] = value.T.astype(BF16)

        def kept(slot, j):
            for c in range(2):
                h_copy(RING - 1, c, slot, j).wait()

        def gate_work():
            def outer(ia, carry):
                delta = lax.rem(3 * ia + 3 * lax.div(ia, 2) + 2 * lax.div(ia, 3), RING)

                def inner(flip, carry):
                    for k, group in enumerate(GATE_STEPS):
                        if group:
                            pl.when(2 * ia + flip == k)(functools.partial(run, group))
                    i = 2 * lax.rem(x + delta, RING) + lax.rem(core + flip, 2)
                    row_load(tok_all, i, 0).start()
                    row_load(tok_all, i, 0).wait()
                    av[chunk_rows(i)] = jnp.dot(rowbuf[0], wv_a[...], preferred_element_type=F32).astype(BF16)
                    return carry

                return lax.fori_loop(0, 2, inner, carry)

            lax.fori_loop(0, RING, outer, 0)

        def up_work(i, xx, c):
            b = jnp.dot(rowbuf[c], held["wv_b"][...], preferred_element_type=F32).astype(BF16)
            bv[chunk_rows(i)] = b
            a, b = av[chunk_rows(i)].astype(F32), b.astype(F32)
            keep(i, xx, c, 0, 2, a * jax.nn.sigmoid(a) * b)

        def post_work(i, xx, c):
            g = jnp.dot(rowbuf[c], wv_a[...], preferred_element_type=F32).astype(BF16).astype(F32)
            a, b = av[chunk_rows(i)].astype(F32), bv[chunk_rows(i)].astype(F32)
            sig = jax.nn.sigmoid(a)
            keep(i, xx, c, 0, 0, g * b * sig * (1.0 + a * (1.0 - sig)))
            keep(i, xx, c, 1, 1, g * (a * sig))

        steps = (exchange, z_first, z_second, first_own, first_forward, block_on, second_forward, second_far, weights_done, chunk_in)

        def run(group):
            for which, *args in group:
                steps[which](*args)

        def rows_ready():
            run(UP_STEPS[-1])
            for r in (1, 2):
                own_rows(r).wait()
                rows_in(r)
            blk_load(plan[0][0], 0, plan[0][1]).start()

        def gather_phase(shard, pieces, wv_b):
            held.update(shard=shard, pieces=pieces, wv_b=wv_b)
            with jax.named_scope("begin"):
                for t in range(3):
                    shard_load(t).start()
                cut_pieces(0)
                pl.semaphore_wait(barrier, len(others))
                for r in range(3):
                    own_rows(r).start()
            with jax.named_scope("gather"):
                cut = {0}
                for step in GATHER_STEPS:
                    if step[0] in (EX, Z1) and step[1] not in cut:
                        cut.add(step[1])
                        cut_pieces(step[1])
                    run((step,))
                own_rows(0).wait()
                w_load(0).wait()
            with jax.named_scope("gate"):
                gate_work()
            with jax.named_scope("up"):
                run(UP_STEPS[0])
                w_load(1).wait()
                chunk_loop(tok_all, up_work, [functools.partial(run, group) for group in ((),) + UP_STEPS[1:-1]] + [rows_ready])
                kept(0, 2)
            for _, t in LATE_STEPS:
                own_wait(t)
            for make, args in started:
                if make is exchange_copy or make is z_first_copy and args[2] == 0:
                    make(*args).wait_send()

        pl.run_scoped(
            gather_phase, pltpu.VMEM((3,) + sg.shape, BF16), pltpu.VMEM((3, n8, dp, nf), BF16), pltpu.VMEM((d, nf), BF16))
        run_order({
            "far_block": far_block, "next_products": next_products, "give_rows": give_rows, "late": functools.partial(run, LATE_STEPS),
        }, EARLY_ORDER)
        with jax.named_scope("down"):
            w_load(2).wait()
            chunk_loop(grad_all, post_work, ())
            kept(0, 0)
            kept(1, 1)
        for make, args in started:
            if not (make is exchange_copy or make is z_first_copy and args[2] == 0):
                make(*args).wait_send()

    def backward_phase(tmp, stage):
        def next_adds(t):
            received(a_copies(t))
            cs = [pltpu.make_async_copy(ra.at[t, at], tmp.at[s, at], tmp_sem.at[s]) for s, at in ((0, lo), (1, hi))]
            start(cs)
            for c, (s, at) in zip(cs, ((0, lo), (1, hi))):
                c.wait()
                nxt[t, s, at] += tmp[s, at]
            for tile in range(tiles):
                start(c for s, c in enumerate(unit_copies(t, tile)) if (s, tile) not in early_units(t))

        def next_blocks(t):
            next_products(t)
            next_adds(t)

        def own_block(t):
            sent(a_copies(t))
            product(t, far.at[t])

        def slot(t):
            return Z_ORDER.index(t) % 2

        def hand_out(t, tile):
            cs = []
            for k in range(1, n8):
                at = pl.ds(hand_at[NEAR[k][0]][NEAR[k][1]], dp)
                cs.append(rcopy(stage.at[slot(t), tile, at], outs[t].at[i8, tile], e_s.at[t, tile, k], e_r.at[t, tile, k], near(*NEAR[k])))
            at = pl.ds(hand_at[0][0], dp)
            return cs, pltpu.make_async_copy(stage.at[slot(t), tile, at], outs[t].at[i8, tile], out_sem.at[t, tile])

        def handed(t, tile):
            cs, mine = hand_out(t, tile)
            sent(cs)
            mine.wait()

        def finish(t, tile):
            received(unit_copies(t, tile))
            at = tile_rows(tile)
            cs = [pltpu.make_async_copy(rb.at[t, s, at], tmp.at[s, at], tmp_sem.at[s]) for s in range(2)]
            start(cs)
            if t == Z_ORDER[2]:
                handed(Z_ORDER[0], tile)
            for c in cs:
                c.wait()
            wide = pl.ds(tile * LANE, LANE)
            stage[slot(t), tile] = (far[t, wide] + tmp[0, wide] + tmp[1, wide]).T
            cs, mine = hand_out(t, tile)
            start(cs + [mine])

        def on_y(r, n):
            return (r == 1) == (n == 1)

        def level(r, n):
            at = ys if on_y(r, n) else xs
            dev = ydev if on_y(r, n) else xdev
            if n == 1:
                def piece(k, h):
                    return part.at[r, pl.ds(2 * h, 2), at[k]] if on_y(r, n) else part.at[r, at[k], pl.ds(2 * h, 2)]
                return dev, piece, ra1, rb1, sd1, (a1_s, a1_r, f1_s, f1_r, d1_s, d1_r)

            def piece(k, h):
                return mid.at[r, at[k], pl.ds(h, 1)]
            return dev, piece, ra2, rb2, sd2, (a2_s, a2_r, f2_s, f2_r, d2_s, d2_r)

        def ring_a(r, n):
            dev, piece, rfar, _, _, sems = level(r, n)
            return [rcopy(piece(2, s), rfar.at[r, s], sems[0].at[r, s], sems[1].at[r, s], dev(1 + 2 * s)) for s in range(2)]

        def ring_f(r, n):
            dev, piece, _, rnear, _, sems = level(r, n)
            return [rcopy(piece(1 + 2 * s, 1 - s), rnear.at[r, s, 1 - s], sems[2].at[r, s], sems[3].at[r, s], dev(1 + 2 * s)) for s in range(2)]

        def ring_d(r, n):
            dev, _, _, rnear, dep, sems = level(r, n)
            return [rcopy(dep.at[r, s], rnear.at[r, s, s], sems[4].at[r, s], sems[5].at[r, s], dev(1 + 2 * s)) for s in range(2)]

        def add(grid, *terms):
            specs = []
            for ref, at, lead in terms:
                tail = ref.shape[lead:]
                specs.append(pl.BlockSpec((1,) * lead + tuple(tail), lambda *i, at=at, rank=len(tail): tuple(at(*i)) + (0,) * rank))

            def body(*refs):
                total = refs[0][...].astype(F32).reshape(refs[0].shape[-2:])
                for ref in refs[1:-1]:
                    total = total + ref[...].astype(F32).reshape(total.shape)
                refs[-1][...] = total.astype(BF16).reshape(refs[-1].shape)

            pltpu.emit_pipeline(body, grid=grid, in_specs=specs[:-1], out_specs=specs[-1:])(*[ref for ref, _, _ in terms])

        def ring_first(r, n):
            start(ring_a(r, n) + ring_f(r, n))

        def ring_dependent(r, n):
            received(ring_a(r, n))
            here = y if on_y(r, n) else x
            if n == 1:
                def near_block(s, i):
                    at = lax.rem(here + 1 + 2 * s, RING)
                    return (2 * s + i, at) if on_y(r, n) else (at, 2 * s + i)

                add((2, 2), (part.at[r], near_block, 2), (ra1.at[r], lambda s, i: (s, i), 2), (sd1.at[r], lambda s, i: (s, i), 2))
            else:
                add((2,), (mid.at[r], lambda s: (lax.rem(here + 1 + 2 * s, RING), s), 2), (ra2.at[r], lambda s: (s, 0), 2),
                    (sd2.at[r], lambda s: (s, 0), 2))
            start(ring_d(r, n))

        def ring_last(r, n):
            received(ring_f(r, n) + ring_d(r, n))
            here = y if on_y(r, n) else x
            if n == 1:
                def own_at(h, i):
                    return (2 * h + i, here) if on_y(r, n) else (here, 2 * h + i)

                add((2, 2), (part.at[r], own_at, 2), (rb1.at[r, 0], lambda h, i: (h, i), 2),
                    (rb1.at[r, 1], lambda h, i: (h, i), 2), (mid.at[r], lambda h, i: (2 * h + i,), 1))
            else:
                own, res = ((tok_own, out), (grad_own, gin))[r]
                add((2,), (own, lambda h: (h,), 1), (mid.at[r], lambda h: (here, h), 2), (rb2.at[r, 0], lambda h: (h, 0), 2),
                    (rb2.at[r, 1], lambda h: (h, 0), 2), (res, lambda h: (h,), 1))

        def keep_rows(r):
            core_copy(r).wait_recv()
            row_products(r, True)

        run_order({
            "far_block": far_block, "next_products": next_products, "next_adds": next_adds, "next_blocks": next_blocks,
            "own_block": own_block, "finish": finish, "give_rows": give_rows, "keep_rows": keep_rows, "ring_first": ring_first,
            "ring_dependent": ring_dependent, "ring_last": ring_last,
        }, LATE_ORDER)

        for t in range(3):
            for tile in range(tiles):
                sent(unit_copies(t, tile))
                received(hand_out(t, tile)[0])
                if t != Z_ORDER[0]:
                    handed(t, tile)
        for r in range(2):
            core_copy(r).wait_send()
            for n in (1, 2):
                sent(ring_a(r, n) + ring_f(r, n) + ring_d(r, n))

    pl.run_scoped(
        forward_phase,
        pltpu.VMEM((2, chunk, d), BF16),
        pltpu.VMEM((tokens, nf), BF16),
        pltpu.VMEM((tokens, nf), BF16),
        pltpu.VMEM((2, 2, chunk, nf), BF16),
        pltpu.VMEM((d, nf), BF16),
    )
    pl.run_scoped(backward_phase, pltpu.VMEM((2, tiles * LANE, cols), F32), pltpu.VMEM((2, tiles, cols, LANE), F32))


def layer(sg, su, sd, tok, grad):
    n8 = 2 * RING
    dp, nf = sg.shape[0], sg.shape[1] // n8
    rows, d = tok.shape
    tokens = rows * RING * n8
    cols = d // RING
    tiles = -(-nf // LANE)
    padded = tiles * LANE
    hbm = pl.BlockSpec(memory_space=pl.ANY)
    dma = pltpu.SemaphoreType.DMA
    sds = jax.ShapeDtypeStruct
    halves = (2, rows // 2, d)
    res = pl.pallas_call(
        layer_kernel,
        out_shape=[sds((n8, tiles, dp, LANE), F32)] * 3 + [sds(halves, BF16)] * 2 + [
            sds((d, nf), BF16), sds((d, nf), BF16), sds((d, nf), BF16), sds((tokens, d), BF16), sds((tokens, d), BF16),
            sds((3, RING, 2, RING * rows, nf), BF16),
            sds((3, nf, cols), F32), sds((3, 2, nf, cols), F32),
            sds((2, RING, RING, rows, d), BF16), sds((2, RING, RING, rows, d), BF16), sds((2, RING, RING, rows, d), BF16),
            sds((2, 2, 2, rows, d), BF16), sds((2, 2, 2, 2, rows, d), BF16), sds((2, 2, 2, rows, d), BF16),
            sds((2, RING, 2, rows // 2, d), BF16),
            sds((2, 2, 1, rows // 2, d), BF16), sds((2, 2, 2, 1, rows // 2, d), BF16), sds((2, 2, 1, rows // 2, d), BF16),
        ],
        in_specs=[hbm] * 7,
        out_specs=[hbm] * 23,
        scratch_shapes=[
            pltpu.VMEM((3, nf, tokens), BF16),
            pltpu.VMEM((2, tokens, cols), BF16),
            pltpu.VMEM((3, padded, cols), F32),
            pltpu.VMEM((3, 2, nf, cols), F32),
            dma((6,)),
            dma((3, n8)), dma((3, n8)),
            dma((3, 2, n8)), dma((3, 2, n8)),
            dma((3, 2, n8 // 2)), dma((3, 2, n8 // 2)),
            dma((3, 2)), dma((3, 2)),
            dma((3, 2)), dma((3, 2)),
            dma((3, 2, RING)), dma((3, 2, RING)),
            dma((3, RING)), dma((3, RING)),
            dma((3, RING, RING)), dma((3, RING, RING)),
            dma((3,)), dma((3,)), dma((2,)), dma((2, 2)), dma((2,)), dma((2,)),
            dma((3, 2)), dma((3, 2)),
            dma((3, 2, tiles)), dma((3, 2, tiles)),
            dma((3, tiles, n8)), dma((3, tiles, n8)),
            dma((3, tiles)),
            dma((2,)), dma((2,)),
        ] + [dma((2, 2))] * 12,
        compiler_params=pltpu.CompilerParams(collective_id=0, has_side_effects=True, vmem_limit_bytes=67043328),
        cost_estimate=pl.CostEstimate(flops=18 * nf * tokens * d, bytes_accessed=300_000_000, transcendentals=0),
        name="layer",
    )(sg, su, sd, tok, grad, tok.reshape(halves), grad.reshape(halves))
    return res[:3], res[3].reshape(rows, d), res[4].reshape(rows, d)


def assemble_kernel(og, ou, od, out, gin, g, u, w, res, gres, buf, flat, in_sem, out_sem, row_buf, row_sem):
    n8, nf = og.shape[0], g.shape[1] // og.shape[0]
    srcs, dsts = (og, ou, od), (g, u, w)
    rows_in = [pltpu.make_async_copy(src, row_buf.at[r], row_sem.at[r]) for r, src in enumerate((out, gin))]
    loads = [pltpu.make_async_copy(src, buf.at[t], in_sem.at[t]) for t, src in enumerate(srcs)]
    stores = [pltpu.make_async_copy(flat.at[t], dst, out_sem.at[t]) for t, dst in enumerate(dsts)]
    for c in loads + rows_in:
        c.start()
    for t in range(3):
        loads[t].wait()
        for j in range(n8):
            flat[t, :, j * nf:(j + 1) * nf] = jnp.concatenate([buf[t, j, tile] for tile in range(buf.shape[2])], axis=1)[:, :nf]
        stores[t].start()
    rows_out = [pltpu.make_async_copy(row_buf.at[r], dst, row_sem.at[r]) for r, dst in enumerate((res, gres))]
    for c in rows_in:
        c.wait()
    for c in rows_out:
        c.start()
    for c in stores + rows_out:
        c.wait()


def assemble(sums, out, gin, ff):
    dp = sums[0].shape[2]
    hbm = pl.BlockSpec(memory_space=pl.ANY)
    dma = pltpu.SemaphoreType.DMA
    sds = jax.ShapeDtypeStruct
    return pl.pallas_call(
        assemble_kernel,
        out_shape=[sds((dp, ff), F32)] * 3 + [sds(out.shape, BF16)] * 2,
        in_specs=[hbm] * 5,
        out_specs=[hbm] * 5,
        scratch_shapes=[
            pltpu.VMEM((3,) + sums[0].shape, F32), pltpu.VMEM((3, dp, ff), F32), dma((3,)), dma((3,)),
            pltpu.VMEM((2,) + out.shape, BF16), dma((2,)),
        ],
        compiler_params=pltpu.CompilerParams(vmem_limit_bytes=63 * 1024 * 1024),
        name="assemble",
    )(*sums, out, gin)


def solution(mesh):
    nz, ny, nd = mesh.shape["datb"], mesh.shape["model"], mesh.shape["data"]
    fine = Mesh(mesh.devices.reshape(nz, ny, nd // 2, 2), ("datb", "model", "x", "core"))

    def local_step(tok_loc, wg_loc, wu_loc, wd_loc, grad_loc):
        sums, out, grad_in = layer(wg_loc, wu_loc, wd_loc.T, tok_loc, grad_loc)
        grad_gate, grad_up, grad_down_t, out, grad_in = assemble(sums, out, grad_in, wg_loc.shape[1])
        return out, grad_in, grad_gate, grad_up, grad_down_t.T

    return jax.shard_map(local_step, mesh=fine, in_specs=(ROW_SPEC, GATE_SPEC, GATE_SPEC, DOWN_SPEC, ROW_SPEC), out_specs=(ROW_SPEC, ROW_SPEC, GATE_SPEC, GATE_SPEC, DOWN_SPEC), check_vma=False)
```

```python
import functools

import jax
import jax.numpy as jnp
from jax import lax
from jax.experimental import pallas as pl
from jax.experimental.pallas import tpu as pltpu
from jax.sharding import Mesh
from jax.sharding import PartitionSpec as P

ROW_SPEC = P(("datb", "x", "core", "model"), None)
GATE_SPEC = P(("datb", "x", "core"), "model")
DOWN_SPEC = P("model", ("datb", "x", "core"))
BF16 = jnp.bfloat16
F32 = jnp.float32
MESH_ID = pl.DeviceIdType.MESH
RING = 4
NEAR = ((0, 0), (0, 1), (1, 0), (3, 0), (1, 1), (3, 1), (2, 0), (2, 1))
DELTAS = (0, 3, 1, 2)
LANE = 128
OUT_COLS = 512
EX, Z1, Z2, P1, P2, BL, Q1, Q2, WD, CI = range(10)
GATHER_STEPS = (
    (Z1, 0, 0), (BL, 0, 0), (P1, 0, 0), (P1, 0, 1), (EX, 0, 1), (EX, 0, 2), (EX, 0, 3), (EX, 0, 4), (EX, 0, 5), (P1, 2, 0), (P1, 2, 1),
    (BL, 1, 0), (EX, 0, 6), (EX, 0, 7), (Z1, 3, 0), (EX, 3, 1), (Z1, 1, 0), (EX, 1, 1), (Z1, 2, 0), (EX, 2, 1), (Z1, 0, 1), (Z1, 3, 1),
    (Z1, 1, 1), (Z1, 2, 1), (Z2, 0, 0, 0), (EX, 3, 2), (EX, 3, 3), (Z2, 3, 0, 0), (EX, 3, 4), (EX, 3, 5), (EX, 3, 6), (EX, 3, 7),
    (Z2, 1, 0, 0), (EX, 1, 2), (EX, 1, 3), (Z2, 2, 0, 0), (Q1, 0, 0, 0), (Q1, 0, 0, 1), (P2, 0, 0), (P2, 0, 1), (Z2, 0, 0, 1),
    (Z2, 3, 0, 1), (Z1, 0, 2), (BL, 0, 1), (P2, 2, 1), (Z1, 0, 3), (EX, 1, 4), (EX, 1, 5), (Z1, 0, 4), (EX, 1, 6), (EX, 1, 7),
    (Q1, 1, 0, 1), (Z1, 0, 5), (Z1, 0, 6), (BL, 0, 2), (EX, 2, 2), (EX, 2, 3), (Z2, 0, 1, 0), (Z1, 0, 7), (EX, 2, 4), (EX, 2, 5),
    (Z2, 0, 1, 1), (Z1, 3, 2), (EX, 2, 6), (EX, 2, 7), (Z1, 3, 3), (Z2, 0, 1, 2), (Q1, 0, 1, 1), (Q2, 0, 0), (Z1, 3, 4), (Z1, 3, 5),
    (Z2, 0, 0, 2), (BL, 0, 3), (P1, 1, 0), (P1, 1, 1), (Z2, 0, 1, 3), (Z2, 0, 0, 3), (Z1, 3, 6), (BL, 2, 2), (Z1, 3, 7), (Z1, 1, 2),
    (Q1, 0, 2, 1), (Z1, 1, 3), (Q1, 0, 1, 0), (BL, 2, 0), (Z2, 3, 1, 0), (Z2, 3, 1, 1), (Z1, 1, 4), (Z2, 3, 0, 2), (Z2, 3, 1, 2),
    (Z2, 3, 0, 3), (Z2, 3, 1, 3), (Q1, 0, 2, 0), (Z1, 1, 5), (Q1, 0, 3, 1), (Z1, 1, 6), (P2, 2, 0), (BL, 2, 1), (WD, 0), (P2, 1, 0),
    (P2, 1, 1), (Z1, 1, 7), (Q1, 1, 0, 0), (Z2, 1, 0, 1), (Z2, 1, 1, 0), (Q1, 0, 3, 0), (Q1, 2, 2, 0), (Q1, 2, 2, 1), (Z2, 1, 0, 2),
    (BL, 1, 1), (Q2, 0, 2), (Z2, 1, 0, 3), (Z2, 1, 1, 1), (Q1, 2, 0, 0), (Q1, 2, 0, 1), (Z1, 2, 2), (BL, 1, 2), (WD, 3), (Z2, 1, 1, 2),
    (CI, 0),
)
GATE_STEPS = (
    (),
    (),
    (
        (Z1, 2, 3), (Z2, 1, 1, 3), (Q2, 0, 1),
    ),
    (
        (Z1, 2, 4), (Q1, 2, 1, 0), (Q1, 2, 1, 1), (Q2, 0, 3), (BL, 2, 3), (BL, 1, 3), (Z1, 2, 5), (CI, 1),
    ),
    (
        (Z1, 2, 6),
    ),
    (
        (Q2, 1, 0), (Q2, 2, 0), (Q2, 2, 2), (Q1, 1, 1, 1), (CI, 2),
    ),
    (
        (Z1, 2, 7),
    ),
    (
        (Z2, 2, 0, 1), (CI, 3),
    ),
    (
        (Q2, 2, 1), (Q1, 1, 1, 0), (Q1, 1, 2, 1), (Q1, 2, 3, 1),
    ),
)
UP_STEPS = (
    (
        (WD, 1), (Z2, 2, 0, 2),
    ),
    (
        (Z2, 2, 1, 0), (Z2, 2, 0, 3), (Q1, 1, 2, 0), (Q1, 1, 3, 1), (Q1, 2, 3, 0),
    ),
    (),
    (
        (Z2, 2, 1, 1),
    ),
    (
        (Q2, 2, 3), (Q2, 1, 2), (Z2, 2, 1, 2), (Q1, 1, 3, 0),
    ),
    (),
    (
        (Z2, 2, 1, 3),
    ),
    (
        (Q2, 1, 1), (Q2, 1, 3),
    ),
)
LATE_STEPS = (
    (WD, 2),
)
Z_ORDER = (2, 0, 1)
EARLY_ORDER = (
    ("far_block", 2), ("next_products", 2), ("late",), ("give_rows", 0),
)
LATE_ORDER = (
    ("next_adds", 2), ("own_block", 2), ("keep_rows", 0), ("ring_first", 0, 1), ("finish", 2, 0), ("far_block", 0), ("give_rows", 1),
    ("finish", 2, 3), ("finish", 2, 1), ("finish", 2, 4), ("ring_dependent", 0, 1), ("finish", 2, 2), ("far_block", 1), ("keep_rows", 1),
    ("ring_first", 1, 1), ("next_blocks", 0), ("own_block", 0), ("next_blocks", 1), ("own_block", 1), ("finish", 0, 0),
    ("ring_dependent", 1, 1), ("finish", 0, 1), ("ring_last", 0, 1), ("ring_first", 0, 2), ("finish", 0, 2), ("finish", 0, 3),
    ("finish", 0, 4), ("ring_last", 1, 1), ("ring_first", 1, 2), ("ring_dependent", 0, 2), ("finish", 1, 0), ("ring_dependent", 1, 2),
    ("ring_last", 0, 2), ("finish", 1, 1), ("finish", 1, 2), ("ring_last", 1, 2), ("finish", 1, 3), ("finish", 1, 4),
)


def dot(a, b, ca, cb):
    return lax.dot_general(a, b, (((ca,), (cb,)), ((), ())), preferred_element_type=F32)


def layer_kernel(sg, su, sd, tok, grad, tok_own, grad_own,
                 og, ou, od, out, gin, wg, wu, wd, wr, tok_all, grad_all, h_main, h_rest, ra, rb, give, rc, part, ra1, rb1, sd1, mid, ra2, rb2, sd2,
                 ff, blk, far, nxt,
                 own_sem, ex_s, ex_r, z1_s, z1_r, z2_s, z2_r, p1_s, p1_r, p2_s, p2_r, q1_s, q1_r, q2_s, q2_r, cc_s, cc_r,
                 sh_sem, wv_sem, row_sem, hst_sem, blk_sem, tmp_sem, a_s, a_r, u_s, u_r, e_s, e_r, out_sem,
                 c_s, c_r, a1_s, a1_r, f1_s, f1_r, d1_s, d1_r, a2_s, a2_r, f2_s, f2_r, d2_s, d2_r):
    z, y = lax.axis_index("datb"), lax.axis_index("model")
    x, core = lax.axis_index("x"), lax.axis_index("core")
    i8 = 2 * x + core
    n8 = 2 * RING
    rows, d = tok.shape
    half_rows = rows // 2
    chunk = RING * rows
    n_chunk = n8
    nf, tokens = ff.shape[1:]
    dp = sg.shape[0]
    half = nf // 2
    main = wg.shape[1]
    rest = nf - main
    packed = wr.shape[1]
    cols = blk.shape[2]
    tiles = far.shape[1] // LANE
    outs = (og, ou, od)

    zs, ys, xs = ([v] + [lax.rem(v + k, RING) for k in range(1, RING)] for v in (z, y, x))
    cores = (core, 1 - core)
    peers = [[2 * v + c for c in cores] for v in xs]
    slot_at = [[[pl.multiple_of((zz * n8 + peers[dx][dc]) * dp, 16) for dc in range(2)] for dx in range(RING)] for zz in zs]
    hand_at = [[pl.multiple_of(p * dp, 8) for p in row] for row in peers]
    rows_at = [[[pl.multiple_of((peers[dx][dc] * RING + yy) * rows, half_rows) for dc in range(2)] for yy in ys] for dx in range(RING)]
    lanes_at = [pl.multiple_of(zz * cols, LANE) for zz in zs]

    def peer(dx, dc):
        return peers[dx][dc]

    def zdev(k):
        return {"datb": zs[k]}

    def xdev(k):
        return {"x": xs[k]}

    def ydev(k):
        return {"model": ys[k]}

    def near(dx, dc):
        return {"x": xs[dx], "core": cores[dc]}

    def copy(src, dst, s, r, dev):
        return pltpu.make_async_remote_copy(src_ref=src, dst_ref=dst, send_sem=s, recv_sem=r, device_id=dev, device_id_type=MESH_ID)

    rcopy = copy

    def start(copies):
        for c in copies:
            c.start()

    def received(copies):
        for c in copies:
            c.wait_recv()

    def sent(copies):
        for c in copies:
            c.wait_send()

    def run_order(fns, order):
        for fn, *args in order:
            with jax.named_scope("_".join(str(v) for v in [fn, *args])):
                fns[fn](*args)

    barrier = pltpu.get_barrier_semaphore()
    others = [zdev(1), zdev(3), ydev(1), ydev(3)] + [near(*n) for n in NEAR[1:]]
    for dev in others:
        pl.semaphore_signal(barrier, inc=1, device_id=dev, device_id_type=MESH_ID)

    def blk_load(t, slot, k):
        src = tok_all if t < 2 else grad_all
        return pltpu.make_async_copy(src.at[:, pl.ds(lanes_at[k], cols)], blk.at[slot], blk_sem.at[slot])

    plan = []
    for fn, *args in EARLY_ORDER + LATE_ORDER:
        plan += [(args[0], k) for k in {"far_block": (2,), "next_blocks": (1, 3), "next_products": (1, 3), "own_block": (0,)}.get(fn, ())]
    taken = []

    def next_block():
        n = len(taken)
        taken.append(n)
        blk_load(plan[n][0], n % 2, plan[n][1]).wait()
        if n + 1 < len(plan):
            blk_load(plan[n + 1][0], (n + 1) % 2, plan[n + 1][1]).start()
        return n % 2

    def product(t, dst):
        slot = next_block()
        step = 2 * LANE

        def one(n, carry):
            lanes = pl.ds(pl.multiple_of(jnp.minimum(n * step, cols - step), LANE), step)
            dst[:nf, lanes] = jnp.dot(ff[t], blk[slot, :, lanes], preferred_element_type=F32)
            return carry

        lax.fori_loop(0, -(-cols // step), one, 0)

    lo, hi = pl.ds(0, half), pl.ds(half, half)

    def a_copies(t):
        return [rcopy(far.at[t, rows], ra.at[t, rows], a_s.at[t, s], a_r.at[t, s], zdev(k)) for s, rows, k in ((0, lo, 1), (1, hi, 3))]

    def tile_rows(tile):
        return pl.ds(tile * LANE, min(LANE, nf - tile * LANE))

    def unit_copies(t, tile):
        at = tile_rows(tile)
        return [rcopy(nxt.at[t, s, at], rb.at[t, s, at], u_s.at[t, s, tile], u_r.at[t, s, tile], zdev(1 + 2 * s)) for s in range(2)]

    def far_block(t):
        product(t, far.at[t])
        start(a_copies(t))

    def early_units(t):
        if ("next_products", t) not in EARLY_ORDER + LATE_ORDER:
            return ()
        free = [(0, tile) for tile in range(tiles) if tile * LANE >= half]
        return free + [(1, tile) for tile in range(tiles) if (tile + 1) * LANE <= half]

    def next_products(t):
        for s in range(2):
            product(t, nxt.at[t, s])
        for s, tile in early_units(t):
            unit_copies(t, tile)[s].start()

    blocks = d // min(OUT_COLS, d)
    width = d // blocks

    def row_products(r, keep):
        side = core if keep else 1 - core
        specs, args = [], []
        for h, j, w in ((h_main, 2, wd), (h_rest, 0, wr)) if r == 0 else ((h_main, 0, wg), (h_main, 1, wu), (h_rest, 1, wr)):
            n = w.shape[1]
            specs += [pl.BlockSpec((1, RING, 1, RING * rows, n), lambda i, j=j: (j, 0, side, 0, 0)), pl.BlockSpec((width, n), lambda i: (i, 0))]
            args += [h, w]
        wide = pl.BlockSpec((RING, RING, rows, width), lambda i: (0, 0, 0, i))
        terms = len(args) // 2
        if keep:
            specs.append(wide)
            args.append(rc.at[r])

        def body(*refs):
            total = None
            for i in range(terms):
                h = refs[2 * i][...].reshape(RING * RING * rows, refs[2 * i].shape[-1])
                prod = dot(h, refs[2 * i + 1][...], 1, 1)
                total = prod if total is None else total + prod
            if keep:
                total = total + refs[-2][...].astype(F32).reshape(total.shape)
            refs[-1][...] = total.astype(BF16).reshape(RING, RING, rows, width)

        pltpu.emit_pipeline(body, grid=(blocks,), in_specs=specs, out_specs=[wide])(*args, (part if keep else give).at[r])

    def core_copy(r):
        return rcopy(give.at[r], rc.at[r], c_s.at[r], c_r.at[r], near(0, 1))

    def give_rows(r):
        row_products(r, False)
        core_copy(r).start()

    def forward_phase(rowbuf, av, bv, hst, hst_rest, wv_a, wv_r):
        held = {}

        fulls = (wg, wu, wd, wr)
        REST = 3
        def shard_load(t):
            return pltpu.make_async_copy((sg, su, sd)[t], held["shard"].at[t], sh_sem.at[t])

        def cut_pieces(t):
            if t == REST:
                for u in range(3):
                    for j in range(n8):
                        held["rests"][j, :, u * rest:(u + 1) * rest] = held["shard"][u, :, j * nf + main:(j + 1) * nf]
            else:
                for j in range(n8):
                    held["pieces"][t, j] = held["shard"][t, :, j * nf:j * nf + main]
            own_piece(t).start()

        def piece(t, j):
            return held["rests"].at[j] if t == REST else held["pieces"].at[t, j]

        def own_piece(t):
            return pltpu.make_async_copy(piece(t, i8), slot(t, 0, NEAR[0]), own_sem.at[t])

        started = []

        def go(make, *args):
            make(*args).start()
            started.append((make, args))

        def slot(t, k, source):
            dx, dc = source
            return fulls[t].at[pl.ds(slot_at[k][dx][dc], dp)]

        def source(k):
            dx, dc = NEAR[k]
            return (RING - dx) % RING, dc

        def back(side):
            return 3 if side == 0 else 1

        def ahead(side):
            return 1 if side == 0 else 3

        def exchange_copy(t, k):
            return copy(piece(t, peer(*NEAR[k])), slot(t, 0, NEAR[0]), ex_s.at[t, k], ex_r.at[t, k], near(*NEAR[k]))

        def exchange(t, k):
            go(exchange_copy, t, k)

        def z_first_copy(t, side, k):
            here = slot(t, 0, source(k))
            return copy(here if k else piece(t, i8), here, z1_s.at[t, side, k], z1_r.at[t, side, k], zdev(ahead(side)))

        def z_first(t, k):
            if k:
                here = slot(t, 0, source(k))
                copy(here, here, ex_s.at[t, k], ex_r.at[t, k], {"datb": z}).wait_recv()
            for side in range(2):
                go(z_first_copy, t, side, k)

        def wait_z_first(t, side, k):
            there = slot(t, back(side), source(k))
            copy(there, there, z1_s.at[t, side, k], z1_r.at[t, side, k], {"datb": z}).wait_recv()

        def z_second_copy(t, side, k):
            there = slot(t, back(side), source(k + side * (n8 // 2)))
            return copy(there, there, z2_s.at[t, side, k], z2_r.at[t, side, k], zdev(ahead(side)))

        def z_second(t, side, k):
            wait_z_first(t, side, k + side * (n8 // 2))
            go(z_second_copy, t, side, k)

        def weights_done(t):
            if (WD, t) not in LATE_STEPS:
                own_wait(t)
            for k in range(n8 // 2):
                wait_z_first(t, 0, n8 // 2 + k)
                wait_z_first(t, 1, k)
                for side in range(2):
                    there = slot(t, 2, source(k + side * (n8 // 2)))
                    copy(there, there, z2_s.at[t, side, k], z2_r.at[t, side, k], {"datb": z}).wait_recv()
            w_load(t).start()

        cut = d // 2
        rings = ((tok, tok_all, pl.ds(0, d), True), (grad, grad_all, pl.ds(0, cut), True), (grad, grad_all, pl.ds(cut, d - cut), False))

        def axis(r, n):
            return xdev if rings[r][3] == (n == 1) else ydev

        def block(r, da, db, flip=0, lo=0, size=rows):
            dx, dy = (da, db) if rings[r][3] else (db, da)
            first = rows_at[dx][dy][flip]
            return rings[r][1].at[pl.ds(pl.multiple_of(first + lo, half_rows) if lo else first, size), rings[r][2]]

        def own_block(r):
            return rings[r][0].at[:, rings[r][2]]

        def to_core_copy(r, ia, ib):
            there = block(r, DELTAS[ia], DELTAS[ib])
            return copy(own_block(r) if ia == 0 and ib == 0 else there, there, cc_s.at[r, ia, ib], cc_r.at[r, ia, ib], near(0, 1))

        def to_core(r, ia, ib):
            go(to_core_copy, r, ia, ib)

        def first_copy(r, side):
            return copy(own_block(r), block(r, 0, 0), p1_s.at[r, side], p1_r.at[r, side], axis(r, 1)(ahead(side)))

        def first_own(r, side):
            go(first_copy, r, side)

        def first_far_copy(r, side):
            part = block(r, back(side), 0, 0, side * half_rows, half_rows)
            return copy(part, part, p2_s.at[r, side], p2_r.at[r, side], axis(r, 1)(ahead(side)))

        def first_forward(r, side):
            there = block(r, back(side), 0)
            copy(there, there, p1_s.at[r, side], p1_r.at[r, side], {"datb": z}).wait_recv()
            go(first_far_copy, r, side)

        def block_on(r, ia):
            for side in range(2 if ia == 3 else 0):
                part = block(r, 2, 0, 0, side * half_rows, half_rows)
                copy(part, part, p2_s.at[r, side], p2_r.at[r, side], {"datb": z}).wait_recv()
            for side in range(2):
                go(second_copy, r, side, ia)
            to_core(r, ia, 0)

        def second_copy(r, side, ia):
            there = block(r, DELTAS[ia], 0)
            return copy(there if ia else own_block(r), there, q1_s.at[r, side, ia], q1_r.at[r, side, ia], axis(r, 2)(ahead(side)))

        def second_far_copy(r, ia):
            side = ia // 2
            there = block(r, DELTAS[ia], back(side))
            return copy(there, there, q2_s.at[r, ia], q2_r.at[r, ia], axis(r, 2)(ahead(side)))

        def second_forward(r, ia, side):
            there = block(r, DELTAS[ia], back(side))
            copy(there, there, q1_s.at[r, side, ia], q1_r.at[r, side, ia], {"datb": z}).wait_recv()
            if ia // 2 == side:
                go(second_far_copy, r, ia)
            to_core(r, ia, 1 if side == 0 else 2)

        def second_far(r, ia):
            there = block(r, DELTAS[ia], 2)
            copy(there, there, q2_s.at[r, ia], q2_r.at[r, ia], {"datb": z}).wait_recv()
            to_core(r, ia, 3)

        def chunk_in(ia):
            rows_in(0, (ia,))

        def rows_in(r, blocks=range(RING)):
            for ia in blocks:
                for ib in range(RING):
                    there = block(r, DELTAS[ia], DELTAS[ib], 1)
                    copy(there, there, cc_s.at[r, ia, ib], cc_r.at[r, ia, ib], {"datb": z}).wait_recv()

        def own_wait(t):
            there = slot(t, 0, NEAR[0])
            pltpu.make_async_copy(there, there, own_sem.at[t]).wait()

        def own_rows(r):
            return pltpu.make_async_copy(own_block(r), block(r, 0, 0), own_sem.at[4 + r])

        def w_load(t):
            return pltpu.make_async_copy(fulls[t], (wv_a, held["wv_b"], wv_a, wv_r)[t], wv_sem.at[t])

        def row_load(src, i, buf):
            return pltpu.make_async_copy(src.at[chunk_rows(i)], rowbuf.at[buf], row_sem.at[buf])

        def chunk_loop(src, work, between):
            row_load(src, 0, 0).start()

            def outer(xx, carry):
                def inner(c, carry):
                    i = 2 * xx + c

                    @pl.when(i + 1 < n_chunk)
                    def _():
                        row_load(src, i + 1, 1 - c).start()

                    for k, step in enumerate(between):
                        pl.when(i == k)(step)
                    row_load(src, i, c).wait()
                    work(i, xx, c)
                    return carry

                return lax.fori_loop(0, 2, inner, carry)

            lax.fori_loop(0, RING, outer, 0)

        def chunk_rows(i):
            return pl.ds(pl.multiple_of(i * chunk, chunk), chunk)

        def main_copy(xx, c, place, j):
            return pltpu.make_async_copy(hst.at[c, place], h_main.at[j, xx, c], hst_sem.at[c, place])

        def rest_copy(xx, c, j):
            return pltpu.make_async_copy(hst_rest.at[j, c], h_rest.at[j, xx, c], hst_sem.at[c, 2])

        def keep(i, xx, c, which, values):
            copies = lambda at: [main_copy(at, c, n, j) for n, (j, _) in enumerate(values)] + [rest_copy(at, c, which)]

            @pl.when(xx >= 1)
            def _():
                for cp in copies(xx - 1):
                    cp.wait()

            for n, (j, v) in enumerate(values):
                low = v.astype(BF16)
                hst[c, n] = low[:, :main]
                hst_rest[which, c, :, j * rest:(j + 1) * rest] = low[:, main:]
                ff[j, :, chunk_rows(i)] = v.T.astype(BF16)
            start(copies(xx))

        def kept(which, names):
            for c in range(2):
                for cp in [main_copy(RING - 1, c, n, j) for n, j in enumerate(names)] + [rest_copy(RING - 1, c, which)]:
                    cp.wait()

        def gate_work():
            def place(k):
                ia, flip = lax.div(k, 2), lax.rem(k, 2)
                delta = lax.rem(3 * ia + 3 * lax.div(ia, 2) + 2 * lax.div(ia, 3), RING)
                return 2 * lax.rem(x + delta, RING) + lax.rem(core + flip, 2)

            def body(k, carry):
                for n, group in enumerate(GATE_STEPS):
                    if group:
                        pl.when(k == n)(functools.partial(run, group))

                @pl.when(k < n_chunk)
                def _():
                    row_load(tok_all, place(k), lax.rem(k, 2)).start()

                @pl.when(k >= 1)
                def _():
                    i, buf = place(k - 1), lax.rem(k - 1, 2)
                    row_load(tok_all, i, buf).wait()
                    rb_ = rowbuf[buf]
                    av[chunk_rows(i), :main] = jnp.dot(rb_, wv_a[...], preferred_element_type=F32).astype(BF16)
                    both = jnp.dot(rb_, wv_r[...], preferred_element_type=F32).astype(BF16)
                    av[chunk_rows(i), main:] = both[:, :rest]
                    bv[chunk_rows(i), main:] = both[:, rest:2 * rest]

                return carry

            lax.fori_loop(0, n_chunk + 1, body, 0)

        def up_work(i, xx, c):
            bv[chunk_rows(i), :main] = jnp.dot(rowbuf[c], held["wv_b"][...], preferred_element_type=F32).astype(BF16)
            a, b = av[chunk_rows(i)].astype(F32), bv[chunk_rows(i)].astype(F32)
            keep(i, xx, c, 0, ((2, a * jax.nn.sigmoid(a) * b),))

        def post_work(i, xx, c):
            rb_ = rowbuf[c]
            lanes = 2 * rest // LANE * LANE
            low = jnp.dot(rb_, wv_r[:, lanes:], preferred_element_type=F32)[:, 2 * rest - lanes:3 * rest - lanes]
            g = jnp.concatenate([jnp.dot(rb_, wv_a[...], preferred_element_type=F32), low], axis=1).astype(BF16).astype(F32)
            a, b = av[chunk_rows(i)].astype(F32), bv[chunk_rows(i)].astype(F32)
            sig = jax.nn.sigmoid(a)
            keep(i, xx, c, 1, ((0, g * b * sig * (1.0 + a * (1.0 - sig))), (1, g * (a * sig))))

        steps = (exchange, z_first, z_second, first_own, first_forward, block_on, second_forward, second_far, weights_done, chunk_in)

        def run(group):
            for which, *args in group:
                steps[which](*args)

        def rows_ready():
            run(UP_STEPS[-1])
            for r in (1, 2):
                own_rows(r).wait()
                rows_in(r)
            blk_load(plan[0][0], 0, plan[0][1]).start()

        def gather_phase(shard, pieces, rests, wv_b):
            held.update(shard=shard, pieces=pieces, rests=rests, wv_b=wv_b)
            with jax.named_scope("begin"):
                for t in range(3):
                    shard_load(t).start()
                shard_load(0).wait()
                cut_pieces(0)
                pl.semaphore_wait(barrier, len(others))
                for r in range(3):
                    own_rows(r).start()
            with jax.named_scope("gather"):
                cut = {0}
                for step in GATHER_STEPS:
                    if step[0] in (EX, Z1) and step[1] not in cut:
                        if len(cut) == 1:
                            rests[...] = jnp.zeros_like(rests)
                            hst_rest[...] = jnp.zeros_like(hst_rest)
                            shard_load(1).wait()
                            shard_load(2).wait()
                        cut.add(step[1])
                        cut_pieces(step[1])
                    run((step,))
                own_rows(0).wait()
                w_load(0).wait()
                w_load(REST).wait()
            with jax.named_scope("gate"):
                gate_work()
            with jax.named_scope("up"):
                run(UP_STEPS[0])
                w_load(1).wait()
                chunk_loop(tok_all, up_work, [functools.partial(run, group) for group in ((),) + UP_STEPS[1:-1]] + [rows_ready])
                kept(0, (2,))
            for _, t in LATE_STEPS:
                own_wait(t)
            for make, args in started:
                if make is exchange_copy or make is z_first_copy and args[2] == 0:
                    make(*args).wait_send()

        pl.run_scoped(
            gather_phase, pltpu.VMEM((3,) + sg.shape, BF16), pltpu.VMEM((3, n8, dp, main), BF16), pltpu.VMEM((n8, dp, packed), BF16),
            pltpu.VMEM((d, main), BF16))
        run_order({
            "far_block": far_block, "next_products": next_products, "give_rows": give_rows, "late": functools.partial(run, LATE_STEPS),
        }, EARLY_ORDER)
        with jax.named_scope("down"):
            w_load(2).wait()
            chunk_loop(grad_all, post_work, ())
            kept(1, (0, 1))
        for make, args in started:
            if not (make is exchange_copy or make is z_first_copy and args[2] == 0):
                make(*args).wait_send()

    def backward_phase(tmp, stage):
        def next_adds(t):
            received(a_copies(t))
            cs = [pltpu.make_async_copy(ra.at[t, at], tmp.at[s, at], tmp_sem.at[s]) for s, at in ((0, lo), (1, hi))]
            start(cs)
            for c, (s, at) in zip(cs, ((0, lo), (1, hi))):
                c.wait()
                nxt[t, s, at] += tmp[s, at]
            for tile in range(tiles):
                start(c for s, c in enumerate(unit_copies(t, tile)) if (s, tile) not in early_units(t))

        def next_blocks(t):
            next_products(t)
            next_adds(t)

        def own_block(t):
            sent(a_copies(t))
            product(t, far.at[t])

        def slot(t):
            return Z_ORDER.index(t) % 2

        def hand_out(t, tile):
            cs = []
            for k in range(1, n8):
                at = pl.ds(hand_at[NEAR[k][0]][NEAR[k][1]], dp)
                cs.append(rcopy(stage.at[slot(t), tile, at], outs[t].at[i8, tile], e_s.at[t, tile, k], e_r.at[t, tile, k], near(*NEAR[k])))
            at = pl.ds(hand_at[0][0], dp)
            return cs, pltpu.make_async_copy(stage.at[slot(t), tile, at], outs[t].at[i8, tile], out_sem.at[t, tile])

        def handed(t, tile):
            cs, mine = hand_out(t, tile)
            sent(cs)
            mine.wait()

        def finish(t, tile):
            received(unit_copies(t, tile))
            at = tile_rows(tile)
            cs = [pltpu.make_async_copy(rb.at[t, s, at], tmp.at[s, at], tmp_sem.at[s]) for s in range(2)]
            start(cs)
            if t == Z_ORDER[2]:
                handed(Z_ORDER[0], tile)
            for c in cs:
                c.wait()
            wide = pl.ds(tile * LANE, LANE)
            stage[slot(t), tile] = (far[t, wide] + tmp[0, wide] + tmp[1, wide]).T
            cs, mine = hand_out(t, tile)
            start(cs + [mine])

        def on_y(r, n):
            return (r == 1) == (n == 1)

        def level(r, n):
            at = ys if on_y(r, n) else xs
            dev = ydev if on_y(r, n) else xdev
            if n == 1:
                def piece(k, h):
                    return part.at[r, pl.ds(2 * h, 2), at[k]] if on_y(r, n) else part.at[r, at[k], pl.ds(2 * h, 2)]
                return dev, piece, ra1, rb1, sd1, (a1_s, a1_r, f1_s, f1_r, d1_s, d1_r)

            def piece(k, h):
                return mid.at[r, at[k], pl.ds(h, 1)]
            return dev, piece, ra2, rb2, sd2, (a2_s, a2_r, f2_s, f2_r, d2_s, d2_r)

        def ring_a(r, n):
            dev, piece, rfar, _, _, sems = level(r, n)
            return [rcopy(piece(2, s), rfar.at[r, s], sems[0].at[r, s], sems[1].at[r, s], dev(1 + 2 * s)) for s in range(2)]

        def ring_f(r, n):
            dev, piece, _, rnear, _, sems = level(r, n)
            return [rcopy(piece(1 + 2 * s, 1 - s), rnear.at[r, s, 1 - s], sems[2].at[r, s], sems[3].at[r, s], dev(1 + 2 * s)) for s in range(2)]

        def ring_d(r, n):
            dev, _, _, rnear, dep, sems = level(r, n)
            return [rcopy(dep.at[r, s], rnear.at[r, s, s], sems[4].at[r, s], sems[5].at[r, s], dev(1 + 2 * s)) for s in range(2)]

        def add(grid, *terms):
            specs = []
            for ref, at, lead in terms:
                tail = ref.shape[lead:]
                specs.append(pl.BlockSpec((1,) * lead + tuple(tail), lambda *i, at=at, rank=len(tail): tuple(at(*i)) + (0,) * rank))

            def body(*refs):
                total = refs[0][...].astype(F32).reshape(refs[0].shape[-2:])
                for ref in refs[1:-1]:
                    total = total + ref[...].astype(F32).reshape(total.shape)
                refs[-1][...] = total.astype(BF16).reshape(refs[-1].shape)

            pltpu.emit_pipeline(body, grid=grid, in_specs=specs[:-1], out_specs=specs[-1:])(*[ref for ref, _, _ in terms])

        def ring_first(r, n):
            start(ring_a(r, n) + ring_f(r, n))

        def ring_dependent(r, n):
            received(ring_a(r, n))
            here = y if on_y(r, n) else x
            if n == 1:
                def near_block(s, i):
                    at = lax.rem(here + 1 + 2 * s, RING)
                    return (2 * s + i, at) if on_y(r, n) else (at, 2 * s + i)

                add((2, 2), (part.at[r], near_block, 2), (ra1.at[r], lambda s, i: (s, i), 2), (sd1.at[r], lambda s, i: (s, i), 2))
            else:
                add((2,), (mid.at[r], lambda s: (lax.rem(here + 1 + 2 * s, RING), s), 2), (ra2.at[r], lambda s: (s, 0), 2),
                    (sd2.at[r], lambda s: (s, 0), 2))
            start(ring_d(r, n))

        def ring_last(r, n):
            received(ring_f(r, n) + ring_d(r, n))
            here = y if on_y(r, n) else x
            if n == 1:
                def own_at(h, i):
                    return (2 * h + i, here) if on_y(r, n) else (here, 2 * h + i)

                add((2, 2), (part.at[r], own_at, 2), (rb1.at[r, 0], lambda h, i: (h, i), 2),
                    (rb1.at[r, 1], lambda h, i: (h, i), 2), (mid.at[r], lambda h, i: (2 * h + i,), 1))
            else:
                own, res = ((tok_own, out), (grad_own, gin))[r]
                add((2,), (own, lambda h: (h,), 1), (mid.at[r], lambda h: (here, h), 2), (rb2.at[r, 0], lambda h: (h, 0), 2),
                    (rb2.at[r, 1], lambda h: (h, 0), 2), (res, lambda h: (h,), 1))

        def keep_rows(r):
            core_copy(r).wait_recv()
            row_products(r, True)

        run_order({
            "far_block": far_block, "next_products": next_products, "next_adds": next_adds, "next_blocks": next_blocks,
            "own_block": own_block, "finish": finish, "give_rows": give_rows, "keep_rows": keep_rows, "ring_first": ring_first,
            "ring_dependent": ring_dependent, "ring_last": ring_last,
        }, LATE_ORDER)

        with jax.named_scope("units_sent"):
            for t in range(3):
                for tile in range(tiles):
                    sent(unit_copies(t, tile))
        for t in Z_ORDER:
            for tile in range(tiles):
                with jax.named_scope(f"handed_{t}_{tile}"):
                    received(hand_out(t, tile)[0])
                    if t != Z_ORDER[0]:
                        handed(t, tile)
        for r in range(2):
            core_copy(r).wait_send()
            for n in (1, 2):
                sent(ring_a(r, n) + ring_f(r, n) + ring_d(r, n))

    pl.run_scoped(
        forward_phase,
        pltpu.VMEM((2, chunk, d), BF16),
        pltpu.VMEM((tokens, nf), BF16),
        pltpu.VMEM((tokens, nf), BF16),
        pltpu.VMEM((2, 2, chunk, main), BF16),
        pltpu.VMEM((2, 2, chunk, packed), BF16),
        pltpu.VMEM((d, main), BF16),
        pltpu.VMEM((d, packed), BF16),
    )
    pl.run_scoped(backward_phase, pltpu.VMEM((2, tiles * LANE, cols), F32), pltpu.VMEM((2, tiles, cols, LANE), F32))


def layer(sg, su, sd, tok, grad):
    n8 = 2 * RING
    dp, nf = sg.shape[0], sg.shape[1] // n8
    rows, d = tok.shape
    tokens = rows * RING * n8
    cols = d // RING
    tiles = -(-nf // LANE)
    padded = tiles * LANE
    main = nf // LANE * LANE
    packed = -(-3 * (nf - main) // LANE) * LANE
    hbm = pl.BlockSpec(memory_space=pl.ANY)
    dma = pltpu.SemaphoreType.DMA
    sds = jax.ShapeDtypeStruct
    halves = (2, rows // 2, d)
    res = pl.pallas_call(
        layer_kernel,
        out_shape=[sds((n8, tiles, dp, LANE), F32)] * 3 + [sds(halves, BF16)] * 2 + [
            sds((d, main), BF16), sds((d, main), BF16), sds((d, main), BF16), sds((d, packed), BF16), sds((tokens, d), BF16), sds((tokens, d), BF16),
            sds((3, RING, 2, RING * rows, main), BF16), sds((2, RING, 2, RING * rows, packed), BF16),
            sds((3, nf, cols), F32), sds((3, 2, nf, cols), F32),
            sds((2, RING, RING, rows, d), BF16), sds((2, RING, RING, rows, d), BF16), sds((2, RING, RING, rows, d), BF16),
            sds((2, 2, 2, rows, d), BF16), sds((2, 2, 2, 2, rows, d), BF16), sds((2, 2, 2, rows, d), BF16),
            sds((2, RING, 2, rows // 2, d), BF16),
            sds((2, 2, 1, rows // 2, d), BF16), sds((2, 2, 2, 1, rows // 2, d), BF16), sds((2, 2, 1, rows // 2, d), BF16),
        ],
        in_specs=[hbm] * 7,
        out_specs=[hbm] * 25,
        scratch_shapes=[
            pltpu.VMEM((3, nf, tokens), BF16),
            pltpu.VMEM((2, tokens, cols), BF16),
            pltpu.VMEM((3, padded, cols), F32),
            pltpu.VMEM((3, 2, nf, cols), F32),
            dma((7,)),
            dma((4, n8)), dma((4, n8)),
            dma((4, 2, n8)), dma((4, 2, n8)),
            dma((4, 2, n8 // 2)), dma((4, 2, n8 // 2)),
            dma((3, 2)), dma((3, 2)),
            dma((3, 2)), dma((3, 2)),
            dma((3, 2, RING)), dma((3, 2, RING)),
            dma((3, RING)), dma((3, RING)),
            dma((3, RING, RING)), dma((3, RING, RING)),
            dma((3,)), dma((4,)), dma((2,)), dma((2, 3)), dma((2,)), dma((2,)),
            dma((3, 2)), dma((3, 2)),
            dma((3, 2, tiles)), dma((3, 2, tiles)),
            dma((3, tiles, n8)), dma((3, tiles, n8)),
            dma((3, tiles)),
            dma((2,)), dma((2,)),
        ] + [dma((2, 2))] * 12,
        compiler_params=pltpu.CompilerParams(collective_id=0, has_side_effects=True, vmem_limit_bytes=67043328),
        cost_estimate=pl.CostEstimate(flops=18 * nf * tokens * d, bytes_accessed=300_000_000, transcendentals=0),
        name="layer",
    )(sg, su, sd, tok, grad, tok.reshape(halves), grad.reshape(halves))
    return res[:3], res[3].reshape(rows, d), res[4].reshape(rows, d)


def assemble_kernel(og, ou, od, out, gin, g, u, w, res, gres, buf, flat, in_sem, out_sem, row_buf, row_sem):
    n8, nf = og.shape[0], g.shape[1] // og.shape[0]
    srcs, dsts = (og, ou, od), (g, u, w)
    rows_in = [pltpu.make_async_copy(src, row_buf.at[r], row_sem.at[r]) for r, src in enumerate((out, gin))]
    loads = [pltpu.make_async_copy(src, buf.at[t], in_sem.at[t]) for t, src in enumerate(srcs)]
    stores = [pltpu.make_async_copy(flat.at[t], dst, out_sem.at[t]) for t, dst in enumerate(dsts)]
    for c in loads + rows_in:
        c.start()
    for t in range(3):
        loads[t].wait()
        for j in range(n8):
            flat[t, :, j * nf:(j + 1) * nf] = jnp.concatenate([buf[t, j, tile] for tile in range(buf.shape[2])], axis=1)[:, :nf]
        stores[t].start()
    rows_out = [pltpu.make_async_copy(row_buf.at[r], dst, row_sem.at[r]) for r, dst in enumerate((res, gres))]
    for c in rows_in:
        c.wait()
    for c in rows_out:
        c.start()
    for c in stores + rows_out:
        c.wait()


def assemble(sums, out, gin, ff):
    dp = sums[0].shape[2]
    hbm = pl.BlockSpec(memory_space=pl.ANY)
    dma = pltpu.SemaphoreType.DMA
    sds = jax.ShapeDtypeStruct
    return pl.pallas_call(
        assemble_kernel,
        out_shape=[sds((dp, ff), F32)] * 3 + [sds(out.shape, BF16)] * 2,
        in_specs=[hbm] * 5,
        out_specs=[hbm] * 5,
        scratch_shapes=[
            pltpu.VMEM((3,) + sums[0].shape, F32), pltpu.VMEM((3, dp, ff), F32), dma((3,)), dma((3,)),
            pltpu.VMEM((2,) + out.shape, BF16), dma((2,)),
        ],
        compiler_params=pltpu.CompilerParams(vmem_limit_bytes=63 * 1024 * 1024),
        name="assemble",
    )(*sums, out, gin)


def solution(mesh):
    nz, ny, nd = mesh.shape["datb"], mesh.shape["model"], mesh.shape["data"]
    fine = Mesh(mesh.devices.reshape(nz, ny, nd // 2, 2), ("datb", "model", "x", "core"))

    def local_step(tok_loc, wg_loc, wu_loc, wd_loc, grad_loc):
        sums, out, grad_in = layer(wg_loc, wu_loc, wd_loc.T, tok_loc, grad_loc)
        grad_gate, grad_up, grad_down_t, out, grad_in = assemble(sums, out, grad_in, wg_loc.shape[1])
        return out, grad_in, grad_gate, grad_up, grad_down_t.T

    return jax.shard_map(local_step, mesh=fine, in_specs=(ROW_SPEC, GATE_SPEC, GATE_SPEC, DOWN_SPEC, ROW_SPEC), out_specs=(ROW_SPEC, ROW_SPEC, GATE_SPEC, GATE_SPEC, DOWN_SPEC), check_vma=False)
```

```python
import functools

import jax
import jax.numpy as jnp
from jax import lax
from jax.experimental import pallas as pl
from jax.experimental.pallas import tpu as pltpu
from jax.sharding import Mesh
from jax.sharding import PartitionSpec as P

ROW_SPEC = P(("datb", "x", "core", "model"), None)
GATE_SPEC = P(("datb", "x", "core"), "model")
DOWN_SPEC = P("model", ("datb", "x", "core"))
BF16 = jnp.bfloat16
F32 = jnp.float32
MESH_ID = pl.DeviceIdType.MESH
RING = 4
NEAR = ((0, 0), (0, 1), (1, 0), (3, 0), (1, 1), (3, 1), (2, 0), (2, 1))
DELTAS = (0, 3, 1, 2)
LANE = 128
OUT_COLS = 512
EX, Z1, Z2, P1, P2, BL, Q1, Q2, WD, CI = range(10)
GATHER_STEPS = (
    (Z1, 0, 0), (BL, 0, 0), (P1, 0, 0), (P1, 0, 1), (EX, 0, 1), (EX, 0, 2), (EX, 0, 3), (EX, 0, 4), (EX, 0, 5), (P1, 2, 0), (P1, 2, 1),
    (BL, 1, 0), (EX, 0, 6), (EX, 0, 7), (Z1, 3, 0), (EX, 3, 1), (Z1, 1, 0), (EX, 1, 1), (Z1, 2, 0), (EX, 2, 1), (Z1, 0, 1), (Z1, 3, 1),
    (Z1, 1, 1), (Z1, 2, 1), (Z2, 0, 0, 0), (EX, 3, 2), (EX, 3, 3), (Z2, 3, 0, 0), (EX, 3, 4), (EX, 3, 5), (EX, 3, 6), (EX, 3, 7),
    (Z2, 1, 0, 0), (EX, 1, 2), (EX, 1, 3), (Z2, 2, 0, 0), (Q1, 0, 0, 0), (Q1, 0, 0, 1), (P2, 0, 0), (P2, 0, 1), (Z2, 0, 0, 1),
    (Z2, 3, 0, 1), (Z1, 0, 2), (BL, 0, 1), (P2, 2, 1), (Z1, 0, 3), (EX, 1, 4), (EX, 1, 5), (Z1, 0, 4), (EX, 1, 6), (EX, 1, 7),
    (Q1, 1, 0, 1), (Z1, 0, 5), (Z1, 0, 6), (BL, 0, 2), (EX, 2, 2), (EX, 2, 3), (Z2, 0, 1, 0), (Z1, 0, 7), (EX, 2, 4), (EX, 2, 5),
    (Z2, 0, 1, 1), (Z1, 3, 2), (EX, 2, 6), (EX, 2, 7), (Z1, 3, 3), (Z2, 0, 1, 2), (Q1, 0, 1, 1), (Q2, 0, 0), (Z1, 3, 4), (Z1, 3, 5),
    (Z2, 0, 0, 2), (BL, 0, 3), (P1, 1, 0), (P1, 1, 1), (Z2, 0, 1, 3), (Z2, 0, 0, 3), (Z1, 3, 6), (BL, 2, 2), (Z1, 3, 7), (Z1, 1, 2),
    (Q1, 0, 2, 1), (Z1, 1, 3), (Q1, 0, 1, 0), (BL, 2, 0), (Z2, 3, 1, 0), (Z2, 3, 1, 1), (Z1, 1, 4), (Z2, 3, 0, 2), (Z2, 3, 1, 2),
    (Z2, 3, 0, 3), (Z2, 3, 1, 3), (Q1, 0, 2, 0), (Z1, 1, 5), (Q1, 0, 3, 1), (Z1, 1, 6), (P2, 2, 0), (BL, 2, 1), (WD, 0), (P2, 1, 0),
    (P2, 1, 1), (Z1, 1, 7), (Q1, 1, 0, 0), (Z2, 1, 0, 1), (Z2, 1, 1, 0), (Q1, 0, 3, 0), (Q1, 2, 2, 0), (Q1, 2, 2, 1), (Z2, 1, 0, 2),
    (BL, 1, 1), (Q2, 0, 2), (Z2, 1, 0, 3), (Z2, 1, 1, 1), (Q1, 2, 0, 0), (Q1, 2, 0, 1), (Z1, 2, 2), (BL, 1, 2), (WD, 3), (Z2, 1, 1, 2),
    (CI, 0),
)
GATE_STEPS = (
    (),
    (),
    (
        (Z1, 2, 3), (Z2, 1, 1, 3), (Q2, 0, 1),
    ),
    (
        (Z1, 2, 4), (Q1, 2, 1, 0), (Q1, 2, 1, 1), (Q2, 0, 3), (BL, 2, 3), (BL, 1, 3), (Z1, 2, 5), (CI, 1),
    ),
    (
        (Z1, 2, 6),
    ),
    (
        (Q2, 1, 0), (Q2, 2, 0), (Q2, 2, 2), (Q1, 1, 1, 1), (CI, 2),
    ),
    (
        (Z1, 2, 7),
    ),
    (
        (Z2, 2, 0, 1), (CI, 3),
    ),
    (
        (Q2, 2, 1), (Q1, 1, 1, 0), (Q1, 1, 2, 1), (Q1, 2, 3, 1),
    ),
)
UP_STEPS = (
    (
        (WD, 1), (Z2, 2, 0, 2),
    ),
    (
        (Z2, 2, 1, 0), (Z2, 2, 0, 3), (Q1, 1, 2, 0), (Q1, 1, 3, 1), (Q1, 2, 3, 0),
    ),
    (),
    (
        (Z2, 2, 1, 1),
    ),
    (
        (Q2, 2, 3), (Q2, 1, 2), (Z2, 2, 1, 2), (Q1, 1, 3, 0),
    ),
    (),
    (
        (Z2, 2, 1, 3),
    ),
    (
        (Q2, 1, 1), (Q2, 1, 3),
    ),
)
LATE_STEPS = (
    (WD, 2),
)
Z_ORDER = (2, 0, 1)
EARLY_ORDER = (
    ("far_block", 2), ("next_products", 2), ("late",), ("give_rows", 0),
)
LATE_ORDER = (
    ("next_adds", 2), ("own_block", 2), ("keep_rows", 0), ("ring_first", 0, 1), ("finish", 2, 0), ("far_block", 0), ("give_rows", 1),
    ("finish", 2, 3), ("finish", 2, 1), ("finish", 2, 4), ("ring_dependent", 0, 1), ("finish", 2, 2), ("far_block", 1), ("keep_rows", 1),
    ("ring_first", 1, 1), ("next_blocks", 0), ("own_block", 0), ("next_blocks", 1), ("own_block", 1), ("finish", 0, 0),
    ("ring_dependent", 1, 1), ("finish", 0, 1), ("ring_last", 0, 1), ("ring_first", 0, 2), ("finish", 0, 2), ("finish", 0, 3),
    ("finish", 0, 4), ("ring_last", 1, 1), ("ring_first", 1, 2), ("ring_dependent", 0, 2), ("finish", 1, 0), ("ring_dependent", 1, 2),
    ("ring_last", 0, 2), ("finish", 1, 1), ("finish", 1, 2), ("ring_last", 1, 2), ("finish", 1, 3), ("finish", 1, 4),
)


def dot(a, b, ca, cb):
    return lax.dot_general(a, b, (((ca,), (cb,)), ((), ())), preferred_element_type=F32)


def layer_kernel(sg, su, sd, tok, grad, tok_own, grad_own,
                 og, ou, od, out, gin, wg, wu, wd, wr, tok_all, grad_all, h_main, h_rest, ra, rb, give, rc, part, ra1, rb1, sd1, mid, ra2, rb2, sd2,
                 ff, blk, far, nxt,
                 own_sem, ex_s, ex_r, z1_s, z1_r, zn_r, z2_s, z2_r, p1_s, p1_r, p2_s, p2_r, q1_s, q1_r, q2_s, q2_r, cc_s, cc_r,
                 sh_sem, wv_sem, row_sem, hst_sem, blk_sem, tmp_sem, a_s, a_r, u_s, u_r, e_s, e_r, out_sem,
                 c_s, c_r, a1_s, a1_r, f1_s, f1_r, d1_s, d1_r, a2_s, a2_r, f2_s, f2_r, d2_s, d2_r):
    z, y = lax.axis_index("datb"), lax.axis_index("model")
    x, core = lax.axis_index("x"), lax.axis_index("core")
    i8 = 2 * x + core
    n8 = 2 * RING
    rows, d = tok.shape
    half_rows = rows // 2
    chunk = RING * rows
    n_chunk = n8
    nf, tokens = ff.shape[1:]
    dp = sg.shape[0]
    half = nf // 2
    main = wg.shape[1]
    rest = nf - main
    packed = wr.shape[1]
    cols = blk.shape[2]
    tiles = far.shape[1] // LANE
    outs = (og, ou, od)

    zs, ys, xs = ([v] + [lax.rem(v + k, RING) for k in range(1, RING)] for v in (z, y, x))
    cores = (core, 1 - core)
    peers = [[2 * v + c for c in cores] for v in xs]
    slot_at = [[[pl.multiple_of((zz * n8 + peers[dx][dc]) * dp, 16) for dc in range(2)] for dx in range(RING)] for zz in zs]
    hand_at = [[pl.multiple_of(p * dp, 8) for p in row] for row in peers]
    rows_at = [[[pl.multiple_of((peers[dx][dc] * RING + yy) * rows, half_rows) for dc in range(2)] for yy in ys] for dx in range(RING)]
    lanes_at = [pl.multiple_of(zz * cols, LANE) for zz in zs]

    def peer(dx, dc):
        return peers[dx][dc]

    def zdev(k):
        return {"datb": zs[k]}

    def xdev(k):
        return {"x": xs[k]}

    def ydev(k):
        return {"model": ys[k]}

    def near(dx, dc):
        return {"x": xs[dx], "core": cores[dc]}

    def copy(src, dst, s, r, dev):
        return pltpu.make_async_remote_copy(src_ref=src, dst_ref=dst, send_sem=s, recv_sem=r, device_id=dev, device_id_type=MESH_ID)

    rcopy = copy

    def all_in(ref, sem):
        copy(ref, ref, sem, sem, zdev(1)).wait_recv()

    def all_out(ref, sem):
        copy(ref, ref, sem, sem, zdev(1)).wait_send()

    def start(copies):
        for c in copies:
            c.start()

    def received(copies):
        for c in copies:
            c.wait_recv()

    def sent(copies):
        for c in copies:
            c.wait_send()

    def run_order(fns, order):
        for fn, *args in order:
            with jax.named_scope("_".join(str(v) for v in [fn, *args])):
                fns[fn](*args)

    barrier = pltpu.get_barrier_semaphore()
    others = [zdev(1), zdev(3), ydev(1), ydev(3)] + [near(*n) for n in NEAR[1:]]
    for dev in others:
        pl.semaphore_signal(barrier, inc=1, device_id=dev, device_id_type=MESH_ID)

    def blk_load(t, slot, k):
        src = tok_all if t < 2 else grad_all
        return pltpu.make_async_copy(src.at[:, pl.ds(lanes_at[k], cols)], blk.at[slot], blk_sem.at[slot])

    plan = []
    for fn, *args in EARLY_ORDER + LATE_ORDER:
        plan += [(args[0], k) for k in {"far_block": (2,), "next_blocks": (1, 3), "next_products": (1, 3), "own_block": (0,)}.get(fn, ())]
    taken = []

    def next_block():
        n = len(taken)
        taken.append(n)
        blk_load(plan[n][0], n % 2, plan[n][1]).wait()
        if n + 1 < len(plan):
            blk_load(plan[n + 1][0], (n + 1) % 2, plan[n + 1][1]).start()
        return n % 2

    def product(t, dst):
        slot = next_block()
        step = 2 * LANE

        def one(n, carry):
            lanes = pl.ds(pl.multiple_of(jnp.minimum(n * step, cols - step), LANE), step)
            dst[:nf, lanes] = jnp.dot(ff[t], blk[slot, :, lanes], preferred_element_type=F32)
            return carry

        lax.fori_loop(0, -(-cols // step), one, 0)

    lo, hi = pl.ds(0, half), pl.ds(half, half)

    def a_copies(t):
        return [rcopy(far.at[t, rows], ra.at[t, rows], a_s.at[t], a_r.at[t], zdev(k)) for s, rows, k in ((0, lo, 1), (1, hi, 3))]

    def tile_rows(tile):
        return pl.ds(tile * LANE, min(LANE, nf - tile * LANE))

    def unit_copies(t, tile):
        at = tile_rows(tile)
        return [rcopy(nxt.at[t, s, at], rb.at[t, s, at], u_s.at[t], u_r.at[t, tile], zdev(1 + 2 * s)) for s in range(2)]

    def far_block(t):
        product(t, far.at[t])
        start(a_copies(t))

    def early_units(t):
        if ("next_products", t) not in EARLY_ORDER + LATE_ORDER:
            return ()
        free = [(0, tile) for tile in range(tiles) if tile * LANE >= half]
        return free + [(1, tile) for tile in range(tiles) if (tile + 1) * LANE <= half]

    def next_products(t):
        for s in range(2):
            product(t, nxt.at[t, s])
        for s, tile in early_units(t):
            unit_copies(t, tile)[s].start()

    blocks = d // min(OUT_COLS, d)
    width = d // blocks

    def row_products(r, keep):
        side = core if keep else 1 - core
        specs, args = [], []
        for h, j, w in ((h_main, 2, wd), (h_rest, 0, wr)) if r == 0 else ((h_main, 0, wg), (h_main, 1, wu), (h_rest, 1, wr)):
            n = w.shape[1]
            specs += [pl.BlockSpec((1, RING, 1, RING * rows, n), lambda i, j=j: (j, 0, side, 0, 0)), pl.BlockSpec((width, n), lambda i: (i, 0))]
            args += [h, w]
        wide = pl.BlockSpec((RING, RING, rows, width), lambda i: (0, 0, 0, i))
        terms = len(args) // 2
        if keep:
            specs.append(wide)
            args.append(rc.at[r])

        def body(*refs):
            total = None
            for i in range(terms):
                h = refs[2 * i][...].reshape(RING * RING * rows, refs[2 * i].shape[-1])
                prod = dot(h, refs[2 * i + 1][...], 1, 1)
                total = prod if total is None else total + prod
            if keep:
                total = total + refs[-2][...].astype(F32).reshape(total.shape)
            refs[-1][...] = total.astype(BF16).reshape(RING, RING, rows, width)

        pltpu.emit_pipeline(body, grid=(blocks,), in_specs=specs, out_specs=[wide])(*args, (part if keep else give).at[r])

    def core_copy(r):
        return rcopy(give.at[r], rc.at[r], c_s.at[r], c_r.at[r], near(0, 1))

    def give_rows(r):
        row_products(r, False)
        core_copy(r).start()

    def forward_phase(rowbuf, av, bv, gv, hst, hst_rest, wv_a, wv_r):
        held = {}

        fulls = (wg, wu, wd, wr)
        REST = 3
        def shard_load(t):
            return pltpu.make_async_copy((sg, su, sd)[t], held["shard"].at[t], sh_sem.at[t])

        def cut_pieces(t):
            if t == REST:
                for u in range(3):
                    for j in range(n8):
                        held["rests"][j, :, u * rest:(u + 1) * rest] = held["shard"][u, :, j * nf + main:(j + 1) * nf]
            else:
                for j in range(n8):
                    held["pieces"][t, j] = held["shard"][t, :, j * nf:j * nf + main]
            own_piece(t).start()

        def piece(t, j):
            return held["rests"].at[j] if t == REST else held["pieces"].at[t, j]

        def own_piece(t):
            return pltpu.make_async_copy(piece(t, i8), slot(t, 0, NEAR[0]), own_sem.at[t])

        def go(make, *args):
            make(*args).start()

        def slot(t, k, source):
            dx, dc = source
            return fulls[t].at[pl.ds(slot_at[k][dx][dc], dp)]

        def source(k):
            dx, dc = NEAR[k]
            return (RING - dx) % RING, dc

        def back(side):
            return 3 if side == 0 else 1

        def ahead(side):
            return 1 if side == 0 else 3

        def exchange_copy(t, k):
            return copy(piece(t, peer(*NEAR[k])), slot(t, 0, NEAR[0]), ex_s.at[t], ex_r.at[t, k], near(*NEAR[k]))

        def exchange(t, k):
            go(exchange_copy, t, k)

        def z_first_copy(t, side, k):
            here = slot(t, 0, source(k))
            return copy(here if k else piece(t, i8), here, z1_s.at[t, side], z1_sem(t, side, k), zdev(ahead(side)))

        def z_first(t, k):
            if k:
                here = slot(t, 0, source(k))
                all_in(here, ex_r.at[t, k])
            for side in range(2):
                go(z_first_copy, t, side, k)

        def z1_sem(t, side, k):
            return z1_r.at[t, side, k % (n8 // 2)] if (k < n8 // 2) == (side == 0) else zn_r.at[t, side]

        def some(t, count):
            return fulls[t].at[pl.ds(0, count * dp)]

        def z_second_copy(t, side, k):
            there = slot(t, back(side), source(k + side * (n8 // 2)))
            return copy(there, there, z2_s.at[t, side], z2_r.at[t, side], zdev(ahead(side)))

        def z_second(t, side, k):
            kk = k + side * (n8 // 2)
            all_in(slot(t, back(side), source(kk)), z1_sem(t, side, kk))
            go(z_second_copy, t, side, k)

        def weights_done(t):
            if (WD, t) not in LATE_STEPS:
                own_wait(t)
            for side in range(2):
                all_in(some(t, n8 // 2), zn_r.at[t, side])
                all_in(some(t, n8 // 2), z2_r.at[t, side])
            w_load(t).start()

        cut = d // 2
        rings = ((tok, tok_all, pl.ds(0, d), True), (grad, grad_all, pl.ds(0, cut), True), (grad, grad_all, pl.ds(cut, d - cut), False))

        def axis(r, n):
            return xdev if rings[r][3] == (n == 1) else ydev

        def block(r, da, db, flip=0, lo=0, size=rows):
            dx, dy = (da, db) if rings[r][3] else (db, da)
            first = rows_at[dx][dy][flip]
            return rings[r][1].at[pl.ds(pl.multiple_of(first + lo, half_rows) if lo else first, size), rings[r][2]]

        def own_block(r):
            return rings[r][0].at[:, rings[r][2]]

        def to_core_copy(r, ia, ib):
            there = block(r, DELTAS[ia], DELTAS[ib])
            return copy(own_block(r) if ia == 0 and ib == 0 else there, there, cc_s.at[r], cc_r.at[ia if r == 0 else RING - 1 + r], near(0, 1))

        def to_core(r, ia, ib):
            go(to_core_copy, r, ia, ib)

        def first_copy(r, side):
            return copy(own_block(r), block(r, 0, 0), p1_s.at[r], p1_r.at[r, side], axis(r, 1)(ahead(side)))

        def first_own(r, side):
            go(first_copy, r, side)

        def first_far_copy(r, side):
            part = block(r, back(side), 0, 0, side * half_rows, half_rows)
            return copy(part, part, p2_s.at[r], p2_r.at[r], axis(r, 1)(ahead(side)))

        def first_forward(r, side):
            there = block(r, back(side), 0)
            all_in(there, p1_r.at[r, side])
            go(first_far_copy, r, side)

        def block_on(r, ia):
            if ia == 3:
                all_in(block(r, 2, 0), p2_r.at[r])
            for side in range(2):
                go(second_copy, r, side, ia)
            to_core(r, ia, 0)

        def second_copy(r, side, ia):
            there = block(r, DELTAS[ia], 0)
            return copy(there if ia else own_block(r), there, q1_s.at[r], q1_r.at[r, side, ia], axis(r, 2)(ahead(side)))

        def second_far_copy(r, ia):
            side = ia // 2
            there = block(r, DELTAS[ia], back(side))
            return copy(there, there, q2_s.at[r], q2_r.at[r, ia], axis(r, 2)(ahead(side)))

        def second_forward(r, ia, side):
            there = block(r, DELTAS[ia], back(side))
            all_in(there, q1_r.at[r, side, ia])
            if ia // 2 == side:
                go(second_far_copy, r, ia)
            to_core(r, ia, 1 if side == 0 else 2)

        def second_far(r, ia):
            there = block(r, DELTAS[ia], 2)
            all_in(there, q2_r.at[r, ia])
            to_core(r, ia, 3)

        def some_rows(r, count):
            return rings[r][1].at[pl.ds(0, count * rows), rings[r][2]]

        def chunk_in(ia):
            all_in(some_rows(0, RING), cc_r.at[ia])

        def rows_in(r):
            all_in(some_rows(r, RING * RING), cc_r.at[RING - 1 + r])

        def own_wait(t):
            there = slot(t, 0, NEAR[0])
            pltpu.make_async_copy(there, there, own_sem.at[t]).wait()

        def own_rows(r):
            return pltpu.make_async_copy(own_block(r), block(r, 0, 0), own_sem.at[4 + r])

        def w_load(t):
            return pltpu.make_async_copy(fulls[t], (wv_a, held["wv_b"], wv_a, wv_r)[t], wv_sem.at[t])

        def row_load(src, i, buf):
            return pltpu.make_async_copy(src.at[chunk_rows(i)], rowbuf.at[buf], row_sem.at[buf])

        def chunk_loop(src, products, elementwise, between):
            row_load(src, 0, 0).start()
            between[0]()
            row_load(src, 1, 1).start()
            row_load(src, 0, 0).wait()
            products(0, 0)

            def body(i, carry):
                buf = lax.rem(i, 2)

                @pl.when(i + 1 < n_chunk)
                def _():
                    row_load(src, i + 1, 1 - buf).start()

                for k, step in enumerate(between[1:], 1):
                    pl.when(i == k)(step)
                row_load(src, i, buf).wait()
                free(elementwise, i - 1)
                elementwise(i - 1, 1 - buf, lambda: products(i, buf))
                return carry

            lax.fori_loop(1, n_chunk, body, 0)
            free(elementwise, n_chunk - 1)
            elementwise(n_chunk - 1, (n_chunk - 1) % 2, lambda: None)

        def free(elementwise, i):
            @pl.when(i >= 2)
            def _():
                for cp in copies_of[elementwise](i - 2):
                    cp.wait()

        def chunk_rows(i):
            return pl.ds(pl.multiple_of(i * chunk, chunk), chunk)

        def h_copies(i, which, names):
            xx, c = lax.div(i, 2), lax.rem(i, 2)
            cs = [pltpu.make_async_copy(hst.at[c, n], h_main.at[j, xx, c], hst_sem.at[c, n]) for n, j in enumerate(names)]
            return cs + [pltpu.make_async_copy(hst_rest.at[which, c], h_rest.at[which, xx, c], hst_sem.at[c, 2])]

        def keep(i, c, values):
            which = len(values) - 1
            for n, (j, v) in enumerate(values):
                low = v.astype(BF16)
                hst[c, n] = low[:, :main]
                hst_rest[which, c, :, j * rest:(j + 1) * rest] = low[:, main:]
                ff[j, :, chunk_rows(i)] = v.T.astype(BF16)

        def kept(elementwise):
            for i in (n_chunk - 2, n_chunk - 1):
                for cp in copies_of[elementwise](i):
                    cp.wait()

        def gate_work():
            def place(k):
                ia, flip = lax.div(k, 2), lax.rem(k, 2)
                delta = lax.rem(3 * ia + 3 * lax.div(ia, 2) + 2 * lax.div(ia, 3), RING)
                return 2 * lax.rem(x + delta, RING) + lax.rem(core + flip, 2)

            def body(k, carry):
                for n, group in enumerate(GATE_STEPS):
                    if group:
                        pl.when(k == n)(functools.partial(run, group))

                @pl.when(k < n_chunk)
                def _():
                    row_load(tok_all, place(k), lax.rem(k, 2)).start()

                @pl.when(k >= 1)
                def _():
                    i, buf = place(k - 1), lax.rem(k - 1, 2)
                    row_load(tok_all, i, buf).wait()
                    rb_ = rowbuf[buf]
                    av[chunk_rows(i), :main] = jnp.dot(rb_, wv_a[...], preferred_element_type=F32).astype(BF16)
                    both = jnp.dot(rb_, wv_r[...], preferred_element_type=F32).astype(BF16)
                    av[chunk_rows(i), main:] = both[:, :rest]
                    bv[chunk_rows(i), main:] = both[:, rest:2 * rest]

                return carry

            lax.fori_loop(0, n_chunk + 1, body, 0)

        def up_products(i, buf):
            bv[chunk_rows(i), :main] = jnp.dot(rowbuf[buf], held["wv_b"][...], preferred_element_type=F32).astype(BF16)

        def hidden(i, c, beside):
            a, b = av[chunk_rows(i)].astype(F32), bv[chunk_rows(i)].astype(F32)
            beside()
            keep(i, c, ((2, a * jax.nn.sigmoid(a) * b),))
            start(copies_of[hidden](i))

        def down_products(i, buf):
            rb_ = rowbuf[buf]
            lanes = 2 * rest // LANE * LANE
            low = jnp.dot(rb_, wv_r[:, lanes:], preferred_element_type=F32)[:, 2 * rest - lanes:3 * rest - lanes]
            gv[buf] = jnp.concatenate([jnp.dot(rb_, wv_a[...], preferred_element_type=F32), low], axis=1).astype(BF16)

        def backward(i, c, beside):
            g = gv[c].astype(F32)
            a, b = av[chunk_rows(i)].astype(F32), bv[chunk_rows(i)].astype(F32)
            beside()
            sig = jax.nn.sigmoid(a)
            keep(i, c, ((0, g * b * sig * (1.0 + a * (1.0 - sig))), (1, g * (a * sig))))
            start(copies_of[backward](i))

        copies_of = {hidden: lambda i: h_copies(i, 0, (2,)), backward: lambda i: h_copies(i, 1, (0, 1))}

        steps = (exchange, z_first, z_second, first_own, first_forward, block_on, second_forward, second_far, weights_done, chunk_in)

        def run(group):
            for which, *args in group:
                steps[which](*args)

        def rows_ready():
            run(UP_STEPS[-1])
            for r in (1, 2):
                own_rows(r).wait()
                rows_in(r)
            blk_load(plan[0][0], 0, plan[0][1]).start()

        def gather_phase(shard, pieces, rests, wv_b):
            held.update(shard=shard, pieces=pieces, rests=rests, wv_b=wv_b)
            with jax.named_scope("begin"):
                for t in range(3):
                    shard_load(t).start()
                shard_load(0).wait()
                cut_pieces(0)
                pl.semaphore_wait(barrier, len(others))
                for r in range(3):
                    own_rows(r).start()
            with jax.named_scope("gather"):
                cut = {0}
                for step in GATHER_STEPS:
                    if step[0] in (EX, Z1) and step[1] not in cut:
                        if len(cut) == 1:
                            rests[...] = jnp.zeros_like(rests)
                            hst_rest[...] = jnp.zeros_like(hst_rest)
                            shard_load(1).wait()
                            shard_load(2).wait()
                        cut.add(step[1])
                        cut_pieces(step[1])
                    run((step,))
                own_rows(0).wait()
                w_load(0).wait()
                w_load(REST).wait()
            with jax.named_scope("gate"):
                gate_work()
            with jax.named_scope("up"):
                run(UP_STEPS[0])
                w_load(1).wait()
                chunk_loop(tok_all, up_products, hidden, [functools.partial(run, group) for group in ((),) + UP_STEPS[1:-1]] + [rows_ready])
                kept(hidden)
            for _, t in LATE_STEPS:
                own_wait(t)
            for t in range(4):
                all_out(some(t, n8 - 1), ex_s.at[t])
                for side in range(2):
                    all_out(some(t, n8), z1_s.at[t, side])

        pl.run_scoped(
            gather_phase, pltpu.VMEM((3,) + sg.shape, BF16), pltpu.VMEM((3, n8, dp, main), BF16), pltpu.VMEM((n8, dp, packed), BF16),
            pltpu.VMEM((d, main), BF16))
        run_order({
            "far_block": far_block, "next_products": next_products, "give_rows": give_rows, "late": functools.partial(run, LATE_STEPS),
        }, EARLY_ORDER)
        with jax.named_scope("down"):
            w_load(2).wait()
            chunk_loop(grad_all, down_products, backward, [lambda: None])
            kept(backward)
        for t in range(4):
            for side in range(2):
                all_out(some(t, n8 // 2), z2_s.at[t, side])
        for r in range(3):
            for count, sem in ((2, p1_s), (1, p2_s), (2 * RING, q1_s), (RING, q2_s), (RING * RING, cc_s)):
                all_out(some_rows(r, count), sem.at[r])

    def backward_phase(tmp, stage):
        def next_adds(t):
            all_in(ra.at[t], a_r.at[t])
            cs = [pltpu.make_async_copy(ra.at[t, at], tmp.at[s, at], tmp_sem.at[s]) for s, at in ((0, lo), (1, hi))]
            start(cs)
            for c, (s, at) in zip(cs, ((0, lo), (1, hi))):
                c.wait()
                nxt[t, s, at] += tmp[s, at]
            for tile in range(tiles):
                start(c for s, c in enumerate(unit_copies(t, tile)) if (s, tile) not in early_units(t))

        def next_blocks(t):
            next_products(t)
            next_adds(t)

        def own_block(t):
            all_out(ra.at[t], a_s.at[t])
            product(t, far.at[t])

        def slot(t):
            return Z_ORDER.index(t) % 2

        def hand_out(t, tile):
            cs = []
            for k in range(1, n8):
                at = pl.ds(hand_at[NEAR[k][0]][NEAR[k][1]], dp)
                cs.append(rcopy(stage.at[slot(t), tile, at], outs[t].at[i8, tile], e_s.at[t], e_r.at[t], near(*NEAR[k])))
            at = pl.ds(hand_at[0][0], dp)
            return cs, pltpu.make_async_copy(stage.at[slot(t), tile, at], outs[t].at[i8, tile], out_sem.at[t])

        def handed(t):
            all_out(outs[t].at[pl.ds(0, n8 - 1)], e_s.at[t])
            pltpu.make_async_copy(outs[t].at[0], outs[t].at[0], out_sem.at[t]).wait()

        given = []

        def finish(t, tile):
            at = tile_rows(tile)
            all_in(rb.at[t, :, at], u_r.at[t, tile])
            cs = [pltpu.make_async_copy(rb.at[t, s, at], tmp.at[s, at], tmp_sem.at[s]) for s in range(2)]
            start(cs)
            if t == Z_ORDER[2] and not given:
                given.append(Z_ORDER[0])
                handed(Z_ORDER[0])
            for c in cs:
                c.wait()
            wide = pl.ds(tile * LANE, LANE)
            stage[slot(t), tile] = (far[t, wide] + tmp[0, wide] + tmp[1, wide]).T
            cs, mine = hand_out(t, tile)
            start(cs + [mine])

        def on_y(r, n):
            return (r == 1) == (n == 1)

        def level(r, n):
            at = ys if on_y(r, n) else xs
            dev = ydev if on_y(r, n) else xdev
            if n == 1:
                def piece(k, h):
                    return part.at[r, pl.ds(2 * h, 2), at[k]] if on_y(r, n) else part.at[r, at[k], pl.ds(2 * h, 2)]
                return dev, piece, ra1, rb1, sd1, (a1_s, a1_r, f1_s, f1_r, d1_s, d1_r)

            def piece(k, h):
                return mid.at[r, at[k], pl.ds(h, 1)]
            return dev, piece, ra2, rb2, sd2, (a2_s, a2_r, f2_s, f2_r, d2_s, d2_r)

        def ring_a(r, n):
            dev, piece, rfar, _, _, sems = level(r, n)
            return [rcopy(piece(2, s), rfar.at[r, s], sems[0].at[r], sems[1].at[r], dev(1 + 2 * s)) for s in range(2)]

        def ring_f(r, n):
            dev, piece, _, rnear, _, sems = level(r, n)
            return [rcopy(piece(1 + 2 * s, 1 - s), rnear.at[r, s, 1 - s], sems[2].at[r], sems[3].at[r], dev(1 + 2 * s)) for s in range(2)]

        def ring_d(r, n):
            dev, _, _, rnear, dep, sems = level(r, n)
            return [rcopy(dep.at[r, s], rnear.at[r, s, s], sems[4].at[r], sems[5].at[r], dev(1 + 2 * s)) for s in range(2)]

        def add(grid, *terms):
            specs = []
            for ref, at, lead in terms:
                tail = ref.shape[lead:]
                specs.append(pl.BlockSpec((1,) * lead + tuple(tail), lambda *i, at=at, rank=len(tail): tuple(at(*i)) + (0,) * rank))

            def body(*refs):
                total = refs[0][...].astype(F32).reshape(refs[0].shape[-2:])
                for ref in refs[1:-1]:
                    total = total + ref[...].astype(F32).reshape(total.shape)
                refs[-1][...] = total.astype(BF16).reshape(refs[-1].shape)

            pltpu.emit_pipeline(body, grid=grid, in_specs=specs[:-1], out_specs=specs[-1:])(*[ref for ref, _, _ in terms])

        def ring_first(r, n):
            start(ring_a(r, n) + ring_f(r, n))

        def ring_dependent(r, n):
            _, _, rfar, _, _, sems = level(r, n)
            all_in(rfar.at[r], sems[1].at[r])
            here = y if on_y(r, n) else x
            if n == 1:
                def near_block(s, i):
                    at = lax.rem(here + 1 + 2 * s, RING)
                    return (2 * s + i, at) if on_y(r, n) else (at, 2 * s + i)

                add((2, 2), (part.at[r], near_block, 2), (ra1.at[r], lambda s, i: (s, i), 2), (sd1.at[r], lambda s, i: (s, i), 2))
            else:
                add((2,), (mid.at[r], lambda s: (lax.rem(here + 1 + 2 * s, RING), s), 2), (ra2.at[r], lambda s: (s, 0), 2),
                    (sd2.at[r], lambda s: (s, 0), 2))
            start(ring_d(r, n))

        def ring_last(r, n):
            _, _, rfar, _, _, sems = level(r, n)
            all_in(rfar.at[r], sems[3].at[r])
            all_in(rfar.at[r], sems[5].at[r])
            here = y if on_y(r, n) else x
            if n == 1:
                def own_at(h, i):
                    return (2 * h + i, here) if on_y(r, n) else (here, 2 * h + i)

                add((2, 2), (part.at[r], own_at, 2), (rb1.at[r, 0], lambda h, i: (h, i), 2),
                    (rb1.at[r, 1], lambda h, i: (h, i), 2), (mid.at[r], lambda h, i: (2 * h + i,), 1))
            else:
                own, res = ((tok_own, out), (grad_own, gin))[r]
                add((2,), (own, lambda h: (h,), 1), (mid.at[r], lambda h: (here, h), 2), (rb2.at[r, 0], lambda h: (h, 0), 2),
                    (rb2.at[r, 1], lambda h: (h, 0), 2), (res, lambda h: (h,), 1))

        def keep_rows(r):
            core_copy(r).wait_recv()
            row_products(r, True)

        run_order({
            "far_block": far_block, "next_products": next_products, "next_adds": next_adds, "next_blocks": next_blocks,
            "own_block": own_block, "finish": finish, "give_rows": give_rows, "keep_rows": keep_rows, "ring_first": ring_first,
            "ring_dependent": ring_dependent, "ring_last": ring_last,
        }, LATE_ORDER)

        for t in range(3):
            all_out(nxt.at[t], u_s.at[t])
        for r in range(2):
            core_copy(r).wait_send()
            for n in (1, 2):
                _, _, rfar, _, _, sems = level(r, n)
                for sem in sems[::2]:
                    all_out(rfar.at[r], sem.at[r])
        for t in Z_ORDER:
            with jax.named_scope(f"handed_{t}"):
                all_in(outs[t].at[pl.ds(0, n8 - 1)], e_r.at[t])
                if t not in given:
                    handed(t)

    pl.run_scoped(
        forward_phase,
        pltpu.VMEM((2, chunk, d), BF16),
        pltpu.VMEM((tokens, nf), BF16),
        pltpu.VMEM((tokens, nf), BF16),
        pltpu.VMEM((2, chunk, nf), BF16),
        pltpu.VMEM((2, 2, chunk, main), BF16),
        pltpu.VMEM((2, 2, chunk, packed), BF16),
        pltpu.VMEM((d, main), BF16),
        pltpu.VMEM((d, packed), BF16),
    )
    pl.run_scoped(backward_phase, pltpu.VMEM((2, tiles * LANE, cols), F32), pltpu.VMEM((2, tiles, cols, LANE), F32))


def layer(sg, su, sd, tok, grad):
    n8 = 2 * RING
    dp, nf = sg.shape[0], sg.shape[1] // n8
    rows, d = tok.shape
    tokens = rows * RING * n8
    cols = d // RING
    tiles = -(-nf // LANE)
    padded = tiles * LANE
    main = nf // LANE * LANE
    packed = -(-3 * (nf - main) // LANE) * LANE
    hbm = pl.BlockSpec(memory_space=pl.ANY)
    dma = pltpu.SemaphoreType.DMA
    sds = jax.ShapeDtypeStruct
    halves = (2, rows // 2, d)
    res = pl.pallas_call(
        layer_kernel,
        out_shape=[sds((n8, tiles, dp, LANE), F32)] * 3 + [sds(halves, BF16)] * 2 + [
            sds((d, main), BF16), sds((d, main), BF16), sds((d, main), BF16), sds((d, packed), BF16), sds((tokens, d), BF16), sds((tokens, d), BF16),
            sds((3, RING, 2, RING * rows, main), BF16), sds((2, RING, 2, RING * rows, packed), BF16),
            sds((3, nf, cols), F32), sds((3, 2, nf, cols), F32),
            sds((2, RING, RING, rows, d), BF16), sds((2, RING, RING, rows, d), BF16), sds((2, RING, RING, rows, d), BF16),
            sds((2, 2, 2, rows, d), BF16), sds((2, 2, 2, 2, rows, d), BF16), sds((2, 2, 2, rows, d), BF16),
            sds((2, RING, 2, rows // 2, d), BF16),
            sds((2, 2, 1, rows // 2, d), BF16), sds((2, 2, 2, 1, rows // 2, d), BF16), sds((2, 2, 1, rows // 2, d), BF16),
        ],
        in_specs=[hbm] * 7,
        out_specs=[hbm] * 25,
        scratch_shapes=[
            pltpu.VMEM((3, nf, tokens), BF16),
            pltpu.VMEM((2, tokens, cols), BF16),
            pltpu.VMEM((3, padded, cols), F32),
            pltpu.VMEM((3, 2, nf, cols), F32),
            dma((7,)),
            dma((4,)), dma((4, n8)),
            dma((4, 2)), dma((4, 2, n8 // 2)), dma((4, 2)),
            dma((4, 2)), dma((4, 2)),
            dma((3,)), dma((3, 2)),
            dma((3,)), dma((3,)),
            dma((3,)), dma((3, 2, RING)),
            dma((3,)), dma((3, RING)),
            dma((3,)), dma((RING + 2,)),
            dma((3,)), dma((4,)), dma((2,)), dma((2, 3)), dma((2,)), dma((2,)),
            dma((3,)), dma((3,)),
            dma((3,)), dma((3, tiles)),
            dma((3,)), dma((3,)),
            dma((3,)),
            dma((2,)), dma((2,)),
        ] + [dma((2,))] * 12,
        compiler_params=pltpu.CompilerParams(collective_id=0, has_side_effects=True, vmem_limit_bytes=67043328),
        cost_estimate=pl.CostEstimate(flops=18 * nf * tokens * d, bytes_accessed=300_000_000, transcendentals=0),
        name="layer",
    )(sg, su, sd, tok, grad, tok.reshape(halves), grad.reshape(halves))
    return res[:3], res[3].reshape(rows, d), res[4].reshape(rows, d)


def assemble_kernel(og, ou, od, out, gin, g, u, w, res, gres, buf, flat, in_sem, out_sem, row_buf, row_sem):
    n8, nf = og.shape[0], g.shape[1] // og.shape[0]
    srcs, dsts = (og, ou, od), (g, u, w)
    rows_in = [pltpu.make_async_copy(src, row_buf.at[r], row_sem.at[r]) for r, src in enumerate((out, gin))]
    loads = [pltpu.make_async_copy(src, buf.at[t], in_sem.at[t]) for t, src in enumerate(srcs)]
    stores = [pltpu.make_async_copy(flat.at[t], dst, out_sem.at[t]) for t, dst in enumerate(dsts)]
    for c in loads + rows_in:
        c.start()
    for t in range(3):
        loads[t].wait()
        for j in range(n8):
            flat[t, :, j * nf:(j + 1) * nf] = jnp.concatenate([buf[t, j, tile] for tile in range(buf.shape[2])], axis=1)[:, :nf]
        stores[t].start()
    rows_out = [pltpu.make_async_copy(row_buf.at[r], dst, row_sem.at[r]) for r, dst in enumerate((res, gres))]
    for c in rows_in:
        c.wait()
    for c in rows_out:
        c.start()
    for c in stores + rows_out:
        c.wait()


def assemble(sums, out, gin, ff):
    dp = sums[0].shape[2]
    hbm = pl.BlockSpec(memory_space=pl.ANY)
    dma = pltpu.SemaphoreType.DMA
    sds = jax.ShapeDtypeStruct
    return pl.pallas_call(
        assemble_kernel,
        out_shape=[sds((dp, ff), F32)] * 3 + [sds(out.shape, BF16)] * 2,
        in_specs=[hbm] * 5,
        out_specs=[hbm] * 5,
        scratch_shapes=[
            pltpu.VMEM((3,) + sums[0].shape, F32), pltpu.VMEM((3, dp, ff), F32), dma((3,)), dma((3,)),
            pltpu.VMEM((2,) + out.shape, BF16), dma((2,)),
        ],
        compiler_params=pltpu.CompilerParams(vmem_limit_bytes=63 * 1024 * 1024),
        name="assemble",
    )(*sums, out, gin)


def solution(mesh):
    nz, ny, nd = mesh.shape["datb"], mesh.shape["model"], mesh.shape["data"]
    fine = Mesh(mesh.devices.reshape(nz, ny, nd // 2, 2), ("datb", "model", "x", "core"))

    def local_step(tok_loc, wg_loc, wu_loc, wd_loc, grad_loc):
        sums, out, grad_in = layer(wg_loc, wu_loc, wd_loc.T, tok_loc, grad_loc)
        grad_gate, grad_up, grad_down_t, out, grad_in = assemble(sums, out, grad_in, wg_loc.shape[1])
        return out, grad_in, grad_gate, grad_up, grad_down_t.T

    return jax.shard_map(local_step, mesh=fine, in_specs=(ROW_SPEC, GATE_SPEC, GATE_SPEC, DOWN_SPEC, ROW_SPEC), out_specs=(ROW_SPEC, ROW_SPEC, GATE_SPEC, GATE_SPEC, DOWN_SPEC), check_vma=False)
```

```python
import functools

import jax
import jax.numpy as jnp
from jax import lax
from jax.experimental import pallas as pl
from jax.experimental.pallas import tpu as pltpu
from jax.sharding import Mesh
from jax.sharding import PartitionSpec as P

ROW_SPEC = P(("datb", "x", "core", "model"), None)
GATE_SPEC = P(("datb", "x", "core"), "model")
DOWN_SPEC = P("model", ("datb", "x", "core"))
BF16 = jnp.bfloat16
F32 = jnp.float32
MESH_ID = pl.DeviceIdType.MESH
RING = 4
NEAR = ((0, 0), (0, 1), (1, 0), (3, 0), (1, 1), (3, 1), (2, 0), (2, 1))
DELTAS = (0, 3, 1, 2)
LANE = 128
OUT_COLS = 512
EX, Z1, Z2, P1, P2, BL, Q1, Q2, WD, CI = range(10)
GATHER_STEPS = (
    (Z1, 0, 0), (P1, 0, 0), (P1, 0, 1), (EX, 0, 1), (BL, 0, 0), (P1, 2, 0), (P1, 2, 1), (EX, 0, 2), (Z1, 3, 0), (EX, 3, 1), (EX, 3, 2),
    (EX, 3, 3), (EX, 3, 4), (EX, 3, 5), (EX, 3, 6), (EX, 3, 7), (Z1, 1, 0), (EX, 1, 1), (Z1, 2, 0), (EX, 2, 1), (EX, 0, 3), (BL, 1, 0),
    (Z1, 3, 1), (EX, 0, 4), (EX, 0, 5), (Z1, 0, 1), (Z1, 1, 1), (Z2, 3, 0, 0), (Z1, 2, 1), (EX, 0, 6), (EX, 0, 7), (Z2, 0, 0, 0),
    (Z2, 1, 0, 0), (EX, 1, 2), (EX, 1, 3), (Z2, 2, 0, 0), (Z2, 3, 0, 1), (P2, 0, 0), (P2, 0, 1), (BL, 0, 1), (Q1, 0, 0, 1), (Z1, 3, 2),
    (Z1, 3, 3), (Z1, 3, 4), (Q1, 0, 0, 0), (Z1, 3, 5), (Z2, 0, 0, 1), (EX, 1, 4), (EX, 1, 5), (P2, 2, 1), (Z1, 3, 6), (EX, 1, 6),
    (EX, 1, 7), (Z1, 3, 7), (Z1, 0, 2), (Q1, 1, 0, 1), (Z2, 3, 1, 0), (Z2, 3, 1, 1), (Z1, 0, 3), (EX, 2, 2), (EX, 2, 3), (Z2, 3, 1, 2),
    (BL, 0, 2), (Z2, 3, 1, 3), (Z1, 0, 4), (EX, 2, 4), (EX, 2, 5), (Z1, 0, 5), (EX, 2, 6), (EX, 2, 7), (Z2, 3, 0, 2), (Q1, 0, 1, 1),
    (Z2, 3, 0, 3), (Z1, 0, 6), (P1, 1, 0), (P1, 1, 1), (Q1, 0, 1, 0), (Z1, 0, 7), (BL, 2, 2), (Z2, 0, 1, 0), (Z1, 1, 2), (Z2, 0, 1, 1),
    (Z2, 0, 0, 2), (Q2, 0, 0), (Z2, 0, 1, 2), (Z2, 0, 0, 3), (BL, 2, 0), (BL, 0, 3), (Q1, 0, 2, 1), (Z2, 0, 1, 3), (Z1, 1, 3), (Z1, 1, 4),
    (WD, 3), (Z1, 1, 5), (Q1, 0, 2, 0), (Z1, 1, 6), (P2, 2, 0), (BL, 2, 1), (P2, 1, 0), (P2, 1, 1), (Z1, 1, 7), (Q1, 0, 3, 1),
    (Q1, 1, 0, 0), (Z2, 1, 0, 1), (Q1, 2, 2, 0), (Q1, 2, 2, 1), (Z2, 1, 0, 2), (BL, 1, 1), (Q2, 0, 1), (WD, 0), (Z2, 1, 1, 0), (CI, 0),
)
GATE_STEPS = (
    (),
    (),
    (
        (Z1, 2, 2),
    ),
    (
        (Q2, 0, 2), (Z2, 1, 1, 1), (Z2, 1, 0, 3), (Q1, 2, 0, 0), (Q1, 2, 0, 1), (BL, 1, 2), (CI, 1),
    ),
    (
        (Z2, 1, 1, 2), (Z1, 2, 3),
    ),
    (
        (Q1, 0, 3, 0), (Z2, 1, 1, 3), (Z1, 2, 4), (CI, 2),
    ),
    (
        (Z1, 2, 5), (Q1, 2, 1, 0), (Q1, 2, 1, 1), (BL, 2, 3), (BL, 1, 3), (Z1, 2, 6), (Q2, 0, 3),
    ),
    (
        (Q2, 1, 0), (Z1, 2, 7), (CI, 3),
    ),
    (
        (Q2, 2, 0), (Q2, 2, 2), (Z2, 2, 0, 1), (Q1, 1, 1, 0), (Q1, 1, 1, 1),
    ),
)
UP_STEPS = (
    (
        (Z2, 2, 0, 2), (Q1, 1, 2, 1), (WD, 1),
    ),
    (
        (Q2, 2, 1), (Q1, 2, 3, 1), (Q1, 1, 2, 0),
    ),
    (
        (Z2, 2, 1, 0), (Z2, 2, 0, 3), (Q1, 1, 3, 1),
    ),
    (
        (Z2, 2, 1, 1), (Q1, 1, 3, 0),
    ),
    (
        (Q2, 1, 2), (Z2, 2, 1, 2), (Q1, 2, 3, 0),
    ),
    (
        (Q2, 1, 1), (Z2, 2, 1, 3),
    ),
    (
        (Q2, 1, 3), (Q2, 2, 3),
    ),
    (),
)
LATE_STEPS = (
    (WD, 2),
)
Z_ORDER = (2, 0, 1)
EARLY_ORDER = (
    ("far_block", 2), ("next_products", 2), ("late",), ("give_rows", 0),
)
LATE_ORDER = (
    ("next_adds", 2), ("own_block", 2), ("keep_rows", 0), ("ring_first", 0, 1), ("finish", 2, 0), ("far_block", 0), ("give_rows", 1),
    ("finish", 2, 3), ("finish", 2, 1), ("finish", 2, 4), ("ring_dependent", 0, 1), ("finish", 2, 2), ("far_block", 1), ("keep_rows", 1),
    ("ring_first", 1, 1), ("next_blocks", 0), ("own_block", 0), ("next_blocks", 1), ("own_block", 1), ("finish", 0, 0),
    ("ring_dependent", 1, 1), ("finish", 0, 1), ("ring_last", 0, 1), ("ring_first", 0, 2), ("finish", 0, 2), ("finish", 0, 3),
    ("finish", 0, 4), ("ring_last", 1, 1), ("ring_first", 1, 2), ("ring_dependent", 0, 2), ("finish", 1, 0), ("ring_dependent", 1, 2),
    ("ring_last", 0, 2), ("finish", 1, 1), ("finish", 1, 2), ("ring_last", 1, 2), ("finish", 1, 3), ("finish", 1, 4),
)


def dot(a, b, ca, cb):
    return lax.dot_general(a, b, (((ca,), (cb,)), ((), ())), preferred_element_type=F32)


def layer_kernel(sg, su, sd, tok, grad, tok_own, grad_own,
                 og, ou, od, out, gin, wg, wu, wd, wr, tok_all, grad_all, h_main, h_rest, ra, rb, give, rc, part, ra1, rb1, sd1, mid, ra2, rb2, sd2,
                 ff, blk, far, nxt,
                 own_sem, ex_s, ex_r, z1_s, z1_r, zn_r, z2_s, z2_r, p1_s, p1_r, p2_s, p2_r, q1_s, q1_r, q2_s, q2_r, cc_s, cc_r,
                 sh_sem, wv_sem, row_sem, hst_sem, blk_sem, tmp_sem, a_s, a_r, u_s, u_r, e_s, e_r, out_sem,
                 c_s, c_r, a1_s, a1_r, f1_s, f1_r, d1_s, d1_r, a2_s, a2_r, f2_s, f2_r, d2_s, d2_r):
    z, y = lax.axis_index("datb"), lax.axis_index("model")
    x, core = lax.axis_index("x"), lax.axis_index("core")
    i8 = 2 * x + core
    n8 = 2 * RING
    rows, d = tok.shape
    half_rows = rows // 2
    chunk = RING * rows
    n_chunk = n8
    nf, tokens = ff.shape[1:]
    dp = sg.shape[0]
    half = nf // 2
    main = wg.shape[1]
    rest = nf - main
    packed = wr.shape[1]
    cols = blk.shape[2]
    tiles = far.shape[1] // LANE
    outs = (og, ou, od)

    zs, ys, xs = ([v] + [lax.rem(v + k, RING) for k in range(1, RING)] for v in (z, y, x))
    cores = (core, 1 - core)
    peers = [[2 * v + c for c in cores] for v in xs]
    slot_at = [[[pl.multiple_of((zz * n8 + peers[dx][dc]) * dp, 16) for dc in range(2)] for dx in range(RING)] for zz in zs]
    hand_at = [[pl.multiple_of(p * dp, 8) for p in row] for row in peers]
    rows_at = [[[pl.multiple_of((peers[dx][dc] * RING + yy) * rows, half_rows) for dc in range(2)] for yy in ys] for dx in range(RING)]
    lanes_at = [pl.multiple_of(zz * cols, LANE) for zz in zs]

    def peer(dx, dc):
        return peers[dx][dc]

    def zdev(k):
        return {"datb": zs[k]}

    def xdev(k):
        return {"x": xs[k]}

    def ydev(k):
        return {"model": ys[k]}

    def near(dx, dc):
        return {"x": xs[dx], "core": cores[dc]}

    def copy(src, dst, s, r, dev):
        return pltpu.make_async_remote_copy(src_ref=src, dst_ref=dst, send_sem=s, recv_sem=r, device_id=dev, device_id_type=MESH_ID)

    rcopy = copy

    def all_in(ref, sem):
        copy(ref, ref, sem, sem, zdev(1)).wait_recv()

    def all_out(ref, sem):
        copy(ref, ref, sem, sem, zdev(1)).wait_send()

    def start(copies):
        for c in copies:
            c.start()

    def received(copies):
        for c in copies:
            c.wait_recv()

    def sent(copies):
        for c in copies:
            c.wait_send()

    def run_order(fns, order):
        for fn, *args in order:
            with jax.named_scope("_".join(str(v) for v in [fn, *args])):
                fns[fn](*args)

    barrier = pltpu.get_barrier_semaphore()
    others = [zdev(1), zdev(3), ydev(1), ydev(3)] + [near(*n) for n in NEAR[1:]]
    for dev in others:
        pl.semaphore_signal(barrier, inc=1, device_id=dev, device_id_type=MESH_ID)

    def blk_load(t, slot, k):
        src = tok_all if t < 2 else grad_all
        return pltpu.make_async_copy(src.at[:, pl.ds(lanes_at[k], cols)], blk.at[slot], blk_sem.at[slot])

    plan = []
    for fn, *args in EARLY_ORDER + LATE_ORDER:
        plan += [(args[0], k) for k in {"far_block": (2,), "next_blocks": (1, 3), "next_products": (1, 3), "own_block": (0,)}.get(fn, ())]
    taken = []

    def next_block():
        n = len(taken)
        taken.append(n)
        blk_load(plan[n][0], n % 2, plan[n][1]).wait()
        if n + 1 < len(plan):
            blk_load(plan[n + 1][0], (n + 1) % 2, plan[n + 1][1]).start()
        return n % 2

    def product(t, dst):
        slot = next_block()
        step = 2 * LANE

        def one(n, carry):
            lanes = pl.ds(pl.multiple_of(jnp.minimum(n * step, cols - step), LANE), step)
            dst[:nf, lanes] = jnp.dot(ff[t], blk[slot, :, lanes], preferred_element_type=F32)
            return carry

        lax.fori_loop(0, -(-cols // step), one, 0)

    lo, hi = pl.ds(0, half), pl.ds(half, half)

    def a_copies(t):
        return [rcopy(far.at[t, rows], ra.at[t, rows], a_s.at[t], a_r.at[t], zdev(k)) for s, rows, k in ((0, lo, 1), (1, hi, 3))]

    def tile_rows(tile):
        return pl.ds(tile * LANE, min(LANE, nf - tile * LANE))

    def unit_parts(t, tile):
        if (t, tile) != (Z_ORDER[2], tiles - 1):
            return [(tile, 0, cols)]
        first = -(-cols // 2 // LANE) * LANE
        return [(tile, 0, first), (tiles, first, cols - first)]

    def unit_copies(t, tile):
        at = tile_rows(tile)
        cs = []
        for n, first, size in unit_parts(t, tile):
            lanes = pl.ds(first, size)
            cs += [rcopy(nxt.at[t, s, at, lanes], rb.at[t, s, at, lanes], u_s.at[t], u_r.at[t, n], zdev(1 + 2 * s)) for s in range(2)]
        return cs

    def far_block(t):
        product(t, far.at[t])
        start(a_copies(t))

    def early_units(t):
        if ("next_products", t) not in EARLY_ORDER + LATE_ORDER:
            return ()
        free = [(0, tile) for tile in range(tiles) if tile * LANE >= half]
        return free + [(1, tile) for tile in range(tiles) if (tile + 1) * LANE <= half]

    def next_products(t):
        for s in range(2):
            product(t, nxt.at[t, s])
        for s, tile in early_units(t):
            unit_copies(t, tile)[s].start()

    blocks = d // min(OUT_COLS, d)
    width = d // blocks

    def row_products(r, keep):
        side = core if keep else 1 - core
        specs, args = [], []
        for h, j, w in ((h_main, 2, wd), (h_rest, 0, wr)) if r == 0 else ((h_main, 0, wg), (h_main, 1, wu), (h_rest, 1, wr)):
            n = w.shape[1]
            specs += [pl.BlockSpec((1, RING, 1, RING * rows, n), lambda i, j=j: (j, 0, side, 0, 0)), pl.BlockSpec((width, n), lambda i: (i, 0))]
            args += [h, w]
        wide = pl.BlockSpec((RING, RING, rows, width), lambda i: (0, 0, 0, i))
        terms = len(args) // 2
        if keep:
            specs.append(wide)
            args.append(rc.at[r])

        def body(*refs):
            total = None
            for i in range(terms):
                h = refs[2 * i][...].reshape(RING * RING * rows, refs[2 * i].shape[-1])
                prod = dot(h, refs[2 * i + 1][...], 1, 1)
                total = prod if total is None else total + prod
            if keep:
                total = total + refs[-2][...].astype(F32).reshape(total.shape)
            refs[-1][...] = total.astype(BF16).reshape(RING, RING, rows, width)

        pltpu.emit_pipeline(body, grid=(blocks,), in_specs=specs, out_specs=[wide])(*args, (part if keep else give).at[r])

    def core_copy(r):
        return rcopy(give.at[r], rc.at[r], c_s.at[r], c_r.at[r], near(0, 1))

    def give_rows(r):
        row_products(r, False)
        core_copy(r).start()

    def forward_phase(rowbuf, av, bv, gv, hst, hst_rest, wv_a, wv_r):
        held = {}

        fulls = (wg, wu, wd, wr)
        REST = 3
        def shard_load(t):
            return pltpu.make_async_copy((sg, su, sd)[t], held["shard"].at[t], sh_sem.at[t])

        def cut_pieces(t):
            if t == REST:
                for u in range(3):
                    for j in range(n8):
                        held["rests"][j, :, u * rest:(u + 1) * rest] = held["shard"][u, :, j * nf + main:(j + 1) * nf]
            else:
                for j in range(n8):
                    held["pieces"][t, j] = held["shard"][t, :, j * nf:j * nf + main]
            own_piece(t).start()

        def piece(t, j):
            return held["rests"].at[j] if t == REST else held["pieces"].at[t, j]

        def own_piece(t):
            return pltpu.make_async_copy(piece(t, i8), slot(t, 0, NEAR[0]), own_sem.at[t])

        def go(make, *args):
            make(*args).start()

        def slot(t, k, source):
            dx, dc = source
            return fulls[t].at[pl.ds(slot_at[k][dx][dc], dp)]

        def source(k):
            dx, dc = NEAR[k]
            return (RING - dx) % RING, dc

        def back(side):
            return 3 if side == 0 else 1

        def ahead(side):
            return 1 if side == 0 else 3

        def exchange_copy(t, k):
            return copy(piece(t, peer(*NEAR[k])), slot(t, 0, NEAR[0]), ex_s.at[t], ex_r.at[t, k], near(*NEAR[k]))

        def exchange(t, k):
            go(exchange_copy, t, k)

        def z_first_copy(t, side, k):
            here = slot(t, 0, source(k))
            return copy(here if k else piece(t, i8), here, z1_s.at[t, side], z1_sem(t, side, k), zdev(ahead(side)))

        def z_first(t, k):
            if k:
                here = slot(t, 0, source(k))
                all_in(here, ex_r.at[t, k])
            for side in range(2):
                go(z_first_copy, t, side, k)

        def z1_sem(t, side, k):
            return z1_r.at[t, side, k % (n8 // 2)] if (k < n8 // 2) == (side == 0) else zn_r.at[t, side]

        def some(t, count):
            return fulls[t].at[pl.ds(0, count * dp)]

        def z_second_copy(t, side, k):
            there = slot(t, back(side), source(k + side * (n8 // 2)))
            return copy(there, there, z2_s.at[t, side], z2_r.at[t, side], zdev(ahead(side)))

        def z_second(t, side, k):
            kk = k + side * (n8 // 2)
            all_in(slot(t, back(side), source(kk)), z1_sem(t, side, kk))
            go(z_second_copy, t, side, k)

        def weights_done(t):
            if (WD, t) not in LATE_STEPS:
                own_wait(t)
            for side in range(2):
                all_in(some(t, n8 // 2), zn_r.at[t, side])
                all_in(some(t, n8 // 2), z2_r.at[t, side])
            w_load(t).start()

        cut = d * 11 // 28
        rings = ((tok, tok_all, pl.ds(0, d), True), (grad, grad_all, pl.ds(0, cut), True), (grad, grad_all, pl.ds(cut, d - cut), False))

        def axis(r, n):
            return xdev if rings[r][3] == (n == 1) else ydev

        def block(r, da, db, flip=0, lo=0, size=rows):
            dx, dy = (da, db) if rings[r][3] else (db, da)
            first = rows_at[dx][dy][flip]
            return rings[r][1].at[pl.ds(pl.multiple_of(first + lo, half_rows) if lo else first, size), rings[r][2]]

        def own_block(r):
            return rings[r][0].at[:, rings[r][2]]

        def to_core_copy(r, ia, ib):
            there = block(r, DELTAS[ia], DELTAS[ib])
            return copy(own_block(r) if ia == 0 and ib == 0 else there, there, cc_s.at[r], cc_r.at[ia if r == 0 else RING - 1 + r], near(0, 1))

        def to_core(r, ia, ib):
            go(to_core_copy, r, ia, ib)

        def first_copy(r, side):
            return copy(own_block(r), block(r, 0, 0), p1_s.at[r], p1_r.at[r, side], axis(r, 1)(ahead(side)))

        def first_own(r, side):
            go(first_copy, r, side)

        def first_far_copy(r, side):
            part = block(r, back(side), 0, 0, side * half_rows, half_rows)
            return copy(part, part, p2_s.at[r], p2_r.at[r], axis(r, 1)(ahead(side)))

        def first_forward(r, side):
            there = block(r, back(side), 0)
            all_in(there, p1_r.at[r, side])
            go(first_far_copy, r, side)

        def block_on(r, ia):
            if ia == 3:
                all_in(block(r, 2, 0), p2_r.at[r])
            for side in range(2):
                go(second_copy, r, side, ia)
            to_core(r, ia, 0)

        def second_copy(r, side, ia):
            there = block(r, DELTAS[ia], 0)
            return copy(there if ia else own_block(r), there, q1_s.at[r], q1_r.at[r, side, ia], axis(r, 2)(ahead(side)))

        def second_far_copy(r, ia):
            side = ia // 2
            there = block(r, DELTAS[ia], back(side))
            return copy(there, there, q2_s.at[r], q2_r.at[r, ia], axis(r, 2)(ahead(side)))

        def second_forward(r, ia, side):
            there = block(r, DELTAS[ia], back(side))
            all_in(there, q1_r.at[r, side, ia])
            if ia // 2 == side:
                go(second_far_copy, r, ia)
            to_core(r, ia, 1 if side == 0 else 2)

        def second_far(r, ia):
            there = block(r, DELTAS[ia], 2)
            all_in(there, q2_r.at[r, ia])
            to_core(r, ia, 3)

        def some_rows(r, count):
            return rings[r][1].at[pl.ds(0, count * rows), rings[r][2]]

        def chunk_in(ia):
            all_in(some_rows(0, RING), cc_r.at[ia])

        def rows_in(r):
            all_in(some_rows(r, RING * RING), cc_r.at[RING - 1 + r])

        def own_wait(t):
            there = slot(t, 0, NEAR[0])
            pltpu.make_async_copy(there, there, own_sem.at[t]).wait()

        def own_rows(r):
            return pltpu.make_async_copy(own_block(r), block(r, 0, 0), own_sem.at[4 + r])

        def w_load(t):
            return pltpu.make_async_copy(fulls[t], (wv_a, held["wv_b"], wv_a, wv_r)[t], wv_sem.at[t])

        def row_load(src, i, buf):
            return pltpu.make_async_copy(src.at[chunk_rows(i)], rowbuf.at[buf], row_sem.at[buf])

        def chunk_loop(src, products, elementwise, between):
            row_load(src, 0, 0).start()
            between[0]()
            row_load(src, 1, 1).start()
            row_load(src, 0, 0).wait()
            products(0, 0)

            def body(i, carry):
                buf = lax.rem(i, 2)

                @pl.when(i + 1 < n_chunk)
                def _():
                    row_load(src, i + 1, 1 - buf).start()

                for k, step in enumerate(between[1:], 1):
                    pl.when(i == k)(step)
                row_load(src, i, buf).wait()
                free(elementwise, i - 1)
                elementwise(i - 1, 1 - buf, lambda: products(i, buf))
                return carry

            lax.fori_loop(1, n_chunk, body, 0)
            free(elementwise, n_chunk - 1)
            elementwise(n_chunk - 1, (n_chunk - 1) % 2, lambda: None)

        def free(elementwise, i):
            @pl.when(i >= 2)
            def _():
                for cp in copies_of[elementwise](i - 2):
                    cp.wait()

        def chunk_rows(i):
            return pl.ds(pl.multiple_of(i * chunk, chunk), chunk)

        def h_copies(i, which, names):
            xx, c = lax.div(i, 2), lax.rem(i, 2)
            cs = [pltpu.make_async_copy(hst.at[c, n], h_main.at[j, xx, c], hst_sem.at[c, n]) for n, j in enumerate(names)]
            return cs + [pltpu.make_async_copy(hst_rest.at[which, c], h_rest.at[which, xx, c], hst_sem.at[c, 2])]

        def keep(i, c, values):
            which = len(values) - 1
            for n, (j, v) in enumerate(values):
                low = v.astype(BF16)
                hst[c, n] = low[:, :main]
                hst_rest[which, c, :, j * rest:(j + 1) * rest] = low[:, main:]
                ff[j, :, chunk_rows(i)] = low.T

        def kept(elementwise):
            for i in (n_chunk - 2, n_chunk - 1):
                for cp in copies_of[elementwise](i):
                    cp.wait()

        def gate_work():
            def place(k):
                ia, flip = lax.div(k, 2), lax.rem(k, 2)
                delta = lax.rem(3 * ia + 3 * lax.div(ia, 2) + 2 * lax.div(ia, 3), RING)
                return 2 * lax.rem(x + delta, RING) + lax.rem(core + flip, 2)

            def body(k, carry):
                for n, group in enumerate(GATE_STEPS):
                    if group:
                        pl.when(k == n)(functools.partial(run, group))

                @pl.when(k < n_chunk)
                def _():
                    row_load(tok_all, place(k), lax.rem(k, 2)).start()

                @pl.when(k >= 1)
                def _():
                    i, buf = place(k - 1), lax.rem(k - 1, 2)
                    row_load(tok_all, i, buf).wait()
                    rb_ = rowbuf[buf]
                    av[chunk_rows(i), :main] = jnp.dot(rb_, wv_a[...], preferred_element_type=F32).astype(BF16)
                    both = jnp.dot(rb_, wv_r[...], preferred_element_type=F32).astype(BF16)
                    av[chunk_rows(i), main:] = both[:, :rest]
                    bv[chunk_rows(i), main:] = both[:, rest:2 * rest]

                return carry

            lax.fori_loop(0, n_chunk + 1, body, 0)

        def up_products(i, buf):
            bv[chunk_rows(i), :main] = jnp.dot(rowbuf[buf], held["wv_b"][...], preferred_element_type=F32).astype(BF16)

        def hidden(i, c, beside):
            a, b = av[chunk_rows(i)].astype(F32), bv[chunk_rows(i)].astype(F32)
            beside()
            keep(i, c, ((2, a * jax.nn.sigmoid(a) * b),))
            start(copies_of[hidden](i))

        def down_products(i, buf):
            rb_ = rowbuf[buf]
            lanes = 2 * rest // LANE * LANE
            low = jnp.dot(rb_, wv_r[:, lanes:], preferred_element_type=F32)[:, 2 * rest - lanes:3 * rest - lanes]
            gv[buf] = jnp.concatenate([jnp.dot(rb_, wv_a[...], preferred_element_type=F32), low], axis=1).astype(BF16)

        def backward(i, c, beside):
            g = gv[c].astype(F32)
            a, b = av[chunk_rows(i)].astype(F32), bv[chunk_rows(i)].astype(F32)
            beside()
            sig = jax.nn.sigmoid(a)
            keep(i, c, ((0, g * b * sig * (1.0 + a * (1.0 - sig))), (1, g * (a * sig))))
            start(copies_of[backward](i))

        copies_of = {hidden: lambda i: h_copies(i, 0, (2,)), backward: lambda i: h_copies(i, 1, (0, 1))}

        steps = (exchange, z_first, z_second, first_own, first_forward, block_on, second_forward, second_far, weights_done, chunk_in)

        def run(group):
            for which, *args in group:
                steps[which](*args)

        def rows_ready():
            run(UP_STEPS[-1])
            for r in (1, 2):
                own_rows(r).wait()
                rows_in(r)
            blk_load(plan[0][0], 0, plan[0][1]).start()

        def gather_phase(shard, pieces, rests, wv_b):
            held.update(shard=shard, pieces=pieces, rests=rests, wv_b=wv_b)
            with jax.named_scope("begin"):
                for t in range(3):
                    shard_load(t).start()
                shard_load(0).wait()
                cut_pieces(0)
                pl.semaphore_wait(barrier, len(others))
                for r in range(3):
                    own_rows(r).start()
            with jax.named_scope("gather"):
                cut = {0}
                for step in GATHER_STEPS:
                    if step[0] in (EX, Z1) and step[1] not in cut:
                        if len(cut) == 1:
                            rests[...] = jnp.zeros_like(rests)
                            hst_rest[...] = jnp.zeros_like(hst_rest)
                            shard_load(1).wait()
                            shard_load(2).wait()
                        cut.add(step[1])
                        cut_pieces(step[1])
                    run((step,))
                own_rows(0).wait()
                w_load(0).wait()
                w_load(REST).wait()
            with jax.named_scope("gate"):
                gate_work()
            with jax.named_scope("up"):
                run(UP_STEPS[0])
                w_load(1).wait()
                chunk_loop(tok_all, up_products, hidden, [functools.partial(run, group) for group in ((),) + UP_STEPS[1:-1]] + [rows_ready])
                kept(hidden)
            for _, t in LATE_STEPS:
                own_wait(t)
            for t in range(4):
                all_out(some(t, n8 - 1), ex_s.at[t])
                for side in range(2):
                    all_out(some(t, n8), z1_s.at[t, side])

        pl.run_scoped(
            gather_phase, pltpu.VMEM((3,) + sg.shape, BF16), pltpu.VMEM((3, n8, dp, main), BF16), pltpu.VMEM((n8, dp, packed), BF16),
            pltpu.VMEM((d, main), BF16))
        run_order({
            "far_block": far_block, "next_products": next_products, "give_rows": give_rows, "late": functools.partial(run, LATE_STEPS),
        }, EARLY_ORDER)
        with jax.named_scope("down"):
            w_load(2).wait()
            chunk_loop(grad_all, down_products, backward, [lambda: None])
            kept(backward)
        for t in range(4):
            for side in range(2):
                all_out(some(t, n8 // 2), z2_s.at[t, side])
        for r in range(3):
            for count, sem in ((2, p1_s), (1, p2_s), (2 * RING, q1_s), (RING, q2_s), (RING * RING, cc_s)):
                all_out(some_rows(r, count), sem.at[r])

    def backward_phase(tmp, stage):
        def next_adds(t):
            all_in(ra.at[t], a_r.at[t])
            cs = [pltpu.make_async_copy(ra.at[t, at], tmp.at[s, at], tmp_sem.at[s]) for s, at in ((0, lo), (1, hi))]
            start(cs)
            for c, (s, at) in zip(cs, ((0, lo), (1, hi))):
                c.wait()
                nxt[t, s, at] += tmp[s, at]
            for tile in range(tiles):
                start(c for s, c in enumerate(unit_copies(t, tile)) if (s, tile) not in early_units(t))

        def next_blocks(t):
            next_products(t)
            next_adds(t)

        def own_block(t):
            all_out(ra.at[t], a_s.at[t])
            product(t, far.at[t])

        def slot(t):
            return Z_ORDER.index(t) % 2

        def hand_out(t, tile, part):
            parts = unit_parts(t, tile)
            for k in range(n8):
                dx, dc = NEAR[k]
                at = pl.ds(hand_at[dx][dc], dp)
                src, dst = stage.at[slot(t), tile, at], outs[t].at[i8, tile]

                def send(k=k, src=src, dst=dst):
                    if k:
                        rcopy(src, dst, e_s.at[t], e_r.at[t], near(*NEAR[k])).start()
                    else:
                        pltpu.make_async_copy(src, dst, out_sem.at[t]).start()

                if len(parts) == 1:
                    send()
                elif part == 0:
                    pl.when(xs[dx] < parts[0][2] // dp // 2)(send)
                else:
                    pl.when(xs[dx] >= parts[0][2] // dp // 2)(send)

        def handed(t):
            all_out(outs[t].at[pl.ds(0, n8 - 1)], e_s.at[t])
            pltpu.make_async_copy(outs[t].at[0], outs[t].at[0], out_sem.at[t]).wait()

        given = []

        def finish(t, tile):
            at = tile_rows(tile)
            wide = pl.ds(tile * LANE, LANE)
            for part, (n, first, size) in enumerate(unit_parts(t, tile)):
                lanes = pl.ds(first, size)
                all_in(rb.at[t, :, at, lanes], u_r.at[t, n])
                cs = [pltpu.make_async_copy(rb.at[t, s, at, lanes], tmp.at[s, at, lanes], tmp_sem.at[s]) for s in range(2)]
                start(cs)
                if t == Z_ORDER[2] and not given:
                    given.append(Z_ORDER[0])
                    handed(Z_ORDER[0])
                for c in cs:
                    c.wait()
                stage[slot(t), tile, lanes] = (far[t, wide, lanes] + tmp[0, wide, lanes] + tmp[1, wide, lanes]).T
                hand_out(t, tile, part)

        def on_y(r, n):
            return (r == 1) == (n == 1)

        def level(r, n):
            at = ys if on_y(r, n) else xs
            dev = ydev if on_y(r, n) else xdev
            if n == 1:
                def piece(k, h):
                    return part.at[r, pl.ds(2 * h, 2), at[k]] if on_y(r, n) else part.at[r, at[k], pl.ds(2 * h, 2)]
                return dev, piece, ra1, rb1, sd1, (a1_s, a1_r, f1_s, f1_r, d1_s, d1_r)

            def piece(k, h):
                return mid.at[r, at[k], pl.ds(h, 1)]
            return dev, piece, ra2, rb2, sd2, (a2_s, a2_r, f2_s, f2_r, d2_s, d2_r)

        def ring_a(r, n):
            dev, piece, rfar, _, _, sems = level(r, n)
            return [rcopy(piece(2, s), rfar.at[r, s], sems[0].at[r], sems[1].at[r], dev(1 + 2 * s)) for s in range(2)]

        def ring_f(r, n):
            dev, piece, _, rnear, _, sems = level(r, n)
            return [rcopy(piece(1 + 2 * s, 1 - s), rnear.at[r, s, 1 - s], sems[2].at[r], sems[3].at[r], dev(1 + 2 * s)) for s in range(2)]

        def ring_d(r, n):
            dev, _, _, rnear, dep, sems = level(r, n)
            return [rcopy(dep.at[r, s], rnear.at[r, s, s], sems[4].at[r], sems[5].at[r], dev(1 + 2 * s)) for s in range(2)]

        def add(grid, *terms):
            specs = []
            for ref, at, lead in terms:
                tail = ref.shape[lead:]
                specs.append(pl.BlockSpec((1,) * lead + tuple(tail), lambda *i, at=at, rank=len(tail): tuple(at(*i)) + (0,) * rank))

            def body(*refs):
                total = refs[0][...].astype(F32).reshape(refs[0].shape[-2:])
                for ref in refs[1:-1]:
                    total = total + ref[...].astype(F32).reshape(total.shape)
                refs[-1][...] = total.astype(BF16).reshape(refs[-1].shape)

            pltpu.emit_pipeline(body, grid=grid, in_specs=specs[:-1], out_specs=specs[-1:])(*[ref for ref, _, _ in terms])

        def ring_first(r, n):
            start(ring_a(r, n) + ring_f(r, n))

        def ring_dependent(r, n):
            _, _, rfar, _, _, sems = level(r, n)
            all_in(rfar.at[r], sems[1].at[r])
            here = y if on_y(r, n) else x
            if n == 1:
                def near_block(s, i):
                    at = lax.rem(here + 1 + 2 * s, RING)
                    return (2 * s + i, at) if on_y(r, n) else (at, 2 * s + i)

                add((2, 2), (part.at[r], near_block, 2), (ra1.at[r], lambda s, i: (s, i), 2), (sd1.at[r], lambda s, i: (s, i), 2))
            else:
                add((2,), (mid.at[r], lambda s: (lax.rem(here + 1 + 2 * s, RING), s), 2), (ra2.at[r], lambda s: (s, 0), 2),
                    (sd2.at[r], lambda s: (s, 0), 2))
            start(ring_d(r, n))

        def ring_last(r, n):
            _, _, rfar, _, _, sems = level(r, n)
            all_in(rfar.at[r], sems[3].at[r])
            all_in(rfar.at[r], sems[5].at[r])
            here = y if on_y(r, n) else x
            if n == 1:
                def own_at(h, i):
                    return (2 * h + i, here) if on_y(r, n) else (here, 2 * h + i)

                add((2, 2), (part.at[r], own_at, 2), (rb1.at[r, 0], lambda h, i: (h, i), 2),
                    (rb1.at[r, 1], lambda h, i: (h, i), 2), (mid.at[r], lambda h, i: (2 * h + i,), 1))
            else:
                own, res = ((tok_own, out), (grad_own, gin))[r]
                add((2,), (own, lambda h: (h,), 1), (mid.at[r], lambda h: (here, h), 2), (rb2.at[r, 0], lambda h: (h, 0), 2),
                    (rb2.at[r, 1], lambda h: (h, 0), 2), (res, lambda h: (h,), 1))

        def keep_rows(r):
            core_copy(r).wait_recv()
            row_products(r, True)

        run_order({
            "far_block": far_block, "next_products": next_products, "next_adds": next_adds, "next_blocks": next_blocks,
            "own_block": own_block, "finish": finish, "give_rows": give_rows, "keep_rows": keep_rows, "ring_first": ring_first,
            "ring_dependent": ring_dependent, "ring_last": ring_last,
        }, LATE_ORDER)

        for t in range(3):
            all_out(nxt.at[t], u_s.at[t])
        for r in range(2):
            core_copy(r).wait_send()
            for n in (1, 2):
                _, _, rfar, _, _, sems = level(r, n)
                for sem in sems[::2]:
                    all_out(rfar.at[r], sem.at[r])
        for t in Z_ORDER:
            with jax.named_scope(f"handed_{t}"):
                all_in(outs[t].at[pl.ds(0, n8 - 1)], e_r.at[t])
                if t not in given:
                    handed(t)

    pl.run_scoped(
        forward_phase,
        pltpu.VMEM((2, chunk, d), BF16),
        pltpu.VMEM((tokens, nf), BF16),
        pltpu.VMEM((tokens, nf), BF16),
        pltpu.VMEM((2, chunk, nf), BF16),
        pltpu.VMEM((2, 2, chunk, main), BF16),
        pltpu.VMEM((2, 2, chunk, packed), BF16),
        pltpu.VMEM((d, main), BF16),
        pltpu.VMEM((d, packed), BF16),
    )
    pl.run_scoped(backward_phase, pltpu.VMEM((2, tiles * LANE, cols), F32), pltpu.VMEM((2, tiles, cols, LANE), F32))


def layer(sg, su, sd, tok, grad):
    n8 = 2 * RING
    dp, nf = sg.shape[0], sg.shape[1] // n8
    rows, d = tok.shape
    tokens = rows * RING * n8
    cols = d // RING
    tiles = -(-nf // LANE)
    padded = tiles * LANE
    main = nf // LANE * LANE
    packed = -(-3 * (nf - main) // LANE) * LANE
    hbm = pl.BlockSpec(memory_space=pl.ANY)
    dma = pltpu.SemaphoreType.DMA
    sds = jax.ShapeDtypeStruct
    halves = (2, rows // 2, d)
    res = pl.pallas_call(
        layer_kernel,
        out_shape=[sds((n8, tiles, dp, LANE), F32)] * 3 + [sds(halves, BF16)] * 2 + [
            sds((d, main), BF16), sds((d, main), BF16), sds((d, main), BF16), sds((d, packed), BF16), sds((tokens, d), BF16), sds((tokens, d), BF16),
            sds((3, RING, 2, RING * rows, main), BF16), sds((2, RING, 2, RING * rows, packed), BF16),
            sds((3, nf, cols), F32), sds((3, 2, nf, cols), F32),
            sds((2, RING, RING, rows, d), BF16), sds((2, RING, RING, rows, d), BF16), sds((2, RING, RING, rows, d), BF16),
            sds((2, 2, 2, rows, d), BF16), sds((2, 2, 2, 2, rows, d), BF16), sds((2, 2, 2, rows, d), BF16),
            sds((2, RING, 2, rows // 2, d), BF16),
            sds((2, 2, 1, rows // 2, d), BF16), sds((2, 2, 2, 1, rows // 2, d), BF16), sds((2, 2, 1, rows // 2, d), BF16),
        ],
        in_specs=[hbm] * 7,
        out_specs=[hbm] * 25,
        scratch_shapes=[
            pltpu.VMEM((3, nf, tokens), BF16),
            pltpu.VMEM((2, tokens, cols), BF16),
            pltpu.VMEM((3, padded, cols), F32),
            pltpu.VMEM((3, 2, nf, cols), F32),
            dma((7,)),
            dma((4,)), dma((4, n8)),
            dma((4, 2)), dma((4, 2, n8 // 2)), dma((4, 2)),
            dma((4, 2)), dma((4, 2)),
            dma((3,)), dma((3, 2)),
            dma((3,)), dma((3,)),
            dma((3,)), dma((3, 2, RING)),
            dma((3,)), dma((3, RING)),
            dma((3,)), dma((RING + 2,)),
            dma((3,)), dma((4,)), dma((2,)), dma((2, 3)), dma((2,)), dma((2,)),
            dma((3,)), dma((3,)),
            dma((3,)), dma((3, tiles + 1)),
            dma((3,)), dma((3,)),
            dma((3,)),
            dma((2,)), dma((2,)),
        ] + [dma((2,))] * 12,
        compiler_params=pltpu.CompilerParams(collective_id=0, has_side_effects=True, vmem_limit_bytes=67043328),
        cost_estimate=pl.CostEstimate(flops=18 * nf * tokens * d, bytes_accessed=300_000_000, transcendentals=0),
        name="layer",
    )(sg, su, sd, tok, grad, tok.reshape(halves), grad.reshape(halves))
    return res[:3], res[3].reshape(rows, d), res[4].reshape(rows, d)


def assemble_kernel(og, ou, od, out, gin, g, u, w, res, gres, buf, flat, in_sem, out_sem, row_buf, row_sem):
    n8, nf = og.shape[0], g.shape[1] // og.shape[0]
    srcs, dsts = (og, ou, od), (g, u, w)
    rows_in = [pltpu.make_async_copy(src, row_buf.at[r], row_sem.at[r]) for r, src in enumerate((out, gin))]
    loads = [pltpu.make_async_copy(src, buf.at[t], in_sem.at[t]) for t, src in enumerate(srcs)]
    stores = [pltpu.make_async_copy(flat.at[t], dst, out_sem.at[t]) for t, dst in enumerate(dsts)]
    for c in loads + rows_in:
        c.start()
    for t in range(3):
        loads[t].wait()
        for j in range(n8):
            flat[t, :, j * nf:(j + 1) * nf] = jnp.concatenate([buf[t, j, tile] for tile in range(buf.shape[2])], axis=1)[:, :nf]
        stores[t].start()
    rows_out = [pltpu.make_async_copy(row_buf.at[r], dst, row_sem.at[r]) for r, dst in enumerate((res, gres))]
    for c in rows_in:
        c.wait()
    for c in rows_out:
        c.start()
    for c in stores + rows_out:
        c.wait()


def assemble(sums, out, gin, ff):
    dp = sums[0].shape[2]
    hbm = pl.BlockSpec(memory_space=pl.ANY)
    dma = pltpu.SemaphoreType.DMA
    sds = jax.ShapeDtypeStruct
    return pl.pallas_call(
        assemble_kernel,
        out_shape=[sds((dp, ff), F32)] * 3 + [sds(out.shape, BF16)] * 2,
        in_specs=[hbm] * 5,
        out_specs=[hbm] * 5,
        scratch_shapes=[
            pltpu.VMEM((3,) + sums[0].shape, F32), pltpu.VMEM((3, dp, ff), F32), dma((3,)), dma((3,)),
            pltpu.VMEM((2,) + out.shape, BF16), dma((2,)),
        ],
        compiler_params=pltpu.CompilerParams(vmem_limit_bytes=63 * 1024 * 1024),
        name="assemble",
    )(*sums, out, gin)


def solution(mesh):
    nz, ny, nd = mesh.shape["datb"], mesh.shape["model"], mesh.shape["data"]
    fine = Mesh(mesh.devices.reshape(nz, ny, nd // 2, 2), ("datb", "model", "x", "core"))

    def local_step(tok_loc, wg_loc, wu_loc, wd_loc, grad_loc):
        sums, out, grad_in = layer(wg_loc, wu_loc, wd_loc.T, tok_loc, grad_loc)
        grad_gate, grad_up, grad_down_t, out, grad_in = assemble(sums, out, grad_in, wg_loc.shape[1])
        return out, grad_in, grad_gate, grad_up, grad_down_t.T

    return jax.shard_map(local_step, mesh=fine, in_specs=(ROW_SPEC, GATE_SPEC, GATE_SPEC, DOWN_SPEC, ROW_SPEC), out_specs=(ROW_SPEC, ROW_SPEC, GATE_SPEC, GATE_SPEC, DOWN_SPEC), check_vma=False)
```

```python
import functools

import jax
import jax.numpy as jnp
from jax import lax
from jax.experimental import pallas as pl
from jax.experimental.pallas import tpu as pltpu
from jax.sharding import Mesh
from jax.sharding import PartitionSpec as P

ROW_SPEC = P(("datb", "x", "core", "model"), None)
GATE_SPEC = P(("datb", "x", "core"), "model")
DOWN_SPEC = P("model", ("datb", "x", "core"))
BF16 = jnp.bfloat16
F32 = jnp.float32
MESH_ID = pl.DeviceIdType.MESH
RING = 4
NEAR = ((0, 0), (0, 1), (1, 0), (3, 0), (1, 1), (3, 1), (2, 0), (2, 1))
DELTAS = (0, 3, 1, 2)
LANE = 128
OUT_COLS = 512
EX, Z1, Z2, P1, P2, BL, Q1, Q2, WD, CI = range(10)
GATHER_STEPS = (
    (Z1, 0, 0), (P1, 0, 0), (P1, 0, 1), (EX, 0, 1), (BL, 0, 0), (P1, 2, 0), (P1, 2, 1), (EX, 0, 2), (Z1, 3, 0), (EX, 3, 1), (EX, 3, 2),
    (EX, 3, 3), (EX, 3, 4), (EX, 3, 5), (EX, 3, 6), (EX, 3, 7), (Z1, 1, 0), (EX, 1, 1), (Z1, 2, 0), (EX, 2, 1), (EX, 0, 3), (BL, 1, 0),
    (Z1, 3, 1), (EX, 0, 4), (EX, 0, 5), (Z1, 0, 1), (Z1, 1, 1), (Z2, 3, 0, 0), (Z1, 2, 1), (EX, 0, 6), (EX, 0, 7), (Z2, 0, 0, 0),
    (Z2, 1, 0, 0), (EX, 1, 2), (EX, 1, 3), (Z2, 2, 0, 0), (Z2, 3, 0, 1), (P2, 0, 0), (P2, 0, 1), (BL, 0, 1), (Q1, 0, 0, 1), (Z1, 3, 2),
    (Z1, 3, 3), (Z1, 3, 4), (Q1, 0, 0, 0), (Z1, 3, 5), (Z2, 0, 0, 1), (EX, 1, 4), (EX, 1, 5), (P2, 2, 1), (Z1, 3, 6), (EX, 1, 6),
    (EX, 1, 7), (Z1, 3, 7), (Z1, 0, 2), (Q1, 1, 0, 1), (Z2, 3, 1, 0), (Z2, 3, 1, 1), (Z1, 0, 3), (EX, 2, 2), (EX, 2, 3), (Z2, 3, 1, 2),
    (BL, 0, 2), (Z2, 3, 1, 3), (Z1, 0, 4), (EX, 2, 4), (EX, 2, 5), (Z1, 0, 5), (EX, 2, 6), (EX, 2, 7), (Z2, 3, 0, 2), (Q1, 0, 1, 1),
    (Z2, 3, 0, 3), (Z1, 0, 6), (P1, 1, 0), (P1, 1, 1), (Q1, 0, 1, 0), (Z1, 0, 7), (BL, 2, 2), (Z2, 0, 1, 0), (Z1, 1, 2), (Z2, 0, 1, 1),
    (Z2, 0, 0, 2), (Q2, 0, 0), (Z2, 0, 1, 2), (Z2, 0, 0, 3), (BL, 2, 0), (BL, 0, 3), (Q1, 0, 2, 1), (Z2, 0, 1, 3), (Z1, 1, 3), (Z1, 1, 4),
    (WD, 3), (Z1, 1, 5), (Q1, 0, 2, 0), (Z1, 1, 6), (P2, 2, 0), (BL, 2, 1), (P2, 1, 0), (P2, 1, 1), (Z1, 1, 7), (Q1, 0, 3, 1),
    (Q1, 1, 0, 0), (Z2, 1, 0, 1), (Q1, 2, 2, 0), (Q1, 2, 2, 1), (Z2, 1, 0, 2), (BL, 1, 1), (Q2, 0, 1), (WD, 0), (Z2, 1, 1, 0), (CI, 0),
)
GATE_STEPS = (
    (),
    (),
    (
        (Z1, 2, 2),
    ),
    (
        (Q2, 0, 2), (Z2, 1, 1, 1), (Z2, 1, 0, 3), (Q1, 2, 0, 0), (Q1, 2, 0, 1), (BL, 1, 2), (CI, 1),
    ),
    (
        (Z2, 1, 1, 2), (Z1, 2, 3),
    ),
    (
        (Q1, 0, 3, 0), (Z2, 1, 1, 3), (Z1, 2, 4), (CI, 2),
    ),
    (
        (Z1, 2, 5), (Q1, 2, 1, 0), (Q1, 2, 1, 1), (BL, 2, 3), (BL, 1, 3), (Z1, 2, 6), (Q2, 0, 3),
    ),
    (
        (Q2, 1, 0), (Z1, 2, 7), (CI, 3),
    ),
    (
        (Q2, 2, 0), (Q2, 2, 2), (Z2, 2, 0, 1), (Q1, 1, 1, 0), (Q1, 1, 1, 1),
    ),
)
UP_STEPS = (
    (
        (Z2, 2, 0, 2), (Q1, 1, 2, 1), (WD, 1),
    ),
    (
        (Q2, 2, 1), (Q1, 2, 3, 1), (Q1, 1, 2, 0),
    ),
    (
        (Z2, 2, 1, 0), (Z2, 2, 0, 3), (Q1, 1, 3, 1),
    ),
    (
        (Z2, 2, 1, 1), (Q1, 1, 3, 0),
    ),
    (
        (Q2, 1, 2), (Z2, 2, 1, 2), (Q1, 2, 3, 0),
    ),
    (
        (Q2, 1, 1), (Z2, 2, 1, 3),
    ),
    (
        (Q2, 1, 3), (Q2, 2, 3),
    ),
    (),
)
LATE_STEPS = (
    (WD, 2),
)
Z_ORDER = (2, 0, 1)
EARLY_ORDER = (
    ("far_block", 2), ("next_products", 2), ("late",), ("give_rows", 0),
)
LATE_ORDER = (
    ("next_adds", 2), ("own_block", 2), ("keep_rows", 0), ("ring_first", 0, 1), ("finish", 2, 0), ("far_block", 0), ("give_rows", 1),
    ("finish", 2, 3), ("finish", 2, 1), ("finish", 2, 4), ("ring_dependent", 0, 1), ("finish", 2, 2), ("far_block", 1), ("keep_rows", 1),
    ("ring_first", 1, 1), ("next_blocks", 0), ("own_block", 0), ("next_blocks", 1), ("own_block", 1), ("finish", 0, 0),
    ("ring_dependent", 1, 1), ("finish", 0, 1), ("ring_last", 0, 1), ("ring_first", 0, 2), ("finish", 0, 2), ("finish", 0, 3),
    ("finish", 0, 4), ("ring_last", 1, 1), ("ring_first", 1, 2), ("ring_dependent", 0, 2), ("finish", 1, 0), ("ring_dependent", 1, 2),
    ("ring_last", 0, 2), ("finish", 1, 1), ("finish", 1, 2), ("ring_last", 1, 2), ("finish", 1, 3), ("finish", 1, 4),
)


def dot(a, b, ca, cb):
    return lax.dot_general(a, b, (((ca,), (cb,)), ((), ())), preferred_element_type=F32)


def layer_kernel(sg, su, sd, tok, grad, tok_own, grad_own,
                 og, ou, od, out, gin, wg, wu, wd, wr, tok_all, grad_all, h_main, h_rest, ra, rb, give, rc, part, ra1, rb1, sd1, mid, ra2, rb2, sd2,
                 ff, blk, far, nxt,
                 own_sem, ex_s, ex_r, z1_s, z1_r, zn_r, z2_s, z2_r, p1_s, p1_r, p2_s, p2_r, q1_s, q1_r, q2_s, q2_r, cc_s, cc_r,
                 sh_sem, wv_sem, row_sem, hst_sem, blk_sem, tmp_sem, a_s, a_r, u_s, u_r, e_s, e_r, out_sem,
                 c_s, c_r, a1_s, a1_r, f1_s, f1_r, d1_s, d1_r, a2_s, a2_r, f2_s, f2_r, d2_s, d2_r):
    z, y = lax.axis_index("datb"), lax.axis_index("model")
    x, core = lax.axis_index("x"), lax.axis_index("core")
    i8 = 2 * x + core
    n8 = 2 * RING
    rows, d = tok.shape
    half_rows = rows // 2
    chunk = RING * rows
    n_chunk = n8
    nf, tokens = ff.shape[1:]
    dp = sg.shape[0]
    half = nf // 2
    main = wg.shape[1]
    rest = nf - main
    packed = wr.shape[1]
    cols = blk.shape[2]
    tiles = far.shape[1] // LANE
    outs = (og, ou, od)

    zs, ys, xs = ([v] + [lax.rem(v + k, RING) for k in range(1, RING)] for v in (z, y, x))
    cores = (core, 1 - core)
    peers = [[2 * v + c for c in cores] for v in xs]
    slot_at = [[[pl.multiple_of((zz * n8 + peers[dx][dc]) * dp, 16) for dc in range(2)] for dx in range(RING)] for zz in zs]
    hand_at = [[pl.multiple_of(p * dp, 8) for p in row] for row in peers]
    rows_at = [[[pl.multiple_of((peers[dx][dc] * RING + yy) * rows, half_rows) for dc in range(2)] for yy in ys] for dx in range(RING)]
    lanes_at = [pl.multiple_of(zz * cols, LANE) for zz in zs]

    def peer(dx, dc):
        return peers[dx][dc]

    def zdev(k):
        return {"datb": zs[k]}

    def xdev(k):
        return {"x": xs[k]}

    def ydev(k):
        return {"model": ys[k]}

    def near(dx, dc):
        return {"x": xs[dx], "core": cores[dc]}

    def copy(src, dst, s, r, dev):
        return pltpu.make_async_remote_copy(src_ref=src, dst_ref=dst, send_sem=s, recv_sem=r, device_id=dev, device_id_type=MESH_ID)

    rcopy = copy

    def all_in(ref, sem):
        copy(ref, ref, sem, sem, zdev(1)).wait_recv()

    def all_out(ref, sem):
        copy(ref, ref, sem, sem, zdev(1)).wait_send()

    def start(copies):
        for c in copies:
            c.start()

    def received(copies):
        for c in copies:
            c.wait_recv()

    def sent(copies):
        for c in copies:
            c.wait_send()

    def run_order(fns, order):
        for fn, *args in order:
            with jax.named_scope("_".join(str(v) for v in [fn, *args])):
                fns[fn](*args)

    barrier = pltpu.get_barrier_semaphore()
    others = [zdev(1), zdev(3), ydev(1), ydev(3)] + [near(*n) for n in NEAR[1:]]
    for dev in others:
        pl.semaphore_signal(barrier, inc=1, device_id=dev, device_id_type=MESH_ID)

    def blk_load(t, slot, k):
        src = tok_all if t < 2 else grad_all
        return pltpu.make_async_copy(src.at[:, pl.ds(lanes_at[k], cols)], blk.at[slot], blk_sem.at[slot])

    plan = []
    for fn, *args in EARLY_ORDER + LATE_ORDER:
        plan += [(args[0], k) for k in {"far_block": (2,), "next_blocks": (1, 3), "next_products": (1, 3), "own_block": (0,)}.get(fn, ())]
    taken = []

    def next_block():
        n = len(taken)
        taken.append(n)
        blk_load(plan[n][0], n % 2, plan[n][1]).wait()
        if n + 1 < len(plan):
            blk_load(plan[n + 1][0], (n + 1) % 2, plan[n + 1][1]).start()
        return n % 2

    def product(t, dst):
        slot = next_block()
        step = 2 * LANE

        def one(n, carry):
            lanes = pl.ds(pl.multiple_of(jnp.minimum(n * step, cols - step), LANE), step)
            dst[:nf, lanes] = jnp.dot(ff[t], blk[slot, :, lanes], preferred_element_type=F32)
            return carry

        lax.fori_loop(0, -(-cols // step), one, 0)

    lo, hi = pl.ds(0, half), pl.ds(half, half)

    def a_copies(t, first=0, size=cols):
        lanes = pl.ds(first, size)
        return [rcopy(far.at[t, at, lanes], ra.at[t, at, lanes], a_s.at[t], a_r.at[t], zdev(k)) for at, k in ((lo, 1), (hi, 3))]

    def tile_rows(tile):
        return pl.ds(tile * LANE, min(LANE, nf - tile * LANE))

    def unit_parts(t, tile):
        if (t, tile) != (Z_ORDER[2], tiles - 1):
            return [(tile, 0, cols)]
        first = -(-cols // 2 // LANE) * LANE
        return [(tile, 0, first), (tiles, first, cols - first)]

    def unit_copies(t, tile):
        at = tile_rows(tile)
        cs = []
        for n, first, size in unit_parts(t, tile):
            lanes = pl.ds(first, size)
            cs += [rcopy(nxt.at[t, s, at, lanes], rb.at[t, s, at, lanes], u_s.at[t], u_r.at[t, n], zdev(1 + 2 * s)) for s in range(2)]
        return cs

    def far_block(t):
        if t == Z_ORDER[0]:
            slot = next_block()
            for first in range(0, cols, 2 * LANE):
                size = min(2 * LANE, cols - first)
                lanes = pl.ds(first, size)
                far[t, :nf, lanes] = jnp.dot(ff[t], blk[slot, :, lanes], preferred_element_type=F32)
                start(a_copies(t, first, size))
        else:
            product(t, far.at[t])
            start(a_copies(t))

    def early_units(t):
        if ("next_products", t) not in EARLY_ORDER + LATE_ORDER:
            return ()
        free = [(0, tile) for tile in range(tiles) if tile * LANE >= half]
        return free + [(1, tile) for tile in range(tiles) if (tile + 1) * LANE <= half]

    def next_products(t):
        for s in range(2):
            product(t, nxt.at[t, s])
        for s, tile in early_units(t):
            unit_copies(t, tile)[s].start()

    blocks = d // min(OUT_COLS, d)
    width = d // blocks

    def row_products(r, keep):
        side = core if keep else 1 - core
        specs, args = [], []
        for h, j, w in ((h_main, 2, wd), (h_rest, 0, wr)) if r == 0 else ((h_main, 0, wg), (h_main, 1, wu), (h_rest, 1, wr)):
            n = w.shape[1]
            specs += [pl.BlockSpec((1, RING, 1, RING * rows, n), lambda i, j=j: (j, 0, side, 0, 0)), pl.BlockSpec((width, n), lambda i: (i, 0))]
            args += [h, w]
        wide = pl.BlockSpec((RING, RING, rows, width), lambda i: (0, 0, 0, i))
        terms = len(args) // 2
        if keep:
            specs.append(wide)
            args.append(rc.at[r])

        def body(*refs):
            total = None
            for i in range(terms):
                h = refs[2 * i][...].reshape(RING * RING * rows, refs[2 * i].shape[-1])
                prod = dot(h, refs[2 * i + 1][...], 1, 1)
                total = prod if total is None else total + prod
            if keep:
                total = total + refs[-2][...].astype(F32).reshape(total.shape)
            refs[-1][...] = total.astype(BF16).reshape(RING, RING, rows, width)

        pltpu.emit_pipeline(body, grid=(blocks,), in_specs=specs, out_specs=[wide])(*args, (part if keep else give).at[r])

    def core_copy(r):
        return rcopy(give.at[r], rc.at[r], c_s.at[r], c_r.at[r], near(0, 1))

    def give_rows(r):
        row_products(r, False)
        core_copy(r).start()

    def forward_phase(rowbuf, av, bv, gv, hst, hst_rest, wv_a, wv_r):
        held = {}

        fulls = (wg, wu, wd, wr)
        REST = 3
        def shard_load(t):
            return pltpu.make_async_copy((sg, su, sd)[t], held["shard"].at[t], sh_sem.at[t])

        def cut_pieces(t):
            if t == REST:
                for u in range(3):
                    for j in range(n8):
                        held["rests"][j, :, u * rest:(u + 1) * rest] = held["shard"][u, :, j * nf + main:(j + 1) * nf]
            else:
                for j in range(n8):
                    held["pieces"][t, j] = held["shard"][t, :, j * nf:j * nf + main]
            own_piece(t).start()

        def piece(t, j):
            return held["rests"].at[j] if t == REST else held["pieces"].at[t, j]

        def own_piece(t):
            return pltpu.make_async_copy(piece(t, i8), slot(t, 0, NEAR[0]), own_sem.at[t])

        def go(make, *args):
            make(*args).start()

        def slot(t, k, source):
            dx, dc = source
            return fulls[t].at[pl.ds(slot_at[k][dx][dc], dp)]

        def source(k):
            dx, dc = NEAR[k]
            return (RING - dx) % RING, dc

        def back(side):
            return 3 if side == 0 else 1

        def ahead(side):
            return 1 if side == 0 else 3

        def exchange_copy(t, k):
            return copy(piece(t, peer(*NEAR[k])), slot(t, 0, NEAR[0]), ex_s.at[t], ex_r.at[t, k], near(*NEAR[k]))

        def exchange(t, k):
            go(exchange_copy, t, k)

        def z_first_copy(t, side, k):
            here = slot(t, 0, source(k))
            return copy(here if k else piece(t, i8), here, z1_s.at[t, side], z1_sem(t, side, k), zdev(ahead(side)))

        def z_first(t, k):
            if k:
                here = slot(t, 0, source(k))
                all_in(here, ex_r.at[t, k])
            for side in range(2):
                go(z_first_copy, t, side, k)

        def z1_sem(t, side, k):
            return z1_r.at[t, side, k % (n8 // 2)] if (k < n8 // 2) == (side == 0) else zn_r.at[t, side]

        def some(t, count):
            return fulls[t].at[pl.ds(0, count * dp)]

        def z_second_copy(t, side, k):
            there = slot(t, back(side), source(k + side * (n8 // 2)))
            return copy(there, there, z2_s.at[t, side], z2_r.at[t, side], zdev(ahead(side)))

        def z_second(t, side, k):
            kk = k + side * (n8 // 2)
            all_in(slot(t, back(side), source(kk)), z1_sem(t, side, kk))
            go(z_second_copy, t, side, k)

        def weights_done(t):
            if (WD, t) not in LATE_STEPS:
                own_wait(t)
            for side in range(2):
                all_in(some(t, n8 // 2), zn_r.at[t, side])
                all_in(some(t, n8 // 2), z2_r.at[t, side])
            w_load(t).start()

        cut = d * 11 // 28
        rings = ((tok, tok_all, pl.ds(0, d), True), (grad, grad_all, pl.ds(0, cut), True), (grad, grad_all, pl.ds(cut, d - cut), False))

        def axis(r, n):
            return xdev if rings[r][3] == (n == 1) else ydev

        def block(r, da, db, flip=0, lo=0, size=rows):
            dx, dy = (da, db) if rings[r][3] else (db, da)
            first = rows_at[dx][dy][flip]
            return rings[r][1].at[pl.ds(pl.multiple_of(first + lo, half_rows) if lo else first, size), rings[r][2]]

        def own_block(r):
            return rings[r][0].at[:, rings[r][2]]

        def to_core_copy(r, ia, ib):
            there = block(r, DELTAS[ia], DELTAS[ib])
            return copy(own_block(r) if ia == 0 and ib == 0 else there, there, cc_s.at[r], cc_r.at[ia if r == 0 else RING - 1 + r], near(0, 1))

        def to_core(r, ia, ib):
            go(to_core_copy, r, ia, ib)

        def first_copy(r, side):
            return copy(own_block(r), block(r, 0, 0), p1_s.at[r], p1_r.at[r, side], axis(r, 1)(ahead(side)))

        def first_own(r, side):
            go(first_copy, r, side)

        def first_far_copy(r, side):
            part = block(r, back(side), 0, 0, side * half_rows, half_rows)
            return copy(part, part, p2_s.at[r], p2_r.at[r], axis(r, 1)(ahead(side)))

        def first_forward(r, side):
            there = block(r, back(side), 0)
            all_in(there, p1_r.at[r, side])
            go(first_far_copy, r, side)

        def block_on(r, ia):
            if ia == 3:
                all_in(block(r, 2, 0), p2_r.at[r])
            for side in range(2):
                go(second_copy, r, side, ia)
            to_core(r, ia, 0)

        def second_copy(r, side, ia):
            there = block(r, DELTAS[ia], 0)
            return copy(there if ia else own_block(r), there, q1_s.at[r], q1_r.at[r, side, ia], axis(r, 2)(ahead(side)))

        def second_far_copy(r, ia):
            side = ia // 2
            there = block(r, DELTAS[ia], back(side))
            return copy(there, there, q2_s.at[r], q2_r.at[r, ia], axis(r, 2)(ahead(side)))

        def second_forward(r, ia, side):
            there = block(r, DELTAS[ia], back(side))
            all_in(there, q1_r.at[r, side, ia])
            if ia // 2 == side:
                go(second_far_copy, r, ia)
            to_core(r, ia, 1 if side == 0 else 2)

        def second_far(r, ia):
            there = block(r, DELTAS[ia], 2)
            all_in(there, q2_r.at[r, ia])
            to_core(r, ia, 3)

        def some_rows(r, count):
            return rings[r][1].at[pl.ds(0, count * rows), rings[r][2]]

        def chunk_in(ia):
            all_in(some_rows(0, RING), cc_r.at[ia])

        def rows_in(r):
            all_in(some_rows(r, RING * RING), cc_r.at[RING - 1 + r])

        def own_wait(t):
            there = slot(t, 0, NEAR[0])
            pltpu.make_async_copy(there, there, own_sem.at[t]).wait()

        def own_rows(r):
            return pltpu.make_async_copy(own_block(r), block(r, 0, 0), own_sem.at[4 + r])

        def w_load(t):
            return pltpu.make_async_copy(fulls[t], (wv_a, held["wv_b"], wv_a, wv_r)[t], wv_sem.at[t])

        def row_load(src, i, buf):
            return pltpu.make_async_copy(src.at[chunk_rows(i)], rowbuf.at[buf], row_sem.at[buf])

        def chunk_loop(src, products, elementwise, between):
            row_load(src, 0, 0).start()
            between[0]()
            row_load(src, 1, 1).start()
            row_load(src, 0, 0).wait()
            products(0, 0)

            def body(i, carry):
                buf = lax.rem(i, 2)

                @pl.when(i + 1 < n_chunk)
                def _():
                    row_load(src, i + 1, 1 - buf).start()

                for k, step in enumerate(between[1:], 1):
                    pl.when(i == k)(step)
                row_load(src, i, buf).wait()
                free(elementwise, i - 1)
                elementwise(i - 1, 1 - buf, lambda: products(i, buf))
                return carry

            lax.fori_loop(1, n_chunk, body, 0)
            free(elementwise, n_chunk - 1)
            elementwise(n_chunk - 1, (n_chunk - 1) % 2, lambda: None)

        def free(elementwise, i):
            @pl.when(i >= 2)
            def _():
                for cp in copies_of[elementwise](i - 2):
                    cp.wait()

        def chunk_rows(i):
            return pl.ds(pl.multiple_of(i * chunk, chunk), chunk)

        def h_copies(i, which, names):
            xx, c = lax.div(i, 2), lax.rem(i, 2)
            cs = [pltpu.make_async_copy(hst.at[c, n], h_main.at[j, xx, c], hst_sem.at[c, n]) for n, j in enumerate(names)]
            return cs + [pltpu.make_async_copy(hst_rest.at[which, c], h_rest.at[which, xx, c], hst_sem.at[c, 2])]

        def keep(i, c, values):
            which = len(values) - 1
            for n, (j, v) in enumerate(values):
                low = v.astype(BF16)
                hst[c, n] = low[:, :main]
                hst_rest[which, c, :, j * rest:(j + 1) * rest] = low[:, main:]
                ff[j, :, chunk_rows(i)] = v.T.astype(BF16)

        def kept(elementwise):
            for i in (n_chunk - 2, n_chunk - 1):
                for cp in copies_of[elementwise](i):
                    cp.wait()

        def gate_work():
            def place(k):
                ia, flip = lax.div(k, 2), lax.rem(k, 2)
                delta = lax.rem(3 * ia + 3 * lax.div(ia, 2) + 2 * lax.div(ia, 3), RING)
                return 2 * lax.rem(x + delta, RING) + lax.rem(core + flip, 2)

            def body(k, carry):
                for n, group in enumerate(GATE_STEPS):
                    if group:
                        pl.when(k == n)(functools.partial(run, group))

                @pl.when(k < n_chunk)
                def _():
                    row_load(tok_all, place(k), lax.rem(k, 2)).start()

                @pl.when(k >= 1)
                def _():
                    i, buf = place(k - 1), lax.rem(k - 1, 2)
                    row_load(tok_all, i, buf).wait()
                    rb_ = rowbuf[buf]
                    av[chunk_rows(i), :main] = jnp.dot(rb_, wv_a[...], preferred_element_type=F32).astype(BF16)
                    both = jnp.dot(rb_, wv_r[...], preferred_element_type=F32).astype(BF16)
                    av[chunk_rows(i), main:] = both[:, :rest]
                    bv[chunk_rows(i), main:] = both[:, rest:2 * rest]

                return carry

            lax.fori_loop(0, n_chunk + 1, body, 0)

        def up_products(i, buf):
            bv[chunk_rows(i), :main] = jnp.dot(rowbuf[buf], held["wv_b"][...], preferred_element_type=F32).astype(BF16)

        def hidden(i, c, beside):
            a, b = av[chunk_rows(i)].astype(F32), bv[chunk_rows(i)].astype(F32)
            beside()
            keep(i, c, ((2, a * jax.nn.sigmoid(a) * b),))
            start(copies_of[hidden](i))

        def down_products(i, buf):
            rb_ = rowbuf[buf]
            lanes = 2 * rest // LANE * LANE
            low = jnp.dot(rb_, wv_r[:, lanes:], preferred_element_type=F32)[:, 2 * rest - lanes:3 * rest - lanes]
            gv[buf] = jnp.concatenate([jnp.dot(rb_, wv_a[...], preferred_element_type=F32), low], axis=1).astype(BF16)

        def backward(i, c, beside):
            g = gv[c].astype(F32)
            a, b = av[chunk_rows(i)].astype(F32), bv[chunk_rows(i)].astype(F32)
            beside()
            sig = jax.nn.sigmoid(a)
            keep(i, c, ((0, g * b * sig * (1.0 + a * (1.0 - sig))), (1, g * (a * sig))))
            start(copies_of[backward](i))

        copies_of = {hidden: lambda i: h_copies(i, 0, (2,)), backward: lambda i: h_copies(i, 1, (0, 1))}

        steps = (exchange, z_first, z_second, first_own, first_forward, block_on, second_forward, second_far, weights_done, chunk_in)

        def run(group):
            for which, *args in group:
                steps[which](*args)

        def rows_ready():
            run(UP_STEPS[-1])
            for r in (1, 2):
                own_rows(r).wait()
                rows_in(r)
            blk_load(plan[0][0], 0, plan[0][1]).start()

        def gather_phase(shard, pieces, rests, wv_b):
            held.update(shard=shard, pieces=pieces, rests=rests, wv_b=wv_b)
            with jax.named_scope("begin"):
                for t in range(3):
                    shard_load(t).start()
                shard_load(0).wait()
                cut_pieces(0)
                pl.semaphore_wait(barrier, len(others))
                for r in range(3):
                    own_rows(r).start()
            with jax.named_scope("gather"):
                cut = {0}
                for step in GATHER_STEPS:
                    if step[0] in (EX, Z1) and step[1] not in cut:
                        if len(cut) == 1:
                            rests[...] = jnp.zeros_like(rests)
                            hst_rest[...] = jnp.zeros_like(hst_rest)
                            shard_load(1).wait()
                            shard_load(2).wait()
                        cut.add(step[1])
                        cut_pieces(step[1])
                    run((step,))
                own_rows(0).wait()
                w_load(0).wait()
                w_load(REST).wait()
            with jax.named_scope("gate"):
                gate_work()
            with jax.named_scope("up"):
                run(UP_STEPS[0])
                w_load(1).wait()
                chunk_loop(tok_all, up_products, hidden, [functools.partial(run, group) for group in ((),) + UP_STEPS[1:-1]] + [rows_ready])
                kept(hidden)
            for _, t in LATE_STEPS:
                own_wait(t)
            for t in range(4):
                all_out(some(t, n8 - 1), ex_s.at[t])
                for side in range(2):
                    all_out(some(t, n8), z1_s.at[t, side])

        pl.run_scoped(
            gather_phase, pltpu.VMEM((3,) + sg.shape, BF16), pltpu.VMEM((3, n8, dp, main), BF16), pltpu.VMEM((n8, dp, packed), BF16),
            pltpu.VMEM((d, main), BF16))
        run_order({
            "far_block": far_block, "next_products": next_products, "give_rows": give_rows, "late": functools.partial(run, LATE_STEPS),
        }, EARLY_ORDER)
        with jax.named_scope("down"):
            w_load(2).wait()
            chunk_loop(grad_all, down_products, backward, [lambda: None])
            kept(backward)
        for t in range(4):
            for side in range(2):
                all_out(some(t, n8 // 2), z2_s.at[t, side])
        for r in range(3):
            for count, sem in ((2, p1_s), (1, p2_s), (2 * RING, q1_s), (RING, q2_s), (RING * RING, cc_s)):
                all_out(some_rows(r, count), sem.at[r])

    def backward_phase(tmp, stage):
        def next_adds(t):
            all_in(ra.at[t], a_r.at[t])
            cs = [pltpu.make_async_copy(ra.at[t, at], tmp.at[s, at], tmp_sem.at[s]) for s, at in ((0, lo), (1, hi))]
            start(cs)
            for c, (s, at) in zip(cs, ((0, lo), (1, hi))):
                c.wait()
                nxt[t, s, at] += tmp[s, at]
            for tile in range(tiles):
                start(c for s, c in enumerate(unit_copies(t, tile)) if (s, tile) not in early_units(t))

        def next_blocks(t):
            next_products(t)
            next_adds(t)

        def own_block(t):
            all_out(ra.at[t], a_s.at[t])
            product(t, far.at[t])

        def slot(t):
            return Z_ORDER.index(t) % 2

        def hand_out(t, tile, part):
            parts = unit_parts(t, tile)
            for k in range(n8):
                dx, dc = NEAR[k]
                at = pl.ds(hand_at[dx][dc], dp)
                src, dst = stage.at[slot(t), tile, at], outs[t].at[i8, tile]

                def send(k=k, src=src, dst=dst):
                    if k:
                        rcopy(src, dst, e_s.at[t], e_r.at[t], near(*NEAR[k])).start()
                    else:
                        pltpu.make_async_copy(src, dst, out_sem.at[t]).start()

                if len(parts) == 1:
                    send()
                elif part == 0:
                    pl.when(xs[dx] < parts[0][2] // dp // 2)(send)
                else:
                    pl.when(xs[dx] >= parts[0][2] // dp // 2)(send)

        def handed(t):
            all_out(outs[t].at[pl.ds(0, n8 - 1)], e_s.at[t])
            pltpu.make_async_copy(outs[t].at[0], outs[t].at[0], out_sem.at[t]).wait()

        given = []

        def finish(t, tile):
            at = tile_rows(tile)
            wide = pl.ds(tile * LANE, LANE)
            for part, (n, first, size) in enumerate(unit_parts(t, tile)):
                lanes = pl.ds(first, size)
                all_in(rb.at[t, :, at, lanes], u_r.at[t, n])
                cs = [pltpu.make_async_copy(rb.at[t, s, at, lanes], tmp.at[s, at, lanes], tmp_sem.at[s]) for s in range(2)]
                start(cs)
                if t == Z_ORDER[2] and not given:
                    given.append(Z_ORDER[0])
                    handed(Z_ORDER[0])
                for c in cs:
                    c.wait()
                stage[slot(t), tile, lanes] = (far[t, wide, lanes] + tmp[0, wide, lanes] + tmp[1, wide, lanes]).T
                hand_out(t, tile, part)

        def on_y(r, n):
            return (r == 1) == (n == 1)

        def level(r, n):
            at = ys if on_y(r, n) else xs
            dev = ydev if on_y(r, n) else xdev
            if n == 1:
                def piece(k, h):
                    return part.at[r, pl.ds(2 * h, 2), at[k]] if on_y(r, n) else part.at[r, at[k], pl.ds(2 * h, 2)]
                return dev, piece, ra1, rb1, sd1, (a1_s, a1_r, f1_s, f1_r, d1_s, d1_r)

            def piece(k, h):
                return mid.at[r, at[k], pl.ds(h, 1)]
            return dev, piece, ra2, rb2, sd2, (a2_s, a2_r, f2_s, f2_r, d2_s, d2_r)

        def ring_a(r, n):
            dev, piece, rfar, _, _, sems = level(r, n)
            return [rcopy(piece(2, s), rfar.at[r, s], sems[0].at[r], sems[1].at[r], dev(1 + 2 * s)) for s in range(2)]

        def ring_f(r, n):
            dev, piece, _, rnear, _, sems = level(r, n)
            return [rcopy(piece(1 + 2 * s, 1 - s), rnear.at[r, s, 1 - s], sems[2].at[r], sems[3].at[r], dev(1 + 2 * s)) for s in range(2)]

        def ring_d(r, n):
            dev, _, _, rnear, dep, sems = level(r, n)
            return [rcopy(dep.at[r, s], rnear.at[r, s, s], sems[4].at[r], sems[5].at[r], dev(1 + 2 * s)) for s in range(2)]

        def add(grid, *terms):
            specs = []
            for ref, at, lead in terms:
                tail = ref.shape[lead:]
                specs.append(pl.BlockSpec((1,) * lead + tuple(tail), lambda *i, at=at, rank=len(tail): tuple(at(*i)) + (0,) * rank))

            def body(*refs):
                total = refs[0][...].astype(F32).reshape(refs[0].shape[-2:])
                for ref in refs[1:-1]:
                    total = total + ref[...].astype(F32).reshape(total.shape)
                refs[-1][...] = total.astype(BF16).reshape(refs[-1].shape)

            pltpu.emit_pipeline(body, grid=grid, in_specs=specs[:-1], out_specs=specs[-1:])(*[ref for ref, _, _ in terms])

        def ring_first(r, n):
            start(ring_a(r, n) + ring_f(r, n))

        def ring_dependent(r, n):
            _, _, rfar, _, _, sems = level(r, n)
            all_in(rfar.at[r], sems[1].at[r])
            here = y if on_y(r, n) else x
            if n == 1:
                def near_block(s, i):
                    at = lax.rem(here + 1 + 2 * s, RING)
                    return (2 * s + i, at) if on_y(r, n) else (at, 2 * s + i)

                add((2, 2), (part.at[r], near_block, 2), (ra1.at[r], lambda s, i: (s, i), 2), (sd1.at[r], lambda s, i: (s, i), 2))
            else:
                add((2,), (mid.at[r], lambda s: (lax.rem(here + 1 + 2 * s, RING), s), 2), (ra2.at[r], lambda s: (s, 0), 2),
                    (sd2.at[r], lambda s: (s, 0), 2))
            start(ring_d(r, n))

        def ring_last(r, n):
            _, _, rfar, _, _, sems = level(r, n)
            all_in(rfar.at[r], sems[3].at[r])
            all_in(rfar.at[r], sems[5].at[r])
            here = y if on_y(r, n) else x
            if n == 1:
                def own_at(h, i):
                    return (2 * h + i, here) if on_y(r, n) else (here, 2 * h + i)

                add((2, 2), (part.at[r], own_at, 2), (rb1.at[r, 0], lambda h, i: (h, i), 2),
                    (rb1.at[r, 1], lambda h, i: (h, i), 2), (mid.at[r], lambda h, i: (2 * h + i,), 1))
            else:
                own, res = ((tok_own, out), (grad_own, gin))[r]
                add((2,), (own, lambda h: (h,), 1), (mid.at[r], lambda h: (here, h), 2), (rb2.at[r, 0], lambda h: (h, 0), 2),
                    (rb2.at[r, 1], lambda h: (h, 0), 2), (res, lambda h: (h,), 1))

        def keep_rows(r):
            core_copy(r).wait_recv()
            row_products(r, True)

        run_order({
            "far_block": far_block, "next_products": next_products, "next_adds": next_adds, "next_blocks": next_blocks,
            "own_block": own_block, "finish": finish, "give_rows": give_rows, "keep_rows": keep_rows, "ring_first": ring_first,
            "ring_dependent": ring_dependent, "ring_last": ring_last,
        }, LATE_ORDER)

        for t in range(3):
            all_out(nxt.at[t], u_s.at[t])
        for r in range(2):
            core_copy(r).wait_send()
            for n in (1, 2):
                _, _, rfar, _, _, sems = level(r, n)
                for sem in sems[::2]:
                    all_out(rfar.at[r], sem.at[r])
        for t in Z_ORDER:
            with jax.named_scope(f"handed_{t}"):
                all_in(outs[t].at[pl.ds(0, n8 - 1)], e_r.at[t])
                if t not in given:
                    handed(t)

    pl.run_scoped(
        forward_phase,
        pltpu.VMEM((2, chunk, d), BF16),
        pltpu.VMEM((tokens, nf), BF16),
        pltpu.VMEM((tokens, nf), BF16),
        pltpu.VMEM((2, chunk, nf), BF16),
        pltpu.VMEM((2, 2, chunk, main), BF16),
        pltpu.VMEM((2, 2, chunk, packed), BF16),
        pltpu.VMEM((d, main), BF16),
        pltpu.VMEM((d, packed), BF16),
    )
    pl.run_scoped(backward_phase, pltpu.VMEM((2, tiles * LANE, cols), F32), pltpu.VMEM((2, tiles, cols, LANE), F32))


def layer(sg, su, sd, tok, grad):
    n8 = 2 * RING
    dp, nf = sg.shape[0], sg.shape[1] // n8
    rows, d = tok.shape
    tokens = rows * RING * n8
    cols = d // RING
    tiles = -(-nf // LANE)
    padded = tiles * LANE
    main = nf // LANE * LANE
    packed = -(-3 * (nf - main) // LANE) * LANE
    hbm = pl.BlockSpec(memory_space=pl.ANY)
    dma = pltpu.SemaphoreType.DMA
    sds = jax.ShapeDtypeStruct
    halves = (2, rows // 2, d)
    res = pl.pallas_call(
        layer_kernel,
        out_shape=[sds((n8, tiles, dp, LANE), F32)] * 3 + [sds(halves, BF16)] * 2 + [
            sds((d, main), BF16), sds((d, main), BF16), sds((d, main), BF16), sds((d, packed), BF16), sds((tokens, d), BF16), sds((tokens, d), BF16),
            sds((3, RING, 2, RING * rows, main), BF16), sds((2, RING, 2, RING * rows, packed), BF16),
            sds((3, nf, cols), F32), sds((3, 2, nf, cols), F32),
            sds((2, RING, RING, rows, d), BF16), sds((2, RING, RING, rows, d), BF16), sds((2, RING, RING, rows, d), BF16),
            sds((2, 2, 2, rows, d), BF16), sds((2, 2, 2, 2, rows, d), BF16), sds((2, 2, 2, rows, d), BF16),
            sds((2, RING, 2, rows // 2, d), BF16),
            sds((2, 2, 1, rows // 2, d), BF16), sds((2, 2, 2, 1, rows // 2, d), BF16), sds((2, 2, 1, rows // 2, d), BF16),
        ],
        in_specs=[hbm] * 7,
        out_specs=[hbm] * 25,
        scratch_shapes=[
            pltpu.VMEM((3, nf, tokens), BF16),
            pltpu.VMEM((2, tokens, cols), BF16),
            pltpu.VMEM((3, padded, cols), F32),
            pltpu.VMEM((3, 2, nf, cols), F32),
            dma((7,)),
            dma((4,)), dma((4, n8)),
            dma((4, 2)), dma((4, 2, n8 // 2)), dma((4, 2)),
            dma((4, 2)), dma((4, 2)),
            dma((3,)), dma((3, 2)),
            dma((3,)), dma((3,)),
            dma((3,)), dma((3, 2, RING)),
            dma((3,)), dma((3, RING)),
            dma((3,)), dma((RING + 2,)),
            dma((3,)), dma((4,)), dma((2,)), dma((2, 3)), dma((2,)), dma((2,)),
            dma((3,)), dma((3,)),
            dma((3,)), dma((3, tiles + 1)),
            dma((3,)), dma((3,)),
            dma((3,)),
            dma((2,)), dma((2,)),
        ] + [dma((2,))] * 12,
        compiler_params=pltpu.CompilerParams(collective_id=0, has_side_effects=True, vmem_limit_bytes=67043328),
        cost_estimate=pl.CostEstimate(flops=18 * nf * tokens * d, bytes_accessed=300_000_000, transcendentals=0),
        name="layer",
    )(sg, su, sd, tok, grad, tok.reshape(halves), grad.reshape(halves))
    return res[:3], res[3].reshape(rows, d), res[4].reshape(rows, d)


def assemble_kernel(og, ou, od, out, gin, g, u, w, res, gres, buf, flat, in_sem, out_sem, row_buf, row_sem):
    n8, nf = og.shape[0], g.shape[1] // og.shape[0]
    srcs, dsts = (og, ou, od), (g, u, w)
    rows_in = [pltpu.make_async_copy(src, row_buf.at[r], row_sem.at[r]) for r, src in enumerate((out, gin))]
    loads = [pltpu.make_async_copy(src, buf.at[t], in_sem.at[t]) for t, src in enumerate(srcs)]
    stores = [pltpu.make_async_copy(flat.at[t], dst, out_sem.at[t]) for t, dst in enumerate(dsts)]
    for c in loads + rows_in:
        c.start()
    for t in range(3):
        loads[t].wait()
        for j in range(n8):
            flat[t, :, j * nf:(j + 1) * nf] = jnp.concatenate([buf[t, j, tile] for tile in range(buf.shape[2])], axis=1)[:, :nf]
        stores[t].start()
    rows_out = [pltpu.make_async_copy(row_buf.at[r], dst, row_sem.at[r]) for r, dst in enumerate((res, gres))]
    for c in rows_in:
        c.wait()
    for c in rows_out:
        c.start()
    for c in stores + rows_out:
        c.wait()


def assemble(sums, out, gin, ff):
    dp = sums[0].shape[2]
    hbm = pl.BlockSpec(memory_space=pl.ANY)
    dma = pltpu.SemaphoreType.DMA
    sds = jax.ShapeDtypeStruct
    return pl.pallas_call(
        assemble_kernel,
        out_shape=[sds((dp, ff), F32)] * 3 + [sds(out.shape, BF16)] * 2,
        in_specs=[hbm] * 5,
        out_specs=[hbm] * 5,
        scratch_shapes=[
            pltpu.VMEM((3,) + sums[0].shape, F32), pltpu.VMEM((3, dp, ff), F32), dma((3,)), dma((3,)),
            pltpu.VMEM((2,) + out.shape, BF16), dma((2,)),
        ],
        compiler_params=pltpu.CompilerParams(vmem_limit_bytes=63 * 1024 * 1024),
        name="assemble",
    )(*sums, out, gin)


def solution(mesh):
    nz, ny, nd = mesh.shape["datb"], mesh.shape["model"], mesh.shape["data"]
    fine = Mesh(mesh.devices.reshape(nz, ny, nd // 2, 2), ("datb", "model", "x", "core"))

    def local_step(tok_loc, wg_loc, wu_loc, wd_loc, grad_loc):
        sums, out, grad_in = layer(wg_loc, wu_loc, wd_loc.T, tok_loc, grad_loc)
        grad_gate, grad_up, grad_down_t, out, grad_in = assemble(sums, out, grad_in, wg_loc.shape[1])
        return out, grad_in, grad_gate, grad_up, grad_down_t.T

    return jax.shard_map(local_step, mesh=fine, in_specs=(ROW_SPEC, GATE_SPEC, GATE_SPEC, DOWN_SPEC, ROW_SPEC), out_specs=(ROW_SPEC, ROW_SPEC, GATE_SPEC, GATE_SPEC, DOWN_SPEC), check_vma=False)
```

```python
import functools

import jax
import jax.numpy as jnp
from jax import lax
from jax.experimental import pallas as pl
from jax.experimental.pallas import tpu as pltpu
from jax.sharding import Mesh
from jax.sharding import PartitionSpec as P

ROW_SPEC = P(("datb", "x", "core", "model"), None)
GATE_SPEC = P(("datb", "x", "core"), "model")
DOWN_SPEC = P("model", ("datb", "x", "core"))
BF16 = jnp.bfloat16
F32 = jnp.float32
MESH_ID = pl.DeviceIdType.MESH
RING = 4
NEAR = ((0, 0), (0, 1), (1, 0), (3, 0), (1, 1), (3, 1), (2, 0), (2, 1))
DELTAS = (0, 3, 1, 2)
LANE = 128
OUT_COLS = 512
EX, Z1, Z2, P1, P2, BL, Q1, Q2, WD, CI = range(10)
GATHER_STEPS = (
    (Z1, 0, 0), (P1, 0, 0), (P1, 0, 1), (EX, 0, 1), (BL, 0, 0), (P1, 2, 0), (P1, 2, 1), (EX, 0, 2), (Z1, 3, 0), (EX, 3, 1), (EX, 3, 2),
    (EX, 3, 3), (EX, 3, 4), (EX, 3, 5), (EX, 3, 6), (EX, 3, 7), (Z1, 1, 0), (EX, 1, 1), (Z1, 2, 0), (EX, 2, 1), (EX, 0, 3), (BL, 1, 0),
    (Z1, 3, 1), (EX, 0, 4), (EX, 0, 5), (Z1, 0, 1), (Z1, 1, 1), (Z2, 3, 0, 0), (Z1, 2, 1), (EX, 0, 6), (EX, 0, 7), (Z2, 0, 0, 0),
    (Z2, 1, 0, 0), (EX, 1, 2), (EX, 1, 3), (Z2, 2, 0, 0), (Z2, 3, 0, 1), (P2, 0, 0), (P2, 0, 1), (BL, 0, 1), (Q1, 0, 0, 1), (Z1, 3, 2),
    (Z1, 3, 3), (Z1, 3, 4), (Q1, 0, 0, 0), (Z1, 3, 5), (Z2, 0, 0, 1), (EX, 1, 4), (EX, 1, 5), (P2, 2, 1), (Z1, 3, 6), (EX, 1, 6),
    (EX, 1, 7), (Z1, 3, 7), (Z1, 0, 2), (Q1, 1, 0, 1), (Z2, 3, 1, 0), (Z2, 3, 1, 1), (Z1, 0, 3), (EX, 2, 2), (EX, 2, 3), (Z2, 3, 1, 2),
    (BL, 0, 2), (Z2, 3, 1, 3), (Z1, 0, 4), (EX, 2, 4), (EX, 2, 5), (Z1, 0, 5), (EX, 2, 6), (EX, 2, 7), (Z2, 3, 0, 2), (Q1, 0, 1, 1),
    (Z2, 3, 0, 3), (Z1, 0, 6), (P1, 1, 0), (P1, 1, 1), (Q1, 0, 1, 0), (Z1, 0, 7), (BL, 2, 2), (Z2, 0, 1, 0), (Z1, 1, 2), (Z2, 0, 1, 1),
    (Z2, 0, 0, 2), (Q2, 0, 0), (Z2, 0, 1, 2), (Z2, 0, 0, 3), (BL, 2, 0), (BL, 0, 3), (Q1, 0, 2, 1), (Z2, 0, 1, 3), (Z1, 1, 3), (Z1, 1, 4),
    (WD, 3), (Z1, 1, 5), (Q1, 0, 2, 0), (Z1, 1, 6), (P2, 2, 0), (BL, 2, 1), (P2, 1, 0), (P2, 1, 1), (Z1, 1, 7), (Q1, 0, 3, 1),
    (Q1, 1, 0, 0), (Z2, 1, 0, 1), (Q1, 2, 2, 0), (Q1, 2, 2, 1), (Z2, 1, 0, 2), (BL, 1, 1), (Q2, 0, 1), (WD, 0), (Z2, 1, 1, 0), (CI, 0),
)
GATE_STEPS = (
    (),
    (),
    (
        (Z1, 2, 2),
    ),
    (
        (Q2, 0, 2), (Z2, 1, 1, 1), (Z2, 1, 0, 3), (Q1, 2, 0, 0), (Q1, 2, 0, 1), (BL, 1, 2), (CI, 1),
    ),
    (
        (Z2, 1, 1, 2), (Z1, 2, 3),
    ),
    (
        (Q1, 0, 3, 0), (Z2, 1, 1, 3), (Z1, 2, 4), (CI, 2),
    ),
    (
        (Z1, 2, 5), (Q1, 2, 1, 0), (Q1, 2, 1, 1), (BL, 2, 3), (BL, 1, 3), (Z1, 2, 6), (Q2, 0, 3),
    ),
    (
        (Q2, 1, 0), (Z1, 2, 7), (CI, 3),
    ),
    (
        (Q2, 2, 0), (Q2, 2, 2), (Z2, 2, 0, 1), (Q1, 1, 1, 0), (Q1, 1, 1, 1),
    ),
)
UP_STEPS = (
    (
        (Z2, 2, 0, 2), (Q1, 1, 2, 1), (WD, 1),
    ),
    (
        (Q2, 2, 1), (Q1, 2, 3, 1), (Q1, 1, 2, 0),
    ),
    (
        (Z2, 2, 1, 0), (Z2, 2, 0, 3), (Q1, 1, 3, 1),
    ),
    (
        (Z2, 2, 1, 1), (Q1, 1, 3, 0),
    ),
    (
        (Q2, 1, 2), (Z2, 2, 1, 2), (Q1, 2, 3, 0),
    ),
    (
        (Q2, 1, 1), (Z2, 2, 1, 3),
    ),
    (
        (Q2, 1, 3), (Q2, 2, 3),
    ),
    (),
)
LATE_STEPS = (
    (WD, 2),
)
Z_ORDER = (2, 0, 1)
EARLY_ORDER = (
    ("far_block", 2), ("next_products", 2), ("late",), ("give_rows", 0),
)
LATE_ORDER = (
    ("next_adds", 2), ("own_block", 2), ("keep_rows", 0), ("ring_first", 0, 1), ("finish", 2, 0), ("far_block", 0), ("give_rows", 1),
    ("finish", 2, 3), ("finish", 2, 1), ("finish", 2, 4), ("ring_dependent", 0, 1), ("finish", 2, 2), ("far_block", 1), ("keep_rows", 1),
    ("ring_first", 1, 1), ("next_blocks", 0), ("own_block", 0), ("next_blocks", 1), ("own_block", 1), ("finish", 0, 0),
    ("ring_dependent", 1, 1), ("finish", 0, 1), ("ring_last", 0, 1), ("ring_first", 0, 2), ("finish", 0, 2), ("finish", 0, 3),
    ("finish", 0, 4), ("ring_last", 1, 1), ("ring_first", 1, 2), ("ring_dependent", 0, 2), ("finish", 1, 0), ("ring_dependent", 1, 2),
    ("ring_last", 0, 2), ("finish", 1, 1), ("finish", 1, 2), ("ring_last", 1, 2), ("finish", 1, 3), ("finish", 1, 4),
)


def dot(a, b, ca, cb):
    return lax.dot_general(a, b, (((ca,), (cb,)), ((), ())), preferred_element_type=F32)


def layer_kernel(sg, su, sd, tok, grad, tok_own, grad_own,
                 og, ou, od, out, gin, wg, wu, wd, wr, tok_all, grad_all, h_main, h_rest, ra, rb, give, rc, part, ra1, rb1, sd1, mid, ra2, rb2, sd2,
                 ff, blk, far, nxt,
                 own_sem, ex_s, ex_r, z1_s, z1_r, zn_r, z2_s, z2_r, p1_s, p1_r, p2_s, p2_r, q1_s, q1_r, q2_s, q2_r, cc_s, cc_r,
                 sh_sem, wv_sem, row_sem, hst_sem, blk_sem, tmp_sem, a_s, a_r, u_s, u_r, e_s, e_r, out_sem,
                 c_s, c_r, a1_s, a1_r, f1_s, f1_r, d1_s, d1_r, a2_s, a2_r, f2_s, f2_r, d2_s, d2_r):
    z, y = lax.axis_index("datb"), lax.axis_index("model")
    x, core = lax.axis_index("x"), lax.axis_index("core")
    i8 = 2 * x + core
    n8 = 2 * RING
    rows, d = tok.shape
    half_rows = rows // 2
    chunk = RING * rows
    n_chunk = n8
    nf, tokens = ff.shape[1:]
    dp = sg.shape[0]
    half = nf // 2
    main = wg.shape[1]
    rest = nf - main
    packed = wr.shape[1]
    cols = blk.shape[2]
    tiles = far.shape[1] // LANE
    outs = (og, ou, od)

    zs, ys, xs = ([v] + [lax.rem(v + k, RING) for k in range(1, RING)] for v in (z, y, x))
    cores = (core, 1 - core)
    peers = [[2 * v + c for c in cores] for v in xs]
    slot_at = [[[pl.multiple_of((zz * n8 + peers[dx][dc]) * dp, 16) for dc in range(2)] for dx in range(RING)] for zz in zs]
    hand_at = [[pl.multiple_of(p * dp, 8) for p in row] for row in peers]
    rows_at = [[[pl.multiple_of((peers[dx][dc] * RING + yy) * rows, half_rows) for dc in range(2)] for yy in ys] for dx in range(RING)]
    lanes_at = [pl.multiple_of(zz * cols, LANE) for zz in zs]

    def peer(dx, dc):
        return peers[dx][dc]

    def zdev(k):
        return {"datb": zs[k]}

    def xdev(k):
        return {"x": xs[k]}

    def ydev(k):
        return {"model": ys[k]}

    def near(dx, dc):
        return {"x": xs[dx], "core": cores[dc]}

    def copy(src, dst, s, r, dev):
        return pltpu.make_async_remote_copy(src_ref=src, dst_ref=dst, send_sem=s, recv_sem=r, device_id=dev, device_id_type=MESH_ID)

    rcopy = copy

    def all_in(ref, sem):
        copy(ref, ref, sem, sem, zdev(1)).wait_recv()

    def all_out(ref, sem):
        copy(ref, ref, sem, sem, zdev(1)).wait_send()

    def start(copies):
        for c in copies:
            c.start()

    def received(copies):
        for c in copies:
            c.wait_recv()

    def sent(copies):
        for c in copies:
            c.wait_send()

    def run_order(fns, order):
        for fn, *args in order:
            with jax.named_scope("_".join(str(v) for v in [fn, *args])):
                fns[fn](*args)

    barrier = pltpu.get_barrier_semaphore()
    others = [zdev(1), zdev(3), ydev(1), ydev(3)] + [near(*n) for n in NEAR[1:]]
    for dev in others:
        pl.semaphore_signal(barrier, inc=1, device_id=dev, device_id_type=MESH_ID)

    def blk_load(t, slot, k):
        src = tok_all if t < 2 else grad_all
        return pltpu.make_async_copy(src.at[:, pl.ds(lanes_at[k], cols)], blk.at[slot], blk_sem.at[slot])

    plan = []
    for fn, *args in EARLY_ORDER + LATE_ORDER:
        plan += [(args[0], k) for k in {"far_block": (2,), "next_blocks": (1, 3), "next_products": (1, 3), "own_block": (0,)}.get(fn, ())]
    taken = []

    def next_block():
        n = len(taken)
        taken.append(n)
        blk_load(plan[n][0], n % 2, plan[n][1]).wait()
        if n + 1 < len(plan):
            blk_load(plan[n + 1][0], (n + 1) % 2, plan[n + 1][1]).start()
        return n % 2

    def product(t, dst, then=None):
        slot = next_block()
        step = 2 * LANE
        count = -(-cols // step)

        def one(n, carry):
            lanes = pl.ds(pl.multiple_of(jnp.minimum(n * step, cols - step), LANE), step)
            dst[:nf, lanes] = jnp.dot(ff[t], blk[slot, :, lanes], preferred_element_type=F32)
            for k in range(count if then else 0):
                first = k * step if k < count - 1 else cols - step
                size = step if k == count - 1 else min(step, cols - step - first)
                if size > 0:
                    pl.when(n == k)(functools.partial(then, first, size))
            return carry

        lax.fori_loop(0, count, one, 0)

    lo, hi = pl.ds(0, half), pl.ds(half, half)

    def a_copies(t, first=0, size=cols):
        lanes = pl.ds(first, size)
        return [rcopy(far.at[t, at, lanes], ra.at[t, at, lanes], a_s.at[t], a_r.at[t], zdev(k)) for at, k in ((lo, 1), (hi, 3))]

    def tile_rows(tile):
        return pl.ds(tile * LANE, min(LANE, nf - tile * LANE))

    def unit_parts(t, tile):
        if (t, tile) != (Z_ORDER[2], tiles - 1):
            return [(tile, 0, cols)]
        first = -(-cols // 2 // LANE) * LANE
        return [(tile, 0, first), (tiles, first, cols - first)]

    def unit_copies(t, tile):
        at = tile_rows(tile)
        cs = []
        for n, first, size in unit_parts(t, tile):
            lanes = pl.ds(first, size)
            cs += [rcopy(nxt.at[t, s, at, lanes], rb.at[t, s, at, lanes], u_s.at[t], u_r.at[t, n], zdev(1 + 2 * s)) for s in range(2)]
        return cs

    def far_block(t):
        if t == Z_ORDER[0]:
            product(t, far.at[t], lambda first, size: start(a_copies(t, first, size)))
        else:
            product(t, far.at[t])
            start(a_copies(t))

    def early_units(t):
        if ("next_products", t) not in EARLY_ORDER + LATE_ORDER:
            return ()
        free = [(0, tile) for tile in range(tiles) if tile * LANE >= half]
        return free + [(1, tile) for tile in range(tiles) if (tile + 1) * LANE <= half]

    def next_products(t):
        for s in range(2):
            product(t, nxt.at[t, s])
        for s, tile in early_units(t):
            unit_copies(t, tile)[s].start()

    blocks = d // min(OUT_COLS, d)
    width = d // blocks

    def row_products(r, keep):
        side = core if keep else 1 - core
        specs, args = [], []
        for h, j, w in ((h_main, 2, wd), (h_rest, 0, wr)) if r == 0 else ((h_main, 0, wg), (h_main, 1, wu), (h_rest, 1, wr)):
            n = w.shape[1]
            specs += [pl.BlockSpec((1, RING, 1, RING * rows, n), lambda i, j=j: (j, 0, side, 0, 0)), pl.BlockSpec((width, n), lambda i: (i, 0))]
            args += [h, w]
        wide = pl.BlockSpec((RING, RING, rows, width), lambda i: (0, 0, 0, i))
        terms = len(args) // 2
        if keep:
            specs.append(wide)
            args.append(rc.at[r])

        def body(*refs):
            total = None
            for i in range(terms):
                h = refs[2 * i][...].reshape(RING * RING * rows, refs[2 * i].shape[-1])
                prod = dot(h, refs[2 * i + 1][...], 1, 1)
                total = prod if total is None else total + prod
            if keep:
                total = total + refs[-2][...].astype(F32).reshape(total.shape)
            refs[-1][...] = total.astype(BF16).reshape(RING, RING, rows, width)

        pltpu.emit_pipeline(body, grid=(blocks,), in_specs=specs, out_specs=[wide])(*args, (part if keep else give).at[r])

    def core_copy(r):
        return rcopy(give.at[r], rc.at[r], c_s.at[r], c_r.at[r], near(0, 1))

    def give_rows(r):
        row_products(r, False)
        core_copy(r).start()

    def forward_phase(rowbuf, av, bv, gv, hst, hst_rest, wv_a, wv_r):
        held = {}

        fulls = (wg, wu, wd, wr)
        REST = 3
        def shard_load(t):
            return pltpu.make_async_copy((sg, su, sd)[t], held["shard"].at[t], sh_sem.at[t])

        def cut_pieces(t):
            if t == REST:
                for u in range(3):
                    for j in range(n8):
                        held["rests"][j, :, u * rest:(u + 1) * rest] = held["shard"][u, :, j * nf + main:(j + 1) * nf]
            else:
                for j in range(n8):
                    held["pieces"][t, j] = held["shard"][t, :, j * nf:j * nf + main]
            own_piece(t).start()

        def piece(t, j):
            return held["rests"].at[j] if t == REST else held["pieces"].at[t, j]

        def own_piece(t):
            return pltpu.make_async_copy(piece(t, i8), slot(t, 0, NEAR[0]), own_sem.at[t])

        def go(make, *args):
            make(*args).start()

        def slot(t, k, source):
            dx, dc = source
            return fulls[t].at[pl.ds(slot_at[k][dx][dc], dp)]

        def source(k):
            dx, dc = NEAR[k]
            return (RING - dx) % RING, dc

        def back(side):
            return 3 if side == 0 else 1

        def ahead(side):
            return 1 if side == 0 else 3

        def exchange_copy(t, k):
            return copy(piece(t, peer(*NEAR[k])), slot(t, 0, NEAR[0]), ex_s.at[t], ex_r.at[t, k], near(*NEAR[k]))

        def exchange(t, k):
            go(exchange_copy, t, k)

        def z_first_copy(t, side, k):
            here = slot(t, 0, source(k))
            return copy(here if k else piece(t, i8), here, z1_s.at[t, side], z1_sem(t, side, k), zdev(ahead(side)))

        def z_first(t, k):
            if k:
                here = slot(t, 0, source(k))
                all_in(here, ex_r.at[t, k])
            for side in range(2):
                go(z_first_copy, t, side, k)

        def z1_sem(t, side, k):
            return z1_r.at[t, side, k % (n8 // 2)] if (k < n8 // 2) == (side == 0) else zn_r.at[t, side]

        def some(t, count):
            return fulls[t].at[pl.ds(0, count * dp)]

        def z_second_copy(t, side, k):
            there = slot(t, back(side), source(k + side * (n8 // 2)))
            return copy(there, there, z2_s.at[t, side], z2_r.at[t, side], zdev(ahead(side)))

        def z_second(t, side, k):
            kk = k + side * (n8 // 2)
            all_in(slot(t, back(side), source(kk)), z1_sem(t, side, kk))
            go(z_second_copy, t, side, k)

        def weights_done(t):
            if (WD, t) not in LATE_STEPS:
                own_wait(t)
            for side in range(2):
                all_in(some(t, n8 // 2), zn_r.at[t, side])
                all_in(some(t, n8 // 2), z2_r.at[t, side])
            w_load(t).start()

        cut = d * 11 // 28
        rings = ((tok, tok_all, pl.ds(0, d), True), (grad, grad_all, pl.ds(0, cut), True), (grad, grad_all, pl.ds(cut, d - cut), False))

        def axis(r, n):
            return xdev if rings[r][3] == (n == 1) else ydev

        def block(r, da, db, flip=0, lo=0, size=rows):
            dx, dy = (da, db) if rings[r][3] else (db, da)
            first = rows_at[dx][dy][flip]
            return rings[r][1].at[pl.ds(pl.multiple_of(first + lo, half_rows) if lo else first, size), rings[r][2]]

        def own_block(r):
            return rings[r][0].at[:, rings[r][2]]

        def to_core_copy(r, ia, ib):
            there = block(r, DELTAS[ia], DELTAS[ib])
            return copy(own_block(r) if ia == 0 and ib == 0 else there, there, cc_s.at[r], cc_r.at[ia if r == 0 else RING - 1 + r], near(0, 1))

        def to_core(r, ia, ib):
            go(to_core_copy, r, ia, ib)

        def first_copy(r, side):
            return copy(own_block(r), block(r, 0, 0), p1_s.at[r], p1_r.at[r, side], axis(r, 1)(ahead(side)))

        def first_own(r, side):
            go(first_copy, r, side)

        def first_far_copy(r, side):
            part = block(r, back(side), 0, 0, side * half_rows, half_rows)
            return copy(part, part, p2_s.at[r], p2_r.at[r], axis(r, 1)(ahead(side)))

        def first_forward(r, side):
            there = block(r, back(side), 0)
            all_in(there, p1_r.at[r, side])
            go(first_far_copy, r, side)

        def block_on(r, ia):
            if ia == 3:
                all_in(block(r, 2, 0), p2_r.at[r])
            for side in range(2):
                go(second_copy, r, side, ia)
            to_core(r, ia, 0)

        def second_copy(r, side, ia):
            there = block(r, DELTAS[ia], 0)
            return copy(there if ia else own_block(r), there, q1_s.at[r], q1_r.at[r, side, ia], axis(r, 2)(ahead(side)))

        def second_far_copy(r, ia):
            side = ia // 2
            there = block(r, DELTAS[ia], back(side))
            return copy(there, there, q2_s.at[r], q2_r.at[r, ia], axis(r, 2)(ahead(side)))

        def second_forward(r, ia, side):
            there = block(r, DELTAS[ia], back(side))
            all_in(there, q1_r.at[r, side, ia])
            if ia // 2 == side:
                go(second_far_copy, r, ia)
            to_core(r, ia, 1 if side == 0 else 2)

        def second_far(r, ia):
            there = block(r, DELTAS[ia], 2)
            all_in(there, q2_r.at[r, ia])
            to_core(r, ia, 3)

        def some_rows(r, count):
            return rings[r][1].at[pl.ds(0, count * rows), rings[r][2]]

        def chunk_in(ia):
            all_in(some_rows(0, RING), cc_r.at[ia])

        def rows_in(r):
            all_in(some_rows(r, RING * RING), cc_r.at[RING - 1 + r])

        def own_wait(t):
            there = slot(t, 0, NEAR[0])
            pltpu.make_async_copy(there, there, own_sem.at[t]).wait()

        def own_rows(r):
            return pltpu.make_async_copy(own_block(r), block(r, 0, 0), own_sem.at[4 + r])

        def w_load(t):
            return pltpu.make_async_copy(fulls[t], (wv_a, held["wv_b"], wv_a, wv_r)[t], wv_sem.at[t])

        def row_load(src, i, buf):
            return pltpu.make_async_copy(src.at[chunk_rows(i)], rowbuf.at[buf], row_sem.at[buf])

        def chunk_loop(src, products, elementwise, between):
            row_load(src, 0, 0).start()
            between[0]()
            row_load(src, 1, 1).start()
            row_load(src, 0, 0).wait()
            products(0, 0)

            def body(i, carry):
                buf = lax.rem(i, 2)

                @pl.when(i + 1 < n_chunk)
                def _():
                    row_load(src, i + 1, 1 - buf).start()

                for k, step in enumerate(between[1:], 1):
                    pl.when(i == k)(step)
                row_load(src, i, buf).wait()
                free(elementwise, i - 1)
                elementwise(i - 1, 1 - buf, lambda: products(i, buf))
                return carry

            lax.fori_loop(1, n_chunk, body, 0)
            free(elementwise, n_chunk - 1)
            elementwise(n_chunk - 1, (n_chunk - 1) % 2, lambda: None)

        def free(elementwise, i):
            @pl.when(i >= 2)
            def _():
                for cp in copies_of[elementwise](i - 2):
                    cp.wait()

        def chunk_rows(i):
            return pl.ds(pl.multiple_of(i * chunk, chunk), chunk)

        def h_copies(i, which, names):
            xx, c = lax.div(i, 2), lax.rem(i, 2)
            cs = [pltpu.make_async_copy(hst.at[c, n], h_main.at[j, xx, c], hst_sem.at[c, n]) for n, j in enumerate(names)]
            return cs + [pltpu.make_async_copy(hst_rest.at[which, c], h_rest.at[which, xx, c], hst_sem.at[c, 2])]

        def keep(i, c, values):
            which = len(values) - 1
            for n, (j, v) in enumerate(values):
                low = v.astype(BF16)
                hst[c, n] = low[:, :main]
                hst_rest[which, c, :, j * rest:(j + 1) * rest] = low[:, main:]
                ff[j, :, chunk_rows(i)] = v.T.astype(BF16)

        def kept(elementwise):
            for i in (n_chunk - 2, n_chunk - 1):
                for cp in copies_of[elementwise](i):
                    cp.wait()

        def gate_work():
            def place(k):
                ia, flip = lax.div(k, 2), lax.rem(k, 2)
                delta = lax.rem(3 * ia + 3 * lax.div(ia, 2) + 2 * lax.div(ia, 3), RING)
                return 2 * lax.rem(x + delta, RING) + lax.rem(core + flip, 2)

            def body(k, carry):
                for n, group in enumerate(GATE_STEPS):
                    if group:
                        pl.when(k == n)(functools.partial(run, group))

                @pl.when(k < n_chunk)
                def _():
                    row_load(tok_all, place(k), lax.rem(k, 2)).start()

                @pl.when(k >= 1)
                def _():
                    i, buf = place(k - 1), lax.rem(k - 1, 2)
                    row_load(tok_all, i, buf).wait()
                    rb_ = rowbuf[buf]
                    av[chunk_rows(i), :main] = jnp.dot(rb_, wv_a[...], preferred_element_type=F32).astype(BF16)
                    both = jnp.dot(rb_, wv_r[...], preferred_element_type=F32).astype(BF16)
                    av[chunk_rows(i), main:] = both[:, :rest]
                    bv[chunk_rows(i), main:] = both[:, rest:2 * rest]

                return carry

            lax.fori_loop(0, n_chunk + 1, body, 0)

        def up_products(i, buf):
            bv[chunk_rows(i), :main] = jnp.dot(rowbuf[buf], held["wv_b"][...], preferred_element_type=F32).astype(BF16)

        def hidden(i, c, beside):
            a, b = av[chunk_rows(i)].astype(F32), bv[chunk_rows(i)].astype(F32)
            beside()
            keep(i, c, ((2, a * jax.nn.sigmoid(a) * b),))
            start(copies_of[hidden](i))

        def down_products(i, buf):
            rb_ = rowbuf[buf]
            lanes = 2 * rest // LANE * LANE
            low = jnp.dot(rb_, wv_r[:, lanes:], preferred_element_type=F32)[:, 2 * rest - lanes:3 * rest - lanes]
            gv[buf] = jnp.concatenate([jnp.dot(rb_, wv_a[...], preferred_element_type=F32), low], axis=1).astype(BF16)

        def backward(i, c, beside):
            g = gv[c].astype(F32)
            a, b = av[chunk_rows(i)].astype(F32), bv[chunk_rows(i)].astype(F32)
            beside()
            sig = jax.nn.sigmoid(a)
            keep(i, c, ((0, g * b * sig * (1.0 + a * (1.0 - sig))), (1, g * (a * sig))))
            start(copies_of[backward](i))

        copies_of = {hidden: lambda i: h_copies(i, 0, (2,)), backward: lambda i: h_copies(i, 1, (0, 1))}

        steps = (exchange, z_first, z_second, first_own, first_forward, block_on, second_forward, second_far, weights_done, chunk_in)

        def run(group):
            for which, *args in group:
                steps[which](*args)

        def rows_ready():
            run(UP_STEPS[-1])
            for r in (1, 2):
                own_rows(r).wait()
                rows_in(r)
            blk_load(plan[0][0], 0, plan[0][1]).start()

        def gather_phase(shard, pieces, rests, wv_b):
            held.update(shard=shard, pieces=pieces, rests=rests, wv_b=wv_b)
            with jax.named_scope("begin"):
                for t in range(3):
                    shard_load(t).start()
                shard_load(0).wait()
                cut_pieces(0)
                pl.semaphore_wait(barrier, len(others))
                for r in range(3):
                    own_rows(r).start()
            with jax.named_scope("gather"):
                cut = {0}
                for step in GATHER_STEPS:
                    if step[0] in (EX, Z1) and step[1] not in cut:
                        if len(cut) == 1:
                            rests[...] = jnp.zeros_like(rests)
                            hst_rest[...] = jnp.zeros_like(hst_rest)
                            shard_load(1).wait()
                            shard_load(2).wait()
                        cut.add(step[1])
                        cut_pieces(step[1])
                    run((step,))
                own_rows(0).wait()
                w_load(0).wait()
                w_load(REST).wait()
            with jax.named_scope("gate"):
                gate_work()
            with jax.named_scope("up"):
                run(UP_STEPS[0])
                w_load(1).wait()
                chunk_loop(tok_all, up_products, hidden, [functools.partial(run, group) for group in ((),) + UP_STEPS[1:-1]] + [rows_ready])
                kept(hidden)
            for _, t in LATE_STEPS:
                own_wait(t)
            for t in range(4):
                all_out(some(t, n8 - 1), ex_s.at[t])
                for side in range(2):
                    all_out(some(t, n8), z1_s.at[t, side])

        pl.run_scoped(
            gather_phase, pltpu.VMEM((3,) + sg.shape, BF16), pltpu.VMEM((3, n8, dp, main), BF16), pltpu.VMEM((n8, dp, packed), BF16),
            pltpu.VMEM((d, main), BF16))
        run_order({
            "far_block": far_block, "next_products": next_products, "give_rows": give_rows, "late": functools.partial(run, LATE_STEPS),
        }, EARLY_ORDER)
        with jax.named_scope("down"):
            w_load(2).wait()
            chunk_loop(grad_all, down_products, backward, [lambda: None])
            kept(backward)
        for t in range(4):
            for side in range(2):
                all_out(some(t, n8 // 2), z2_s.at[t, side])
        for r in range(3):
            for count, sem in ((2, p1_s), (1, p2_s), (2 * RING, q1_s), (RING, q2_s), (RING * RING, cc_s)):
                all_out(some_rows(r, count), sem.at[r])

    def backward_phase(tmp, stage):
        def next_adds(t):
            all_in(ra.at[t], a_r.at[t])
            cs = [pltpu.make_async_copy(ra.at[t, at], tmp.at[s, at], tmp_sem.at[s]) for s, at in ((0, lo), (1, hi))]
            start(cs)
            for c, (s, at) in zip(cs, ((0, lo), (1, hi))):
                c.wait()
                nxt[t, s, at] += tmp[s, at]
            for tile in range(tiles):
                start(c for s, c in enumerate(unit_copies(t, tile)) if (s, tile) not in early_units(t))

        def next_blocks(t):
            next_products(t)
            next_adds(t)

        def own_block(t):
            all_out(ra.at[t], a_s.at[t])
            product(t, far.at[t])

        def slot(t):
            return Z_ORDER.index(t) % 2

        def hand_out(t, tile, part):
            parts = unit_parts(t, tile)
            for k in range(n8):
                dx, dc = NEAR[k]
                at = pl.ds(hand_at[dx][dc], dp)
                src, dst = stage.at[slot(t), tile, at], outs[t].at[i8, tile]

                def send(k=k, src=src, dst=dst):
                    if k:
                        rcopy(src, dst, e_s.at[t], e_r.at[t], near(*NEAR[k])).start()
                    else:
                        pltpu.make_async_copy(src, dst, out_sem.at[t]).start()

                if len(parts) == 1:
                    send()
                elif part == 0:
                    pl.when(xs[dx] < parts[0][2] // dp // 2)(send)
                else:
                    pl.when(xs[dx] >= parts[0][2] // dp // 2)(send)

        def handed(t):
            all_out(outs[t].at[pl.ds(0, n8 - 1)], e_s.at[t])
            pltpu.make_async_copy(outs[t].at[0], outs[t].at[0], out_sem.at[t]).wait()

        given = []

        def finish(t, tile):
            at = tile_rows(tile)
            wide = pl.ds(tile * LANE, LANE)
            for part, (n, first, size) in enumerate(unit_parts(t, tile)):
                lanes = pl.ds(first, size)
                all_in(rb.at[t, :, at, lanes], u_r.at[t, n])
                cs = [pltpu.make_async_copy(rb.at[t, s, at, lanes], tmp.at[s, at, lanes], tmp_sem.at[s]) for s in range(2)]
                start(cs)
                if t == Z_ORDER[2] and not given:
                    given.append(Z_ORDER[0])
                    handed(Z_ORDER[0])
                for c in cs:
                    c.wait()
                stage[slot(t), tile, lanes] = (far[t, wide, lanes] + tmp[0, wide, lanes] + tmp[1, wide, lanes]).T
                hand_out(t, tile, part)

        def on_y(r, n):
            return (r == 1) == (n == 1)

        def level(r, n):
            at = ys if on_y(r, n) else xs
            dev = ydev if on_y(r, n) else xdev
            if n == 1:
                def piece(k, h):
                    return part.at[r, pl.ds(2 * h, 2), at[k]] if on_y(r, n) else part.at[r, at[k], pl.ds(2 * h, 2)]
                return dev, piece, ra1, rb1, sd1, (a1_s, a1_r, f1_s, f1_r, d1_s, d1_r)

            def piece(k, h):
                return mid.at[r, at[k], pl.ds(h, 1)]
            return dev, piece, ra2, rb2, sd2, (a2_s, a2_r, f2_s, f2_r, d2_s, d2_r)

        def ring_a(r, n):
            dev, piece, rfar, _, _, sems = level(r, n)
            return [rcopy(piece(2, s), rfar.at[r, s], sems[0].at[r], sems[1].at[r], dev(1 + 2 * s)) for s in range(2)]

        def ring_f(r, n):
            dev, piece, _, rnear, _, sems = level(r, n)
            return [rcopy(piece(1 + 2 * s, 1 - s), rnear.at[r, s, 1 - s], sems[2].at[r], sems[3].at[r], dev(1 + 2 * s)) for s in range(2)]

        def ring_d(r, n):
            dev, _, _, rnear, dep, sems = level(r, n)
            return [rcopy(dep.at[r, s], rnear.at[r, s, s], sems[4].at[r], sems[5].at[r], dev(1 + 2 * s)) for s in range(2)]

        def add(grid, *terms):
            specs = []
            for ref, at, lead in terms:
                tail = ref.shape[lead:]
                specs.append(pl.BlockSpec((1,) * lead + tuple(tail), lambda *i, at=at, rank=len(tail): tuple(at(*i)) + (0,) * rank))

            def body(*refs):
                total = refs[0][...].astype(F32).reshape(refs[0].shape[-2:])
                for ref in refs[1:-1]:
                    total = total + ref[...].astype(F32).reshape(total.shape)
                refs[-1][...] = total.astype(BF16).reshape(refs[-1].shape)

            pltpu.emit_pipeline(body, grid=grid, in_specs=specs[:-1], out_specs=specs[-1:])(*[ref for ref, _, _ in terms])

        def ring_first(r, n):
            start(ring_a(r, n) + ring_f(r, n))

        def ring_dependent(r, n):
            _, _, rfar, _, _, sems = level(r, n)
            all_in(rfar.at[r], sems[1].at[r])
            here = y if on_y(r, n) else x
            if n == 1:
                def near_block(s, i):
                    at = lax.rem(here + 1 + 2 * s, RING)
                    return (2 * s + i, at) if on_y(r, n) else (at, 2 * s + i)

                add((2, 2), (part.at[r], near_block, 2), (ra1.at[r], lambda s, i: (s, i), 2), (sd1.at[r], lambda s, i: (s, i), 2))
            else:
                add((2,), (mid.at[r], lambda s: (lax.rem(here + 1 + 2 * s, RING), s), 2), (ra2.at[r], lambda s: (s, 0), 2),
                    (sd2.at[r], lambda s: (s, 0), 2))
            start(ring_d(r, n))

        def ring_last(r, n):
            _, _, rfar, _, _, sems = level(r, n)
            all_in(rfar.at[r], sems[3].at[r])
            all_in(rfar.at[r], sems[5].at[r])
            here = y if on_y(r, n) else x
            if n == 1:
                def own_at(h, i):
                    return (2 * h + i, here) if on_y(r, n) else (here, 2 * h + i)

                add((2, 2), (part.at[r], own_at, 2), (rb1.at[r, 0], lambda h, i: (h, i), 2),
                    (rb1.at[r, 1], lambda h, i: (h, i), 2), (mid.at[r], lambda h, i: (2 * h + i,), 1))
            else:
                own, res = ((tok_own, out), (grad_own, gin))[r]
                add((2,), (own, lambda h: (h,), 1), (mid.at[r], lambda h: (here, h), 2), (rb2.at[r, 0], lambda h: (h, 0), 2),
                    (rb2.at[r, 1], lambda h: (h, 0), 2), (res, lambda h: (h,), 1))

        def keep_rows(r):
            core_copy(r).wait_recv()
            row_products(r, True)

        run_order({
            "far_block": far_block, "next_products": next_products, "next_adds": next_adds, "next_blocks": next_blocks,
            "own_block": own_block, "finish": finish, "give_rows": give_rows, "keep_rows": keep_rows, "ring_first": ring_first,
            "ring_dependent": ring_dependent, "ring_last": ring_last,
        }, LATE_ORDER)

        for t in range(3):
            all_out(nxt.at[t], u_s.at[t])
        for r in range(2):
            core_copy(r).wait_send()
            for n in (1, 2):
                _, _, rfar, _, _, sems = level(r, n)
                for sem in sems[::2]:
                    all_out(rfar.at[r], sem.at[r])
        for t in Z_ORDER:
            with jax.named_scope(f"handed_{t}"):
                all_in(outs[t].at[pl.ds(0, n8 - 1)], e_r.at[t])
                if t not in given:
                    handed(t)

    pl.run_scoped(
        forward_phase,
        pltpu.VMEM((2, chunk, d), BF16),
        pltpu.VMEM((tokens, nf), BF16),
        pltpu.VMEM((tokens, nf), BF16),
        pltpu.VMEM((2, chunk, nf), BF16),
        pltpu.VMEM((2, 2, chunk, main), BF16),
        pltpu.VMEM((2, 2, chunk, packed), BF16),
        pltpu.VMEM((d, main), BF16),
        pltpu.VMEM((d, packed), BF16),
    )
    pl.run_scoped(backward_phase, pltpu.VMEM((2, tiles * LANE, cols), F32), pltpu.VMEM((2, tiles, cols, LANE), F32))


def layer(sg, su, sd, tok, grad):
    n8 = 2 * RING
    dp, nf = sg.shape[0], sg.shape[1] // n8
    rows, d = tok.shape
    tokens = rows * RING * n8
    cols = d // RING
    tiles = -(-nf // LANE)
    padded = tiles * LANE
    main = nf // LANE * LANE
    packed = -(-3 * (nf - main) // LANE) * LANE
    hbm = pl.BlockSpec(memory_space=pl.ANY)
    dma = pltpu.SemaphoreType.DMA
    sds = jax.ShapeDtypeStruct
    halves = (2, rows // 2, d)
    res = pl.pallas_call(
        layer_kernel,
        out_shape=[sds((n8, tiles, dp, LANE), F32)] * 3 + [sds(halves, BF16)] * 2 + [
            sds((d, main), BF16), sds((d, main), BF16), sds((d, main), BF16), sds((d, packed), BF16), sds((tokens, d), BF16), sds((tokens, d), BF16),
            sds((3, RING, 2, RING * rows, main), BF16), sds((2, RING, 2, RING * rows, packed), BF16),
            sds((3, nf, cols), F32), sds((3, 2, nf, cols), F32),
            sds((2, RING, RING, rows, d), BF16), sds((2, RING, RING, rows, d), BF16), sds((2, RING, RING, rows, d), BF16),
            sds((2, 2, 2, rows, d), BF16), sds((2, 2, 2, 2, rows, d), BF16), sds((2, 2, 2, rows, d), BF16),
            sds((2, RING, 2, rows // 2, d), BF16),
            sds((2, 2, 1, rows // 2, d), BF16), sds((2, 2, 2, 1, rows // 2, d), BF16), sds((2, 2, 1, rows // 2, d), BF16),
        ],
        in_specs=[hbm] * 7,
        out_specs=[hbm] * 25,
        scratch_shapes=[
            pltpu.VMEM((3, nf, tokens), BF16),
            pltpu.VMEM((2, tokens, cols), BF16),
            pltpu.VMEM((3, padded, cols), F32),
            pltpu.VMEM((3, 2, nf, cols), F32),
            dma((7,)),
            dma((4,)), dma((4, n8)),
            dma((4, 2)), dma((4, 2, n8 // 2)), dma((4, 2)),
            dma((4, 2)), dma((4, 2)),
            dma((3,)), dma((3, 2)),
            dma((3,)), dma((3,)),
            dma((3,)), dma((3, 2, RING)),
            dma((3,)), dma((3, RING)),
            dma((3,)), dma((RING + 2,)),
            dma((3,)), dma((4,)), dma((2,)), dma((2, 3)), dma((2,)), dma((2,)),
            dma((3,)), dma((3,)),
            dma((3,)), dma((3, tiles + 1)),
            dma((3,)), dma((3,)),
            dma((3,)),
            dma((2,)), dma((2,)),
        ] + [dma((2,))] * 12,
        compiler_params=pltpu.CompilerParams(collective_id=0, has_side_effects=True, vmem_limit_bytes=67043328),
        cost_estimate=pl.CostEstimate(flops=18 * nf * tokens * d, bytes_accessed=300_000_000, transcendentals=0),
        name="layer",
    )(sg, su, sd, tok, grad, tok.reshape(halves), grad.reshape(halves))
    return res[:3], res[3].reshape(rows, d), res[4].reshape(rows, d)


def assemble_kernel(og, ou, od, out, gin, g, u, w, res, gres, buf, flat, in_sem, out_sem, row_buf, row_sem):
    n8, tiles, dp = og.shape[:3]
    nf = g.shape[1] // n8
    srcs, dsts = (og, ou, od), (g, u, w)
    half = dp // 2
    parts = [(t, h) for t in range(3) for h in range(2)]

    def load(n):
        t, h = parts[n]
        at = pl.ds(h * half, half)
        return pltpu.make_async_copy(srcs[t].at[:, :, at], buf.at[t, :, :, at], in_sem.at[n])

    def store(n):
        t, h = parts[n]
        at = pl.ds(h * half, half)
        return pltpu.make_async_copy(flat.at[t, at], dsts[t].at[at], out_sem.at[n])

    rows_in = [pltpu.make_async_copy(src, row_buf.at[r], row_sem.at[r]) for r, src in enumerate((out, gin))]
    rows_out = [pltpu.make_async_copy(row_buf.at[r], dst, row_sem.at[r]) for r, dst in enumerate((res, gres))]
    for n in range(2):
        load(n).start()
    for c in rows_in:
        c.start()
    for n, (t, h) in enumerate(parts):
        load(n).wait()
        if n + 2 < len(parts):
            load(n + 2).start()
        at = pl.ds(h * half, half)
        for j in range(n8):
            flat[t, at, j * nf:(j + 1) * nf] = jnp.concatenate([buf[t, j, tile, at] for tile in range(tiles)], axis=1)[:, :nf]
        store(n).start()
        if n < 2:
            rows_in[n].wait()
            rows_out[n].start()
    for n in range(len(parts)):
        store(n).wait()
    for c in rows_out:
        c.wait()


def assemble(sums, out, gin, ff):
    dp = sums[0].shape[2]
    hbm = pl.BlockSpec(memory_space=pl.ANY)
    dma = pltpu.SemaphoreType.DMA
    sds = jax.ShapeDtypeStruct
    return pl.pallas_call(
        assemble_kernel,
        out_shape=[sds((dp, ff), F32)] * 3 + [sds(out.shape, BF16)] * 2,
        in_specs=[hbm] * 5,
        out_specs=[hbm] * 5,
        scratch_shapes=[
            pltpu.VMEM((3,) + sums[0].shape, F32), pltpu.VMEM((3, dp, ff), F32), dma((6,)), dma((6,)),
            pltpu.VMEM((2,) + out.shape, BF16), dma((2,)),
        ],
        compiler_params=pltpu.CompilerParams(vmem_limit_bytes=63 * 1024 * 1024),
        name="assemble",
    )(*sums, out, gin)


def solution(mesh):
    nz, ny, nd = mesh.shape["datb"], mesh.shape["model"], mesh.shape["data"]
    fine = Mesh(mesh.devices.reshape(nz, ny, nd // 2, 2), ("datb", "model", "x", "core"))

    def local_step(tok_loc, wg_loc, wu_loc, wd_loc, grad_loc):
        sums, out, grad_in = layer(wg_loc, wu_loc, wd_loc.T, tok_loc, grad_loc)
        grad_gate, grad_up, grad_down_t, out, grad_in = assemble(sums, out, grad_in, wg_loc.shape[1])
        return out, grad_in, grad_gate, grad_up, grad_down_t.T

    return jax.shard_map(local_step, mesh=fine, in_specs=(ROW_SPEC, GATE_SPEC, GATE_SPEC, DOWN_SPEC, ROW_SPEC), out_specs=(ROW_SPEC, ROW_SPEC, GATE_SPEC, GATE_SPEC, DOWN_SPEC), check_vma=False)
```

```python
import functools

import jax
import jax.numpy as jnp
from jax import lax
from jax.experimental import pallas as pl
from jax.experimental.pallas import tpu as pltpu
from jax.sharding import Mesh
from jax.sharding import PartitionSpec as P

ROW_SPEC = P(("datb", "x", "core", "model"), None)
GATE_SPEC = P(("datb", "x", "core"), "model")
DOWN_SPEC = P("model", ("datb", "x", "core"))
BF16 = jnp.bfloat16
F32 = jnp.float32
MESH_ID = pl.DeviceIdType.MESH
RING = 4
NEAR = ((0, 0), (0, 1), (1, 0), (3, 0), (1, 1), (3, 1), (2, 0), (2, 1))
DELTAS = (0, 3, 1, 2)
LANE = 128
OUT_COLS = 512
EX, Z1, Z2, P1, P2, BL, Q1, Q2, WD, CI = range(10)
GATHER_STEPS = (
    (Z1, 0, 0), (P1, 0, 0), (P1, 0, 1), (EX, 0, 1), (BL, 0, 0), (P1, 2, 0), (P1, 2, 1), (EX, 0, 2), (Z1, 3, 0), (EX, 3, 1), (EX, 3, 2),
    (EX, 3, 3), (EX, 3, 4), (EX, 3, 5), (EX, 3, 6), (EX, 3, 7), (Z1, 1, 0), (EX, 1, 1), (Z1, 2, 0), (EX, 2, 1), (EX, 0, 3), (BL, 1, 0),
    (Z1, 3, 1), (EX, 0, 4), (EX, 0, 5), (Z1, 0, 1), (Z1, 1, 1), (Z2, 3, 0, 0), (Z1, 2, 1), (EX, 0, 6), (EX, 0, 7), (Z2, 0, 0, 0),
    (Z2, 1, 0, 0), (EX, 1, 2), (EX, 1, 3), (Z2, 2, 0, 0), (Z2, 3, 0, 1), (P2, 0, 0), (P2, 0, 1), (BL, 0, 1), (Q1, 0, 0, 1), (Z1, 3, 2),
    (Z1, 3, 3), (Z1, 3, 4), (Q1, 0, 0, 0), (Z1, 3, 5), (Z2, 0, 0, 1), (EX, 1, 4), (EX, 1, 5), (P2, 2, 1), (Z1, 3, 6), (EX, 1, 6),
    (EX, 1, 7), (Z1, 3, 7), (Z1, 0, 2), (Q1, 1, 0, 1), (Z2, 3, 1, 0), (Z2, 3, 1, 1), (Z1, 0, 3), (EX, 2, 2), (EX, 2, 3), (Z2, 3, 1, 2),
    (BL, 0, 2), (Z2, 3, 1, 3), (Z1, 0, 4), (EX, 2, 4), (EX, 2, 5), (Z1, 0, 5), (EX, 2, 6), (EX, 2, 7), (Z2, 3, 0, 2), (Q1, 0, 1, 1),
    (Z2, 3, 0, 3), (Z1, 0, 6), (P1, 1, 0), (P1, 1, 1), (Q1, 0, 1, 0), (Z1, 0, 7), (BL, 2, 2), (Z2, 0, 1, 0), (Z1, 1, 2), (Z2, 0, 1, 1),
    (Z2, 0, 0, 2), (Q2, 0, 0), (Z2, 0, 1, 2), (Z2, 0, 0, 3), (BL, 2, 0), (BL, 0, 3), (Q1, 0, 2, 1), (Z2, 0, 1, 3), (Z1, 1, 3), (Z1, 1, 4),
    (WD, 3), (Z1, 1, 5), (Q1, 0, 2, 0), (Z1, 1, 6), (P2, 2, 0), (BL, 2, 1), (P2, 1, 0), (P2, 1, 1), (Z1, 1, 7), (Q1, 0, 3, 1),
    (Q1, 1, 0, 0), (Z2, 1, 0, 1), (Q1, 2, 2, 0), (Q1, 2, 2, 1), (Z2, 1, 0, 2), (BL, 1, 1), (Q2, 0, 1), (WD, 0), (Z2, 1, 1, 0), (CI, 0),
)
GATE_STEPS = (
    (),
    (),
    (
        (Z1, 2, 2),
    ),
    (
        (Q2, 0, 2), (Z2, 1, 1, 1), (Z2, 1, 0, 3), (Q1, 2, 0, 0), (Q1, 2, 0, 1), (BL, 1, 2), (CI, 1),
    ),
    (
        (Z2, 1, 1, 2), (Z1, 2, 3),
    ),
    (
        (Q1, 0, 3, 0), (Z2, 1, 1, 3), (Z1, 2, 4), (CI, 2),
    ),
    (
        (Z1, 2, 5), (Q1, 2, 1, 0), (Q1, 2, 1, 1), (BL, 2, 3), (BL, 1, 3), (Z1, 2, 6), (Q2, 0, 3),
    ),
    (
        (Q2, 1, 0), (Z1, 2, 7), (CI, 3),
    ),
    (
        (Q2, 2, 0), (Q2, 2, 2), (Z2, 2, 0, 1), (Q1, 1, 1, 0), (Q1, 1, 1, 1),
    ),
)
UP_STEPS = (
    (
        (Z2, 2, 0, 2), (Q1, 1, 2, 1), (WD, 1),
    ),
    (
        (Q2, 2, 1), (Q1, 2, 3, 1), (Q1, 1, 2, 0),
    ),
    (
        (Z2, 2, 1, 0), (Z2, 2, 0, 3), (Q1, 1, 3, 1),
    ),
    (
        (Z2, 2, 1, 1), (Q1, 1, 3, 0),
    ),
    (
        (Q2, 1, 2), (Z2, 2, 1, 2), (Q1, 2, 3, 0),
    ),
    (
        (Q2, 1, 1), (Z2, 2, 1, 3),
    ),
    (
        (Q2, 1, 3), (Q2, 2, 3),
    ),
    (),
)
LATE_STEPS = (
    (WD, 2),
)
Z_ORDER = (2, 0, 1)
EARLY_ORDER = (
    ("far_block", 2), ("next_products", 2), ("late",), ("give_rows", 0),
)
LATE_ORDER = (
    ("next_adds", 2), ("own_block", 2), ("keep_rows", 0), ("ring_first", 0, 1), ("finish", 2, 0), ("far_block", 0), ("give_rows", 1),
    ("finish", 2, 3), ("finish", 2, 1), ("finish", 2, 4), ("ring_dependent", 0, 1), ("finish", 2, 2), ("far_block", 1), ("keep_rows", 1),
    ("ring_first", 1, 1), ("next_blocks", 0), ("own_block", 0), ("next_blocks", 1), ("own_block", 1), ("finish", 0, 0),
    ("ring_dependent", 1, 1), ("finish", 0, 1), ("ring_last", 0, 1), ("ring_first", 0, 2), ("finish", 0, 2), ("finish", 0, 3),
    ("finish", 0, 4), ("ring_last", 1, 1), ("ring_first", 1, 2), ("ring_dependent", 0, 2), ("finish", 1, 0), ("ring_dependent", 1, 2),
    ("ring_last", 0, 2), ("finish", 1, 1), ("finish", 1, 2), ("ring_last", 1, 2), ("finish", 1, 3), ("finish", 1, 4),
)


def dot(a, b, ca, cb):
    return lax.dot_general(a, b, (((ca,), (cb,)), ((), ())), preferred_element_type=F32)


def layer_kernel(sg, su, sd, tok, grad, tok_own, grad_own,
                 og, ou, od, out, gin, wg, wu, wd, wr, tok_all, grad_all, h_main, h_rest, ra, rb, give, rc, part, ra1, rb1, sd1, mid, ra2, rb2, sd2,
                 ff, blk, far, nxt,
                 own_sem, ex_s, ex_r, z1_s, z1_r, zn_r, z2_s, p1_s, p1_r, p2_s, p2_r, q1_s, q1_r, q2_s, q2_r, cc_s, cc_r,
                 sh_sem, wv_sem, row_sem, hst_sem, blk_sem, tmp_sem, a_s, a_r, u_s, u_r, e_s, e_r, out_sem,
                 c_s, c_r, a1_s, a1_r, f1_s, f1_r, a2_s, a2_r, f2_s, f2_r):
    z, y = lax.axis_index("datb"), lax.axis_index("model")
    x, core = lax.axis_index("x"), lax.axis_index("core")
    i8 = 2 * x + core
    n8 = 2 * RING
    rows, d = tok.shape
    half_rows = rows // 2
    chunk = RING * rows
    n_chunk = n8
    nf, tokens = ff.shape[1:]
    dp = sg.shape[0]
    half = nf // 2
    main = wg.shape[1]
    rest = nf - main
    packed = wr.shape[1]
    cols = blk.shape[2]
    tiles = far.shape[1] // LANE
    outs = (og, ou, od)

    zs, ys, xs = ([v] + [lax.rem(v + k, RING) for k in range(1, RING)] for v in (z, y, x))
    cores = (core, 1 - core)
    peers = [[2 * v + c for c in cores] for v in xs]
    slot_at = [[[pl.multiple_of((zz * n8 + peers[dx][dc]) * dp, 16) for dc in range(2)] for dx in range(RING)] for zz in zs]
    hand_at = [[pl.multiple_of(p * dp, 8) for p in row] for row in peers]
    rows_at = [[[pl.multiple_of((peers[dx][dc] * RING + yy) * rows, half_rows) for dc in range(2)] for yy in ys] for dx in range(RING)]
    lanes_at = [pl.multiple_of(zz * cols, LANE) for zz in zs]

    def peer(dx, dc):
        return peers[dx][dc]

    def zdev(k):
        return {"datb": zs[k]}

    def xdev(k):
        return {"x": xs[k]}

    def ydev(k):
        return {"model": ys[k]}

    def near(dx, dc):
        return {"x": xs[dx], "core": cores[dc]}

    def copy(src, dst, s, r, dev):
        return pltpu.make_async_remote_copy(src_ref=src, dst_ref=dst, send_sem=s, recv_sem=r, device_id=dev, device_id_type=MESH_ID)

    rcopy = copy

    def all_in(ref, sem):
        copy(ref, ref, sem, sem, zdev(1)).wait_recv()

    def all_out(ref, sem):
        copy(ref, ref, sem, sem, zdev(1)).wait_send()

    def start(copies):
        for c in copies:
            c.start()

    def received(copies):
        for c in copies:
            c.wait_recv()

    def sent(copies):
        for c in copies:
            c.wait_send()

    def run_order(fns, order):
        for fn, *args in order:
            with jax.named_scope("_".join(str(v) for v in [fn, *args])):
                fns[fn](*args)

    barrier = pltpu.get_barrier_semaphore()
    others = [zdev(1), zdev(3), ydev(1), ydev(3)] + [near(*n) for n in NEAR[1:]]
    for dev in others:
        pl.semaphore_signal(barrier, inc=1, device_id=dev, device_id_type=MESH_ID)

    def blk_load(t, slot, k):
        src = tok_all if t < 2 else grad_all
        return pltpu.make_async_copy(src.at[:, pl.ds(lanes_at[k], cols)], blk.at[slot], blk_sem.at[slot])

    plan = []
    for fn, *args in EARLY_ORDER + LATE_ORDER:
        plan += [(args[0], k) for k in {"far_block": (2,), "next_blocks": (1, 3), "next_products": (1, 3), "own_block": (0,)}.get(fn, ())]
    taken = []

    def next_block():
        n = len(taken)
        taken.append(n)
        blk_load(plan[n][0], n % 2, plan[n][1]).wait()
        if n + 1 < len(plan):
            blk_load(plan[n + 1][0], (n + 1) % 2, plan[n + 1][1]).start()
        return n % 2

    def product(t, dst, then=None):
        slot = next_block()
        step = 2 * LANE
        count = -(-cols // step)

        def one(n, carry):
            lanes = pl.ds(pl.multiple_of(jnp.minimum(n * step, cols - step), LANE), step)
            dst[:nf, lanes] = jnp.dot(ff[t], blk[slot, :, lanes], preferred_element_type=F32)
            for k in range(count if then else 0):
                first = k * step if k < count - 1 else cols - step
                size = step if k == count - 1 else min(step, cols - step - first)
                if size > 0:
                    pl.when(n == k)(functools.partial(then, first, size))
            return carry

        lax.fori_loop(0, count, one, 0)

    lo, hi = pl.ds(0, half), pl.ds(half, half)

    def a_copies(t, first=0, size=cols):
        lanes = pl.ds(first, size)
        return [rcopy(far.at[t, at, lanes], ra.at[t, at, lanes], a_s.at[t], a_r.at[t], zdev(k)) for at, k in ((lo, 1), (hi, 3))]

    def tile_rows(tile):
        return pl.ds(tile * LANE, min(LANE, nf - tile * LANE))

    def unit_parts(t, tile):
        if (t, tile) != (Z_ORDER[2], tiles - 1):
            return [(tile, 0, cols)]
        first = -(-cols // 2 // LANE) * LANE
        return [(tile, 0, first), (tiles, first, cols - first)]

    def unit_copies(t, tile):
        at = tile_rows(tile)
        cs = []
        for n, first, size in unit_parts(t, tile):
            lanes = pl.ds(first, size)
            cs += [rcopy(nxt.at[t, s, at, lanes], rb.at[t, s, at, lanes], u_s.at[t], u_r.at[t, n], zdev(1 + 2 * s)) for s in range(2)]
        return cs

    def far_block(t):
        if t == Z_ORDER[0]:
            product(t, far.at[t], lambda first, size: start(a_copies(t, first, size)))
        else:
            product(t, far.at[t])
            start(a_copies(t))

    def early_units(t):
        if ("next_products", t) not in EARLY_ORDER + LATE_ORDER:
            return ()
        free = [(0, tile) for tile in range(tiles) if tile * LANE >= half]
        return free + [(1, tile) for tile in range(tiles) if (tile + 1) * LANE <= half]

    def next_products(t):
        for s in range(2):
            product(t, nxt.at[t, s])
        for s, tile in early_units(t):
            unit_copies(t, tile)[s].start()

    blocks = d // min(OUT_COLS, d)
    width = d // blocks

    def row_products(r, keep):
        side = core if keep else 1 - core
        specs, args = [], []
        for h, j, w in ((h_main, 2, wd), (h_rest, 0, wr)) if r == 0 else ((h_main, 0, wg), (h_main, 1, wu), (h_rest, 1, wr)):
            n = w.shape[1]
            specs += [pl.BlockSpec((1, RING, 1, RING * rows, n), lambda i, j=j: (j, 0, side, 0, 0)), pl.BlockSpec((width, n), lambda i: (i, 0))]
            args += [h, w]
        wide = pl.BlockSpec((RING, RING, rows, width), lambda i: (0, 0, 0, i))
        terms = len(args) // 2
        if keep:
            specs.append(wide)
            args.append(rc.at[r])

        def body(*refs):
            total = None
            for i in range(terms):
                h = refs[2 * i][...].reshape(RING * RING * rows, refs[2 * i].shape[-1])
                prod = dot(h, refs[2 * i + 1][...], 1, 1)
                total = prod if total is None else total + prod
            if keep:
                total = total + refs[-2][...].astype(F32).reshape(total.shape)
            refs[-1][...] = total.astype(BF16).reshape(RING, RING, rows, width)

        pltpu.emit_pipeline(body, grid=(blocks,), in_specs=specs, out_specs=[wide])(*args, (part if keep else give).at[r])

    def core_copy(r):
        return rcopy(give.at[r], rc.at[r], c_s.at[r], c_r.at[r], near(0, 1))

    def give_rows(r):
        row_products(r, False)
        core_copy(r).start()

    def forward_phase(rowbuf, av, bv, gv, hst, hst_rest, wv_a, wv_r):
        held = {}

        fulls = (wg, wu, wd, wr)
        REST = 3
        def shard_load(t):
            return pltpu.make_async_copy((sg, su, sd)[t], held["shard"].at[t], sh_sem.at[t])

        def cut_pieces(t):
            if t == REST:
                for u in range(3):
                    for j in range(n8):
                        held["rests"][j, :, u * rest:(u + 1) * rest] = held["shard"][u, :, j * nf + main:(j + 1) * nf]
            else:
                for j in range(n8):
                    held["pieces"][t, j] = held["shard"][t, :, j * nf:j * nf + main]
            own_piece(t).start()

        def piece(t, j):
            return held["rests"].at[j] if t == REST else held["pieces"].at[t, j]

        def own_piece(t):
            return pltpu.make_async_copy(piece(t, i8), slot(t, 0, NEAR[0]), own_sem.at[t])

        def go(make, *args):
            make(*args).start()

        def slot(t, k, source):
            dx, dc = source
            return fulls[t].at[pl.ds(slot_at[k][dx][dc], dp)]

        def source(k):
            dx, dc = NEAR[k]
            return (RING - dx) % RING, dc

        def back(side):
            return 3 if side == 0 else 1

        def ahead(side):
            return 1 if side == 0 else 3

        def exchange_copy(t, k):
            return copy(piece(t, peer(*NEAR[k])), slot(t, 0, NEAR[0]), ex_s.at[t], ex_r.at[t, k], near(*NEAR[k]))

        def exchange(t, k):
            go(exchange_copy, t, k)

        def z_first_copy(t, side, k):
            here = slot(t, 0, source(k))
            return copy(here if k else piece(t, i8), here, z1_s.at[t], z1_sem(t, side, k), zdev(ahead(side)))

        def z_first(t, k):
            if k:
                here = slot(t, 0, source(k))
                all_in(here, ex_r.at[t, k])
            for side in range(2):
                go(z_first_copy, t, side, k)

        def z1_sem(t, side, k):
            return z1_r.at[t, side, k % (n8 // 2)] if (k < n8 // 2) == (side == 0) else zn_r.at[t]

        def some(t, count):
            return fulls[t].at[pl.ds(0, count * dp)]

        def z_second_copy(t, side, k):
            there = slot(t, back(side), source(k + side * (n8 // 2)))
            return copy(there, there, z2_s.at[t], zn_r.at[t], zdev(ahead(side)))

        def z_second(t, side, k):
            kk = k + side * (n8 // 2)
            all_in(slot(t, back(side), source(kk)), z1_sem(t, side, kk))
            go(z_second_copy, t, side, k)

        def weights_done(t):
            if (WD, t) not in LATE_STEPS:
                own_wait(t)
            all_in(some(t, 2 * n8), zn_r.at[t])
            w_load(t).start()

        cut = d * 11 // 28
        rings = ((tok, tok_all, pl.ds(0, d), True), (grad, grad_all, pl.ds(0, cut), True), (grad, grad_all, pl.ds(cut, d - cut), False))

        def axis(r, n):
            return xdev if rings[r][3] == (n == 1) else ydev

        def block(r, da, db, flip=0, lo=0, size=rows):
            dx, dy = (da, db) if rings[r][3] else (db, da)
            first = rows_at[dx][dy][flip]
            return rings[r][1].at[pl.ds(pl.multiple_of(first + lo, half_rows) if lo else first, size), rings[r][2]]

        def own_block(r):
            return rings[r][0].at[:, rings[r][2]]

        def to_core_copy(r, ia, ib):
            there = block(r, DELTAS[ia], DELTAS[ib])
            return copy(own_block(r) if ia == 0 and ib == 0 else there, there, cc_s.at[r], cc_r.at[ia if r == 0 else RING - 1 + r], near(0, 1))

        def to_core(r, ia, ib):
            go(to_core_copy, r, ia, ib)

        def first_copy(r, side):
            return copy(own_block(r), block(r, 0, 0), p1_s.at[r], p1_r.at[r, side], axis(r, 1)(ahead(side)))

        def first_own(r, side):
            go(first_copy, r, side)

        def first_far_copy(r, side):
            part = block(r, back(side), 0, 0, side * half_rows, half_rows)
            return copy(part, part, p2_s.at[r], p2_r.at[r], axis(r, 1)(ahead(side)))

        def first_forward(r, side):
            there = block(r, back(side), 0)
            all_in(there, p1_r.at[r, side])
            go(first_far_copy, r, side)

        def block_on(r, ia):
            if ia == 3:
                all_in(block(r, 2, 0), p2_r.at[r])
            for side in range(2):
                go(second_copy, r, side, ia)
            to_core(r, ia, 0)

        def second_copy(r, side, ia):
            there = block(r, DELTAS[ia], 0)
            return copy(there if ia else own_block(r), there, q1_s.at[r], q1_r.at[r, side, ia], axis(r, 2)(ahead(side)))

        def second_far_copy(r, ia):
            side = ia // 2
            there = block(r, DELTAS[ia], back(side))
            return copy(there, there, q2_s.at[r], q2_r.at[r, ia], axis(r, 2)(ahead(side)))

        def second_forward(r, ia, side):
            there = block(r, DELTAS[ia], back(side))
            all_in(there, q1_r.at[r, side, ia])
            if ia // 2 == side:
                go(second_far_copy, r, ia)
            to_core(r, ia, 1 if side == 0 else 2)

        def second_far(r, ia):
            there = block(r, DELTAS[ia], 2)
            all_in(there, q2_r.at[r, ia])
            to_core(r, ia, 3)

        def some_rows(r, count):
            return rings[r][1].at[pl.ds(0, count * rows), rings[r][2]]

        def chunk_in(ia):
            all_in(some_rows(0, RING), cc_r.at[ia])

        def rows_in(r):
            all_in(some_rows(r, RING * RING), cc_r.at[RING - 1 + r])

        def own_wait(t):
            there = slot(t, 0, NEAR[0])
            pltpu.make_async_copy(there, there, own_sem.at[t]).wait()

        def own_rows(r):
            return pltpu.make_async_copy(own_block(r), block(r, 0, 0), own_sem.at[4 + r])

        def w_load(t):
            return pltpu.make_async_copy(fulls[t], (wv_a, held["wv_b"], wv_a, wv_r)[t], wv_sem.at[t])

        def row_load(src, i, buf):
            return pltpu.make_async_copy(src.at[chunk_rows(i)], rowbuf.at[buf], row_sem.at[buf])

        def chunk_loop(src, products, elementwise, between, last=lambda: None):
            row_load(src, 0, 0).start()
            between[0]()
            row_load(src, 1, 1).start()
            row_load(src, 0, 0).wait()
            products(0, 0)

            def body(i, carry):
                buf = lax.rem(i, 2)

                @pl.when(i + 1 < n_chunk)
                def _():
                    row_load(src, i + 1, 1 - buf).start()

                for k, step in enumerate(between[1:], 1):
                    pl.when(i == k)(step)
                row_load(src, i, buf).wait()
                free(elementwise, i - 1)
                elementwise(i - 1, 1 - buf, lambda: products(i, buf))
                return carry

            lax.fori_loop(1, n_chunk, body, 0)
            last()
            free(elementwise, n_chunk - 1)
            elementwise(n_chunk - 1, (n_chunk - 1) % 2, lambda: None)

        def free(elementwise, i):
            @pl.when(i >= 2)
            def _():
                for cp in copies_of[elementwise](i - 2):
                    cp.wait()

        def chunk_rows(i):
            return pl.ds(pl.multiple_of(i * chunk, chunk), chunk)

        def h_copies(i, which, names):
            xx, c = lax.div(i, 2), lax.rem(i, 2)
            cs = [pltpu.make_async_copy(hst.at[c, n], h_main.at[j, xx, c], hst_sem.at[c, n]) for n, j in enumerate(names)]
            return cs + [pltpu.make_async_copy(hst_rest.at[which, c], h_rest.at[which, xx, c], hst_sem.at[c, 2])]

        def keep(i, c, values):
            which = len(values) - 1
            for n, (j, v) in enumerate(values):
                low = v.astype(BF16)
                hst[c, n] = low[:, :main]
                hst_rest[which, c, :, j * rest:(j + 1) * rest] = low[:, main:]
                ff[j, :, chunk_rows(i)] = v.T.astype(BF16)

        def kept(elementwise):
            for i in (n_chunk - 2, n_chunk - 1):
                for cp in copies_of[elementwise](i):
                    cp.wait()

        def gate_work():
            def place(k):
                ia, flip = lax.div(k, 2), lax.rem(k, 2)
                delta = lax.rem(3 * ia + 3 * lax.div(ia, 2) + 2 * lax.div(ia, 3), RING)
                return 2 * lax.rem(x + delta, RING) + lax.rem(core + flip, 2)

            def body(k, carry):
                for n, group in enumerate(GATE_STEPS):
                    if group:
                        pl.when(k == n)(functools.partial(run, group))

                @pl.when(k < n_chunk)
                def _():
                    row_load(tok_all, place(k), lax.rem(k, 2)).start()

                @pl.when(k >= 1)
                def _():
                    i, buf = place(k - 1), lax.rem(k - 1, 2)
                    row_load(tok_all, i, buf).wait()
                    rb_ = rowbuf[buf]
                    av[chunk_rows(i), :main] = jnp.dot(rb_, wv_a[...], preferred_element_type=F32).astype(BF16)
                    both = jnp.dot(rb_, wv_r[...], preferred_element_type=F32).astype(BF16)
                    av[chunk_rows(i), main:] = both[:, :rest]
                    bv[chunk_rows(i), main:] = both[:, rest:2 * rest]

                return carry

            lax.fori_loop(0, n_chunk + 1, body, 0)

        def up_products(i, buf):
            bv[chunk_rows(i), :main] = jnp.dot(rowbuf[buf], held["wv_b"][...], preferred_element_type=F32).astype(BF16)

        def hidden(i, c, beside):
            a, b = av[chunk_rows(i)].astype(F32), bv[chunk_rows(i)].astype(F32)
            beside()
            keep(i, c, ((2, a * jax.nn.sigmoid(a) * b),))
            start(copies_of[hidden](i))

        def down_products(i, buf):
            rb_ = rowbuf[buf]
            lanes = 2 * rest // LANE * LANE
            low = jnp.dot(rb_, wv_r[:, lanes:], preferred_element_type=F32)[:, 2 * rest - lanes:3 * rest - lanes]
            gv[buf] = jnp.concatenate([jnp.dot(rb_, wv_a[...], preferred_element_type=F32), low], axis=1).astype(BF16)

        def backward(i, c, beside):
            g = gv[c].astype(F32)
            a, b = av[chunk_rows(i)].astype(F32), bv[chunk_rows(i)].astype(F32)
            beside()
            sig = jax.nn.sigmoid(a)
            keep(i, c, ((0, g * b * sig * (1.0 + a * (1.0 - sig))), (1, g * (a * sig))))
            start(copies_of[backward](i))

        copies_of = {hidden: lambda i: h_copies(i, 0, (2,)), backward: lambda i: h_copies(i, 1, (0, 1))}

        steps = (exchange, z_first, z_second, first_own, first_forward, block_on, second_forward, second_far, weights_done, chunk_in)

        def run(group):
            for which, *args in group:
                steps[which](*args)

        def rows_ready():
            for r in (1, 2):
                own_rows(r).wait()
                rows_in(r)
            blk_load(plan[0][0], 0, plan[0][1]).start()

        def gather_phase(shard, pieces, rests, wv_b):
            held.update(shard=shard, pieces=pieces, rests=rests, wv_b=wv_b)
            with jax.named_scope("begin"):
                shard_load(0).start()
                shard_load(0).wait()
                for t in (1, 2):
                    shard_load(t).start()
                cut_pieces(0)
                pl.semaphore_wait(barrier, len(others))
                for r in range(3):
                    own_rows(r).start()
            with jax.named_scope("gather"):
                cut = {0}
                for step in GATHER_STEPS:
                    if step[0] in (EX, Z1) and step[1] not in cut:
                        if len(cut) == 1:
                            rests[...] = jnp.zeros_like(rests)
                            hst_rest[...] = jnp.zeros_like(hst_rest)
                            shard_load(1).wait()
                            shard_load(2).wait()
                        cut.add(step[1])
                        cut_pieces(step[1])
                    run((step,))
                own_rows(0).wait()
                w_load(0).wait()
                w_load(REST).wait()
            with jax.named_scope("gate"):
                gate_work()
            with jax.named_scope("up"):
                run(UP_STEPS[0])
                w_load(1).wait()
                chunk_loop(tok_all, up_products, hidden, [functools.partial(run, group) for group in ((),) + UP_STEPS[1:]], rows_ready)
                kept(hidden)
            for _, t in LATE_STEPS:
                own_wait(t)
            for t in range(4):
                all_out(some(t, n8 - 1), ex_s.at[t])
                all_out(some(t, 2 * n8), z1_s.at[t])

        pl.run_scoped(
            gather_phase, pltpu.VMEM((3,) + sg.shape, BF16), pltpu.VMEM((3, n8, dp, main), BF16), pltpu.VMEM((n8, dp, packed), BF16),
            pltpu.VMEM((d, main), BF16))
        run_order({
            "far_block": far_block, "next_products": next_products, "give_rows": give_rows, "late": functools.partial(run, LATE_STEPS),
        }, EARLY_ORDER)
        with jax.named_scope("down"):
            w_load(2).wait()
            chunk_loop(grad_all, down_products, backward, [lambda: None])
            kept(backward)
        for t in range(4):
            all_out(some(t, n8), z2_s.at[t])
        for r in range(3):
            for count, sem in ((2, p1_s), (1, p2_s), (2 * RING, q1_s), (RING, q2_s), (RING * RING, cc_s)):
                all_out(some_rows(r, count), sem.at[r])

    def backward_phase(tmp, stage):
        def next_adds(t):
            all_in(ra.at[t], a_r.at[t])
            cs = [pltpu.make_async_copy(ra.at[t, at], tmp.at[s, at], tmp_sem.at[s]) for s, at in ((0, lo), (1, hi))]
            start(cs)
            for c, (s, at) in zip(cs, ((0, lo), (1, hi))):
                c.wait()
                nxt[t, s, at] += tmp[s, at]
            for tile in range(tiles):
                start(c for s, c in enumerate(unit_copies(t, tile)) if (s, tile) not in early_units(t))

        def next_blocks(t):
            next_products(t)
            next_adds(t)

        def own_block(t):
            all_out(ra.at[t], a_s.at[t])
            product(t, far.at[t])

        def slot(t):
            return Z_ORDER.index(t) % 2

        def hand_out(t, tile, part):
            parts = unit_parts(t, tile)
            for k in range(n8):
                dx, dc = NEAR[k]
                at = pl.ds(hand_at[dx][dc], dp)
                src, dst = stage.at[slot(t), tile, at], outs[t].at[i8, tile]

                def send(k=k, src=src, dst=dst):
                    if k:
                        rcopy(src, dst, e_s.at[t], e_r.at[t], near(*NEAR[k])).start()
                    else:
                        pltpu.make_async_copy(src, dst, out_sem.at[t]).start()

                if len(parts) == 1:
                    send()
                elif part == 0:
                    pl.when(xs[dx] < parts[0][2] // dp // 2)(send)
                else:
                    pl.when(xs[dx] >= parts[0][2] // dp // 2)(send)

        def handed(t):
            all_out(outs[t].at[pl.ds(0, n8 - 1)], e_s.at[t])
            pltpu.make_async_copy(outs[t].at[0], outs[t].at[0], out_sem.at[t]).wait()

        given = []

        def finish(t, tile):
            at = tile_rows(tile)
            wide = pl.ds(tile * LANE, LANE)
            for part, (n, first, size) in enumerate(unit_parts(t, tile)):
                lanes = pl.ds(first, size)
                all_in(rb.at[t, :, at, lanes], u_r.at[t, n])
                cs = [pltpu.make_async_copy(rb.at[t, s, at, lanes], tmp.at[s, at, lanes], tmp_sem.at[s]) for s in range(2)]
                start(cs)
                if t == Z_ORDER[2] and not given:
                    given.append(Z_ORDER[0])
                    handed(Z_ORDER[0])
                for c in cs:
                    c.wait()
                stage[slot(t), tile, lanes] = (far[t, wide, lanes] + tmp[0, wide, lanes] + tmp[1, wide, lanes]).T
                hand_out(t, tile, part)

        def on_y(r, n):
            return (r == 1) == (n == 1)

        def level(r, n):
            at = ys if on_y(r, n) else xs
            dev = ydev if on_y(r, n) else xdev
            if n == 1:
                def piece(k, h):
                    return part.at[r, pl.ds(2 * h, 2), at[k]] if on_y(r, n) else part.at[r, at[k], pl.ds(2 * h, 2)]
                return dev, piece, ra1, rb1, sd1, (a1_s, a1_r, f1_s, f1_r)

            def piece(k, h):
                return mid.at[r, at[k], pl.ds(h, 1)]
            return dev, piece, ra2, rb2, sd2, (a2_s, a2_r, f2_s, f2_r)

        def ring_a(r, n):
            dev, piece, rfar, _, _, sems = level(r, n)
            return [rcopy(piece(2, s), rfar.at[r, s], sems[0].at[r], sems[1].at[r], dev(1 + 2 * s)) for s in range(2)]

        def ring_f(r, n):
            dev, piece, _, rnear, _, sems = level(r, n)
            return [rcopy(piece(1 + 2 * s, 1 - s), rnear.at[r, s, 1 - s], sems[2].at[r], sems[3].at[r], dev(1 + 2 * s)) for s in range(2)]

        def ring_d(r, n):
            dev, _, _, rnear, dep, sems = level(r, n)
            return [rcopy(dep.at[r, s], rnear.at[r, s, s], sems[2].at[r], sems[3].at[r], dev(1 + 2 * s)) for s in range(2)]

        def add(grid, *terms):
            specs = []
            for ref, at, lead in terms:
                tail = ref.shape[lead:]
                specs.append(pl.BlockSpec((1,) * lead + tuple(tail), lambda *i, at=at, rank=len(tail): tuple(at(*i)) + (0,) * rank))

            def body(*refs):
                total = refs[0][...].astype(F32).reshape(refs[0].shape[-2:])
                for ref in refs[1:-1]:
                    total = total + ref[...].astype(F32).reshape(total.shape)
                refs[-1][...] = total.astype(BF16).reshape(refs[-1].shape)

            pltpu.emit_pipeline(body, grid=grid, in_specs=specs[:-1], out_specs=specs[-1:])(*[ref for ref, _, _ in terms])

        def ring_first(r, n):
            start(ring_a(r, n) + ring_f(r, n))

        def ring_dependent(r, n):
            _, _, rfar, _, _, sems = level(r, n)
            all_in(rfar.at[r], sems[1].at[r])
            here = y if on_y(r, n) else x
            if n == 1:
                def near_block(s, i):
                    at = lax.rem(here + 1 + 2 * s, RING)
                    return (2 * s + i, at) if on_y(r, n) else (at, 2 * s + i)

                add((2, 2), (part.at[r], near_block, 2), (ra1.at[r], lambda s, i: (s, i), 2), (sd1.at[r], lambda s, i: (s, i), 2))
            else:
                add((2,), (mid.at[r], lambda s: (lax.rem(here + 1 + 2 * s, RING), s), 2), (ra2.at[r], lambda s: (s, 0), 2),
                    (sd2.at[r], lambda s: (s, 0), 2))
            start(ring_d(r, n))

        def ring_last(r, n):
            _, _, _, rnear, _, sems = level(r, n)
            all_in(rnear.at[r], sems[3].at[r])
            here = y if on_y(r, n) else x
            if n == 1:
                def own_at(h, i):
                    return (2 * h + i, here) if on_y(r, n) else (here, 2 * h + i)

                add((2, 2), (part.at[r], own_at, 2), (rb1.at[r, 0], lambda h, i: (h, i), 2),
                    (rb1.at[r, 1], lambda h, i: (h, i), 2), (mid.at[r], lambda h, i: (2 * h + i,), 1))
            else:
                own, res = ((tok_own, out), (grad_own, gin))[r]
                add((2,), (own, lambda h: (h,), 1), (mid.at[r], lambda h: (here, h), 2), (rb2.at[r, 0], lambda h: (h, 0), 2),
                    (rb2.at[r, 1], lambda h: (h, 0), 2), (res, lambda h: (h,), 1))

        def keep_rows(r):
            core_copy(r).wait_recv()
            row_products(r, True)

        run_order({
            "far_block": far_block, "next_products": next_products, "next_adds": next_adds, "next_blocks": next_blocks,
            "own_block": own_block, "finish": finish, "give_rows": give_rows, "keep_rows": keep_rows, "ring_first": ring_first,
            "ring_dependent": ring_dependent, "ring_last": ring_last,
        }, LATE_ORDER)

        for t in range(3):
            all_out(nxt.at[t], u_s.at[t])
        for r in range(2):
            core_copy(r).wait_send()
            for n in (1, 2):
                _, _, rfar, rnear, _, sems = level(r, n)
                all_out(rfar.at[r], sems[0].at[r])
                all_out(rnear.at[r], sems[2].at[r])
        for t in Z_ORDER:
            with jax.named_scope(f"handed_{t}"):
                all_in(outs[t].at[pl.ds(0, n8 - 1)], e_r.at[t])
                if t not in given:
                    handed(t)

    pl.run_scoped(
        forward_phase,
        pltpu.VMEM((2, chunk, d), BF16),
        pltpu.VMEM((tokens, nf), BF16),
        pltpu.VMEM((tokens, nf), BF16),
        pltpu.VMEM((2, chunk, nf), BF16),
        pltpu.VMEM((2, 2, chunk, main), BF16),
        pltpu.VMEM((2, 2, chunk, packed), BF16),
        pltpu.VMEM((d, main), BF16),
        pltpu.VMEM((d, packed), BF16),
    )
    pl.run_scoped(backward_phase, pltpu.VMEM((2, tiles * LANE, cols), F32), pltpu.VMEM((2, tiles, cols, LANE), F32))


def layer(sg, su, sd, tok, grad):
    n8 = 2 * RING
    dp, nf = sg.shape[0], sg.shape[1] // n8
    rows, d = tok.shape
    tokens = rows * RING * n8
    cols = d // RING
    tiles = -(-nf // LANE)
    padded = tiles * LANE
    main = nf // LANE * LANE
    packed = -(-3 * (nf - main) // LANE) * LANE
    hbm = pl.BlockSpec(memory_space=pl.ANY)
    dma = pltpu.SemaphoreType.DMA
    sds = jax.ShapeDtypeStruct
    halves = (2, rows // 2, d)
    res = pl.pallas_call(
        layer_kernel,
        out_shape=[sds((n8, tiles, dp, LANE), F32)] * 3 + [sds(halves, BF16)] * 2 + [
            sds((d, main), BF16), sds((d, main), BF16), sds((d, main), BF16), sds((d, packed), BF16), sds((tokens, d), BF16), sds((tokens, d), BF16),
            sds((3, RING, 2, RING * rows, main), BF16), sds((2, RING, 2, RING * rows, packed), BF16),
            sds((3, nf, cols), F32), sds((3, 2, nf, cols), F32),
            sds((2, RING, RING, rows, d), BF16), sds((2, RING, RING, rows, d), BF16), sds((2, RING, RING, rows, d), BF16),
            sds((2, 2, 2, rows, d), BF16), sds((2, 2, 2, 2, rows, d), BF16), sds((2, 2, 2, rows, d), BF16),
            sds((2, RING, 2, rows // 2, d), BF16),
            sds((2, 2, 1, rows // 2, d), BF16), sds((2, 2, 2, 1, rows // 2, d), BF16), sds((2, 2, 1, rows // 2, d), BF16),
        ],
        in_specs=[hbm] * 7,
        out_specs=[hbm] * 25,
        scratch_shapes=[
            pltpu.VMEM((3, nf, tokens), BF16),
            pltpu.VMEM((2, tokens, cols), BF16),
            pltpu.VMEM((3, padded, cols), F32),
            pltpu.VMEM((3, 2, nf, cols), F32),
            dma((7,)),
            dma((4,)), dma((4, n8)),
            dma((4,)), dma((4, 2, n8 // 2)), dma((4,)),
            dma((4,)),
            dma((3,)), dma((3, 2)),
            dma((3,)), dma((3,)),
            dma((3,)), dma((3, 2, RING)),
            dma((3,)), dma((3, RING)),
            dma((3,)), dma((RING + 2,)),
            dma((3,)), dma((4,)), dma((2,)), dma((2, 3)), dma((2,)), dma((2,)),
            dma((3,)), dma((3,)),
            dma((3,)), dma((3, tiles + 1)),
            dma((3,)), dma((3,)),
            dma((3,)),
            dma((2,)), dma((2,)),
        ] + [dma((2,))] * 8,
        compiler_params=pltpu.CompilerParams(collective_id=0, has_side_effects=True, vmem_limit_bytes=67043328),
        cost_estimate=pl.CostEstimate(flops=18 * nf * tokens * d, bytes_accessed=300_000_000, transcendentals=0),
        name="layer",
    )(sg, su, sd, tok, grad, tok.reshape(halves), grad.reshape(halves))
    return res[:3], res[3].reshape(rows, d), res[4].reshape(rows, d)


def assemble_kernel(og, ou, od, out, gin, g, u, w, res, gres, buf, flat, in_sem, out_sem, row_buf, row_sem):
    n8, nf = og.shape[0], g.shape[1] // og.shape[0]
    srcs, dsts = (og, ou, od), (g, u, w)
    rows_in = [pltpu.make_async_copy(src, row_buf.at[r], row_sem.at[r]) for r, src in enumerate((out, gin))]
    loads = [pltpu.make_async_copy(src, buf.at[t], in_sem.at[t]) for t, src in enumerate(srcs)]
    stores = [pltpu.make_async_copy(flat.at[t], dst, out_sem.at[t]) for t, dst in enumerate(dsts)]
    for c in loads + rows_in:
        c.start()
    for t in range(3):
        loads[t].wait()
        for j in range(n8):
            flat[t, :, j * nf:(j + 1) * nf] = jnp.concatenate([buf[t, j, tile] for tile in range(buf.shape[2])], axis=1)[:, :nf]
        stores[t].start()
    rows_out = [pltpu.make_async_copy(row_buf.at[r], dst, row_sem.at[r]) for r, dst in enumerate((res, gres))]
    for c in rows_in:
        c.wait()
    for c in rows_out:
        c.start()
    for c in stores + rows_out:
        c.wait()


def assemble(sums, out, gin, ff):
    dp = sums[0].shape[2]
    hbm = pl.BlockSpec(memory_space=pl.ANY)
    dma = pltpu.SemaphoreType.DMA
    sds = jax.ShapeDtypeStruct
    return pl.pallas_call(
        assemble_kernel,
        out_shape=[sds((dp, ff), F32)] * 3 + [sds(out.shape, BF16)] * 2,
        in_specs=[hbm] * 5,
        out_specs=[hbm] * 5,
        scratch_shapes=[
            pltpu.VMEM((3,) + sums[0].shape, F32), pltpu.VMEM((3, dp, ff), F32), dma((3,)), dma((3,)),
            pltpu.VMEM((2,) + out.shape, BF16), dma((2,)),
        ],
        compiler_params=pltpu.CompilerParams(vmem_limit_bytes=63 * 1024 * 1024),
        name="assemble",
    )(*sums, out, gin)


def solution(mesh):
    nz, ny, nd = mesh.shape["datb"], mesh.shape["model"], mesh.shape["data"]
    fine = Mesh(mesh.devices.reshape(nz, ny, nd // 2, 2), ("datb", "model", "x", "core"))

    def local_step(tok_loc, wg_loc, wu_loc, wd_loc, grad_loc):
        sums, out, grad_in = layer(wg_loc, wu_loc, wd_loc.T, tok_loc, grad_loc)
        grad_gate, grad_up, grad_down_t, out, grad_in = assemble(sums, out, grad_in, wg_loc.shape[1])
        return out, grad_in, grad_gate, grad_up, grad_down_t.T

    return jax.shard_map(local_step, mesh=fine, in_specs=(ROW_SPEC, GATE_SPEC, GATE_SPEC, DOWN_SPEC, ROW_SPEC), out_specs=(ROW_SPEC, ROW_SPEC, GATE_SPEC, GATE_SPEC, DOWN_SPEC), check_vma=False)
```

```python
import functools

import jax
import jax.numpy as jnp
from jax import lax
from jax.experimental import pallas as pl
from jax.experimental.pallas import tpu as pltpu
from jax.sharding import Mesh
from jax.sharding import PartitionSpec as P

ROW_SPEC = P(("datb", "x", "core", "model"), None)
GATE_SPEC = P(("datb", "x", "core"), "model")
DOWN_SPEC = P("model", ("datb", "x", "core"))
BF16 = jnp.bfloat16
F32 = jnp.float32
MESH_ID = pl.DeviceIdType.MESH
RING = 4
NEAR = ((0, 0), (0, 1), (1, 0), (3, 0), (1, 1), (3, 1), (2, 0), (2, 1))
DELTAS = (0, 3, 1, 2)
LANE = 128
OUT_COLS = 512
EX, Z1, Z2, P1, P2, BL, Q1, Q2, WD, CI = range(10)
GATHER_STEPS = (
    (Z1, 0, 0), (P1, 0, 0), (P1, 0, 1), (EX, 0, 1), (BL, 0, 0), (P1, 2, 0), (P1, 2, 1), (EX, 0, 2), (Z1, 3, 0), (EX, 3, 1), (EX, 3, 2),
    (EX, 3, 3), (EX, 3, 4), (EX, 3, 5), (EX, 3, 6), (EX, 3, 7), (Z1, 1, 0), (EX, 1, 1), (Z1, 2, 0), (EX, 2, 1), (EX, 0, 3), (BL, 1, 0),
    (Z1, 3, 1), (EX, 0, 4), (EX, 0, 5), (Z1, 0, 1), (Z1, 1, 1), (Z2, 3, 0, 0), (Z1, 2, 1), (EX, 0, 6), (EX, 0, 7), (Z2, 0, 0, 0),
    (Z2, 1, 0, 0), (EX, 1, 2), (EX, 1, 3), (Z2, 2, 0, 0), (Z2, 3, 0, 1), (P2, 0, 0), (P2, 0, 1), (BL, 0, 1), (Q1, 0, 0, 1), (Z1, 3, 2),
    (Z1, 3, 3), (Z1, 3, 4), (Q1, 0, 0, 0), (Z1, 3, 5), (Z2, 0, 0, 1), (EX, 1, 4), (EX, 1, 5), (P2, 2, 1), (Z1, 3, 6), (EX, 1, 6),
    (EX, 1, 7), (Z1, 3, 7), (Z1, 0, 2), (Q1, 1, 0, 1), (Z2, 3, 1, 0), (Z2, 3, 1, 1), (Z1, 0, 3), (EX, 2, 2), (EX, 2, 3), (Z2, 3, 1, 2),
    (BL, 0, 2), (Z2, 3, 1, 3), (Z1, 0, 4), (EX, 2, 4), (EX, 2, 5), (Z1, 0, 5), (EX, 2, 6), (EX, 2, 7), (Z2, 3, 0, 2), (Q1, 0, 1, 1),
    (Z2, 3, 0, 3), (Z1, 0, 6), (P1, 1, 0), (P1, 1, 1), (Q1, 0, 1, 0), (Z1, 0, 7), (BL, 2, 2), (Z2, 0, 1, 0), (Z1, 1, 2), (Z2, 0, 1, 1),
    (Z2, 0, 0, 2), (Q2, 0, 0), (Z2, 0, 1, 2), (Z2, 0, 0, 3), (BL, 2, 0), (BL, 0, 3), (Q1, 0, 2, 1), (Z2, 0, 1, 3), (Z1, 1, 3), (Z1, 1, 4),
    (WD, 3), (Z1, 1, 5), (Q1, 0, 2, 0), (Z1, 1, 6), (P2, 2, 0), (BL, 2, 1), (P2, 1, 0), (P2, 1, 1), (Z1, 1, 7), (Q1, 0, 3, 1),
    (Q1, 1, 0, 0), (Z2, 1, 0, 1), (Q1, 2, 2, 0), (Q1, 2, 2, 1), (Z2, 1, 0, 2), (BL, 1, 1), (Q2, 0, 1), (WD, 0), (Z2, 1, 1, 0), (CI, 0),
)
GATE_STEPS = (
    (),
    (),
    (
        (Z1, 2, 2),
    ),
    (
        (Q2, 0, 2), (Z2, 1, 1, 1), (Z2, 1, 0, 3), (Q1, 2, 0, 0), (Q1, 2, 0, 1), (BL, 1, 2), (CI, 1),
    ),
    (
        (Z2, 1, 1, 2), (Z1, 2, 3),
    ),
    (
        (Q1, 0, 3, 0), (Z2, 1, 1, 3), (Z1, 2, 4), (CI, 2),
    ),
    (
        (Z1, 2, 5), (Q1, 2, 1, 0), (Q1, 2, 1, 1), (BL, 2, 3), (BL, 1, 3), (Z1, 2, 6), (Q2, 0, 3),
    ),
    (
        (Q2, 1, 0), (Z1, 2, 7), (CI, 3),
    ),
    (
        (Q2, 2, 0), (Q2, 2, 2), (Z2, 2, 0, 1), (Q1, 1, 1, 0), (Q1, 1, 1, 1),
    ),
)
UP_STEPS = (
    (
        (Z2, 2, 0, 2), (Q1, 1, 2, 1), (WD, 1),
    ),
    (
        (Q2, 2, 1), (Q1, 2, 3, 1), (Q1, 1, 2, 0),
    ),
    (
        (Z2, 2, 1, 0), (Z2, 2, 0, 3), (Q1, 1, 3, 1),
    ),
    (
        (Z2, 2, 1, 1), (Q1, 1, 3, 0),
    ),
    (
        (Q2, 1, 2), (Z2, 2, 1, 2), (Q1, 2, 3, 0),
    ),
    (
        (Q2, 1, 1), (Z2, 2, 1, 3),
    ),
    (
        (Q2, 1, 3), (Q2, 2, 3),
    ),
    (),
)
LATE_STEPS = (
    (WD, 2),
)
Z_ORDER = (2, 0, 1)
EARLY_ORDER = (
    ("far_block", 2), ("next_products", 2), ("late",), ("give_rows", 0),
)
LATE_ORDER = (
    ("next_adds", 2), ("own_block", 2), ("keep_rows", 0), ("ring_first", 0, 1), ("finish", 2, 0), ("far_block", 0), ("give_rows", 1),
    ("finish", 2, 3), ("finish", 2, 1), ("finish", 2, 4), ("ring_dependent", 0, 1), ("finish", 2, 2), ("far_block", 1), ("keep_rows", 1),
    ("ring_first", 1, 1), ("next_blocks", 0), ("own_block", 0), ("next_blocks", 1), ("own_block", 1), ("finish", 0, 0),
    ("ring_dependent", 1, 1), ("finish", 0, 1), ("ring_last", 0, 1), ("ring_first", 0, 2), ("finish", 0, 2), ("finish", 0, 3),
    ("finish", 0, 4), ("ring_last", 1, 1), ("ring_first", 1, 2), ("ring_dependent", 0, 2), ("finish", 1, 0), ("ring_dependent", 1, 2),
    ("ring_last", 0, 2), ("finish", 1, 1), ("finish", 1, 2), ("ring_last", 1, 2), ("finish", 1, 3), ("finish", 1, 4),
)


def dot(a, b, ca, cb):
    return lax.dot_general(a, b, (((ca,), (cb,)), ((), ())), preferred_element_type=F32)


def layer_kernel(sg, su, sd, tok, grad, tok_own, grad_own,
                 og, ou, od, out, gin, wg, wu, wd, wr, tok_all, grad_all, h_main, h_rest, ra, rb, give, rc, part, ra1, rb1, sd1, mid, ra2, rb2, sd2,
                 ff, blk, far, nxt,
                 own_sem, ex_s, ex_r, z1_s, z1_r, zn_r, z2_s, p1_s, p1_r, p2_s, p2_r, q1_s, q1_r, q2_s, q2_r, cc_s, cc_r,
                 sh_sem, wv_sem, row_sem, hst_sem, blk_sem, tmp_sem, a_s, a_r, u_s, u_r, e_s, e_r, out_sem,
                 c_s, c_r, a1_s, a1_r, f1_s, f1_r, a2_s, a2_r, f2_s, f2_r):
    z, y = lax.axis_index("datb"), lax.axis_index("model")
    x, core = lax.axis_index("x"), lax.axis_index("core")
    i8 = 2 * x + core
    n8 = 2 * RING
    rows, d = tok.shape
    half_rows = rows // 2
    chunk = RING * rows
    n_chunk = n8
    nf, tokens = ff.shape[1:]
    dp = sg.shape[0]
    half = nf // 2
    main = wg.shape[1]
    rest = nf - main
    packed = wr.shape[1]
    cols = blk.shape[2]
    tiles = far.shape[1] // LANE
    outs = (og, ou, od)

    zs, ys, xs = ([v] + [lax.rem(v + k, RING) for k in range(1, RING)] for v in (z, y, x))
    cores = (core, 1 - core)
    peers = [[2 * v + c for c in cores] for v in xs]
    slot_at = [[[pl.multiple_of((zz * n8 + peers[dx][dc]) * dp, 16) for dc in range(2)] for dx in range(RING)] for zz in zs]
    hand_at = [[pl.multiple_of(p * dp, 8) for p in row] for row in peers]
    rows_at = [[[pl.multiple_of((peers[dx][dc] * RING + yy) * rows, half_rows) for dc in range(2)] for yy in ys] for dx in range(RING)]
    lanes_at = [pl.multiple_of(zz * cols, LANE) for zz in zs]

    def peer(dx, dc):
        return peers[dx][dc]

    def zdev(k):
        return {"datb": zs[k]}

    def xdev(k):
        return {"x": xs[k]}

    def ydev(k):
        return {"model": ys[k]}

    def near(dx, dc):
        return {"x": xs[dx], "core": cores[dc]}

    def copy(src, dst, s, r, dev):
        return pltpu.make_async_remote_copy(src_ref=src, dst_ref=dst, send_sem=s, recv_sem=r, device_id=dev, device_id_type=MESH_ID)

    rcopy = copy

    def all_in(ref, sem):
        copy(ref, ref, sem, sem, zdev(1)).wait_recv()

    def all_out(ref, sem):
        copy(ref, ref, sem, sem, zdev(1)).wait_send()

    def start(copies):
        for c in copies:
            c.start()

    def received(copies):
        for c in copies:
            c.wait_recv()

    def sent(copies):
        for c in copies:
            c.wait_send()

    def run_order(fns, order):
        for fn, *args in order:
            with jax.named_scope("_".join(str(v) for v in [fn, *args])):
                fns[fn](*args)

    barrier = pltpu.get_barrier_semaphore()
    others = [zdev(1), zdev(3), ydev(1), ydev(3)] + [near(*n) for n in NEAR[1:]]
    for dev in others:
        pl.semaphore_signal(barrier, inc=1, device_id=dev, device_id_type=MESH_ID)

    def blk_load(t, slot, k):
        src = tok_all if t < 2 else grad_all
        return pltpu.make_async_copy(src.at[:, pl.ds(lanes_at[k], cols)], blk.at[slot], blk_sem.at[slot])

    plan = []
    for fn, *args in EARLY_ORDER + LATE_ORDER:
        plan += [(args[0], k) for k in {"far_block": (2,), "next_blocks": (1, 3), "next_products": (1, 3), "own_block": (0,)}.get(fn, ())]
    taken = []

    def next_block():
        n = len(taken)
        taken.append(n)
        blk_load(plan[n][0], n % 2, plan[n][1]).wait()
        if n + 1 < len(plan):
            blk_load(plan[n + 1][0], (n + 1) % 2, plan[n + 1][1]).start()
        return n % 2

    def product(t, dst, then=None):
        slot = next_block()
        step = 2 * LANE
        count = -(-cols // step)

        def one(n, carry):
            lanes = pl.ds(pl.multiple_of(jnp.minimum(n * step, cols - step), LANE), step)
            dst[:nf, lanes] = jnp.dot(ff[t], blk[slot, :, lanes], preferred_element_type=F32)
            for k in range(count if then else 0):
                first = k * step if k < count - 1 else cols - step
                size = step if k == count - 1 else min(step, cols - step - first)
                if size > 0:
                    pl.when(n == k)(functools.partial(then, first, size))
            return carry

        lax.fori_loop(0, count, one, 0)

    lo, hi = pl.ds(0, half), pl.ds(half, half)

    def a_copies(t, first=0, size=cols):
        lanes = pl.ds(first, size)
        return [rcopy(far.at[t, at, lanes], ra.at[t, at, lanes], a_s.at[t], a_r.at[t], zdev(k)) for at, k in ((lo, 1), (hi, 3))]

    def tile_rows(tile):
        return pl.ds(tile * LANE, min(LANE, nf - tile * LANE))

    def unit_parts(t, tile):
        if (t, tile) != (Z_ORDER[2], tiles - 1):
            return [(tile, 0, cols)]
        first = -(-cols // 2 // LANE) * LANE
        return [(tile, 0, first), (tiles, first, cols - first)]

    def unit_copies(t, tile):
        at = tile_rows(tile)
        cs = []
        for n, first, size in unit_parts(t, tile):
            lanes = pl.ds(first, size)
            cs += [rcopy(nxt.at[t, s, at, lanes], rb.at[t, s, at, lanes], u_s.at[t], u_r.at[t, n], zdev(1 + 2 * s)) for s in range(2)]
        return cs

    def far_block(t):
        if t == Z_ORDER[0]:
            product(t, far.at[t], lambda first, size: start(a_copies(t, first, size)))
        else:
            product(t, far.at[t])
            start(a_copies(t))

    def early_units(t):
        if ("next_products", t) not in EARLY_ORDER + LATE_ORDER:
            return ()
        free = [(0, tile) for tile in range(tiles) if tile * LANE >= half]
        return free + [(1, tile) for tile in range(tiles) if (tile + 1) * LANE <= half]

    def next_products(t):
        for s in range(2):
            product(t, nxt.at[t, s])
        for s, tile in early_units(t):
            unit_copies(t, tile)[s].start()

    blocks = d // min(OUT_COLS, d)
    width = d // blocks

    def row_products(r, keep):
        side = core if keep else 1 - core
        specs, args = [], []
        for h, j, w in ((h_main, 2, wd), (h_rest, 0, wr)) if r == 0 else ((h_main, 0, wg), (h_main, 1, wu), (h_rest, 1, wr)):
            n = w.shape[1]
            specs += [pl.BlockSpec((1, RING, 1, RING * rows, n), lambda i, j=j: (j, 0, side, 0, 0)), pl.BlockSpec((width, n), lambda i: (i, 0))]
            args += [h, w]
        wide = pl.BlockSpec((RING, RING, rows, width), lambda i: (0, 0, 0, i))
        terms = len(args) // 2
        if keep:
            specs.append(wide)
            args.append(rc.at[r])

        def body(*refs):
            total = None
            for i in range(terms):
                h = refs[2 * i][...].reshape(RING * RING * rows, refs[2 * i].shape[-1])
                prod = dot(h, refs[2 * i + 1][...], 1, 1)
                total = prod if total is None else total + prod
            if keep:
                total = total + refs[-2][...].astype(F32).reshape(total.shape)
            refs[-1][...] = total.astype(BF16).reshape(RING, RING, rows, width)

        pltpu.emit_pipeline(body, grid=(blocks,), in_specs=specs, out_specs=[wide])(*args, (part if keep else give).at[r])

    def core_copy(r):
        return rcopy(give.at[r], rc.at[r], c_s.at[r], c_r.at[r], near(0, 1))

    def give_rows(r):
        row_products(r, False)
        core_copy(r).start()

    def forward_phase(rowbuf, av, bv, gv, hst, hst_rest, wv_a):
        held = {}

        fulls = (wg, wu, wd, wr)
        REST = 3
        def shard_load(t):
            return pltpu.make_async_copy((sg, su, sd)[t], held["shard"].at[t], sh_sem.at[t])

        def cut_pieces(t):
            if t == REST:
                for u in range(3):
                    for j in range(n8):
                        held["rests"][j, :, u * rest:(u + 1) * rest] = held["shard"][u, :, j * nf + main:(j + 1) * nf]
            else:
                for j in range(n8):
                    held["pieces"][t, j] = held["shard"][t, :, j * nf:j * nf + main]
            own_piece(t).start()

        def piece(t, j):
            return held["rests"].at[j] if t == REST else held["pieces"].at[t, j]

        def own_piece(t):
            return pltpu.make_async_copy(piece(t, i8), slot(t, 0, NEAR[0]), own_sem.at[t])

        def go(make, *args):
            make(*args).start()

        def slot(t, k, source):
            dx, dc = source
            return fulls[t].at[pl.ds(slot_at[k][dx][dc], dp)]

        def source(k):
            dx, dc = NEAR[k]
            return (RING - dx) % RING, dc

        def back(side):
            return 3 if side == 0 else 1

        def ahead(side):
            return 1 if side == 0 else 3

        def exchange_copy(t, k):
            return copy(piece(t, peer(*NEAR[k])), slot(t, 0, NEAR[0]), ex_s.at[t], ex_r.at[t, k], near(*NEAR[k]))

        def exchange(t, k):
            go(exchange_copy, t, k)

        def z_first_copy(t, side, k):
            here = slot(t, 0, source(k))
            return copy(here if k else piece(t, i8), here, z1_s.at[t], z1_sem(t, side, k), zdev(ahead(side)))

        def z_first(t, k):
            if k:
                here = slot(t, 0, source(k))
                all_in(here, ex_r.at[t, k])
            for side in range(2):
                go(z_first_copy, t, side, k)

        def z1_sem(t, side, k):
            return z1_r.at[t, side, k % (n8 // 2)] if (k < n8 // 2) == (side == 0) else zn_r.at[t]

        def some(t, count):
            return fulls[t].at[pl.ds(0, count * dp)]

        def z_second_copy(t, side, k):
            there = slot(t, back(side), source(k + side * (n8 // 2)))
            return copy(there, there, z2_s.at[t], zn_r.at[t], zdev(ahead(side)))

        def z_second(t, side, k):
            kk = k + side * (n8 // 2)
            all_in(slot(t, back(side), source(kk)), z1_sem(t, side, kk))
            go(z_second_copy, t, side, k)

        def weights_done(t):
            if (WD, t) not in LATE_STEPS:
                own_wait(t)
            all_in(some(t, 2 * n8), zn_r.at[t])
            w_load(t).start()

        cut = d * 11 // 28
        rings = ((tok, tok_all, pl.ds(0, d), True), (grad, grad_all, pl.ds(0, cut), True), (grad, grad_all, pl.ds(cut, d - cut), False))

        def axis(r, n):
            return xdev if rings[r][3] == (n == 1) else ydev

        def block(r, da, db, flip=0, lo=0, size=rows):
            dx, dy = (da, db) if rings[r][3] else (db, da)
            first = rows_at[dx][dy][flip]
            return rings[r][1].at[pl.ds(pl.multiple_of(first + lo, half_rows) if lo else first, size), rings[r][2]]

        def own_block(r):
            return rings[r][0].at[:, rings[r][2]]

        def to_core_copy(r, ia, ib):
            there = block(r, DELTAS[ia], DELTAS[ib])
            return copy(own_block(r) if ia == 0 and ib == 0 else there, there, cc_s.at[r], cc_r.at[ia if r == 0 else RING - 1 + r], near(0, 1))

        def to_core(r, ia, ib):
            go(to_core_copy, r, ia, ib)

        def first_copy(r, side):
            return copy(own_block(r), block(r, 0, 0), p1_s.at[r], p1_r.at[r, side], axis(r, 1)(ahead(side)))

        def first_own(r, side):
            go(first_copy, r, side)

        def first_far_copy(r, side):
            part = block(r, back(side), 0, 0, side * half_rows, half_rows)
            return copy(part, part, p2_s.at[r], p2_r.at[r], axis(r, 1)(ahead(side)))

        def first_forward(r, side):
            there = block(r, back(side), 0)
            all_in(there, p1_r.at[r, side])
            go(first_far_copy, r, side)

        def block_on(r, ia):
            if ia == 3:
                all_in(block(r, 2, 0), p2_r.at[r])
            for side in range(2):
                go(second_copy, r, side, ia)
            to_core(r, ia, 0)

        def second_copy(r, side, ia):
            there = block(r, DELTAS[ia], 0)
            return copy(there if ia else own_block(r), there, q1_s.at[r], q1_r.at[r, side, ia], axis(r, 2)(ahead(side)))

        def second_far_copy(r, ia):
            side = ia // 2
            there = block(r, DELTAS[ia], back(side))
            return copy(there, there, q2_s.at[r], q2_r.at[r, ia], axis(r, 2)(ahead(side)))

        def second_forward(r, ia, side):
            there = block(r, DELTAS[ia], back(side))
            all_in(there, q1_r.at[r, side, ia])
            if ia // 2 == side:
                go(second_far_copy, r, ia)
            to_core(r, ia, 1 if side == 0 else 2)

        def second_far(r, ia):
            there = block(r, DELTAS[ia], 2)
            all_in(there, q2_r.at[r, ia])
            to_core(r, ia, 3)

        def some_rows(r, count):
            return rings[r][1].at[pl.ds(0, count * rows), rings[r][2]]

        def chunk_in(ia):
            all_in(some_rows(0, RING), cc_r.at[ia])

        def rows_in(r):
            all_in(some_rows(r, RING * RING), cc_r.at[RING - 1 + r])

        def own_wait(t):
            there = slot(t, 0, NEAR[0])
            pltpu.make_async_copy(there, there, own_sem.at[t]).wait()

        def own_rows(r):
            return pltpu.make_async_copy(own_block(r), block(r, 0, 0), own_sem.at[4 + r])

        def w_load(t):
            return pltpu.make_async_copy(fulls[t], (wv_a.at[:, pl.ds(0, main)], held["wv_b"], wv_a.at[:, pl.ds(0, main)], wv_a.at[:, pl.ds(main, packed)])[t], wv_sem.at[t])

        def row_load(src, i, buf):
            return pltpu.make_async_copy(src.at[chunk_rows(i)], rowbuf.at[buf], row_sem.at[buf])

        def chunk_loop(src, products, elementwise, between):
            row_load(src, 0, 0).start()
            between[0]()
            row_load(src, 1, 1).start()
            row_load(src, 0, 0).wait()
            products(0, 0)

            def body(i, carry):
                buf = lax.rem(i, 2)

                @pl.when(i + 1 < n_chunk)
                def _():
                    row_load(src, i + 1, 1 - buf).start()

                for k, step in enumerate(between[1:], 1):
                    pl.when(i == k)(step)
                row_load(src, i, buf).wait()
                free(elementwise, i - 1)
                elementwise(i - 1, 1 - buf, lambda: products(i, buf))
                return carry

            lax.fori_loop(1, n_chunk, body, 0)
            free(elementwise, n_chunk - 1)
            elementwise(n_chunk - 1, (n_chunk - 1) % 2, lambda: None)

        def free(elementwise, i):
            @pl.when(i >= 2)
            def _():
                for cp in copies_of[elementwise](i - 2):
                    cp.wait()

        def chunk_rows(i):
            return pl.ds(pl.multiple_of(i * chunk, chunk), chunk)

        def h_copies(i, which, names):
            xx, c = lax.div(i, 2), lax.rem(i, 2)
            cs = [pltpu.make_async_copy(hst.at[c, n], h_main.at[j, xx, c], hst_sem.at[c, n]) for n, j in enumerate(names)]
            return cs + [pltpu.make_async_copy(hst_rest.at[which, c], h_rest.at[which, xx, c], hst_sem.at[c, 2])]

        def keep(i, c, values):
            which = len(values) - 1
            for n, (j, v) in enumerate(values):
                low = v.astype(BF16)
                hst[c, n] = low[:, :main]
                hst_rest[which, c, :, j * rest:(j + 1) * rest] = low[:, main:]
                ff[j, :, chunk_rows(i)] = v.T.astype(BF16)

        def kept(elementwise):
            for i in (n_chunk - 2, n_chunk - 1):
                for cp in copies_of[elementwise](i):
                    cp.wait()

        def gate_work():
            def place(k):
                ia, flip = lax.div(k, 2), lax.rem(k, 2)
                delta = lax.rem(3 * ia + 3 * lax.div(ia, 2) + 2 * lax.div(ia, 3), RING)
                return 2 * lax.rem(x + delta, RING) + lax.rem(core + flip, 2)

            def body(k, carry):
                for n, group in enumerate(GATE_STEPS):
                    if group:
                        pl.when(k == n)(functools.partial(run, group))

                @pl.when(k < n_chunk)
                def _():
                    row_load(tok_all, place(k), lax.rem(k, 2)).start()

                @pl.when(k >= 1)
                def _():
                    i, buf = place(k - 1), lax.rem(k - 1, 2)
                    row_load(tok_all, i, buf).wait()
                    rb_ = rowbuf[buf]
                    full = jnp.dot(rb_, wv_a[...], preferred_element_type=F32).astype(BF16)
                    av[chunk_rows(i)] = full[:, :nf]
                    bv[chunk_rows(i), main:] = full[:, nf:nf + rest]

                return carry

            lax.fori_loop(0, n_chunk + 1, body, 0)

        def up_products(i, buf):
            bv[chunk_rows(i), :main] = jnp.dot(rowbuf[buf], held["wv_b"][...], preferred_element_type=F32).astype(BF16)

        def hidden(i, c, beside):
            a, b = av[chunk_rows(i)].astype(F32), bv[chunk_rows(i)].astype(F32)
            beside()
            keep(i, c, ((2, a * jax.nn.sigmoid(a) * b),))
            start(copies_of[hidden](i))

        def down_products(i, buf):
            full = jnp.dot(rowbuf[buf], wv_a[...], preferred_element_type=F32).astype(BF16)
            gv[buf, :, :main] = full[:, :main]
            gv[buf, :, main:] = full[:, main + 2 * rest:main + 3 * rest]

        def backward(i, c, beside):
            g = gv[c].astype(F32)
            a, b = av[chunk_rows(i)].astype(F32), bv[chunk_rows(i)].astype(F32)
            beside()
            sig = jax.nn.sigmoid(a)
            keep(i, c, ((0, g * b * sig * (1.0 + a * (1.0 - sig))), (1, g * (a * sig))))
            start(copies_of[backward](i))

        copies_of = {hidden: lambda i: h_copies(i, 0, (2,)), backward: lambda i: h_copies(i, 1, (0, 1))}

        steps = (exchange, z_first, z_second, first_own, first_forward, block_on, second_forward, second_far, weights_done, chunk_in)

        def run(group):
            for which, *args in group:
                steps[which](*args)

        def rows_ready():
            run(UP_STEPS[-1])
            for r in (1, 2):
                own_rows(r).wait()
                rows_in(r)
            blk_load(plan[0][0], 0, plan[0][1]).start()

        def gather_phase(shard, pieces, rests, wv_b):
            held.update(shard=shard, pieces=pieces, rests=rests, wv_b=wv_b)
            with jax.named_scope("begin"):
                shard_load(0).start()
                shard_load(0).wait()
                for t in (1, 2):
                    shard_load(t).start()
                cut_pieces(0)
                pl.semaphore_wait(barrier, len(others))
                for r in range(3):
                    own_rows(r).start()
            with jax.named_scope("gather"):
                cut = {0}
                for step in GATHER_STEPS:
                    if step[0] in (EX, Z1) and step[1] not in cut:
                        if len(cut) == 1:
                            rests[...] = jnp.zeros_like(rests)
                            hst_rest[...] = jnp.zeros_like(hst_rest)
                            shard_load(1).wait()
                            shard_load(2).wait()
                        cut.add(step[1])
                        cut_pieces(step[1])
                    run((step,))
                own_rows(0).wait()
                w_load(0).wait()
                w_load(REST).wait()
            with jax.named_scope("gate"):
                gate_work()
            with jax.named_scope("up"):
                run(UP_STEPS[0])
                w_load(1).wait()
                chunk_loop(tok_all, up_products, hidden, [functools.partial(run, group) for group in ((),) + UP_STEPS[1:-1]] + [rows_ready])
                kept(hidden)
            for _, t in LATE_STEPS:
                own_wait(t)
            for t in range(4):
                all_out(some(t, n8 - 1), ex_s.at[t])
                all_out(some(t, 2 * n8), z1_s.at[t])

        pl.run_scoped(
            gather_phase, pltpu.VMEM((3,) + sg.shape, BF16), pltpu.VMEM((3, n8, dp, main), BF16), pltpu.VMEM((n8, dp, packed), BF16),
            pltpu.VMEM((d, main), BF16))
        run_order({
            "far_block": far_block, "next_products": next_products, "give_rows": give_rows, "late": functools.partial(run, LATE_STEPS),
        }, EARLY_ORDER)
        with jax.named_scope("down"):
            w_load(2).wait()
            chunk_loop(grad_all, down_products, backward, [lambda: None])
            kept(backward)
        for t in range(4):
            all_out(some(t, n8), z2_s.at[t])
        for r in range(3):
            for count, sem in ((2, p1_s), (1, p2_s), (2 * RING, q1_s), (RING, q2_s), (RING * RING, cc_s)):
                all_out(some_rows(r, count), sem.at[r])

    def backward_phase(tmp, stage):
        def next_adds(t):
            all_in(ra.at[t], a_r.at[t])
            cs = [pltpu.make_async_copy(ra.at[t, at], tmp.at[s, at], tmp_sem.at[s]) for s, at in ((0, lo), (1, hi))]
            start(cs)
            for c, (s, at) in zip(cs, ((0, lo), (1, hi))):
                c.wait()
                nxt[t, s, at] += tmp[s, at]
            for tile in range(tiles):
                start(c for s, c in enumerate(unit_copies(t, tile)) if (s, tile) not in early_units(t))

        def next_blocks(t):
            next_products(t)
            next_adds(t)

        def own_block(t):
            all_out(ra.at[t], a_s.at[t])
            product(t, far.at[t])

        def slot(t):
            return Z_ORDER.index(t) % 2

        def hand_out(t, tile, part):
            parts = unit_parts(t, tile)
            for k in range(n8):
                dx, dc = NEAR[k]
                at = pl.ds(hand_at[dx][dc], dp)
                src, dst = stage.at[slot(t), tile, at], outs[t].at[i8, tile]

                def send(k=k, src=src, dst=dst):
                    if k:
                        rcopy(src, dst, e_s.at[t], e_r.at[t], near(*NEAR[k])).start()
                    else:
                        pltpu.make_async_copy(src, dst, out_sem.at[t]).start()

                if len(parts) == 1:
                    send()
                elif part == 0:
                    pl.when(xs[dx] < parts[0][2] // dp // 2)(send)
                else:
                    pl.when(xs[dx] >= parts[0][2] // dp // 2)(send)

        def handed(t):
            all_out(outs[t].at[pl.ds(0, n8 - 1)], e_s.at[t])
            pltpu.make_async_copy(outs[t].at[0], outs[t].at[0], out_sem.at[t]).wait()

        given = []

        def finish(t, tile):
            at = tile_rows(tile)
            wide = pl.ds(tile * LANE, LANE)
            for part, (n, first, size) in enumerate(unit_parts(t, tile)):
                lanes = pl.ds(first, size)
                all_in(rb.at[t, :, at, lanes], u_r.at[t, n])
                cs = [pltpu.make_async_copy(rb.at[t, s, at, lanes], tmp.at[s, at, lanes], tmp_sem.at[s]) for s in range(2)]
                start(cs)
                if t == Z_ORDER[2] and not given:
                    given.append(Z_ORDER[0])
                    handed(Z_ORDER[0])
                for c in cs:
                    c.wait()
                stage[slot(t), tile, lanes] = (far[t, wide, lanes] + tmp[0, wide, lanes] + tmp[1, wide, lanes]).T
                hand_out(t, tile, part)

        def on_y(r, n):
            return (r == 1) == (n == 1)

        def level(r, n):
            at = ys if on_y(r, n) else xs
            dev = ydev if on_y(r, n) else xdev
            if n == 1:
                def piece(k, h):
                    return part.at[r, pl.ds(2 * h, 2), at[k]] if on_y(r, n) else part.at[r, at[k], pl.ds(2 * h, 2)]
                return dev, piece, ra1, rb1, sd1, (a1_s, a1_r, f1_s, f1_r)

            def piece(k, h):
                return mid.at[r, at[k], pl.ds(h, 1)]
            return dev, piece, ra2, rb2, sd2, (a2_s, a2_r, f2_s, f2_r)

        def ring_a(r, n):
            dev, piece, rfar, _, _, sems = level(r, n)
            return [rcopy(piece(2, s), rfar.at[r, s], sems[0].at[r], sems[1].at[r], dev(1 + 2 * s)) for s in range(2)]

        def ring_f(r, n):
            dev, piece, _, rnear, _, sems = level(r, n)
            return [rcopy(piece(1 + 2 * s, 1 - s), rnear.at[r, s, 1 - s], sems[2].at[r], sems[3].at[r], dev(1 + 2 * s)) for s in range(2)]

        def ring_d(r, n):
            dev, _, _, rnear, dep, sems = level(r, n)
            return [rcopy(dep.at[r, s], rnear.at[r, s, s], sems[2].at[r], sems[3].at[r], dev(1 + 2 * s)) for s in range(2)]

        def add(grid, *terms):
            specs = []
            for ref, at, lead in terms:
                tail = ref.shape[lead:]
                specs.append(pl.BlockSpec((1,) * lead + tuple(tail), lambda *i, at=at, rank=len(tail): tuple(at(*i)) + (0,) * rank))

            def body(*refs):
                total = refs[0][...].astype(F32).reshape(refs[0].shape[-2:])
                for ref in refs[1:-1]:
                    total = total + ref[...].astype(F32).reshape(total.shape)
                refs[-1][...] = total.astype(BF16).reshape(refs[-1].shape)

            pltpu.emit_pipeline(body, grid=grid, in_specs=specs[:-1], out_specs=specs[-1:])(*[ref for ref, _, _ in terms])

        def ring_first(r, n):
            start(ring_a(r, n) + ring_f(r, n))

        def ring_dependent(r, n):
            _, _, rfar, _, _, sems = level(r, n)
            all_in(rfar.at[r], sems[1].at[r])
            here = y if on_y(r, n) else x
            if n == 1:
                def near_block(s, i):
                    at = lax.rem(here + 1 + 2 * s, RING)
                    return (2 * s + i, at) if on_y(r, n) else (at, 2 * s + i)

                add((2, 2), (part.at[r], near_block, 2), (ra1.at[r], lambda s, i: (s, i), 2), (sd1.at[r], lambda s, i: (s, i), 2))
            else:
                add((2,), (mid.at[r], lambda s: (lax.rem(here + 1 + 2 * s, RING), s), 2), (ra2.at[r], lambda s: (s, 0), 2),
                    (sd2.at[r], lambda s: (s, 0), 2))
            start(ring_d(r, n))

        def ring_last(r, n):
            _, _, _, rnear, _, sems = level(r, n)
            all_in(rnear.at[r], sems[3].at[r])
            here = y if on_y(r, n) else x
            if n == 1:
                def own_at(h, i):
                    return (2 * h + i, here) if on_y(r, n) else (here, 2 * h + i)

                add((2, 2), (part.at[r], own_at, 2), (rb1.at[r, 0], lambda h, i: (h, i), 2),
                    (rb1.at[r, 1], lambda h, i: (h, i), 2), (mid.at[r], lambda h, i: (2 * h + i,), 1))
            else:
                own, res = ((tok_own, out), (grad_own, gin))[r]
                add((2,), (own, lambda h: (h,), 1), (mid.at[r], lambda h: (here, h), 2), (rb2.at[r, 0], lambda h: (h, 0), 2),
                    (rb2.at[r, 1], lambda h: (h, 0), 2), (res, lambda h: (h,), 1))

        def keep_rows(r):
            core_copy(r).wait_recv()
            row_products(r, True)

        run_order({
            "far_block": far_block, "next_products": next_products, "next_adds": next_adds, "next_blocks": next_blocks,
            "own_block": own_block, "finish": finish, "give_rows": give_rows, "keep_rows": keep_rows, "ring_first": ring_first,
            "ring_dependent": ring_dependent, "ring_last": ring_last,
        }, LATE_ORDER)

        for t in range(3):
            all_out(nxt.at[t], u_s.at[t])
        for r in range(2):
            core_copy(r).wait_send()
            for n in (1, 2):
                _, _, rfar, rnear, _, sems = level(r, n)
                all_out(rfar.at[r], sems[0].at[r])
                all_out(rnear.at[r], sems[2].at[r])
        for t in Z_ORDER:
            with jax.named_scope(f"handed_{t}"):
                all_in(outs[t].at[pl.ds(0, n8 - 1)], e_r.at[t])
                if t not in given:
                    handed(t)

    pl.run_scoped(
        forward_phase,
        pltpu.VMEM((2, chunk, d), BF16),
        pltpu.VMEM((tokens, nf), BF16),
        pltpu.VMEM((tokens, nf), BF16),
        pltpu.VMEM((2, chunk, nf), BF16),
        pltpu.VMEM((2, 2, chunk, main), BF16),
        pltpu.VMEM((2, 2, chunk, packed), BF16),
        pltpu.VMEM((d, main + packed), BF16),
    )
    pl.run_scoped(backward_phase, pltpu.VMEM((2, tiles * LANE, cols), F32), pltpu.VMEM((2, tiles, cols, LANE), F32))


def layer(sg, su, sd, tok, grad):
    n8 = 2 * RING
    dp, nf = sg.shape[0], sg.shape[1] // n8
    rows, d = tok.shape
    tokens = rows * RING * n8
    cols = d // RING
    tiles = -(-nf // LANE)
    padded = tiles * LANE
    main = nf // LANE * LANE
    packed = -(-3 * (nf - main) // LANE) * LANE
    hbm = pl.BlockSpec(memory_space=pl.ANY)
    dma = pltpu.SemaphoreType.DMA
    sds = jax.ShapeDtypeStruct
    halves = (2, rows // 2, d)
    res = pl.pallas_call(
        layer_kernel,
        out_shape=[sds((n8, tiles, dp, LANE), F32)] * 3 + [sds(halves, BF16)] * 2 + [
            sds((d, main), BF16), sds((d, main), BF16), sds((d, main), BF16), sds((d, packed), BF16), sds((tokens, d), BF16), sds((tokens, d), BF16),
            sds((3, RING, 2, RING * rows, main), BF16), sds((2, RING, 2, RING * rows, packed), BF16),
            sds((3, nf, cols), F32), sds((3, 2, nf, cols), F32),
            sds((2, RING, RING, rows, d), BF16), sds((2, RING, RING, rows, d), BF16), sds((2, RING, RING, rows, d), BF16),
            sds((2, 2, 2, rows, d), BF16), sds((2, 2, 2, 2, rows, d), BF16), sds((2, 2, 2, rows, d), BF16),
            sds((2, RING, 2, rows // 2, d), BF16),
            sds((2, 2, 1, rows // 2, d), BF16), sds((2, 2, 2, 1, rows // 2, d), BF16), sds((2, 2, 1, rows // 2, d), BF16),
        ],
        in_specs=[hbm] * 7,
        out_specs=[hbm] * 25,
        scratch_shapes=[
            pltpu.VMEM((3, nf, tokens), BF16),
            pltpu.VMEM((2, tokens, cols), BF16),
            pltpu.VMEM((3, padded, cols), F32),
            pltpu.VMEM((3, 2, nf, cols), F32),
            dma((7,)),
            dma((4,)), dma((4, n8)),
            dma((4,)), dma((4, 2, n8 // 2)), dma((4,)),
            dma((4,)),
            dma((3,)), dma((3, 2)),
            dma((3,)), dma((3,)),
            dma((3,)), dma((3, 2, RING)),
            dma((3,)), dma((3, RING)),
            dma((3,)), dma((RING + 2,)),
            dma((3,)), dma((4,)), dma((2,)), dma((2, 3)), dma((2,)), dma((2,)),
            dma((3,)), dma((3,)),
            dma((3,)), dma((3, tiles + 1)),
            dma((3,)), dma((3,)),
            dma((3,)),
            dma((2,)), dma((2,)),
        ] + [dma((2,))] * 8,
        compiler_params=pltpu.CompilerParams(collective_id=0, has_side_effects=True, vmem_limit_bytes=67043328),
        cost_estimate=pl.CostEstimate(flops=18 * nf * tokens * d, bytes_accessed=300_000_000, transcendentals=0),
        name="layer",
    )(sg, su, sd, tok, grad, tok.reshape(halves), grad.reshape(halves))
    return res[:3], res[3].reshape(rows, d), res[4].reshape(rows, d)


def assemble_kernel(og, ou, od, out, gin, g, u, w, res, gres, buf, flat, in_sem, out_sem, row_buf, row_sem):
    n8, nf = og.shape[0], g.shape[1] // og.shape[0]
    srcs, dsts = (og, ou, od), (g, u, w)
    rows_in = [pltpu.make_async_copy(src, row_buf.at[r], row_sem.at[r]) for r, src in enumerate((out, gin))]
    loads = [pltpu.make_async_copy(src, buf.at[t], in_sem.at[t]) for t, src in enumerate(srcs)]
    stores = [pltpu.make_async_copy(flat.at[t], dst, out_sem.at[t]) for t, dst in enumerate(dsts)]
    for c in loads + rows_in:
        c.start()
    for t in range(3):
        loads[t].wait()
        for j in range(n8):
            flat[t, :, j * nf:(j + 1) * nf] = jnp.concatenate([buf[t, j, tile] for tile in range(buf.shape[2])], axis=1)[:, :nf]
        stores[t].start()
    rows_out = [pltpu.make_async_copy(row_buf.at[r], dst, row_sem.at[r]) for r, dst in enumerate((res, gres))]
    for c in rows_in:
        c.wait()
    for c in rows_out:
        c.start()
    for c in stores + rows_out:
        c.wait()


def assemble(sums, out, gin, ff):
    dp = sums[0].shape[2]
    hbm = pl.BlockSpec(memory_space=pl.ANY)
    dma = pltpu.SemaphoreType.DMA
    sds = jax.ShapeDtypeStruct
    return pl.pallas_call(
        assemble_kernel,
        out_shape=[sds((dp, ff), F32)] * 3 + [sds(out.shape, BF16)] * 2,
        in_specs=[hbm] * 5,
        out_specs=[hbm] * 5,
        scratch_shapes=[
            pltpu.VMEM((3,) + sums[0].shape, F32), pltpu.VMEM((3, dp, ff), F32), dma((3,)), dma((3,)),
            pltpu.VMEM((2,) + out.shape, BF16), dma((2,)),
        ],
        compiler_params=pltpu.CompilerParams(vmem_limit_bytes=63 * 1024 * 1024),
        name="assemble",
    )(*sums, out, gin)


def solution(mesh):
    nz, ny, nd = mesh.shape["datb"], mesh.shape["model"], mesh.shape["data"]
    fine = Mesh(mesh.devices.reshape(nz, ny, nd // 2, 2), ("datb", "model", "x", "core"))

    def local_step(tok_loc, wg_loc, wu_loc, wd_loc, grad_loc):
        sums, out, grad_in = layer(wg_loc, wu_loc, wd_loc.T, tok_loc, grad_loc)
        grad_gate, grad_up, grad_down_t, out, grad_in = assemble(sums, out, grad_in, wg_loc.shape[1])
        return out, grad_in, grad_gate, grad_up, grad_down_t.T

    return jax.shard_map(local_step, mesh=fine, in_specs=(ROW_SPEC, GATE_SPEC, GATE_SPEC, DOWN_SPEC, ROW_SPEC), out_specs=(ROW_SPEC, ROW_SPEC, GATE_SPEC, GATE_SPEC, DOWN_SPEC), check_vma=False)
```

```python
import functools

import jax
import jax.numpy as jnp
from jax import lax
from jax.experimental import pallas as pl
from jax.experimental.pallas import tpu as pltpu
from jax.sharding import Mesh
from jax.sharding import PartitionSpec as P

ROW_SPEC = P(("datb", "x", "core", "model"), None)
GATE_SPEC = P(("datb", "x", "core"), "model")
DOWN_SPEC = P("model", ("datb", "x", "core"))
BF16 = jnp.bfloat16
F32 = jnp.float32
MESH_ID = pl.DeviceIdType.MESH
RING = 4
NEAR = ((0, 0), (0, 1), (1, 0), (3, 0), (1, 1), (3, 1), (2, 0), (2, 1))
DELTAS = (0, 3, 1, 2)
LANE = 128
OUT_COLS = 512
EX, Z1, Z2, P1, P2, BL, Q1, Q2, WD, CI = range(10)
GATHER_STEPS = (
    (Z1, 0, 0), (P1, 0, 0), (P1, 0, 1), (EX, 0, 1), (BL, 0, 0), (P1, 2, 0), (P1, 2, 1), (EX, 0, 2), (Z1, 3, 0), (EX, 3, 1), (EX, 3, 2),
    (EX, 3, 3), (EX, 3, 4), (EX, 3, 5), (EX, 3, 6), (EX, 3, 7), (Z1, 1, 0), (EX, 1, 1), (Z1, 2, 0), (EX, 2, 1), (EX, 0, 3), (BL, 1, 0),
    (Z1, 3, 1), (EX, 0, 4), (EX, 0, 5), (Z1, 0, 1), (Z1, 1, 1), (Z2, 3, 0, 0), (Z1, 2, 1), (EX, 0, 6), (EX, 0, 7), (Z2, 0, 0, 0),
    (Z2, 1, 0, 0), (EX, 1, 2), (EX, 1, 3), (Z2, 2, 0, 0), (Z2, 3, 0, 1), (P2, 0, 0), (P2, 0, 1), (BL, 0, 1), (Q1, 0, 0, 1), (Z1, 3, 2),
    (Z1, 3, 3), (Z1, 3, 4), (Q1, 0, 0, 0), (Z1, 3, 5), (Z2, 0, 0, 1), (EX, 1, 4), (EX, 1, 5), (P2, 2, 1), (Z1, 3, 6), (EX, 1, 6),
    (EX, 1, 7), (Z1, 3, 7), (Z1, 0, 2), (Q1, 1, 0, 1), (Z2, 3, 1, 0), (Z2, 3, 1, 1), (Z1, 0, 3), (EX, 2, 2), (EX, 2, 3), (Z2, 3, 1, 2),
    (BL, 0, 2), (Z2, 3, 1, 3), (Z1, 0, 4), (EX, 2, 4), (EX, 2, 5), (Z1, 0, 5), (EX, 2, 6), (EX, 2, 7), (Z2, 3, 0, 2), (Q1, 0, 1, 1),
    (Z2, 3, 0, 3), (Z1, 0, 6), (P1, 1, 0), (P1, 1, 1), (Q1, 0, 1, 0), (Z1, 0, 7), (BL, 2, 2), (Z2, 0, 1, 0), (Z1, 1, 2), (Z2, 0, 1, 1),
    (Z2, 0, 0, 2), (Q2, 0, 0), (Z2, 0, 1, 2), (Z2, 0, 0, 3), (BL, 2, 0), (BL, 0, 3), (Q1, 0, 2, 1), (Z2, 0, 1, 3), (Z1, 1, 3), (Z1, 1, 4),
    (WD, 3), (Z1, 1, 5), (Q1, 0, 2, 0), (Z1, 1, 6), (P2, 2, 0), (BL, 2, 1), (P2, 1, 0), (P2, 1, 1), (Z1, 1, 7), (Q1, 0, 3, 1),
    (Q1, 1, 0, 0), (Z2, 1, 0, 1), (Q1, 2, 2, 0), (Q1, 2, 2, 1), (Z2, 1, 0, 2), (BL, 1, 1), (Q2, 0, 1), (WD, 0), (Z2, 1, 1, 0), (CI, 0),
)
GATE_STEPS = (
    (),
    (),
    (
        (Z1, 2, 2),
    ),
    (
        (Q2, 0, 2), (Z2, 1, 1, 1), (Z2, 1, 0, 3), (Q1, 2, 0, 0), (Q1, 2, 0, 1), (BL, 1, 2), (CI, 1),
    ),
    (
        (Z2, 1, 1, 2), (Z1, 2, 3),
    ),
    (
        (Q1, 0, 3, 0), (Z2, 1, 1, 3), (Z1, 2, 4), (CI, 2),
    ),
    (
        (Z1, 2, 5), (Q1, 2, 1, 0), (Q1, 2, 1, 1), (BL, 2, 3), (BL, 1, 3), (Z1, 2, 6), (Q2, 0, 3),
    ),
    (
        (Q2, 1, 0), (Z1, 2, 7), (CI, 3),
    ),
    (
        (Q2, 2, 0), (Q2, 2, 2), (Z2, 2, 0, 1), (Q1, 1, 1, 0), (Q1, 1, 1, 1),
    ),
)
UP_STEPS = (
    (
        (Z2, 2, 0, 2), (Q1, 1, 2, 1), (WD, 1),
    ),
    (
        (Q2, 2, 1), (Q1, 2, 3, 1), (Q1, 1, 2, 0),
    ),
    (
        (Z2, 2, 1, 0), (Z2, 2, 0, 3), (Q1, 1, 3, 1),
    ),
    (
        (Z2, 2, 1, 1), (Q1, 1, 3, 0),
    ),
    (
        (Q2, 1, 2), (Z2, 2, 1, 2), (Q1, 2, 3, 0),
    ),
    (
        (Q2, 1, 1), (Z2, 2, 1, 3),
    ),
    (
        (Q2, 1, 3), (Q2, 2, 3),
    ),
    (),
)
LATE_STEPS = (
    (WD, 2),
)
Z_ORDER = (2, 0, 1)
EARLY_ORDER = (
    ("far_block", 2), ("next_products", 2), ("late",), ("give_rows", 0),
)
LATE_ORDER = (
    ("next_adds", 2), ("own_block", 2), ("keep_rows", 0), ("ring_first", 0, 1), ("finish", 2, 0), ("far_block", 0), ("give_rows", 1),
    ("finish", 2, 3), ("finish", 2, 1), ("finish", 2, 4), ("ring_dependent", 0, 1), ("finish", 2, 2), ("far_block", 1), ("keep_rows", 1),
    ("ring_first", 1, 1), ("next_blocks", 0), ("own_block", 0), ("next_blocks", 1), ("own_block", 1), ("finish", 0, 0),
    ("ring_dependent", 1, 1), ("finish", 0, 1), ("ring_last", 0, 1), ("ring_first", 0, 2), ("finish", 0, 2), ("finish", 0, 3),
    ("finish", 0, 4), ("ring_last", 1, 1), ("ring_first", 1, 2), ("ring_dependent", 0, 2), ("finish", 1, 0), ("ring_dependent", 1, 2),
    ("ring_last", 0, 2), ("finish", 1, 1), ("finish", 1, 2), ("ring_last", 1, 2), ("finish", 1, 3), ("finish", 1, 4),
)


def dot(a, b, ca, cb):
    return lax.dot_general(a, b, (((ca,), (cb,)), ((), ())), preferred_element_type=F32)


def layer_kernel(sg, su, sd, tok, grad, tok_own, grad_own,
                 og, ou, od, out, gin, wg, wu, wd, wr, tok_all, grad_all, h_main, h_rest, ra, rb, give, rc, part, ra1, rb1, sd1, mid, ra2, rb2, sd2,
                 ff, blk, far, nxt,
                 own_sem, ex_s, ex_r, z1_s, z1_r, zn_r, z2_s, p1_s, p1_r, p2_s, p2_r, q1_s, q1_r, q2_s, q2_r, cc_s, cc_r,
                 sh_sem, wv_sem, row_sem, hst_sem, blk_sem, tmp_sem, a_s, a_r, u_s, u_r, e_s, e_r, out_sem,
                 c_s, c_r, a1_s, a1_r, f1_s, f1_r, a2_s, a2_r, f2_s, f2_r):
    z, y = lax.axis_index("datb"), lax.axis_index("model")
    x, core = lax.axis_index("x"), lax.axis_index("core")
    i8 = 2 * x + core
    n8 = 2 * RING
    rows, d = tok.shape
    half_rows = rows // 2
    chunk = RING * rows
    n_chunk = n8
    nf, tokens = ff.shape[1:]
    dp = sg.shape[0]
    half = nf // 2
    main = wg.shape[1]
    rest = nf - main
    packed = wr.shape[1]
    cols = blk.shape[2]
    tiles = far.shape[1] // LANE
    outs = (og, ou, od)

    zs, ys, xs = ([v] + [lax.rem(v + k, RING) for k in range(1, RING)] for v in (z, y, x))
    cores = (core, 1 - core)
    peers = [[2 * v + c for c in cores] for v in xs]
    slot_at = [[[pl.multiple_of((zz * n8 + peers[dx][dc]) * dp, 16) for dc in range(2)] for dx in range(RING)] for zz in zs]
    hand_at = [[pl.multiple_of(p * dp, 8) for p in row] for row in peers]
    rows_at = [[[pl.multiple_of((peers[dx][dc] * RING + yy) * rows, half_rows) for dc in range(2)] for yy in ys] for dx in range(RING)]
    lanes_at = [pl.multiple_of(zz * cols, LANE) for zz in zs]

    def peer(dx, dc):
        return peers[dx][dc]

    def zdev(k):
        return {"datb": zs[k]}

    def xdev(k):
        return {"x": xs[k]}

    def ydev(k):
        return {"model": ys[k]}

    def near(dx, dc):
        return {"x": xs[dx], "core": cores[dc]}

    def copy(src, dst, s, r, dev):
        return pltpu.make_async_remote_copy(src_ref=src, dst_ref=dst, send_sem=s, recv_sem=r, device_id=dev, device_id_type=MESH_ID)

    rcopy = copy

    def all_in(ref, sem):
        copy(ref, ref, sem, sem, zdev(1)).wait_recv()

    def all_out(ref, sem):
        copy(ref, ref, sem, sem, zdev(1)).wait_send()

    def start(copies):
        for c in copies:
            c.start()

    def received(copies):
        for c in copies:
            c.wait_recv()

    def sent(copies):
        for c in copies:
            c.wait_send()

    def run_order(fns, order):
        for fn, *args in order:
            with jax.named_scope("_".join(str(v) for v in [fn, *args])):
                fns[fn](*args)

    barrier = pltpu.get_barrier_semaphore()
    others = [zdev(1), zdev(3), ydev(1), ydev(3)] + [near(*n) for n in NEAR[1:]]
    for dev in others:
        pl.semaphore_signal(barrier, inc=1, device_id=dev, device_id_type=MESH_ID)

    def blk_load(t, slot, k):
        src = tok_all if t < 2 else grad_all
        return pltpu.make_async_copy(src.at[:, pl.ds(lanes_at[k], cols)], blk.at[slot], blk_sem.at[slot])

    plan = []
    for fn, *args in EARLY_ORDER + LATE_ORDER:
        plan += [(args[0], k) for k in {"far_block": (2,), "next_blocks": (1, 3), "next_products": (1, 3), "own_block": (0,)}.get(fn, ())]
    taken = []

    def next_block():
        n = len(taken)
        taken.append(n)
        blk_load(plan[n][0], n % 2, plan[n][1]).wait()
        if n + 1 < len(plan):
            blk_load(plan[n + 1][0], (n + 1) % 2, plan[n + 1][1]).start()
        return n % 2

    def product(t, dst, then=None):
        slot = next_block()
        step = 2 * LANE
        count = -(-cols // step)

        def one(n, carry):
            lanes = pl.ds(pl.multiple_of(jnp.minimum(n * step, cols - step), LANE), step)
            dst[:nf, lanes] = jnp.dot(ff[t], blk[slot, :, lanes], preferred_element_type=F32)
            for k in range(count if then else 0):
                first = k * step if k < count - 1 else cols - step
                size = step if k == count - 1 else min(step, cols - step - first)
                if size > 0:
                    pl.when(n == k)(functools.partial(then, first, size))
            return carry

        lax.fori_loop(0, count, one, 0)

    lo, hi = pl.ds(0, half), pl.ds(half, half)

    def a_copies(t, first=0, size=cols):
        lanes = pl.ds(first, size)
        return [rcopy(far.at[t, at, lanes], ra.at[t, at, lanes], a_s.at[t], a_r.at[t], zdev(k)) for at, k in ((lo, 1), (hi, 3))]

    def tile_rows(tile):
        return pl.ds(tile * LANE, min(LANE, nf - tile * LANE))

    def unit_parts(t, tile):
        if (t, tile) != (Z_ORDER[2], tiles - 1):
            return [(tile, 0, cols)]
        first = -(-cols // 2 // LANE) * LANE
        return [(tile, 0, first), (tiles, first, cols - first)]

    def unit_copies(t, tile):
        at = tile_rows(tile)
        cs = []
        for n, first, size in unit_parts(t, tile):
            lanes = pl.ds(first, size)
            cs += [rcopy(nxt.at[t, s, at, lanes], rb.at[t, s, at, lanes], u_s.at[t], u_r.at[t, n], zdev(1 + 2 * s)) for s in range(2)]
        return cs

    def far_block(t):
        if t == Z_ORDER[0]:
            product(t, far.at[t], lambda first, size: start(a_copies(t, first, size)))
        else:
            product(t, far.at[t])
            start(a_copies(t))

    def early_units(t):
        if ("next_products", t) not in EARLY_ORDER + LATE_ORDER:
            return ()
        free = [(0, tile) for tile in range(tiles) if tile * LANE >= half]
        return free + [(1, tile) for tile in range(tiles) if (tile + 1) * LANE <= half]

    def next_products(t):
        for s in range(2):
            product(t, nxt.at[t, s])
        for s, tile in early_units(t):
            unit_copies(t, tile)[s].start()

    blocks = d // min(OUT_COLS, d)
    width = d // blocks

    def row_products(r, keep):
        side = core if keep else 1 - core
        specs, args = [], []
        for h, j, w in ((h_main, 2, wd), (h_rest, 0, wr)) if r == 0 else ((h_main, 0, wg), (h_main, 1, wu), (h_rest, 1, wr)):
            n = w.shape[1]
            specs += [pl.BlockSpec((1, RING, 1, RING * rows, n), lambda i, j=j: (j, 0, side, 0, 0)), pl.BlockSpec((width, n), lambda i: (i, 0))]
            args += [h, w]
        wide = pl.BlockSpec((RING, RING, rows, width), lambda i: (0, 0, 0, i))
        terms = len(args) // 2
        if keep:
            specs.append(wide)
            args.append(rc.at[r])

        def body(*refs):
            total = None
            for i in range(terms):
                h = refs[2 * i][...].reshape(RING * RING * rows, refs[2 * i].shape[-1])
                prod = dot(h, refs[2 * i + 1][...], 1, 1)
                total = prod if total is None else total + prod
            if keep:
                total = total + refs[-2][...].astype(F32).reshape(total.shape)
            refs[-1][...] = total.astype(BF16).reshape(RING, RING, rows, width)

        pltpu.emit_pipeline(body, grid=(blocks,), in_specs=specs, out_specs=[wide])(*args, (part if keep else give).at[r])

    def core_copy(r):
        return rcopy(give.at[r], rc.at[r], c_s.at[r], c_r.at[r], near(0, 1))

    def give_rows(r):
        row_products(r, False)
        core_copy(r).start()

    def forward_phase(rowbuf, av, bv, gv, hst, hst_rest, wv_a, wv_r):
        held = {}

        fulls = (wg, wu, wd, wr)
        REST = 3
        def shard_load(t):
            return pltpu.make_async_copy((sg, su, sd)[t], held["shard"].at[t], sh_sem.at[t])

        def cut_pieces(t):
            if t == REST:
                for u in range(3):
                    for j in range(n8):
                        held["rests"][j, :, u * rest:(u + 1) * rest] = held["shard"][u, :, j * nf + main:(j + 1) * nf]
            else:
                for j in range(n8):
                    held["pieces"][t, j] = held["shard"][t, :, j * nf:j * nf + main]
            own_piece(t).start()

        def piece(t, j):
            return held["rests"].at[j] if t == REST else held["pieces"].at[t, j]

        def own_piece(t):
            return pltpu.make_async_copy(piece(t, i8), slot(t, 0, NEAR[0]), own_sem.at[t])

        def go(make, *args):
            make(*args).start()

        def slot(t, k, source):
            dx, dc = source
            return fulls[t].at[pl.ds(slot_at[k][dx][dc], dp)]

        def source(k):
            dx, dc = NEAR[k]
            return (RING - dx) % RING, dc

        def back(side):
            return 3 if side == 0 else 1

        def ahead(side):
            return 1 if side == 0 else 3

        def exchange_copy(t, k):
            return copy(piece(t, peer(*NEAR[k])), slot(t, 0, NEAR[0]), ex_s.at[t], ex_r.at[t, k], near(*NEAR[k]))

        def exchange(t, k):
            go(exchange_copy, t, k)

        def z_first_copy(t, side, k):
            here = slot(t, 0, source(k))
            return copy(here if k else piece(t, i8), here, z1_s.at[t], z1_sem(t, side, k), zdev(ahead(side)))

        def z_first(t, k):
            if k:
                here = slot(t, 0, source(k))
                all_in(here, ex_r.at[t, k])
            for side in range(2):
                go(z_first_copy, t, side, k)

        def z1_sem(t, side, k):
            return z1_r.at[t, side, k % (n8 // 2)] if (k < n8 // 2) == (side == 0) else zn_r.at[t]

        def some(t, count):
            return fulls[t].at[pl.ds(0, count * dp)]

        def z_second_copy(t, side, k):
            there = slot(t, back(side), source(k + side * (n8 // 2)))
            return copy(there, there, z2_s.at[t], zn_r.at[t], zdev(ahead(side)))

        def z_second(t, side, k):
            kk = k + side * (n8 // 2)
            all_in(slot(t, back(side), source(kk)), z1_sem(t, side, kk))
            go(z_second_copy, t, side, k)

        def weights_done(t):
            if (WD, t) not in LATE_STEPS:
                own_wait(t)
            all_in(some(t, 2 * n8), zn_r.at[t])
            w_load(t).start()

        cut = d * 11 // 28
        rings = ((tok, tok_all, pl.ds(0, d), True), (grad, grad_all, pl.ds(0, cut), True), (grad, grad_all, pl.ds(cut, d - cut), False))

        def axis(r, n):
            return xdev if rings[r][3] == (n == 1) else ydev

        def block(r, da, db, flip=0, lo=0, size=rows):
            dx, dy = (da, db) if rings[r][3] else (db, da)
            first = rows_at[dx][dy][flip]
            return rings[r][1].at[pl.ds(pl.multiple_of(first + lo, half_rows) if lo else first, size), rings[r][2]]

        def own_block(r):
            return rings[r][0].at[:, rings[r][2]]

        def to_core_copy(r, ia, ib):
            there = block(r, DELTAS[ia], DELTAS[ib])
            return copy(own_block(r) if ia == 0 and ib == 0 else there, there, cc_s.at[r], cc_r.at[ia if r == 0 else RING - 1 + r], near(0, 1))

        def to_core(r, ia, ib):
            go(to_core_copy, r, ia, ib)

        def first_copy(r, side):
            return copy(own_block(r), block(r, 0, 0), p1_s.at[r], p1_r.at[r, side], axis(r, 1)(ahead(side)))

        def first_own(r, side):
            go(first_copy, r, side)

        def first_far_copy(r, side):
            part = block(r, back(side), 0, 0, side * half_rows, half_rows)
            return copy(part, part, p2_s.at[r], p2_r.at[r], axis(r, 1)(ahead(side)))

        def first_forward(r, side):
            there = block(r, back(side), 0)
            all_in(there, p1_r.at[r, side])
            go(first_far_copy, r, side)

        def block_on(r, ia):
            if ia == 3:
                all_in(block(r, 2, 0), p2_r.at[r])
            for side in range(2):
                go(second_copy, r, side, ia)
            to_core(r, ia, 0)

        def second_copy(r, side, ia):
            there = block(r, DELTAS[ia], 0)
            return copy(there if ia else own_block(r), there, q1_s.at[r], q1_r.at[r, side, ia], axis(r, 2)(ahead(side)))

        def second_far_copy(r, ia):
            side = ia // 2
            there = block(r, DELTAS[ia], back(side))
            return copy(there, there, q2_s.at[r], q2_r.at[r, ia], axis(r, 2)(ahead(side)))

        def second_forward(r, ia, side):
            there = block(r, DELTAS[ia], back(side))
            all_in(there, q1_r.at[r, side, ia])
            if ia // 2 == side:
                go(second_far_copy, r, ia)
            to_core(r, ia, 1 if side == 0 else 2)

        def second_far(r, ia):
            there = block(r, DELTAS[ia], 2)
            all_in(there, q2_r.at[r, ia])
            to_core(r, ia, 3)

        def some_rows(r, count):
            return rings[r][1].at[pl.ds(0, count * rows), rings[r][2]]

        def chunk_in(ia):
            all_in(some_rows(0, RING), cc_r.at[ia])

        def rows_in(r):
            all_in(some_rows(r, RING * RING), cc_r.at[RING - 1 + r])

        def own_wait(t):
            there = slot(t, 0, NEAR[0])
            pltpu.make_async_copy(there, there, own_sem.at[t]).wait()

        def own_rows(r):
            return pltpu.make_async_copy(own_block(r), block(r, 0, 0), own_sem.at[4 + r])

        def w_load(t):
            return pltpu.make_async_copy(fulls[t], (wv_a, held["wv_b"], wv_a, wv_r)[t], wv_sem.at[t])

        def row_load(src, i, buf):
            return pltpu.make_async_copy(src.at[chunk_rows(i)], rowbuf.at[buf], row_sem.at[buf])

        def chunk_loop(src, products, elementwise, between):
            row_load(src, 0, 0).start()
            between[0]()
            row_load(src, 1, 1).start()
            row_load(src, 0, 0).wait()
            products(0, 0)

            def body(i, carry):
                buf = lax.rem(i, 2)

                @pl.when(i + 1 < n_chunk)
                def _():
                    row_load(src, i + 1, 1 - buf).start()

                for k, step in enumerate(between[1:], 1):
                    pl.when(i == k)(step)
                row_load(src, i, buf).wait()
                free(elementwise, i - 1)
                elementwise(i - 1, 1 - buf, lambda: products(i, buf))
                return carry

            lax.fori_loop(1, n_chunk, body, 0)
            free(elementwise, n_chunk - 1)
            elementwise(n_chunk - 1, (n_chunk - 1) % 2, lambda: None)

        def free(elementwise, i):
            @pl.when(i >= 2)
            def _():
                for cp in copies_of[elementwise](i - 2):
                    cp.wait()

        def chunk_rows(i):
            return pl.ds(pl.multiple_of(i * chunk, chunk), chunk)

        def h_copies(i, which, names):
            xx, c = lax.div(i, 2), lax.rem(i, 2)
            cs = [pltpu.make_async_copy(hst.at[c, n], h_main.at[j, xx, c], hst_sem.at[c, n]) for n, j in enumerate(names)]
            return cs + [pltpu.make_async_copy(hst_rest.at[which, c], h_rest.at[which, xx, c], hst_sem.at[c, 2])]

        def keep(i, c, values):
            which = len(values) - 1
            for n, (j, v) in enumerate(values):
                low = v.astype(BF16)
                hst[c, n] = low[:, :main]
                hst_rest[which, c, :, j * rest:(j + 1) * rest] = low[:, main:]
                ff[j, :, chunk_rows(i)] = v.T.astype(BF16)

        def kept(elementwise):
            for i in (n_chunk - 2, n_chunk - 1):
                for cp in copies_of[elementwise](i):
                    cp.wait()

        def gate_work():
            def place(k):
                ia, flip = lax.div(k, 2), lax.rem(k, 2)
                delta = lax.rem(3 * ia + 3 * lax.div(ia, 2) + 2 * lax.div(ia, 3), RING)
                return 2 * lax.rem(x + delta, RING) + lax.rem(core + flip, 2)

            def body(k, carry):
                for n, group in enumerate(GATE_STEPS):
                    if group:
                        pl.when(k == n)(functools.partial(run, group))

                @pl.when(k < n_chunk)
                def _():
                    row_load(tok_all, place(k), lax.rem(k, 2)).start()

                @pl.when(k >= 1)
                def _():
                    i, buf = place(k - 1), lax.rem(k - 1, 2)
                    row_load(tok_all, i, buf).wait()
                    rb_ = rowbuf[buf]
                    av[chunk_rows(i), :main] = jnp.dot(rb_, wv_a[...], preferred_element_type=F32).astype(BF16)
                    both = jnp.dot(rb_, wv_r[...], preferred_element_type=F32).astype(BF16)
                    av[chunk_rows(i), main:] = both[:, :rest]
                    bv[chunk_rows(i), main:] = both[:, rest:2 * rest]

                return carry

            lax.fori_loop(0, n_chunk + 1, body, 0)

        def up_products(i, buf):
            bv[chunk_rows(i), :main] = jnp.dot(rowbuf[buf], held["wv_b"][...], preferred_element_type=F32).astype(BF16)

        def hidden(i, c, beside):
            a, b = av[chunk_rows(i)].astype(F32), bv[chunk_rows(i)].astype(F32)
            beside()
            keep(i, c, ((2, a * jax.nn.sigmoid(a) * b),))
            start(copies_of[hidden](i))

        def down_products(i, buf):
            rb_ = rowbuf[buf]
            lanes = 2 * rest // LANE * LANE
            low = jnp.dot(rb_, wv_r[:, lanes:], preferred_element_type=F32)[:, 2 * rest - lanes:3 * rest - lanes]
            gv[buf] = jnp.concatenate([jnp.dot(rb_, wv_a[...], preferred_element_type=F32), low], axis=1).astype(BF16)

        def backward(i, c, beside):
            g = gv[c].astype(F32)
            a, b = av[chunk_rows(i)].astype(F32), bv[chunk_rows(i)].astype(F32)
            beside()
            sig = jax.nn.sigmoid(a)
            keep(i, c, ((0, g * b * sig * (1.0 + a * (1.0 - sig))), (1, g * (a * sig))))
            start(copies_of[backward](i))

        copies_of = {hidden: lambda i: h_copies(i, 0, (2,)), backward: lambda i: h_copies(i, 1, (0, 1))}

        steps = (exchange, z_first, z_second, first_own, first_forward, block_on, second_forward, second_far, weights_done, chunk_in)

        def run(group):
            for which, *args in group:
                steps[which](*args)

        def rows_ready():
            run(UP_STEPS[-1])
            for r in (1, 2):
                own_rows(r).wait()
                rows_in(r)
            blk_load(plan[0][0], 0, plan[0][1]).start()

        def gather_phase(shard, pieces, rests, wv_b):
            held.update(shard=shard, pieces=pieces, rests=rests, wv_b=wv_b)
            with jax.named_scope("begin"):
                shard_load(0).start()
                shard_load(0).wait()
                for t in (1, 2):
                    shard_load(t).start()
                cut_pieces(0)
                pl.semaphore_wait(barrier, len(others))
                for r in range(3):
                    own_rows(r).start()
            with jax.named_scope("gather"):
                cut = {0}
                for step in GATHER_STEPS:
                    if step[0] in (EX, Z1) and step[1] not in cut:
                        if len(cut) == 1:
                            rests[...] = jnp.zeros_like(rests)
                            hst_rest[...] = jnp.zeros_like(hst_rest)
                            shard_load(1).wait()
                            shard_load(2).wait()
                        cut.add(step[1])
                        cut_pieces(step[1])
                    run((step,))
                own_rows(0).wait()
                w_load(0).wait()
                w_load(REST).wait()
            with jax.named_scope("gate"):
                gate_work()
            with jax.named_scope("up"):
                run(UP_STEPS[0])
                w_load(1).wait()
                chunk_loop(tok_all, up_products, hidden, [functools.partial(run, group) for group in ((),) + UP_STEPS[1:-1]] + [rows_ready])
                kept(hidden)
            for _, t in LATE_STEPS:
                own_wait(t)
            for t in range(4):
                all_out(some(t, n8 - 1), ex_s.at[t])
                all_out(some(t, 2 * n8), z1_s.at[t])

        pl.run_scoped(
            gather_phase, pltpu.VMEM((3,) + sg.shape, BF16), pltpu.VMEM((3, n8, dp, main), BF16), pltpu.VMEM((n8, dp, packed), BF16),
            pltpu.VMEM((d, main), BF16))
        run_order({
            "far_block": far_block, "next_products": next_products, "give_rows": give_rows, "late": functools.partial(run, LATE_STEPS),
        }, EARLY_ORDER)
        with jax.named_scope("down"):
            w_load(2).wait()
            chunk_loop(grad_all, down_products, backward, [lambda: None])
            kept(backward)
        for t in range(4):
            all_out(some(t, n8), z2_s.at[t])
        for r in range(3):
            for count, sem in ((2, p1_s), (1, p2_s), (2 * RING, q1_s), (RING, q2_s), (RING * RING, cc_s)):
                all_out(some_rows(r, count), sem.at[r])

    def backward_phase(tmp, stage):
        def next_adds(t):
            all_in(ra.at[t], a_r.at[t])
            cs = [pltpu.make_async_copy(ra.at[t, at], tmp.at[s, at], tmp_sem.at[s]) for s, at in ((0, lo), (1, hi))]
            start(cs)
            for c, (s, at) in zip(cs, ((0, lo), (1, hi))):
                c.wait()
                nxt[t, s, at] += tmp[s, at]
            for tile in range(tiles):
                start(c for s, c in enumerate(unit_copies(t, tile)) if (s, tile) not in early_units(t))

        def next_blocks(t):
            next_products(t)
            next_adds(t)

        def own_block(t):
            all_out(ra.at[t], a_s.at[t])
            product(t, far.at[t])

        def slot(t):
            return Z_ORDER.index(t) % 2

        def hand_out(t, tile, part):
            parts = unit_parts(t, tile)
            for k in reversed(range(n8)):
                dx, dc = NEAR[k]
                at = pl.ds(hand_at[dx][dc], dp)
                src, dst = stage.at[slot(t), tile, at], outs[t].at[i8, tile]

                def send(k=k, src=src, dst=dst):
                    if k:
                        rcopy(src, dst, e_s.at[t], e_r.at[t], near(*NEAR[k])).start()
                    else:
                        pltpu.make_async_copy(src, dst, out_sem.at[t]).start()

                if len(parts) == 1:
                    send()
                elif part == 0:
                    pl.when(xs[dx] < parts[0][2] // dp // 2)(send)
                else:
                    pl.when(xs[dx] >= parts[0][2] // dp // 2)(send)

        def handed(t):
            all_out(outs[t].at[pl.ds(0, n8 - 1)], e_s.at[t])
            pltpu.make_async_copy(outs[t].at[0], outs[t].at[0], out_sem.at[t]).wait()

        given = []

        def finish(t, tile):
            at = tile_rows(tile)
            wide = pl.ds(tile * LANE, LANE)
            for part, (n, first, size) in enumerate(unit_parts(t, tile)):
                lanes = pl.ds(first, size)
                all_in(rb.at[t, :, at, lanes], u_r.at[t, n])
                cs = [pltpu.make_async_copy(rb.at[t, s, at, lanes], tmp.at[s, at, lanes], tmp_sem.at[s]) for s in range(2)]
                start(cs)
                if t == Z_ORDER[2] and not given:
                    given.append(Z_ORDER[0])
                    handed(Z_ORDER[0])
                for c in cs:
                    c.wait()
                stage[slot(t), tile, lanes] = (far[t, wide, lanes] + tmp[0, wide, lanes] + tmp[1, wide, lanes]).T
                hand_out(t, tile, part)

        def on_y(r, n):
            return (r == 1) == (n == 1)

        def level(r, n):
            at = ys if on_y(r, n) else xs
            dev = ydev if on_y(r, n) else xdev
            if n == 1:
                def piece(k, h):
                    return part.at[r, pl.ds(2 * h, 2), at[k]] if on_y(r, n) else part.at[r, at[k], pl.ds(2 * h, 2)]
                return dev, piece, ra1, rb1, sd1, (a1_s, a1_r, f1_s, f1_r)

            def piece(k, h):
                return mid.at[r, at[k], pl.ds(h, 1)]
            return dev, piece, ra2, rb2, sd2, (a2_s, a2_r, f2_s, f2_r)

        def ring_a(r, n):
            dev, piece, rfar, _, _, sems = level(r, n)
            return [rcopy(piece(2, s), rfar.at[r, s], sems[0].at[r], sems[1].at[r], dev(1 + 2 * s)) for s in range(2)]

        def ring_f(r, n):
            dev, piece, _, rnear, _, sems = level(r, n)
            return [rcopy(piece(1 + 2 * s, 1 - s), rnear.at[r, s, 1 - s], sems[2].at[r], sems[3].at[r], dev(1 + 2 * s)) for s in range(2)]

        def ring_d(r, n):
            dev, _, _, rnear, dep, sems = level(r, n)
            return [rcopy(dep.at[r, s], rnear.at[r, s, s], sems[2].at[r], sems[3].at[r], dev(1 + 2 * s)) for s in range(2)]

        def add(grid, *terms):
            specs = []
            for ref, at, lead in terms:
                tail = ref.shape[lead:]
                specs.append(pl.BlockSpec((1,) * lead + tuple(tail), lambda *i, at=at, rank=len(tail): tuple(at(*i)) + (0,) * rank))

            def body(*refs):
                total = refs[0][...].astype(F32).reshape(refs[0].shape[-2:])
                for ref in refs[1:-1]:
                    total = total + ref[...].astype(F32).reshape(total.shape)
                refs[-1][...] = total.astype(BF16).reshape(refs[-1].shape)

            pltpu.emit_pipeline(body, grid=grid, in_specs=specs[:-1], out_specs=specs[-1:])(*[ref for ref, _, _ in terms])

        def ring_first(r, n):
            start(ring_a(r, n) + ring_f(r, n))

        def ring_dependent(r, n):
            _, _, rfar, _, _, sems = level(r, n)
            all_in(rfar.at[r], sems[1].at[r])
            here = y if on_y(r, n) else x
            if n == 1:
                def near_block(s, i):
                    at = lax.rem(here + 1 + 2 * s, RING)
                    return (2 * s + i, at) if on_y(r, n) else (at, 2 * s + i)

                add((2, 2), (part.at[r], near_block, 2), (ra1.at[r], lambda s, i: (s, i), 2), (sd1.at[r], lambda s, i: (s, i), 2))
            else:
                add((2,), (mid.at[r], lambda s: (lax.rem(here + 1 + 2 * s, RING), s), 2), (ra2.at[r], lambda s: (s, 0), 2),
                    (sd2.at[r], lambda s: (s, 0), 2))
            start(ring_d(r, n))

        def ring_last(r, n):
            _, _, _, rnear, _, sems = level(r, n)
            all_in(rnear.at[r], sems[3].at[r])
            here = y if on_y(r, n) else x
            if n == 1:
                def own_at(h, i):
                    return (2 * h + i, here) if on_y(r, n) else (here, 2 * h + i)

                add((2, 2), (part.at[r], own_at, 2), (rb1.at[r, 0], lambda h, i: (h, i), 2),
                    (rb1.at[r, 1], lambda h, i: (h, i), 2), (mid.at[r], lambda h, i: (2 * h + i,), 1))
            else:
                own, res = ((tok_own, out), (grad_own, gin))[r]
                add((2,), (own, lambda h: (h,), 1), (mid.at[r], lambda h: (here, h), 2), (rb2.at[r, 0], lambda h: (h, 0), 2),
                    (rb2.at[r, 1], lambda h: (h, 0), 2), (res, lambda h: (h,), 1))

        def keep_rows(r):
            core_copy(r).wait_recv()
            row_products(r, True)

        run_order({
            "far_block": far_block, "next_products": next_products, "next_adds": next_adds, "next_blocks": next_blocks,
            "own_block": own_block, "finish": finish, "give_rows": give_rows, "keep_rows": keep_rows, "ring_first": ring_first,
            "ring_dependent": ring_dependent, "ring_last": ring_last,
        }, LATE_ORDER)

        for t in range(3):
            all_out(nxt.at[t], u_s.at[t])
        for r in range(2):
            core_copy(r).wait_send()
            for n in (1, 2):
                _, _, rfar, rnear, _, sems = level(r, n)
                all_out(rfar.at[r], sems[0].at[r])
                all_out(rnear.at[r], sems[2].at[r])
        for t in Z_ORDER:
            with jax.named_scope(f"handed_{t}"):
                all_in(outs[t].at[pl.ds(0, n8 - 1)], e_r.at[t])
                if t not in given:
                    handed(t)

    pl.run_scoped(
        forward_phase,
        pltpu.VMEM((2, chunk, d), BF16),
        pltpu.VMEM((tokens, nf), BF16),
        pltpu.VMEM((tokens, nf), BF16),
        pltpu.VMEM((2, chunk, nf), BF16),
        pltpu.VMEM((2, 2, chunk, main), BF16),
        pltpu.VMEM((2, 2, chunk, packed), BF16),
        pltpu.VMEM((d, main), BF16),
        pltpu.VMEM((d, packed), BF16),
    )
    pl.run_scoped(backward_phase, pltpu.VMEM((2, tiles * LANE, cols), F32), pltpu.VMEM((2, tiles, cols, LANE), F32))


def layer(sg, su, sd, tok, grad):
    n8 = 2 * RING
    dp, nf = sg.shape[0], sg.shape[1] // n8
    rows, d = tok.shape
    tokens = rows * RING * n8
    cols = d // RING
    tiles = -(-nf // LANE)
    padded = tiles * LANE
    main = nf // LANE * LANE
    packed = -(-3 * (nf - main) // LANE) * LANE
    hbm = pl.BlockSpec(memory_space=pl.ANY)
    dma = pltpu.SemaphoreType.DMA
    sds = jax.ShapeDtypeStruct
    halves = (2, rows // 2, d)
    res = pl.pallas_call(
        layer_kernel,
        out_shape=[sds((n8, tiles, dp, LANE), F32)] * 3 + [sds(halves, BF16)] * 2 + [
            sds((d, main), BF16), sds((d, main), BF16), sds((d, main), BF16), sds((d, packed), BF16), sds((tokens, d), BF16), sds((tokens, d), BF16),
            sds((3, RING, 2, RING * rows, main), BF16), sds((2, RING, 2, RING * rows, packed), BF16),
            sds((3, nf, cols), F32), sds((3, 2, nf, cols), F32),
            sds((2, RING, RING, rows, d), BF16), sds((2, RING, RING, rows, d), BF16), sds((2, RING, RING, rows, d), BF16),
            sds((2, 2, 2, rows, d), BF16), sds((2, 2, 2, 2, rows, d), BF16), sds((2, 2, 2, rows, d), BF16),
            sds((2, RING, 2, rows // 2, d), BF16),
            sds((2, 2, 1, rows // 2, d), BF16), sds((2, 2, 2, 1, rows // 2, d), BF16), sds((2, 2, 1, rows // 2, d), BF16),
        ],
        in_specs=[hbm] * 7,
        out_specs=[hbm] * 25,
        scratch_shapes=[
            pltpu.VMEM((3, nf, tokens), BF16),
            pltpu.VMEM((2, tokens, cols), BF16),
            pltpu.VMEM((3, padded, cols), F32),
            pltpu.VMEM((3, 2, nf, cols), F32),
            dma((7,)),
            dma((4,)), dma((4, n8)),
            dma((4,)), dma((4, 2, n8 // 2)), dma((4,)),
            dma((4,)),
            dma((3,)), dma((3, 2)),
            dma((3,)), dma((3,)),
            dma((3,)), dma((3, 2, RING)),
            dma((3,)), dma((3, RING)),
            dma((3,)), dma((RING + 2,)),
            dma((3,)), dma((4,)), dma((2,)), dma((2, 3)), dma((2,)), dma((2,)),
            dma((3,)), dma((3,)),
            dma((3,)), dma((3, tiles + 1)),
            dma((3,)), dma((3,)),
            dma((3,)),
            dma((2,)), dma((2,)),
        ] + [dma((2,))] * 8,
        compiler_params=pltpu.CompilerParams(collective_id=0, has_side_effects=True, vmem_limit_bytes=67043328),
        cost_estimate=pl.CostEstimate(flops=18 * nf * tokens * d, bytes_accessed=300_000_000, transcendentals=0),
        name="layer",
    )(sg, su, sd, tok, grad, tok.reshape(halves), grad.reshape(halves))
    return res[:3], res[3].reshape(rows, d), res[4].reshape(rows, d)


def assemble_kernel(og, ou, od, out, gin, g, u, w, res, gres, buf, flat, in_sem, out_sem, row_buf, row_sem):
    n8, nf = og.shape[0], g.shape[1] // og.shape[0]
    srcs, dsts = (og, ou, od), (g, u, w)
    rows_in = [pltpu.make_async_copy(src, row_buf.at[r], row_sem.at[r]) for r, src in enumerate((out, gin))]
    loads = [pltpu.make_async_copy(src, buf.at[t], in_sem.at[t]) for t, src in enumerate(srcs)]
    stores = [pltpu.make_async_copy(flat.at[t], dst, out_sem.at[t]) for t, dst in enumerate(dsts)]
    for c in loads + rows_in:
        c.start()
    for t in range(3):
        loads[t].wait()
        for j in range(n8):
            flat[t, :, j * nf:(j + 1) * nf] = jnp.concatenate([buf[t, j, tile] for tile in range(buf.shape[2])], axis=1)[:, :nf]
        stores[t].start()
    rows_out = [pltpu.make_async_copy(row_buf.at[r], dst, row_sem.at[r]) for r, dst in enumerate((res, gres))]
    for c in rows_in:
        c.wait()
    for c in rows_out:
        c.start()
    for c in stores + rows_out:
        c.wait()


def assemble(sums, out, gin, ff):
    dp = sums[0].shape[2]
    hbm = pl.BlockSpec(memory_space=pl.ANY)
    dma = pltpu.SemaphoreType.DMA
    sds = jax.ShapeDtypeStruct
    return pl.pallas_call(
        assemble_kernel,
        out_shape=[sds((dp, ff), F32)] * 3 + [sds(out.shape, BF16)] * 2,
        in_specs=[hbm] * 5,
        out_specs=[hbm] * 5,
        scratch_shapes=[
            pltpu.VMEM((3,) + sums[0].shape, F32), pltpu.VMEM((3, dp, ff), F32), dma((3,)), dma((3,)),
            pltpu.VMEM((2,) + out.shape, BF16), dma((2,)),
        ],
        compiler_params=pltpu.CompilerParams(vmem_limit_bytes=63 * 1024 * 1024),
        name="assemble",
    )(*sums, out, gin)


def solution(mesh):
    nz, ny, nd = mesh.shape["datb"], mesh.shape["model"], mesh.shape["data"]
    fine = Mesh(mesh.devices.reshape(nz, ny, nd // 2, 2), ("datb", "model", "x", "core"))

    def local_step(tok_loc, wg_loc, wu_loc, wd_loc, grad_loc):
        sums, out, grad_in = layer(wg_loc, wu_loc, wd_loc.T, tok_loc, grad_loc)
        grad_gate, grad_up, grad_down_t, out, grad_in = assemble(sums, out, grad_in, wg_loc.shape[1])
        return out, grad_in, grad_gate, grad_up, grad_down_t.T

    return jax.shard_map(local_step, mesh=fine, in_specs=(ROW_SPEC, GATE_SPEC, GATE_SPEC, DOWN_SPEC, ROW_SPEC), out_specs=(ROW_SPEC, ROW_SPEC, GATE_SPEC, GATE_SPEC, DOWN_SPEC), check_vma=False)
```

```python
import functools

import jax
import jax.numpy as jnp
from jax import lax
from jax.experimental import pallas as pl
from jax.experimental.pallas import tpu as pltpu
from jax.sharding import Mesh
from jax.sharding import PartitionSpec as P

ROW_SPEC = P(("datb", "x", "core", "model"), None)
GATE_SPEC = P(("datb", "x", "core"), "model")
DOWN_SPEC = P("model", ("datb", "x", "core"))
BF16 = jnp.bfloat16
F32 = jnp.float32
MESH_ID = pl.DeviceIdType.MESH
RING = 4
NEAR = ((0, 0), (0, 1), (1, 0), (3, 0), (1, 1), (3, 1), (2, 0), (2, 1))
DELTAS = (0, 3, 1, 2)
LANE = 128
OUT_COLS = 512
EX, Z1, Z2, P1, P2, BL, Q1, Q2, WD, CI = range(10)
GATHER_STEPS = (
    (Z1, 0, 0), (P1, 0, 0), (P1, 0, 1), (EX, 0, 1), (BL, 0, 0), (P1, 2, 0), (P1, 2, 1), (EX, 0, 2), (Z1, 3, 0), (EX, 3, 1), (EX, 3, 2),
    (EX, 3, 3), (EX, 3, 4), (EX, 3, 5), (EX, 3, 6), (EX, 3, 7), (Z1, 1, 0), (EX, 1, 1), (Z1, 2, 0), (EX, 2, 1), (EX, 0, 3), (BL, 1, 0),
    (Z1, 3, 1), (EX, 0, 4), (EX, 0, 5), (Z1, 0, 1), (Z1, 1, 1), (Z2, 3, 0, 0), (Z1, 2, 1), (EX, 0, 6), (EX, 0, 7), (Z2, 0, 0, 0),
    (Z2, 1, 0, 0), (EX, 1, 2), (EX, 1, 3), (Z2, 2, 0, 0), (Z2, 3, 0, 1), (P2, 0, 0), (P2, 0, 1), (BL, 0, 1), (Q1, 0, 0, 1), (Z1, 3, 2),
    (Z1, 3, 3), (Z1, 3, 4), (Q1, 0, 0, 0), (Z1, 3, 5), (Z2, 0, 0, 1), (EX, 1, 4), (EX, 1, 5), (P2, 2, 1), (Z1, 3, 6), (EX, 1, 6),
    (EX, 1, 7), (Z1, 3, 7), (Z1, 0, 2), (Q1, 1, 0, 1), (Z2, 3, 1, 0), (Z2, 3, 1, 1), (Z1, 0, 3), (EX, 2, 2), (EX, 2, 3), (Z2, 3, 1, 2),
    (BL, 0, 2), (Z2, 3, 1, 3), (Z1, 0, 4), (EX, 2, 4), (EX, 2, 5), (Z1, 0, 5), (EX, 2, 6), (EX, 2, 7), (Z2, 3, 0, 2), (Q1, 0, 1, 1),
    (Z2, 3, 0, 3), (Z1, 0, 6), (P1, 1, 0), (P1, 1, 1), (Q1, 0, 1, 0), (Z1, 0, 7), (BL, 2, 2), (Z2, 0, 1, 0), (Z1, 1, 2), (Z2, 0, 1, 1),
    (Z2, 0, 0, 2), (Q2, 0, 0), (Z2, 0, 1, 2), (Z2, 0, 0, 3), (BL, 2, 0), (BL, 0, 3), (Q1, 0, 2, 1), (Z2, 0, 1, 3), (Z1, 1, 3), (Z1, 1, 4),
    (WD, 3), (Z1, 1, 5), (Q1, 0, 2, 0), (Z1, 1, 6), (P2, 2, 0), (BL, 2, 1), (P2, 1, 0), (P2, 1, 1), (Z1, 1, 7), (Q1, 0, 3, 1),
    (Q1, 1, 0, 0), (Z2, 1, 0, 1), (Q1, 2, 2, 0), (Q1, 2, 2, 1), (Z2, 1, 0, 2), (BL, 1, 1), (Q2, 0, 1), (WD, 0), (Z2, 1, 1, 0), (CI, 0),
)
GATE_STEPS = (
    (),
    (),
    (
        (Z1, 2, 2),
    ),
    (
        (Q2, 0, 2), (Z2, 1, 1, 1), (Z2, 1, 0, 3), (Q1, 2, 0, 0), (Q1, 2, 0, 1), (BL, 1, 2), (CI, 1),
    ),
    (
        (Z2, 1, 1, 2), (Z1, 2, 3),
    ),
    (
        (Q1, 0, 3, 0), (Z2, 1, 1, 3), (Z1, 2, 4), (CI, 2),
    ),
    (
        (Z1, 2, 5), (Q1, 2, 1, 0), (Q1, 2, 1, 1), (BL, 2, 3), (BL, 1, 3), (Z1, 2, 6), (Q2, 0, 3),
    ),
    (
        (Q2, 1, 0), (Z1, 2, 7), (CI, 3),
    ),
    (
        (Q2, 2, 0), (Q2, 2, 2), (Z2, 2, 0, 1), (Q1, 1, 1, 0), (Q1, 1, 1, 1),
    ),
)
UP_STEPS = (
    (
        (Z2, 2, 0, 2), (Q1, 1, 2, 1), (WD, 1),
    ),
    (
        (Q2, 2, 1), (Q1, 2, 3, 1), (Q1, 1, 2, 0),
    ),
    (
        (Z2, 2, 1, 0), (Z2, 2, 0, 3), (Q1, 1, 3, 1),
    ),
    (
        (Z2, 2, 1, 1), (Q1, 1, 3, 0),
    ),
    (
        (Q2, 1, 2), (Z2, 2, 1, 2), (Q1, 2, 3, 0),
    ),
    (
        (Q2, 1, 1), (Z2, 2, 1, 3),
    ),
    (
        (Q2, 1, 3), (Q2, 2, 3),
    ),
    (),
)
LATE_STEPS = (
    (WD, 2),
)
Z_ORDER = (2, 0, 1)
EARLY_ORDER = (
    ("far_block", 2), ("next_products", 2), ("late",), ("give_rows", 0),
)
LATE_ORDER = (
    ("next_adds", 2), ("own_block", 2), ("keep_rows", 0), ("ring_first", 0, 1), ("finish", 2, 0), ("far_block", 0), ("give_rows", 1),
    ("finish", 2, 3), ("finish", 2, 1), ("finish", 2, 4), ("ring_dependent", 0, 1), ("finish", 2, 2), ("far_block", 1), ("keep_rows", 1),
    ("ring_first", 1, 1), ("next_blocks", 0), ("own_block", 0), ("next_blocks", 1), ("own_block", 1), ("finish", 0, 0),
    ("ring_dependent", 1, 1), ("finish", 0, 1), ("ring_last", 0, 1), ("ring_first", 0, 2), ("finish", 0, 2), ("finish", 0, 3),
    ("finish", 0, 4), ("ring_last", 1, 1), ("ring_first", 1, 2), ("ring_dependent", 0, 2), ("finish", 1, 0), ("ring_dependent", 1, 2),
    ("ring_last", 0, 2), ("finish", 1, 1), ("finish", 1, 2), ("ring_last", 1, 2), ("finish", 1, 3), ("finish", 1, 4),
)


def dot(a, b, ca, cb):
    return lax.dot_general(a, b, (((ca,), (cb,)), ((), ())), preferred_element_type=F32)


def layer_kernel(sg, su, sd, tok, grad, tok_own, grad_own,
                 og, ou, od, out, gin, wg, wu, wd, wr, tok_all, grad_all, h_main, h_rest, ra, rb, give, rc, part, ra1, rb1, sd1, mid, ra2, rb2, sd2,
                 ff, blk, far, nxt,
                 own_sem, ex_s, ex_r, z1_s, z1_r, zn_r, z2_s, p1_s, p1_r, p2_s, p2_r, q1_s, q1_r, q2_s, q2_r, cc_s, cc_r,
                 sh_sem, wv_sem, row_sem, hst_sem, blk_sem, tmp_sem, a_s, a_r, u_s, u_r, e_s, e_r, out_sem,
                 c_s, c_r, a1_s, a1_r, f1_s, f1_r, a2_s, a2_r, f2_s, f2_r):
    z, y = lax.axis_index("datb"), lax.axis_index("model")
    x, core = lax.axis_index("x"), lax.axis_index("core")
    i8 = 2 * x + core
    n8 = 2 * RING
    rows, d = tok.shape
    half_rows = rows // 2
    chunk = RING * rows
    n_chunk = n8
    nf, tokens = ff.shape[1:]
    dp = sg.shape[0]
    half = nf // 2
    main = wg.shape[1]
    rest = nf - main
    packed = wr.shape[1]
    cols = blk.shape[2]
    tiles = far.shape[1] // LANE
    outs = (og, ou, od)

    zs, ys, xs = ([v] + [lax.rem(v + k, RING) for k in range(1, RING)] for v in (z, y, x))
    cores = (core, 1 - core)
    peers = [[2 * v + c for c in cores] for v in xs]
    slot_at = [[[pl.multiple_of((zz * n8 + peers[dx][dc]) * dp, 16) for dc in range(2)] for dx in range(RING)] for zz in zs]
    hand_at = [[pl.multiple_of(p * dp, 8) for p in row] for row in peers]
    rows_at = [[[pl.multiple_of((peers[dx][dc] * RING + yy) * rows, half_rows) for dc in range(2)] for yy in ys] for dx in range(RING)]
    lanes_at = [pl.multiple_of(zz * cols, LANE) for zz in zs]

    def peer(dx, dc):
        return peers[dx][dc]

    def zdev(k):
        return {"datb": zs[k]}

    def xdev(k):
        return {"x": xs[k]}

    def ydev(k):
        return {"model": ys[k]}

    def near(dx, dc):
        return {"x": xs[dx], "core": cores[dc]}

    def copy(src, dst, s, r, dev):
        return pltpu.make_async_remote_copy(src_ref=src, dst_ref=dst, send_sem=s, recv_sem=r, device_id=dev, device_id_type=MESH_ID)

    rcopy = copy

    def all_in(ref, sem):
        copy(ref, ref, sem, sem, zdev(1)).wait_recv()

    def all_out(ref, sem):
        copy(ref, ref, sem, sem, zdev(1)).wait_send()

    def start(copies):
        for c in copies:
            c.start()

    def received(copies):
        for c in copies:
            c.wait_recv()

    def sent(copies):
        for c in copies:
            c.wait_send()

    def run_order(fns, order):
        for fn, *args in order:
            with jax.named_scope("_".join(str(v) for v in [fn, *args])):
                fns[fn](*args)

    barrier = pltpu.get_barrier_semaphore()
    others = [zdev(1), zdev(3), ydev(1), ydev(3)] + [near(*n) for n in NEAR[1:]]
    for dev in others:
        pl.semaphore_signal(barrier, inc=1, device_id=dev, device_id_type=MESH_ID)

    def blk_load(t, slot, k):
        src = tok_all if t < 2 else grad_all
        return pltpu.make_async_copy(src.at[:, pl.ds(lanes_at[k], cols)], blk.at[slot], blk_sem.at[slot])

    plan = []
    for fn, *args in EARLY_ORDER + LATE_ORDER:
        plan += [(args[0], k) for k in {"far_block": (2,), "next_blocks": (1, 3), "next_products": (1, 3), "own_block": (0,)}.get(fn, ())]
    taken = []

    def next_block():
        n = len(taken)
        taken.append(n)
        blk_load(plan[n][0], n % 2, plan[n][1]).wait()
        if n + 1 < len(plan):
            blk_load(plan[n + 1][0], (n + 1) % 2, plan[n + 1][1]).start()
        return n % 2

    def product(t, dst, then=None):
        slot = next_block()
        step = 2 * LANE
        count = -(-cols // step)

        def one(n, carry):
            lanes = pl.ds(pl.multiple_of(jnp.minimum(n * step, cols - step), LANE), step)
            dst[:nf, lanes] = jnp.dot(ff[t], blk[slot, :, lanes], preferred_element_type=F32)
            for k in range(count if then else 0):
                first = k * step if k < count - 1 else cols - step
                size = step if k == count - 1 else min(step, cols - step - first)
                if size > 0:
                    pl.when(n == k)(functools.partial(then, first, size))
            return carry

        lax.fori_loop(0, count, one, 0)

    lo, hi = pl.ds(0, half), pl.ds(half, half)

    def a_copies(t, first=0, size=cols):
        lanes = pl.ds(first, size)
        return [rcopy(far.at[t, at, lanes], ra.at[t, at, lanes], a_s.at[t], a_r.at[t], zdev(k)) for at, k in ((lo, 1), (hi, 3))]

    def tile_rows(tile):
        return pl.ds(tile * LANE, min(LANE, nf - tile * LANE))

    def unit_parts(t, tile):
        if (t, tile) != (Z_ORDER[2], tiles - 1):
            return [(tile, 0, cols)]
        first = -(-cols // 2 // LANE) * LANE
        return [(tile, 0, first), (tiles, first, cols - first)]

    def unit_copies(t, tile):
        at = tile_rows(tile)
        cs = []
        for n, first, size in unit_parts(t, tile):
            lanes = pl.ds(first, size)
            cs += [rcopy(nxt.at[t, s, at, lanes], rb.at[t, s, at, lanes], u_s.at[t], u_r.at[t, n], zdev(1 + 2 * s)) for s in range(2)]
        return cs

    def far_block(t):
        if t == Z_ORDER[0]:
            product(t, far.at[t], lambda first, size: start(a_copies(t, first, size)))
        else:
            product(t, far.at[t])
            start(a_copies(t))

    def early_units(t):
        if ("next_products", t) not in EARLY_ORDER + LATE_ORDER:
            return ()
        free = [(0, tile) for tile in range(tiles) if tile * LANE >= half]
        return free + [(1, tile) for tile in range(tiles) if (tile + 1) * LANE <= half]

    def next_products(t):
        for s in range(2):
            product(t, nxt.at[t, s])
        for s, tile in early_units(t):
            unit_copies(t, tile)[s].start()

    blocks = d // min(OUT_COLS, d)
    width = d // blocks

    def row_products(r, keep):
        side = core if keep else 1 - core
        specs, args = [], []
        for h, j, w in ((h_main, 2, wd), (h_rest, 0, wr)) if r == 0 else ((h_main, 0, wg), (h_main, 1, wu), (h_rest, 1, wr)):
            n = w.shape[1]
            specs += [pl.BlockSpec((1, RING, 1, RING * rows, n), lambda i, j=j: (j, 0, side, 0, 0)), pl.BlockSpec((width, n), lambda i: (i, 0))]
            args += [h, w]
        wide = pl.BlockSpec((RING, RING, rows, width), lambda i: (0, 0, 0, i))
        terms = len(args) // 2
        if keep:
            specs.append(wide)
            args.append(rc.at[r])

        def body(*refs):
            total = None
            for i in range(terms):
                h = refs[2 * i][...].reshape(RING * RING * rows, refs[2 * i].shape[-1])
                prod = dot(h, refs[2 * i + 1][...], 1, 1)
                total = prod if total is None else total + prod
            if keep:
                total = total + refs[-2][...].astype(F32).reshape(total.shape)
            refs[-1][...] = total.astype(BF16).reshape(RING, RING, rows, width)

        pltpu.emit_pipeline(body, grid=(blocks,), in_specs=specs, out_specs=[wide])(*args, (part if keep else give).at[r])

    def core_copy(r):
        return rcopy(give.at[r], rc.at[r], c_s.at[r], c_r.at[r], near(0, 1))

    def give_rows(r):
        row_products(r, False)
        core_copy(r).start()

    def forward_phase(rowbuf, av, bv, gv, hst, hst_rest, wv_a, wv_r):
        held = {}

        fulls = (wg, wu, wd, wr)
        REST = 3
        def shard_load(t):
            return pltpu.make_async_copy((sg, su, sd)[t], held["shard"].at[t], sh_sem.at[t])

        def cut_pieces(t):
            if t == REST:
                for u in range(3):
                    for j in range(n8):
                        held["rests"][j, :, u * rest:(u + 1) * rest] = held["shard"][u, :, j * nf + main:(j + 1) * nf]
            else:
                for j in range(n8):
                    held["pieces"][t, j] = held["shard"][t, :, j * nf:j * nf + main]
            own_piece(t).start()

        def piece(t, j):
            return held["rests"].at[j] if t == REST else held["pieces"].at[t, j]

        def own_piece(t):
            return pltpu.make_async_copy(piece(t, i8), slot(t, 0, NEAR[0]), own_sem.at[t])

        def go(make, *args):
            make(*args).start()

        def slot(t, k, source):
            dx, dc = source
            return fulls[t].at[pl.ds(slot_at[k][dx][dc], dp)]

        def source(k):
            dx, dc = NEAR[k]
            return (RING - dx) % RING, dc

        def back(side):
            return 3 if side == 0 else 1

        def ahead(side):
            return 1 if side == 0 else 3

        def exchange_copy(t, k):
            return copy(piece(t, peer(*NEAR[k])), slot(t, 0, NEAR[0]), ex_s.at[t], ex_r.at[t, k], near(*NEAR[k]))

        def exchange(t, k):
            go(exchange_copy, t, k)

        def z_first_copy(t, side, k):
            here = slot(t, 0, source(k))
            return copy(here if k else piece(t, i8), here, z1_s.at[t], z1_sem(t, side, k), zdev(ahead(side)))

        def z_first(t, k):
            if k:
                here = slot(t, 0, source(k))
                all_in(here, ex_r.at[t, k])
            for side in range(2):
                go(z_first_copy, t, side, k)

        def z1_sem(t, side, k):
            return z1_r.at[t, side, k % (n8 // 2)] if (k < n8 // 2) == (side == 0) else zn_r.at[t]

        def some(t, count):
            return fulls[t].at[pl.ds(0, count * dp)]

        def z_second_copy(t, side, k):
            there = slot(t, back(side), source(k + side * (n8 // 2)))
            return copy(there, there, z2_s.at[t], zn_r.at[t], zdev(ahead(side)))

        def z_second(t, side, k):
            kk = k + side * (n8 // 2)
            all_in(slot(t, back(side), source(kk)), z1_sem(t, side, kk))
            go(z_second_copy, t, side, k)

        def weights_done(t):
            if (WD, t) not in LATE_STEPS:
                own_wait(t)
            all_in(some(t, 2 * n8), zn_r.at[t])
            w_load(t).start()

        cut = d * 11 // 28
        rings = ((tok, tok_all, pl.ds(0, d), True), (grad, grad_all, pl.ds(0, cut), True), (grad, grad_all, pl.ds(cut, d - cut), False))

        def axis(r, n):
            return xdev if rings[r][3] == (n == 1) else ydev

        def block(r, da, db, flip=0, lo=0, size=rows):
            dx, dy = (da, db) if rings[r][3] else (db, da)
            first = rows_at[dx][dy][flip]
            return rings[r][1].at[pl.ds(pl.multiple_of(first + lo, half_rows) if lo else first, size), rings[r][2]]

        def own_block(r):
            return rings[r][0].at[:, rings[r][2]]

        def to_core_copy(r, ia, ib):
            there = block(r, DELTAS[ia], DELTAS[ib])
            return copy(own_block(r) if ia == 0 and ib == 0 else there, there, cc_s.at[r], cc_r.at[ia if r == 0 else RING - 1 + r], near(0, 1))

        def to_core(r, ia, ib):
            go(to_core_copy, r, ia, ib)

        def first_copy(r, side):
            return copy(own_block(r), block(r, 0, 0), p1_s.at[r], p1_r.at[r, side], axis(r, 1)(ahead(side)))

        def first_own(r, side):
            go(first_copy, r, side)

        def first_far_copy(r, side):
            part = block(r, back(side), 0, 0, side * half_rows, half_rows)
            return copy(part, part, p2_s.at[r], p2_r.at[r], axis(r, 1)(ahead(side)))

        def first_forward(r, side):
            there = block(r, back(side), 0)
            all_in(there, p1_r.at[r, side])
            go(first_far_copy, r, side)

        def block_on(r, ia):
            if ia == 3:
                all_in(block(r, 2, 0), p2_r.at[r])
            for side in range(2):
                go(second_copy, r, side, ia)
            to_core(r, ia, 0)

        def second_copy(r, side, ia):
            there = block(r, DELTAS[ia], 0)
            return copy(there if ia else own_block(r), there, q1_s.at[r], q1_r.at[r, side, ia], axis(r, 2)(ahead(side)))

        def second_far_copy(r, ia):
            side = ia // 2
            there = block(r, DELTAS[ia], back(side))
            return copy(there, there, q2_s.at[r], q2_r.at[r, ia], axis(r, 2)(ahead(side)))

        def second_forward(r, ia, side):
            there = block(r, DELTAS[ia], back(side))
            all_in(there, q1_r.at[r, side, ia])
            if ia // 2 == side:
                go(second_far_copy, r, ia)
            to_core(r, ia, 1 if side == 0 else 2)

        def second_far(r, ia):
            there = block(r, DELTAS[ia], 2)
            all_in(there, q2_r.at[r, ia])
            to_core(r, ia, 3)

        def some_rows(r, count):
            return rings[r][1].at[pl.ds(0, count * rows), rings[r][2]]

        def chunk_in(ia):
            all_in(some_rows(0, RING), cc_r.at[ia])

        def rows_in(r):
            all_in(some_rows(r, RING * RING), cc_r.at[RING - 1 + r])

        def own_wait(t):
            there = slot(t, 0, NEAR[0])
            pltpu.make_async_copy(there, there, own_sem.at[t]).wait()

        def own_rows(r):
            return pltpu.make_async_copy(own_block(r), block(r, 0, 0), own_sem.at[4 + r])

        def w_load(t):
            return pltpu.make_async_copy(fulls[t], (wv_a, held["wv_b"], wv_a, wv_r)[t], wv_sem.at[t])

        def row_load(src, i, buf):
            return pltpu.make_async_copy(src.at[chunk_rows(i)], rowbuf.at[buf], row_sem.at[buf])

        def chunk_loop(src, products, elementwise, between):
            row_load(src, 0, 0).start()
            between[0]()
            row_load(src, 1, 1).start()
            row_load(src, 0, 0).wait()
            products(0, 0)

            def body(i, carry):
                buf = lax.rem(i, 2)

                @pl.when(i + 1 < n_chunk)
                def _():
                    row_load(src, i + 1, 1 - buf).start()

                for k, step in enumerate(between[1:], 1):
                    pl.when(i == k)(step)
                row_load(src, i, buf).wait()
                free(elementwise, i - 1)
                elementwise(i - 1, 1 - buf, lambda: products(i, buf))
                return carry

            lax.fori_loop(1, n_chunk, body, 0)
            free(elementwise, n_chunk - 1)
            elementwise(n_chunk - 1, (n_chunk - 1) % 2, lambda: None)

        def free(elementwise, i):
            @pl.when(i >= 2)
            def _():
                for cp in copies_of[elementwise](i - 2):
                    cp.wait()

        def chunk_rows(i):
            return pl.ds(pl.multiple_of(i * chunk, chunk), chunk)

        def h_copies(i, which, names):
            xx, c = lax.div(i, 2), lax.rem(i, 2)
            cs = [pltpu.make_async_copy(hst.at[c, n], h_main.at[j, xx, c], hst_sem.at[c, n]) for n, j in enumerate(names)]
            return cs + [pltpu.make_async_copy(hst_rest.at[which, c], h_rest.at[which, xx, c], hst_sem.at[c, 2])]

        def keep(i, c, values):
            which = len(values) - 1
            for n, (j, v) in enumerate(values):
                low = v.astype(BF16)
                hst[c, n] = low[:, :main]
                hst_rest[which, c, :, j * rest:(j + 1) * rest] = low[:, main:]
                ff[j, :, chunk_rows(i)] = v.T.astype(BF16)

        def kept(elementwise):
            for i in (n_chunk - 2, n_chunk - 1):
                for cp in copies_of[elementwise](i):
                    cp.wait()

        def gate_work():
            def place(k):
                ia, flip = lax.div(k, 2), lax.rem(k, 2)
                delta = lax.rem(3 * ia + 3 * lax.div(ia, 2) + 2 * lax.div(ia, 3), RING)
                return 2 * lax.rem(x + delta, RING) + lax.rem(core + flip, 2)

            def body(k, carry):
                for n, group in enumerate(GATE_STEPS):
                    if group:
                        pl.when(k == n)(functools.partial(run, group))

                @pl.when(k < n_chunk)
                def _():
                    row_load(tok_all, place(k), lax.rem(k, 2)).start()

                @pl.when(k >= 1)
                def _():
                    i, buf = place(k - 1), lax.rem(k - 1, 2)
                    row_load(tok_all, i, buf).wait()
                    rb_ = rowbuf[buf]
                    av[chunk_rows(i), :main] = jnp.dot(rb_, wv_a[...], preferred_element_type=F32).astype(BF16)
                    both = jnp.dot(rb_, wv_r[...], preferred_element_type=F32).astype(BF16)
                    av[chunk_rows(i), main:] = both[:, :rest]
                    bv[chunk_rows(i), main:] = both[:, rest:2 * rest]

                return carry

            lax.fori_loop(0, n_chunk + 1, body, 0)

        def up_products(i, buf):
            bv[chunk_rows(i), :main] = jnp.dot(rowbuf[buf], held["wv_b"][...], preferred_element_type=F32).astype(BF16)

        def hidden(i, c, beside):
            a, b = av[chunk_rows(i)].astype(F32), bv[chunk_rows(i)].astype(F32)
            beside()
            keep(i, c, ((2, a * jax.nn.sigmoid(a) * b),))
            start(copies_of[hidden](i))

        def down_products(i, buf):
            rb_ = rowbuf[buf]
            lanes = 2 * rest // LANE * LANE
            low = jnp.dot(rb_, wv_r[:, lanes:], preferred_element_type=F32)[:, 2 * rest - lanes:3 * rest - lanes]
            gv[buf] = jnp.concatenate([jnp.dot(rb_, wv_a[...], preferred_element_type=F32), low], axis=1).astype(BF16)

        def backward(i, c, beside):
            g = gv[c].astype(F32)
            a, b = av[chunk_rows(i)].astype(F32), bv[chunk_rows(i)].astype(F32)
            beside()
            sig = jax.nn.sigmoid(a)
            keep(i, c, ((0, g * b * sig * (1.0 + a * (1.0 - sig))), (1, g * (a * sig))))
            start(copies_of[backward](i))

        copies_of = {hidden: lambda i: h_copies(i, 0, (2,)), backward: lambda i: h_copies(i, 1, (0, 1))}

        steps = (exchange, z_first, z_second, first_own, first_forward, block_on, second_forward, second_far, weights_done, chunk_in)

        def run(group):
            for which, *args in group:
                steps[which](*args)

        def rows_ready():
            run(UP_STEPS[-1])
            for r in (1, 2):
                own_rows(r).wait()
                rows_in(r)
            blk_load(plan[0][0], 0, plan[0][1]).start()

        def gather_phase(shard, pieces, rests, wv_b):
            held.update(shard=shard, pieces=pieces, rests=rests, wv_b=wv_b)
            with jax.named_scope("begin"):
                shard_load(0).start()
                shard_load(0).wait()
                for t in (1, 2):
                    shard_load(t).start()
                cut_pieces(0)
                pl.semaphore_wait(barrier, len(others))
                for r in range(3):
                    own_rows(r).start()
            with jax.named_scope("gather"):
                cut = {0}
                for step in GATHER_STEPS:
                    if step[0] in (EX, Z1) and step[1] not in cut:
                        if len(cut) == 1:
                            rests[...] = jnp.zeros_like(rests)
                            hst_rest[...] = jnp.zeros_like(hst_rest)
                            shard_load(1).wait()
                            shard_load(2).wait()
                        cut.add(step[1])
                        cut_pieces(step[1])
                    run((step,))
                own_rows(0).wait()
                w_load(0).wait()
                w_load(REST).wait()
            with jax.named_scope("gate"):
                gate_work()
            with jax.named_scope("up"):
                run(UP_STEPS[0])
                w_load(1).wait()
                chunk_loop(tok_all, up_products, hidden, [functools.partial(run, group) for group in ((),) + UP_STEPS[1:-1]] + [rows_ready])
                kept(hidden)
            for _, t in LATE_STEPS:
                own_wait(t)
            for t in range(4):
                all_out(some(t, n8 - 1), ex_s.at[t])
                all_out(some(t, 2 * n8), z1_s.at[t])

        pl.run_scoped(
            gather_phase, pltpu.VMEM((3,) + sg.shape, BF16), pltpu.VMEM((3, n8, dp, main), BF16), pltpu.VMEM((n8, dp, packed), BF16),
            pltpu.VMEM((d, main), BF16))
        run_order({
            "far_block": far_block, "next_products": next_products, "give_rows": give_rows, "late": functools.partial(run, LATE_STEPS),
        }, EARLY_ORDER)
        with jax.named_scope("down"):
            w_load(2).wait()
            chunk_loop(grad_all, down_products, backward, [lambda: None])
            kept(backward)
        for t in range(4):
            all_out(some(t, n8), z2_s.at[t])
        for r in range(3):
            for count, sem in ((2, p1_s), (1, p2_s), (2 * RING, q1_s), (RING, q2_s), (RING * RING, cc_s)):
                all_out(some_rows(r, count), sem.at[r])

    def backward_phase(tmp, stage):
        def next_adds(t):
            all_in(ra.at[t], a_r.at[t])
            cs = [pltpu.make_async_copy(ra.at[t, at], tmp.at[s, at], tmp_sem.at[s]) for s, at in ((0, lo), (1, hi))]
            start(cs)
            for c, (s, at) in zip(cs, ((0, lo), (1, hi))):
                c.wait()
                nxt[t, s, at] += tmp[s, at]
            for tile in range(tiles):
                start(c for s, c in enumerate(unit_copies(t, tile)) if (s, tile) not in early_units(t))

        def next_blocks(t):
            next_products(t)
            next_adds(t)

        def own_block(t):
            all_out(ra.at[t], a_s.at[t])
            product(t, far.at[t])

        def slot(t):
            return Z_ORDER.index(t) % 2

        def hand_out(t, tile, part):
            parts = unit_parts(t, tile)
            for k in reversed(range(n8)):
                dx, dc = NEAR[k]
                at = pl.ds(hand_at[dx][dc], dp)
                src, dst = stage.at[slot(t), tile, at], outs[t].at[i8, tile]

                def send(k=k, src=src, dst=dst):
                    if k:
                        rcopy(src, dst, e_s.at[t], e_r.at[t], near(*NEAR[k])).start()
                    else:
                        pltpu.make_async_copy(src, dst, out_sem.at[t]).start()

                if len(parts) == 1:
                    send()
                elif part == 0:
                    pl.when(xs[dx] < parts[0][2] // dp // 2)(send)
                else:
                    pl.when(xs[dx] >= parts[0][2] // dp // 2)(send)

        def handed(t):
            all_out(outs[t].at[pl.ds(0, n8 - 1)], e_s.at[t])
            pltpu.make_async_copy(outs[t].at[0], outs[t].at[0], out_sem.at[t]).wait()

        given = []

        def finish(t, tile):
            at = tile_rows(tile)
            wide = pl.ds(tile * LANE, LANE)
            for part, (n, first, size) in enumerate(unit_parts(t, tile)):
                lanes = pl.ds(first, size)
                all_in(rb.at[t, :, at, lanes], u_r.at[t, n])
                cs = [pltpu.make_async_copy(rb.at[t, s, at, lanes], tmp.at[s, at, lanes], tmp_sem.at[s]) for s in range(2)]
                start(cs)
                if t == Z_ORDER[2] and not given:
                    given.append(Z_ORDER[0])
                    handed(Z_ORDER[0])
                for c in cs:
                    c.wait()
                stage[slot(t), tile, lanes] = (far[t, wide, lanes] + tmp[0, wide, lanes] + tmp[1, wide, lanes]).T
                hand_out(t, tile, part)

        def on_y(r, n):
            return (r == 1) == (n == 1)

        def level(r, n):
            at = ys if on_y(r, n) else xs
            dev = ydev if on_y(r, n) else xdev
            if n == 1:
                def piece(k, h):
                    return part.at[r, pl.ds(2 * h, 2), at[k]] if on_y(r, n) else part.at[r, at[k], pl.ds(2 * h, 2)]
                return dev, piece, ra1, rb1, sd1, (a1_s, a1_r, f1_s, f1_r)

            def piece(k, h):
                return mid.at[r, at[k], pl.ds(h, 1)]
            return dev, piece, ra2, rb2, sd2, (a2_s, a2_r, f2_s, f2_r)

        def ring_a(r, n):
            dev, piece, rfar, _, _, sems = level(r, n)
            return [rcopy(piece(2, s), rfar.at[r, s], sems[0].at[r], sems[1].at[r], dev(1 + 2 * s)) for s in range(2)]

        def ring_f(r, n):
            dev, piece, _, rnear, _, sems = level(r, n)
            return [rcopy(piece(1 + 2 * s, 1 - s), rnear.at[r, s, 1 - s], sems[2].at[r], sems[3].at[r], dev(1 + 2 * s)) for s in range(2)]

        def ring_d(r, n):
            dev, _, _, rnear, dep, sems = level(r, n)
            return [rcopy(dep.at[r, s], rnear.at[r, s, s], sems[2].at[r], sems[3].at[r], dev(1 + 2 * s)) for s in range(2)]

        def add(grid, *terms):
            specs = []
            for ref, at, lead in terms:
                tail = ref.shape[lead:]
                specs.append(pl.BlockSpec((1,) * lead + tuple(tail), lambda *i, at=at, rank=len(tail): tuple(at(*i)) + (0,) * rank))

            def body(*refs):
                total = refs[0][...].astype(F32).reshape(refs[0].shape[-2:])
                for ref in refs[1:-1]:
                    total = total + ref[...].astype(F32).reshape(total.shape)
                refs[-1][...] = total.astype(BF16).reshape(refs[-1].shape)

            pltpu.emit_pipeline(body, grid=grid, in_specs=specs[:-1], out_specs=specs[-1:])(*[ref for ref, _, _ in terms])

        def ring_first(r, n):
            start(ring_a(r, n) + ring_f(r, n))

        def ring_dependent(r, n):
            _, _, rfar, _, _, sems = level(r, n)
            all_in(rfar.at[r], sems[1].at[r])
            here = y if on_y(r, n) else x
            if n == 1:
                def near_block(s, i):
                    at = lax.rem(here + 1 + 2 * s, RING)
                    return (2 * s + i, at) if on_y(r, n) else (at, 2 * s + i)

                add((2, 2), (part.at[r], near_block, 2), (ra1.at[r], lambda s, i: (s, i), 2), (sd1.at[r], lambda s, i: (s, i), 2))
            else:
                add((2,), (mid.at[r], lambda s: (lax.rem(here + 1 + 2 * s, RING), s), 2), (ra2.at[r], lambda s: (s, 0), 2),
                    (sd2.at[r], lambda s: (s, 0), 2))
            start(ring_d(r, n))

        def ring_last(r, n):
            _, _, _, rnear, _, sems = level(r, n)
            all_in(rnear.at[r], sems[3].at[r])
            here = y if on_y(r, n) else x
            if n == 1:
                def own_at(h, i):
                    return (2 * h + i, here) if on_y(r, n) else (here, 2 * h + i)

                add((2, 2), (part.at[r], own_at, 2), (rb1.at[r, 0], lambda h, i: (h, i), 2),
                    (rb1.at[r, 1], lambda h, i: (h, i), 2), (mid.at[r], lambda h, i: (2 * h + i,), 1))
            else:
                own, res = ((tok_own, out), (grad_own, gin))[r]
                add((2,), (own, lambda h: (h,), 1), (mid.at[r], lambda h: (here, h), 2), (rb2.at[r, 0], lambda h: (h, 0), 2),
                    (rb2.at[r, 1], lambda h: (h, 0), 2), (res, lambda h: (h,), 1))

        def keep_rows(r):
            core_copy(r).wait_recv()
            row_products(r, True)

        run_order({
            "far_block": far_block, "next_products": next_products, "next_adds": next_adds, "next_blocks": next_blocks,
            "own_block": own_block, "finish": finish, "give_rows": give_rows, "keep_rows": keep_rows, "ring_first": ring_first,
            "ring_dependent": ring_dependent, "ring_last": ring_last,
        }, LATE_ORDER)

        for t in range(3):
            all_out(nxt.at[t], u_s.at[t])
        for r in range(2):
            core_copy(r).wait_send()
            for n in (1, 2):
                _, _, rfar, rnear, _, sems = level(r, n)
                all_out(rfar.at[r], sems[0].at[r])
                all_out(rnear.at[r], sems[2].at[r])
        for t in Z_ORDER:
            with jax.named_scope(f"handed_{t}"):
                all_in(outs[t].at[pl.ds(0, n8 - 1)], e_r.at[t])
                if t not in given:
                    handed(t)

    pl.run_scoped(
        forward_phase,
        pltpu.VMEM((2, chunk, d), BF16),
        pltpu.VMEM((tokens, nf), BF16),
        pltpu.VMEM((tokens, nf), BF16),
        pltpu.VMEM((2, chunk, nf), BF16),
        pltpu.VMEM((2, 2, chunk, main), BF16),
        pltpu.VMEM((2, 2, chunk, packed), BF16),
        pltpu.VMEM((d, main), BF16),
        pltpu.VMEM((d, packed), BF16),
    )
    pl.run_scoped(backward_phase, pltpu.VMEM((2, tiles * LANE, cols), F32), pltpu.VMEM((2, tiles, cols, LANE), F32))


def layer(sg, su, sd, tok, grad):
    n8 = 2 * RING
    dp, nf = sg.shape[0], sg.shape[1] // n8
    rows, d = tok.shape
    tokens = rows * RING * n8
    cols = d // RING
    tiles = -(-nf // LANE)
    padded = tiles * LANE
    main = nf // LANE * LANE
    packed = -(-3 * (nf - main) // LANE) * LANE
    hbm = pl.BlockSpec(memory_space=pl.ANY)
    dma = pltpu.SemaphoreType.DMA
    sds = jax.ShapeDtypeStruct
    halves = (2, rows // 2, d)
    res = pl.pallas_call(
        layer_kernel,
        out_shape=[sds((n8, tiles, dp, LANE), F32)] * 3 + [sds(halves, BF16)] * 2 + [
            sds((d, main), BF16), sds((d, main), BF16), sds((d, main), BF16), sds((d, packed), BF16), sds((tokens, d), BF16), sds((tokens, d), BF16),
            sds((3, RING, 2, RING * rows, main), BF16), sds((2, RING, 2, RING * rows, packed), BF16),
            sds((3, nf, cols), F32), sds((3, 2, nf, cols), F32),
            sds((2, RING, RING, rows, d), BF16), sds((2, RING, RING, rows, d), BF16), sds((2, RING, RING, rows, d), BF16),
            sds((2, 2, 2, rows, d), BF16), sds((2, 2, 2, 2, rows, d), BF16), sds((2, 2, 2, rows, d), BF16),
            sds((2, RING, 2, rows // 2, d), BF16),
            sds((2, 2, 1, rows // 2, d), BF16), sds((2, 2, 2, 1, rows // 2, d), BF16), sds((2, 2, 1, rows // 2, d), BF16),
        ],
        in_specs=[hbm] * 7,
        out_specs=[hbm] * 25,
        scratch_shapes=[
            pltpu.VMEM((3, nf, tokens), BF16),
            pltpu.VMEM((2, tokens, cols), BF16),
            pltpu.VMEM((3, padded, cols), F32),
            pltpu.VMEM((3, 2, nf, cols), F32),
            dma((7,)),
            dma((4,)), dma((4, n8)),
            dma((4,)), dma((4, 2, n8 // 2)), dma((4,)),
            dma((4,)),
            dma((3,)), dma((3, 2)),
            dma((3,)), dma((3,)),
            dma((3,)), dma((3, 2, RING)),
            dma((3,)), dma((3, RING)),
            dma((3,)), dma((RING + 2,)),
            dma((3,)), dma((4,)), dma((2,)), dma((2, 3)), dma((2,)), dma((2,)),
            dma((3,)), dma((3,)),
            dma((3,)), dma((3, tiles + 1)),
            dma((3,)), dma((3,)),
            dma((3,)),
            dma((2,)), dma((2,)),
        ] + [dma((2,))] * 8,
        compiler_params=pltpu.CompilerParams(collective_id=0, has_side_effects=True, vmem_limit_bytes=67043328),
        cost_estimate=pl.CostEstimate(flops=18 * nf * tokens * d, bytes_accessed=300_000_000, transcendentals=0),
        name="layer",
    )(sg, su, sd, tok, grad, tok.reshape(halves), grad.reshape(halves))
    return res[:3], res[3].reshape(rows, d), res[4].reshape(rows, d)


def assemble_kernel(og, ou, od, out, gin, g, u, w, res, gres, buf, flat, in_sem, out_sem, row_buf, row_sem):
    n8, nf = og.shape[0], g.shape[1] // og.shape[0]
    srcs, dsts = (og, ou, od), (g, u, w)
    rows_in = [pltpu.make_async_copy(src, row_buf.at[r], row_sem.at[r]) for r, src in enumerate((out, gin))]
    some = n8 // 2
    loads = [
        pltpu.make_async_copy(src.at[pl.ds(h * some, some)], buf.at[t, pl.ds(h * some, some)], in_sem.at[2 * t + h])
        for t, src in enumerate(srcs) for h in range(2)
    ]
    stores = [pltpu.make_async_copy(flat.at[t], dst, out_sem.at[t]) for t, dst in enumerate(dsts)]
    for c in loads + rows_in:
        c.start()
    for t in range(3):
        for j in range(n8):
            if j % some == 0:
                loads[2 * t + j // some].wait()
            flat[t, :, j * nf:(j + 1) * nf] = jnp.concatenate([buf[t, j, tile] for tile in range(buf.shape[2])], axis=1)[:, :nf]
        stores[t].start()
    rows_out = [pltpu.make_async_copy(row_buf.at[r], dst, row_sem.at[r]) for r, dst in enumerate((res, gres))]
    for c in rows_in:
        c.wait()
    for c in rows_out:
        c.start()
    for c in stores + rows_out:
        c.wait()


def assemble(sums, out, gin, ff):
    dp = sums[0].shape[2]
    hbm = pl.BlockSpec(memory_space=pl.ANY)
    dma = pltpu.SemaphoreType.DMA
    sds = jax.ShapeDtypeStruct
    return pl.pallas_call(
        assemble_kernel,
        out_shape=[sds((dp, ff), F32)] * 3 + [sds(out.shape, BF16)] * 2,
        in_specs=[hbm] * 5,
        out_specs=[hbm] * 5,
        scratch_shapes=[
            pltpu.VMEM((3,) + sums[0].shape, F32), pltpu.VMEM((3, dp, ff), F32), dma((6,)), dma((3,)),
            pltpu.VMEM((2,) + out.shape, BF16), dma((2,)),
        ],
        compiler_params=pltpu.CompilerParams(vmem_limit_bytes=63 * 1024 * 1024),
        name="assemble",
    )(*sums, out, gin)


def solution(mesh):
    nz, ny, nd = mesh.shape["datb"], mesh.shape["model"], mesh.shape["data"]
    fine = Mesh(mesh.devices.reshape(nz, ny, nd // 2, 2), ("datb", "model", "x", "core"))

    def local_step(tok_loc, wg_loc, wu_loc, wd_loc, grad_loc):
        sums, out, grad_in = layer(wg_loc, wu_loc, wd_loc.T, tok_loc, grad_loc)
        grad_gate, grad_up, grad_down_t, out, grad_in = assemble(sums, out, grad_in, wg_loc.shape[1])
        return out, grad_in, grad_gate, grad_up, grad_down_t.T

    return jax.shard_map(local_step, mesh=fine, in_specs=(ROW_SPEC, GATE_SPEC, GATE_SPEC, DOWN_SPEC, ROW_SPEC), out_specs=(ROW_SPEC, ROW_SPEC, GATE_SPEC, GATE_SPEC, DOWN_SPEC), check_vma=False)
```
